8 devices in a mesh: dp: 8 (over z, y, x, core).
Axes of the slice: x: 2, y: 2, z: 1, core: 2. Of those that a mesh axis runs over, the one named last changes fastest.
Arguments:
- tokens: bfloat16 [8192, 1024], P('dp')
- w_one: bfloat16 [1024, 512], replicated
- w_two: bfloat16 [512, 256], replicated
- wi_one: bfloat16 [256, 512], replicated
- wi_two: bfloat16 [512, 256], replicated
- item_table: bfloat16 [262144, 256], P('dp')
- cand_ids: int32 [4096], replicated
- log_q: float32 [4096], replicated
- targets: int32 [8192], P('dp')
Outputs:
- output 1: float32 [], replicated
- output 2: float32 [262144, 256], P('dp')
- output 3: float32 [1024, 512], replicated
- output 4: float32 [512, 256], replicated
- output 5: float32 [256, 512], replicated
- output 6: float32 [512, 256], replicated
All inputs are finite; a program needn't handle non-finite values.
Results may differ from the reference program's by a relative error of at most 0.00982284.
Values are sent between devices in bfloat16 or wider.
A program may use at most 1 GiB of HBM per device.

```python
import math
import jax
import jax.numpy as jnp
from jax import lax

DIN = 1024
FF = 512
D = 256
FF2 = 512
TOK_DEV = 1024
CANDS = 4096
ROWS_DEV = 32768
DEVS = 8

TOKENS = TOK_DEV * DEVS
ROWS = ROWS_DEV * DEVS
HEAD_ROWS = 4 * CANDS
SCORE_GAIN = 3.0
HIT_VALUE = -1e9


def setup_inputs(seed: int = 0) -> dict:
    root_key = jax.random.key(seed)
    val_keys = jax.random.split(root_key, 7)
    tokens = jax.random.normal(val_keys[0], (TOKENS, DIN), jnp.float32).astype(jnp.bfloat16)
    w_one = (jax.random.normal(val_keys[1], (DIN, FF), jnp.float32) * DIN ** -0.5).astype(jnp.bfloat16)
    w_two = (jax.random.normal(val_keys[2], (FF, D), jnp.float32) * FF ** -0.5).astype(jnp.bfloat16)
    wi_one = (jax.random.normal(val_keys[3], (D, FF2), jnp.float32) * D ** -0.5).astype(jnp.bfloat16)
    wi_two = (jax.random.normal(val_keys[4], (FF2, D), jnp.float32) * FF2 ** -0.5).astype(jnp.bfloat16)
    item_table = jax.random.normal(val_keys[5], (ROWS, D), jnp.float32).astype(jnp.bfloat16)
    log_q = math.log(CANDS) + jax.random.uniform(val_keys[6], (CANDS,), jnp.float32, -3.0, 3.0)
    int_keys = jax.random.split(jax.random.fold_in(root_key, 1), 7)
    head_ids = jax.random.permutation(int_keys[0], HEAD_ROWS)[: CANDS // 2]
    tail_ids = HEAD_ROWS + jax.random.permutation(int_keys[1], ROWS - HEAD_ROWS)[: CANDS - CANDS // 2]
    cand_ids = jnp.concatenate([head_ids, tail_ids])[jax.random.permutation(int_keys[2], CANDS)].astype(jnp.int32)
    pick_mode = jax.random.randint(int_keys[3], (TOKENS,), 0, 4)
    from_cands = cand_ids[jax.random.randint(int_keys[4], (TOKENS,), 0, CANDS)]
    from_head = jax.random.randint(int_keys[5], (TOKENS,), 0, HEAD_ROWS)
    from_all = jax.random.randint(int_keys[6], (TOKENS,), 0, ROWS)
    targets = jnp.where(pick_mode == 0, from_cands, jnp.where(pick_mode == 1, from_head, from_all)).astype(jnp.int32)
    return {"tokens": tokens, "w_one": w_one, "w_two": w_two, "wi_one": wi_one, "wi_two": wi_two, "item_table": item_table, "cand_ids": cand_ids, "log_q": log_q, "targets": targets}


def tower_fwd(row_block, w_in, w_out):
    pre_act = jnp.dot(row_block, w_in, preferred_element_type=jnp.float32)
    hidden = jax.nn.gelu(pre_act).astype(jnp.bfloat16)
    tower_out = jnp.dot(hidden, w_out, preferred_element_type=jnp.float32).astype(jnp.bfloat16)
    return pre_act, hidden, tower_out


def tower_back(row_block, w_out, pre_act, hidden, grad_out):
    dw_out = jnp.dot(hidden.T, grad_out, preferred_element_type=jnp.float32)
    grad_hidden = jnp.dot(grad_out, w_out.T, preferred_element_type=jnp.float32)
    gelu_back = jax.vjp(jax.nn.gelu, pre_act)[1]
    grad_pre = gelu_back(grad_hidden)[0].astype(jnp.bfloat16)
    dw_in = jnp.dot(row_block.T, grad_pre, preferred_element_type=jnp.float32)
    return grad_pre, dw_in, dw_out


def reference(tokens, w_one, w_two, wi_one, wi_two, item_table, cand_ids, log_q, targets):
    logit_scale = SCORE_GAIN / math.sqrt(D)
    cand_raw = item_table[cand_ids]
    c_pre, c_hidden, cand_vec = tower_fwd(cand_raw, wi_one, wi_two)

    def block_step(carry, blk):
        loss_acc, dcand_acc, dw_one_acc, dw_two_acc, dwi_one_acc, dwi_two_acc = carry
        tok_blk, targ_blk = blk
        q_pre, q_hidden, query = tower_fwd(tok_blk, w_one, w_two)
        targ_raw = item_table[targ_blk]
        t_pre, t_hidden, targ_vec = tower_fwd(targ_raw, wi_one, wi_two)
        z_targ = jnp.sum(query.astype(jnp.float32) * targ_vec.astype(jnp.float32), axis=1) * logit_scale
        z_cand = jnp.dot(query, cand_vec.T, preferred_element_type=jnp.float32) * logit_scale - log_q[None, :]
        z_cand = jnp.where(targ_blk[:, None] == cand_ids[None, :], HIT_VALUE, z_cand)
        row_max = jnp.maximum(z_targ, jnp.max(z_cand, axis=1))
        e_targ = jnp.exp(z_targ - row_max)
        e_cand = jnp.exp(z_cand - row_max[:, None])
        denom_sum = e_targ + jnp.sum(e_cand, axis=1)
        loss_blk = jnp.sum(jnp.log(denom_sum) + row_max - z_targ)
        dz_targ = ((e_targ / denom_sum - 1.0) / TOKENS).astype(jnp.bfloat16).astype(jnp.float32)
        dz_cand = (e_cand / denom_sum[:, None] / TOKENS).astype(jnp.bfloat16)
        d_query = ((dz_targ[:, None] * targ_vec.astype(jnp.float32) + jnp.dot(dz_cand, cand_vec, preferred_element_type=jnp.float32)) * logit_scale).astype(jnp.bfloat16)
        d_targ_vec = (logit_scale * dz_targ[:, None] * query.astype(jnp.float32)).astype(jnp.bfloat16)
        dcand_new = dcand_acc + jnp.dot(dz_cand.T, query, preferred_element_type=jnp.float32)
        dw_one_blk, dw_two_blk = tower_back(tok_blk, w_two, q_pre, q_hidden, d_query)[1:]
        t_grad_pre, dwi_one_blk, dwi_two_blk = tower_back(targ_raw, wi_two, t_pre, t_hidden, d_targ_vec)
        d_targ_raw = jnp.dot(t_grad_pre, wi_one.T, preferred_element_type=jnp.float32).astype(jnp.bfloat16)
        new_carry = (loss_acc + loss_blk, dcand_new, dw_one_acc + dw_one_blk, dw_two_acc + dw_two_blk, dwi_one_acc + dwi_one_blk, dwi_two_acc + dwi_two_blk)
        return new_carry, d_targ_raw

    init_carry = (jnp.zeros((), jnp.float32), jnp.zeros((CANDS, D), jnp.float32), jnp.zeros((DIN, FF), jnp.float32), jnp.zeros((FF, D), jnp.float32), jnp.zeros((D, FF2), jnp.float32), jnp.zeros((FF2, D), jnp.float32))
    tok_blocks = tokens.reshape(DEVS, TOK_DEV, DIN)
    targ_blocks = targets.reshape(DEVS, TOK_DEV)
    final_carry, d_targ_rows = lax.scan(block_step, init_carry, (tok_blocks, targ_blocks))
    loss_acc, dcand_acc, dw_one, dw_two, dwi_one_t, dwi_two_t = final_carry
    d_cand_vec = (logit_scale * dcand_acc).astype(jnp.bfloat16)
    c_grad_pre, dwi_one_c, dwi_two_c = tower_back(cand_raw, wi_two, c_pre, c_hidden, d_cand_vec)
    d_cand_raw = jnp.dot(c_grad_pre, wi_one.T, preferred_element_type=jnp.float32).astype(jnp.bfloat16)
    row_grads = jnp.concatenate([d_cand_raw, d_targ_rows.reshape(TOKENS, D)]).astype(jnp.float32)
    row_ids = jnp.concatenate([cand_ids, targets])
    d_table = jax.ops.segment_sum(row_grads, row_ids, num_segments=ROWS)
    return loss_acc / TOKENS, d_table, dw_one, dw_two, dwi_one_t + dwi_one_c, dwi_two_t + dwi_two_c
```

```python
import functools
import math
import jax
import jax.numpy as jnp
from jax import lax
from jax.experimental import pallas as pl
from jax.experimental.pallas import tpu as pltpu
from jax.sharding import PartitionSpec as P

SCORE_GAIN = 3.0
HIT_VALUE = -1e9


def tower_fwd(row_block, w_in, w_out):
    pre_act = jnp.dot(row_block, w_in, preferred_element_type=jnp.float32)
    hidden = jax.nn.gelu(pre_act).astype(jnp.bfloat16)
    tower_out = jnp.dot(hidden, w_out, preferred_element_type=jnp.float32).astype(jnp.bfloat16)
    return pre_act, hidden, tower_out


def tower_back(row_block, w_out, pre_act, hidden, grad_out):
    dw_out = jnp.einsum("nf,nd->fd", hidden, grad_out, preferred_element_type=jnp.float32)
    grad_hidden = jnp.einsum("nd,fd->nf", grad_out, w_out, preferred_element_type=jnp.float32)
    gelu_back = jax.vjp(jax.nn.gelu, pre_act)[1]
    grad_pre = gelu_back(grad_hidden)[0].astype(jnp.bfloat16)
    dw_in = jnp.einsum("ne,nf->ef", row_block, grad_pre, preferred_element_type=jnp.float32)
    return grad_pre, dw_in, dw_out


def owned_rows(table_loc, row_ids, row_base):
    local_ids = row_ids - row_base
    num_rows = table_loc.shape[0]
    is_owned = (local_ids >= 0) & (local_ids < num_rows)
    picked = jnp.take(table_loc, jnp.clip(local_ids, 0, num_rows - 1), axis=0)
    return jnp.where(is_owned[:, None], picked, 0)


GROUP = 16
BATCH = 128


def scatter_body(ids_s, ids_v, cand_ref, targ_ref, out_ref, acc, g2, sem):
    rows = out_ref.shape[0]
    width = out_ref.shape[1]
    n_cand = cand_ref.shape[0]
    n_all = n_cand + targ_ref.shape[0]
    zero_rows = 256

    @pl.loop(0, rows // zero_rows)
    def _(i):
        acc[pl.ds(i * zero_rows, zero_rows), :] = jnp.zeros((zero_rows, width), jnp.float32)

    row_i = lax.broadcasted_iota(jnp.int32, (BATCH, BATCH), 0) // GROUP
    col_i = lax.broadcasted_iota(jnp.int32, (BATCH, BATCH), 1) // GROUP
    same_group = row_i == col_i

    def one_batch(b, src, src_base):
        idr = jnp.broadcast_to(ids_v[pl.ds(b, 1), :], (BATCH, BATCH))
        same = jnp.where((idr == idr.T) & same_group, 1.0, 0.0).astype(jnp.bfloat16)
        g2[...] = jnp.dot(same, src[pl.ds(pl.multiple_of(b * BATCH - src_base, BATCH), BATCH), :], preferred_element_type=jnp.float32)
        for g in range(BATCH // GROUP):
            idx = [ids_s[b * BATCH + g * GROUP + r] for r in range(GROUP)]
            old = [acc[pl.ds(idx[r], 1), :] for r in range(GROUP)]
            new = [old[r] + g2[g * GROUP + r : g * GROUP + r + 1, :] for r in range(GROUP)]
            for r in range(GROUP):
                acc[pl.ds(idx[r], 1), :] = new[r]

    @pl.loop(0, n_cand // BATCH)
    def _(b):
        one_batch(b, cand_ref, 0)

    @pl.loop(n_cand // BATCH, n_all // BATCH)
    def _(b):
        one_batch(b, targ_ref, n_cand)

    n_out = 8
    step = rows // n_out
    copies = [pltpu.make_async_copy(acc.at[pl.ds(i * step, step)], out_ref.at[pl.ds(i * step, step)], sem) for i in range(n_out)]
    for c in copies:
        c.start()
    for c in copies:
        c.wait()


def scatter_rows(local_ids, back_cand, back_targ, rows_loc):
    n_all = local_ids.shape[0]
    width = back_cand.shape[1]
    return pl.pallas_call(
        scatter_body,
        out_shape=jax.ShapeDtypeStruct((rows_loc, width), jnp.float32),
        in_specs=[pl.BlockSpec(memory_space=pltpu.SMEM), pl.BlockSpec(memory_space=pltpu.VMEM), pl.BlockSpec(memory_space=pltpu.VMEM), pl.BlockSpec(memory_space=pltpu.VMEM)],
        out_specs=pl.BlockSpec(memory_space=pl.ANY),
        scratch_shapes=[pltpu.VMEM((rows_loc + 8, width), jnp.float32), pltpu.VMEM((BATCH, width), jnp.float32), pltpu.SemaphoreType.DMA],
        compiler_params=pltpu.CompilerParams(vmem_limit_bytes=56 * 1024 * 1024),
        name="scatter_rows",
    )(local_ids, local_ids.reshape(n_all // BATCH, BATCH), back_cand, back_targ)


TOK_BLK = 256
CHUNK = 512


def softmax_body(tok_total, h_ref, v_ref, u_ref, ut_ref, lq_ref, cid_ref, tid_ref, loss_ref, dh_ref, dv_ref, du_ref, z_s, dz_s):
    step = pl.program_id(0)
    n_cand, width = u_ref.shape
    scale = SCORE_GAIN / math.sqrt(width)
    h = h_ref[...]
    hf = h.astype(jnp.float32)
    vf = v_ref[...].astype(jnp.float32)
    ht = hf.T.astype(jnp.bfloat16)
    zt = jnp.sum(hf * vf, axis=1, keepdims=True) * scale
    zt = jnp.broadcast_to(zt, (TOK_BLK, 128)).T[0:1, :]
    tid = tid_ref[0]
    m8 = jnp.broadcast_to(zt, (8, TOK_BLK))
    n_chunk = n_cand // CHUNK

    def z_chunk(i, m8):
        off = pl.multiple_of(i * CHUNK, CHUNK)
        z = jnp.dot(u_ref[pl.ds(off, CHUNK), :], ht, preferred_element_type=jnp.float32) * scale
        lq = lq_ref[pl.ds(off, CHUNK), :]
        cid = cid_ref[pl.ds(off, CHUNK), :]
        z = z - jnp.concatenate([lq] * (TOK_BLK // 128), axis=1)
        z = jnp.where(jnp.concatenate([cid] * (TOK_BLK // 128), axis=1) == tid, HIT_VALUE, z)
        z_s[pl.ds(off, CHUNK), :] = z
        return jnp.maximum(m8, jnp.max(z.reshape(CHUNK // 8, 8, TOK_BLK), axis=0))

    m8 = lax.fori_loop(0, n_chunk, z_chunk, m8)
    m = jnp.max(m8, axis=0, keepdims=True)

    def e_chunk(i, s8):
        off = pl.multiple_of(i * CHUNK, CHUNK)
        e = jnp.exp(z_s[pl.ds(off, CHUNK), :] - m)
        z_s[pl.ds(off, CHUNK), :] = e
        return s8 + jnp.sum(e.reshape(CHUNK // 8, 8, TOK_BLK), axis=0)

    s8 = lax.fori_loop(0, n_chunk, e_chunk, jnp.zeros((8, TOK_BLK), jnp.float32))
    et = jnp.exp(zt - m)
    den = et + jnp.sum(s8, axis=0, keepdims=True)
    part = jnp.sum(jnp.log(den) + m - zt, axis=1, keepdims=True)
    dzt = ((et / den - 1.0) / tok_total).astype(jnp.bfloat16).astype(jnp.float32)
    inv = 1.0 / den / tok_total

    @pl.when(step == 0)
    def _():
        loss_ref[...] = jnp.zeros_like(loss_ref)
        du_ref[...] = jnp.zeros_like(du_ref)

    loss_ref[...] += jnp.broadcast_to(part, loss_ref.shape)

    def dz_chunk(i, dht):
        off = pl.multiple_of(i * CHUNK, CHUNK)
        dz = (z_s[pl.ds(off, CHUNK), :] * inv).astype(jnp.bfloat16)
        du_ref[pl.ds(off, CHUNK), :] += jnp.dot(dz, h, preferred_element_type=jnp.float32)
        return dht + jnp.dot(ut_ref[:, pl.ds(off, CHUNK)], dz, preferred_element_type=jnp.float32)

    dht = lax.fori_loop(0, n_chunk, dz_chunk, jnp.zeros((width, TOK_BLK), jnp.float32))
    dzt_c = jnp.broadcast_to(dzt, (128, TOK_BLK)).T[:, 0:1]
    dh_ref[...] = ((dzt_c * vf + dht.T) * scale).astype(jnp.bfloat16)
    dv_ref[...] = (scale * dzt_c * hf).astype(jnp.bfloat16)


def softmax_grads(query, targ_vec, cand_vec, log_q, targ_ids, cand_ids, tok_total):
    n_tok, width = query.shape
    n_cand = cand_vec.shape[0]
    steps = n_tok // TOK_BLK
    whole = lambda s: (0, 0)
    lq_b = jnp.broadcast_to(log_q[:, None], (n_cand, 128))
    cid_b = jnp.broadcast_to(cand_ids[:, None], (n_cand, 128))
    return pl.pallas_call(
        functools.partial(softmax_body, tok_total),
        grid=(steps,),
        out_shape=(jax.ShapeDtypeStruct((8, 128), jnp.float32), jax.ShapeDtypeStruct((n_tok, width), jnp.bfloat16), jax.ShapeDtypeStruct((n_tok, width), jnp.bfloat16), jax.ShapeDtypeStruct((n_cand, width), jnp.float32)),
        in_specs=[
            pl.BlockSpec((TOK_BLK, width), lambda s: (s, 0)),
            pl.BlockSpec((TOK_BLK, width), lambda s: (s, 0)),
            pl.BlockSpec((n_cand, width), whole),
            pl.BlockSpec((width, n_cand), whole),
            pl.BlockSpec((n_cand, 128), whole),
            pl.BlockSpec((n_cand, 128), whole),
            pl.BlockSpec((1, 1, TOK_BLK), lambda s: (s, 0, 0)),
        ],
        out_specs=(
            pl.BlockSpec((8, 128), whole),
            pl.BlockSpec((TOK_BLK, width), lambda s: (s, 0)),
            pl.BlockSpec((TOK_BLK, width), lambda s: (s, 0)),
            pl.BlockSpec((n_cand, width), whole),
        ),
        scratch_shapes=[pltpu.VMEM((n_cand, TOK_BLK), jnp.float32), pltpu.VMEM((8, 128), jnp.bfloat16)],
        compiler_params=pltpu.CompilerParams(vmem_limit_bytes=48 * 1024 * 1024, dimension_semantics=("arbitrary",)),
        cost_estimate=pl.CostEstimate(flops=6 * n_tok * n_cand * width, bytes_accessed=16 << 20, transcendentals=n_tok * n_cand),
        name="softmax_grads",
    )(query, targ_vec, cand_vec, cand_vec.T, lq_b, cid_b, targ_ids.reshape(steps, 1, TOK_BLK))


def solution(mesh):
    num_dev = mesh.shape["dp"]

    def local_step(tokens, w_one, w_two, wi_one, wi_two, table_loc, cand_ids, log_q, targ_loc):
        my_index = lax.axis_index("dp")
        rows_loc = table_loc.shape[0]
        row_base = my_index * rows_loc
        tok_total = tokens.shape[0] * num_dev
        cand_mine = lax.psum_scatter(owned_rows(table_loc, cand_ids, row_base), "dp", scatter_dimension=0, tiled=True)
        c_pre, c_hidden, cand_vec_mine = tower_fwd(cand_mine, wi_one, wi_two)
        cand_vec = lax.all_gather(cand_vec_mine, "dp", axis=0, tiled=True)
        targ_all = lax.all_gather(targ_loc, "dp", axis=0, tiled=True)
        targ_raw = lax.psum_scatter(owned_rows(table_loc, targ_all, row_base), "dp", scatter_dimension=0, tiled=True)
        t_pre, t_hidden, targ_vec = tower_fwd(targ_raw, wi_one, wi_two)
        q_pre, q_hidden, query = tower_fwd(tokens, w_one, w_two)
        logit_scale = SCORE_GAIN / math.sqrt(query.shape[1])
        loss_part, d_query, d_targ_vec, d_cand_part = softmax_grads(query, targ_vec, cand_vec, log_q, targ_loc, cand_ids, tok_total)
        loss_sum = loss_part[0, 0]
        d_cand_vec = (lax.psum_scatter(d_cand_part, "dp", scatter_dimension=0, tiled=True) * logit_scale).astype(jnp.bfloat16)
        dw_one, dw_two = tower_back(tokens, w_two, q_pre, q_hidden, d_query)[1:]
        t_grad_pre, dwi_one_t, dwi_two_t = tower_back(targ_raw, wi_two, t_pre, t_hidden, d_targ_vec)
        c_grad_pre, dwi_one_c, dwi_two_c = tower_back(cand_mine, wi_two, c_pre, c_hidden, d_cand_vec)
        d_targ_raw = jnp.einsum("nf,df->nd", t_grad_pre, wi_one, preferred_element_type=jnp.float32).astype(jnp.bfloat16)
        d_cand_raw = jnp.einsum("nf,df->nd", c_grad_pre, wi_one, preferred_element_type=jnp.float32).astype(jnp.bfloat16)
        weight_grads = lax.psum((dw_one, dw_two, dwi_one_t + dwi_one_c, dwi_two_t + dwi_two_c), "dp")
        back_cand = lax.all_gather(d_cand_raw, "dp", axis=0, tiled=True)
        back_targ = lax.all_gather(d_targ_raw, "dp", axis=0, tiled=True)
        local_ids = jnp.concatenate([cand_ids, targ_all]) - row_base
        local_ids = jnp.where((local_ids >= 0) & (local_ids < rows_loc), local_ids, rows_loc)
        d_table = scatter_rows(local_ids, back_cand, back_targ, rows_loc)
        loss = lax.psum(loss_sum, "dp") / tok_total
        return (loss, d_table) + tuple(weight_grads)

    return jax.shard_map(local_step, mesh=mesh, in_specs=(P("dp", None), P(), P(), P(), P(), P("dp", None), P(), P(), P("dp")), out_specs=(P(), P("dp", None), P(), P(), P(), P()), check_vma=False)
```

```python
import functools
import math
import jax
import jax.numpy as jnp
from jax import lax
from jax.experimental import pallas as pl
from jax.experimental.pallas import tpu as pltpu
from jax.sharding import PartitionSpec as P

SCORE_GAIN = 3.0
HIT_VALUE = -1e9


def tower_fwd(row_block, w_in, w_out):
    pre_act = jnp.dot(row_block, w_in, preferred_element_type=jnp.float32)
    hidden = jax.nn.gelu(pre_act).astype(jnp.bfloat16)
    tower_out = jnp.dot(hidden, w_out, preferred_element_type=jnp.float32).astype(jnp.bfloat16)
    return pre_act, hidden, tower_out


def over_rows(a, b):
    return lax.dot_general(a, b, (((0,), (0,)), ((), ())), preferred_element_type=jnp.float32)


def by_transpose(a, b):
    return lax.dot_general(a, b, (((1,), (1,)), ((), ())), preferred_element_type=jnp.float32)


def tower_back(row_block, w_out, pre_act, hidden, grad_out):
    dw_out = over_rows(hidden, grad_out)
    grad_hidden = by_transpose(grad_out, w_out)
    gelu_back = jax.vjp(jax.nn.gelu, pre_act)[1]
    grad_pre = gelu_back(grad_hidden)[0].astype(jnp.bfloat16)
    dw_in = over_rows(row_block, grad_pre)
    return grad_pre, dw_in, dw_out


GROUP = 16
BATCH = 128
STAGE_ROWS = 2048
OUT_ROWS = 1024


def pick_body(ids_s, table, cand_out, targ_out, wide, stage, rows_f, stage_sem):
    rows_loc, width = table.shape
    lane = width // 2
    n_stage = rows_loc // STAGE_ROWS

    def stage_copy(i, slot):
        return pltpu.make_async_copy(table.at[pl.ds(i * STAGE_ROWS, STAGE_ROWS)], stage.at[slot], stage_sem.at[slot])

    for i in range(3):
        stage_copy(i, i).start()
    wide[pl.ds(2 * rows_loc, 8), :] = jnp.zeros((8, lane), jnp.float32)

    @pl.loop(0, n_stage)
    def _(i):
        slot = i % 4

        @pl.when(i + 3 < n_stage)
        def _():
            stage_copy(i + 3, (i + 3) % 4).start()

        stage_copy(i, slot).wait()

        @pl.loop(0, STAGE_ROWS // 128)
        def _(j):
            block = stage[slot, pl.ds(pl.multiple_of(j * 128, 128), 128), :].astype(jnp.float32)
            base = pl.multiple_of((i * STAGE_ROWS + j * 128) * 2, 256)
            wide[pl.ds(base, 128, 2), :] = block[:, :lane]
            wide[pl.ds(base + 1, 128, 2), :] = block[:, lane:]

    def fill(out, first):
        @pl.loop(0, out.shape[0] // BATCH)
        def _(b):
            for r in range(BATCH):
                at = pl.multiple_of(ids_s[first + b * BATCH + r], 2)
                rows_f[pl.ds(2 * r, 2), :] = wide[pl.ds(at, 2), :]
            rows = pl.ds(pl.multiple_of(b * BATCH, BATCH), BATCH)
            out[rows, :lane] = rows_f[pl.ds(0, BATCH, 2), :].astype(jnp.bfloat16)
            out[rows, lane:] = rows_f[pl.ds(1, BATCH, 2), :].astype(jnp.bfloat16)

    fill(cand_out, 0)
    fill(targ_out, cand_out.shape[0])


def pick_rows(ids_two, table_loc, n_cand):
    rows_loc, width = table_loc.shape
    n_targ = ids_two.shape[0] - n_cand
    vmem = pl.BlockSpec(memory_space=pltpu.VMEM)
    return pl.pallas_call(
        pick_body,
        out_shape=(jax.ShapeDtypeStruct((n_cand, width), jnp.bfloat16), jax.ShapeDtypeStruct((n_targ, width), jnp.bfloat16)),
        in_specs=[pl.BlockSpec(memory_space=pltpu.SMEM), pl.BlockSpec(memory_space=pl.ANY)],
        out_specs=(vmem, vmem),
        scratch_shapes=[
            pltpu.VMEM((2 * rows_loc + 8, width // 2), jnp.float32),
            pltpu.VMEM((4, STAGE_ROWS, width), jnp.bfloat16),
            pltpu.VMEM((2 * BATCH, width // 2), jnp.float32),
            pltpu.SemaphoreType.DMA((4,)),
        ],
        compiler_params=pltpu.CompilerParams(vmem_limit_bytes=50 * 1024 * 1024),
        name="pick_rows",
    )(ids_two, table_loc)


def scatter_body(ids_s, ids_v, cand_ref, targ_ref, out_ref, acc, g2, out_stage, sem):
    rows, width = out_ref.shape
    lane = width // 2
    n_cand = cand_ref.shape[0]
    n_all = n_cand + targ_ref.shape[0]

    @pl.loop(0, 2 * rows // 512)
    def _(i):
        acc[pl.ds(pl.multiple_of(i * 512, 512), 512), :] = jnp.zeros((512, lane), jnp.float32)

    row_i = lax.broadcasted_iota(jnp.int32, (BATCH, BATCH), 0) // GROUP
    col_i = lax.broadcasted_iota(jnp.int32, (BATCH, BATCH), 1) // GROUP
    same_group = row_i == col_i

    def one_batch(b, src, src_base):
        idr = jnp.broadcast_to(ids_v[pl.ds(b, 1), :], (BATCH, BATCH))
        same = jnp.where((idr == idr.T) & same_group, 1.0, 0.0).astype(jnp.bfloat16)
        part = jnp.dot(same, src[pl.ds(pl.multiple_of(b * BATCH - src_base, BATCH), BATCH), :], preferred_element_type=jnp.float32)
        g2[pl.ds(0, BATCH, 2), :] = part[:, :lane]
        g2[pl.ds(1, BATCH, 2), :] = part[:, lane:]
        for g in range(BATCH // GROUP):
            idx = [pl.multiple_of(ids_s[b * BATCH + g * GROUP + r], 2) for r in range(GROUP)]
            new = [acc[pl.ds(idx[r], 2), :] + g2[pl.ds(2 * (g * GROUP + r), 2), :] for r in range(GROUP)]
            for r in range(GROUP):
                acc[pl.ds(idx[r], 2), :] = new[r]

    @pl.loop(0, n_cand // BATCH)
    def _(b):
        one_batch(b, cand_ref, 0)

    @pl.loop(n_cand // BATCH, n_all // BATCH)
    def _(b):
        one_batch(b, targ_ref, n_cand)

    n_out = rows // OUT_ROWS

    def out_copy(i, slot):
        return pltpu.make_async_copy(out_stage.at[slot], out_ref.at[pl.ds(i * OUT_ROWS, OUT_ROWS)], sem.at[slot])

    @pl.loop(0, n_out)
    def _(i):
        slot = i % 4

        @pl.when(i >= 4)
        def _():
            out_copy(i - 4, slot).wait()

        @pl.loop(0, OUT_ROWS // 128)
        def _(j):
            base = pl.multiple_of((i * OUT_ROWS + j * 128) * 2, 256)
            here = pl.ds(pl.multiple_of(j * 128, 128), 128)
            out_stage[slot, here, :lane] = acc[pl.ds(base, 128, 2), :]
            out_stage[slot, here, lane:] = acc[pl.ds(base + 1, 128, 2), :]

        out_copy(i, slot).start()

    for i in range(n_out - 4, n_out):
        out_copy(i, i % 4).wait()


def scatter_rows(ids_two, back_cand, back_targ, rows_loc):
    n_all = ids_two.shape[0]
    width = back_cand.shape[1]
    vmem = pl.BlockSpec(memory_space=pltpu.VMEM)
    return pl.pallas_call(
        scatter_body,
        out_shape=jax.ShapeDtypeStruct((rows_loc, width), jnp.float32),
        in_specs=[pl.BlockSpec(memory_space=pltpu.SMEM), vmem, vmem, vmem],
        out_specs=pl.BlockSpec(memory_space=pl.ANY),
        scratch_shapes=[
            pltpu.VMEM((2 * rows_loc + 8, width // 2), jnp.float32),
            pltpu.VMEM((2 * BATCH, width // 2), jnp.float32),
            pltpu.VMEM((4, OUT_ROWS, width), jnp.float32),
            pltpu.SemaphoreType.DMA((4,)),
        ],
        compiler_params=pltpu.CompilerParams(vmem_limit_bytes=52 * 1024 * 1024),
        cost_estimate=pl.CostEstimate(flops=60_000_000_000, bytes_accessed=40 << 20, transcendentals=0),
        name="scatter_rows",
    )(ids_two, ids_two.reshape(n_all // BATCH, BATCH), back_cand, back_targ)


TOK_BLK = 256
CHUNK = 512


def softmax_body(tok_total, h_ref, v_ref, u_ref, ut_ref, lq_ref, cid_ref, tid_ref, loss_ref, dh_ref, dv_ref, du_ref, z_s, dz_s):
    step = pl.program_id(0)
    n_cand, width = u_ref.shape
    scale = SCORE_GAIN / math.sqrt(width)
    h = h_ref[...]
    hf = h.astype(jnp.float32)
    vf = v_ref[...].astype(jnp.float32)
    ht = hf.T.astype(jnp.bfloat16)
    zt = jnp.sum(hf * vf, axis=1, keepdims=True) * scale
    zt = jnp.broadcast_to(zt, (TOK_BLK, 128)).T[0:1, :]
    tid = tid_ref[0]
    m8 = jnp.broadcast_to(zt, (8, TOK_BLK))
    n_chunk = n_cand // CHUNK

    def z_chunk(i, m8):
        off = pl.multiple_of(i * CHUNK, CHUNK)
        z = jnp.dot(u_ref[pl.ds(off, CHUNK), :], ht, preferred_element_type=jnp.float32) * scale
        lq = lq_ref[pl.ds(off, CHUNK), :]
        cid = cid_ref[pl.ds(off, CHUNK), :]
        z = z - jnp.concatenate([lq] * (TOK_BLK // 128), axis=1)
        z = jnp.where(jnp.concatenate([cid] * (TOK_BLK // 128), axis=1) == tid, HIT_VALUE, z)
        z_s[pl.ds(off, CHUNK), :] = z
        return jnp.maximum(m8, jnp.max(z.reshape(CHUNK // 8, 8, TOK_BLK), axis=0))

    m8 = lax.fori_loop(0, n_chunk, z_chunk, m8)
    m = jnp.max(m8, axis=0, keepdims=True)

    def e_chunk(i, s8):
        off = pl.multiple_of(i * CHUNK, CHUNK)
        e = jnp.exp(z_s[pl.ds(off, CHUNK), :] - m)
        z_s[pl.ds(off, CHUNK), :] = e
        return s8 + jnp.sum(e.reshape(CHUNK // 8, 8, TOK_BLK), axis=0)

    s8 = lax.fori_loop(0, n_chunk, e_chunk, jnp.zeros((8, TOK_BLK), jnp.float32))
    et = jnp.exp(zt - m)
    den = et + jnp.sum(s8, axis=0, keepdims=True)
    part = jnp.sum(jnp.log(den) + m - zt, axis=1, keepdims=True)
    dzt = ((et / den - 1.0) / tok_total).astype(jnp.bfloat16).astype(jnp.float32)
    inv = 1.0 / den / tok_total

    @pl.when(step == 0)
    def _():
        loss_ref[...] = jnp.zeros_like(loss_ref)
        du_ref[...] = jnp.zeros_like(du_ref)

    loss_ref[...] += jnp.broadcast_to(part, loss_ref.shape)

    def dz_chunk(i, dht):
        off = pl.multiple_of(i * CHUNK, CHUNK)
        dz = (z_s[pl.ds(off, CHUNK), :] * inv).astype(jnp.bfloat16)
        du_ref[pl.ds(off, CHUNK), :] += jnp.dot(dz, h, preferred_element_type=jnp.float32)
        return dht + jnp.dot(ut_ref[:, pl.ds(off, CHUNK)], dz, preferred_element_type=jnp.float32)

    dht = lax.fori_loop(0, n_chunk, dz_chunk, jnp.zeros((width, TOK_BLK), jnp.float32))
    dzt_c = jnp.broadcast_to(dzt, (128, TOK_BLK)).T[:, 0:1]
    dh_ref[...] = ((dzt_c * vf + dht.T) * scale).astype(jnp.bfloat16)
    dv_ref[...] = (scale * dzt_c * hf).astype(jnp.bfloat16)


def softmax_grads(query, targ_vec, cand_vec, log_q, targ_ids, cand_ids, tok_total):
    n_tok, width = query.shape
    n_cand = cand_vec.shape[0]
    steps = n_tok // TOK_BLK
    whole = lambda s: (0, 0)
    lq_b = jnp.broadcast_to(log_q[:, None], (n_cand, 128))
    cid_b = jnp.broadcast_to(cand_ids[:, None], (n_cand, 128))
    return pl.pallas_call(
        functools.partial(softmax_body, tok_total),
        grid=(steps,),
        out_shape=(jax.ShapeDtypeStruct((8, 128), jnp.float32), jax.ShapeDtypeStruct((n_tok, width), jnp.bfloat16), jax.ShapeDtypeStruct((n_tok, width), jnp.bfloat16), jax.ShapeDtypeStruct((n_cand, width), jnp.float32)),
        in_specs=[
            pl.BlockSpec((TOK_BLK, width), lambda s: (s, 0)),
            pl.BlockSpec((TOK_BLK, width), lambda s: (s, 0)),
            pl.BlockSpec((n_cand, width), whole),
            pl.BlockSpec((width, n_cand), whole),
            pl.BlockSpec((n_cand, 128), whole),
            pl.BlockSpec((n_cand, 128), whole),
            pl.BlockSpec((1, 1, TOK_BLK), lambda s: (s, 0, 0)),
        ],
        out_specs=(
            pl.BlockSpec((8, 128), whole),
            pl.BlockSpec((TOK_BLK, width), lambda s: (s, 0)),
            pl.BlockSpec((TOK_BLK, width), lambda s: (s, 0)),
            pl.BlockSpec((n_cand, width), whole),
        ),
        scratch_shapes=[pltpu.VMEM((n_cand, TOK_BLK), jnp.float32), pltpu.VMEM((8, 128), jnp.bfloat16)],
        compiler_params=pltpu.CompilerParams(vmem_limit_bytes=48 * 1024 * 1024, dimension_semantics=("arbitrary",)),
        cost_estimate=pl.CostEstimate(flops=6 * n_tok * n_cand * width, bytes_accessed=16 << 20, transcendentals=n_tok * n_cand),
        name="softmax_grads",
    )(query, targ_vec, cand_vec, cand_vec.T, lq_b, cid_b, targ_ids.reshape(steps, 1, TOK_BLK))


MESH = pl.DeviceIdType.MESH


def my_place():
    me = lax.axis_index("dp")
    return me, me // 4, (me // 2) % 2, me % 2


def peer_of(place, dy, dx, dc):
    me, y, x, c = place
    return me + dy * (4 - 8 * y) + dx * (2 - 4 * x) + dc * (1 - 2 * c)


def meet(place):
    barrier = pltpu.get_barrier_semaphore()
    for k in range(1, 8):
        pl.semaphore_signal(barrier, inc=1, device_id=(peer_of(place, k // 4, (k // 2) % 2, k % 2),), device_id_type=MESH)
    pl.semaphore_wait(barrier, 7)


def push(src, dst, send_sem, recv_sem, peer):
    copy = pltpu.make_async_remote_copy(src_ref=src, dst_ref=dst, send_sem=send_sem, recv_sem=recv_sem, device_id=(peer,), device_id_type=MESH)
    copy.start()
    return copy


class Reduce:
    def __init__(self, place, data, in_one, mid, in_xa, in_yb, part_a, part_b, in_ya, in_xb, send_sem, recv_sem):
        self.place, self.data = place, data
        self.in_one, self.mid, self.in_xa, self.in_yb = in_one, mid, in_xa, in_yb
        self.part_a, self.part_b, self.in_ya, self.in_xb = part_a, part_b, in_ya, in_xb
        self.send_sem, self.recv_sem = send_sem, recv_sem
        self.half = data.shape[3] // 2
        self.copies = []

    def push(self, k, src, dst, dy, dx, dc):
        copy = push(src, dst, self.send_sem.at[k], self.recv_sem.at[k], peer_of(self.place, dy, dx, dc))
        self.copies.append(copy)

    def one(self):
        c = self.place[3]
        self.push(0, self.data.at[:, :, 1 - c], self.in_one, 0, 0, 1)

    def two(self):
        _, y, x, c = self.place
        half = self.half
        self.copies[0].wait_recv()
        for i in range(2):
            for j in range(2):
                self.mid[i, j] = self.data[i, j, c] + self.in_one[i, j]
        self.push(1, self.mid.at[:, 1 - x, pl.ds(0, half)], self.in_xa, 0, 1, 0)
        self.push(2, self.mid.at[1 - y, :, pl.ds(half, half)], self.in_yb, 1, 0, 0)

    def three(self):
        _, y, x, c = self.place
        half = self.half
        self.copies[1].wait_recv()
        for i in range(2):
            self.part_a[i] = self.mid[i, x, 0:half] + self.in_xa[i]
        self.push(3, self.part_a.at[1 - y], self.in_ya, 1, 0, 0)
        self.copies[2].wait_recv()
        for i in range(2):
            self.part_b[i] = self.mid[y, i, half : 2 * half] + self.in_yb[i]
        self.push(4, self.part_b.at[1 - x], self.in_xb, 0, 1, 0)

    def last(self):
        _, y, x, c = self.place
        self.copies[3].wait_recv()
        first = self.part_a[y] + self.in_ya[...]
        self.copies[4].wait_recv()
        return first, self.part_b[x] + self.in_xb[...]

    def drain(self):
        for copy in self.copies:
            copy.wait_send()


def reduce_scratch(n, rows, width, dtype):
    half = rows // 2
    return [
        pltpu.VMEM((n, 2, 2, rows, width), dtype),
        pltpu.VMEM((n, 2, 2, rows, width), dtype),
        pltpu.VMEM((n, 2, half, width), dtype),
        pltpu.VMEM((n, 2, half, width), dtype),
        pltpu.VMEM((n, 2, half, width), dtype),
        pltpu.VMEM((n, 2, half, width), dtype),
        pltpu.VMEM((n, half, width), dtype),
        pltpu.VMEM((n, half, width), dtype),
        pltpu.SemaphoreType.DMA((n, 5)),
        pltpu.SemaphoreType.DMA((n, 5)),
    ]


class Gather:
    def __init__(self, place, full, send_sem, recv_sem):
        self.place, self.full = place, full
        self.send_sem, self.recv_sem = send_sem, recv_sem
        self.half = full.shape[3] // 2
        self.copies = []

    def push(self, k, ref, dy, dx, dc):
        copy = push(ref, ref, self.send_sem.at[k], self.recv_sem.at[k], peer_of(self.place, dy, dx, dc))
        self.copies.append(copy)

    def one(self):
        _, y, x, c = self.place
        half = self.half
        self.push(0, self.full.at[y, x, c, pl.ds(0, half)], 0, 1, 0)
        self.push(1, self.full.at[y, x, c, pl.ds(half, half)], 1, 0, 0)

    def two(self):
        _, y, x, c = self.place
        half = self.half
        self.copies[0].wait_recv()
        self.push(2, self.full.at[y, :, c, pl.ds(0, half)], 1, 0, 0)
        self.copies[1].wait_recv()
        self.push(3, self.full.at[:, x, c, pl.ds(half, half)], 0, 1, 0)

    def three(self):
        c = self.place[3]
        self.copies[2].wait_recv()
        self.copies[3].wait_recv()
        self.push(4, self.full.at[:, :, c], 0, 0, 1)

    def last(self):
        self.copies[4].wait_recv()

    def drain(self):
        for copy in self.copies:
            copy.wait_send()


def gather_sems():
    return [pltpu.SemaphoreType.DMA((5,)), pltpu.SemaphoreType.DMA((5,))]


def ids_body(mine, full, send_sem, recv_sem):
    place = my_place()
    meet(place)
    full[place[0]] = mine[...]
    copies = []
    for k in range(1, 8):
        copies.append(push(mine, full.at[place[0]], send_sem.at[k], recv_sem.at[k], peer_of(place, k // 4, (k // 2) % 2, k % 2)))
    for copy in copies:
        copy.wait()


def share_ids(targ_loc):
    vmem = pl.BlockSpec(memory_space=pltpu.VMEM)
    return pl.pallas_call(
        ids_body,
        out_shape=jax.ShapeDtypeStruct((8, 8, 128), jnp.int32),
        in_specs=[vmem],
        out_specs=vmem,
        scratch_shapes=[pltpu.SemaphoreType.DMA((8,)), pltpu.SemaphoreType.DMA((8,))],
        compiler_params=pltpu.CompilerParams(collective_id=0, has_side_effects=True),
        name="share_ids",
    )(targ_loc.reshape(8, 128))


PIECE = 256


def fetch_body(data_c, data_t, wi_one, wi_two, tokens, w_one, w_two, cand_raw, c_pre, c_hid, cand_vec, targ_raw, t_pre, t_hid, targ_vec, q_pre, q_hid, query, in_one, mid, in_xa, in_yb, part_a, part_b, in_ya, in_xb, rs_send, rs_recv, ag_send, ag_recv):
    place = my_place()
    me, y, x, c = place
    half = PIECE // 2
    meet(place)
    reduces = []
    for k in range(6):
        data = data_c.at[:, :, :, pl.ds(k * PIECE, PIECE)] if k < 2 else data_t.at[:, :, :, pl.ds((k - 2) * PIECE, PIECE)]
        reduces.append(Reduce(place, data, in_one.at[k], mid.at[k], in_xa.at[k], in_yb.at[k], part_a.at[k], part_b.at[k], in_ya.at[k], in_xb.at[k], rs_send.at[k], rs_recv.at[k]))
    ag = Gather(place, cand_vec, ag_send, ag_recv)

    def close(k, out, base):
        first, second = reduces[k].last()
        out[base : base + half, :] = first
        out[base + half : base + PIECE, :] = second

    def tower(rows_ref, at, w_in, w_out, pre_ref, hid_ref):
        pre, hid, vec = tower_fwd(rows_ref[at, :], w_in[...], w_out[...])
        pre_ref[at, :] = pre
        hid_ref[at, :] = hid
        return vec

    for k in range(6):
        reduces[k].one()
    reduces[0].two()
    reduces[1].two()
    reduces[2].two()
    query[0:256, :] = tower(tokens, slice(0, 256), w_one, w_two, q_pre, q_hid)
    reduces[0].three()
    reduces[1].three()
    reduces[3].two()
    query[256:512, :] = tower(tokens, slice(256, 512), w_one, w_two, q_pre, q_hid)
    close(0, cand_raw, 0)
    close(1, cand_raw, PIECE)
    cand_vec[y, x, c] = tower(cand_raw, slice(0, 512), wi_one, wi_two, c_pre, c_hid)
    ag.one()
    reduces[2].three()
    reduces[4].two()
    query[512:768, :] = tower(tokens, slice(512, 768), w_one, w_two, q_pre, q_hid)
    ag.two()
    reduces[3].three()
    reduces[5].two()
    query[768:1024, :] = tower(tokens, slice(768, 1024), w_one, w_two, q_pre, q_hid)
    close(2, targ_raw, 0)
    targ_vec[0:256, :] = tower(targ_raw, slice(0, 256), wi_one, wi_two, t_pre, t_hid)
    reduces[4].three()
    ag.three()
    close(3, targ_raw, PIECE)
    targ_vec[256:512, :] = tower(targ_raw, slice(256, 512), wi_one, wi_two, t_pre, t_hid)
    reduces[5].three()
    close(4, targ_raw, 2 * PIECE)
    targ_vec[512:768, :] = tower(targ_raw, slice(512, 768), wi_one, wi_two, t_pre, t_hid)
    close(5, targ_raw, 3 * PIECE)
    targ_vec[768:1024, :] = tower(targ_raw, slice(768, 1024), wi_one, wi_two, t_pre, t_hid)
    ag.last()
    for red in reduces:
        red.drain()
    ag.drain()


def fetch_rows(data_c, data_t, wi_one, wi_two, tokens, w_one, w_two):
    n_mine, width = data_c.shape[3:]
    n_tok = data_t.shape[3]
    ff = wi_one.shape[1]
    vmem = pl.BlockSpec(memory_space=pltpu.VMEM)

    def outs(n):
        return [jax.ShapeDtypeStruct((n, ff), jnp.float32), jax.ShapeDtypeStruct((n, ff), jnp.bfloat16)]

    def rows(n):
        return [jax.ShapeDtypeStruct((n, width), jnp.bfloat16)]

    full = [jax.ShapeDtypeStruct((2, 2, 2, n_mine, width), jnp.bfloat16)]
    return pl.pallas_call(
        fetch_body,
        out_shape=tuple(rows(n_mine) + outs(n_mine) + full + rows(n_tok) + outs(n_tok) + rows(n_tok) + outs(n_tok) + rows(n_tok)),
        in_specs=[vmem] * 7,
        out_specs=(vmem,) * 11,
        scratch_shapes=reduce_scratch(6, PIECE, width, jnp.bfloat16) + gather_sems(),
        compiler_params=pltpu.CompilerParams(vmem_limit_bytes=56 * 1024 * 1024, collective_id=1, has_side_effects=True),
        name="fetch_rows",
    )(data_c, data_t, wi_one, wi_two, tokens, w_one, w_two)


def back_body(d_part, loss_in, d_query, d_targ, tokens, q_pre, q_hid, w_two, targ_raw, t_pre, t_hid, cand_raw, c_pre, c_hid, wi_one, wi_two, back_t, back_c, w_mine, loss_out, *scratch):
    place = my_place()
    me, y, x, c = place
    rs_u, rs_w = scratch[0:10], scratch[10:20]
    at_send, at_recv, ac_send, ac_recv, l_send, l_recv, w_data, l_all = scratch[20:28]
    width = d_query.shape[1]
    scale = SCORE_GAIN / math.sqrt(width)
    meet(place)
    red_u = []
    for k in range(2):
        red_u.append(Reduce(place, d_part.at[:, :, :, pl.ds(k * PIECE, PIECE)], *[s.at[k] for s in rs_u]))
    red_w = Reduce(place, w_data, *[s.at[0] for s in rs_w])
    ag_t = Gather(place, back_t, at_send, at_recv)
    ag_c = Gather(place, back_c, ac_send, ac_recv)
    red_u[0].one()
    red_u[1].one()
    l_all[me] = loss_in[...]
    l_copies = []
    for k in range(1, 8):
        l_copies.append(push(loss_in, l_all.at[me], l_send.at[k], l_recv.at[k], peer_of(place, k // 4, (k // 2) % 2, k % 2)))

    def put(first, value):
        n = value.shape[0] // 8
        for b in range(8):
            w_data[b // 4, (b // 2) % 2, b % 2, first : first + n, :] = value[b * n : (b + 1) * n, :]

    t_q, dwi_one, dwi_two = tower_back(targ_raw[...], wi_two[...], t_pre[...], t_hid[...], d_targ[...])
    back_t[y, x, c] = by_transpose(t_q, wi_one[...]).astype(jnp.bfloat16)
    red_u[0].two()
    red_u[1].two()
    ag_t.one()
    _, dw_one, dw_two = tower_back(tokens[...], w_two[...], q_pre[...], q_hid[...], d_query[...])
    put(0, dw_one[:, :width])
    put(128, dw_one[:, width:])
    put(256, dw_two)
    red_u[0].three()
    red_u[1].three()
    ag_t.two()
    parts = []
    for k in range(2):
        first, second = red_u[k].last()
        parts += [first, second]
    d_cand = (jnp.concatenate(parts, axis=0) * scale).astype(jnp.bfloat16)
    c_q, dwi_one_c, dwi_two_c = tower_back(cand_raw[...], wi_two[...], c_pre[...], c_hid[...], d_cand)
    back_c[y, x, c] = by_transpose(c_q, wi_one[...]).astype(jnp.bfloat16)
    ag_c.one()
    dwi_one = dwi_one + dwi_one_c
    put(320, dwi_one[:, :width])
    put(352, dwi_one[:, width:])
    put(384, dwi_two + dwi_two_c)
    red_w.one()
    for copy in l_copies:
        copy.wait()
    loss_out[...] = jnp.sum(l_all[...], axis=0)
    ag_c.two()
    red_w.two()
    ag_t.three()
    red_w.three()
    ag_c.three()
    first, second = red_w.last()
    half = first.shape[0]
    w_mine[0:half, :] = first
    w_mine[half : 2 * half, :] = second
    ag_t.last()
    ag_c.last()
    for part in red_u + [red_w, ag_t, ag_c]:
        part.drain()


W_ROWS = 448


def back_rows(d_part, loss_part, *rest):
    n_mine, width = d_part.shape[3:]
    n_tok = rest[0].shape[0]
    vmem = pl.BlockSpec(memory_space=pltpu.VMEM)
    sems = [pltpu.SemaphoreType.DMA((8,)), pltpu.SemaphoreType.DMA((8,))]
    return pl.pallas_call(
        back_body,
        out_shape=(
            jax.ShapeDtypeStruct((2, 2, 2, n_tok, width), jnp.bfloat16),
            jax.ShapeDtypeStruct((2, 2, 2, n_mine, width), jnp.bfloat16),
            jax.ShapeDtypeStruct((W_ROWS, width), jnp.float32),
            jax.ShapeDtypeStruct((8, 128), jnp.float32),
        ),
        in_specs=[vmem] * 16,
        out_specs=(vmem,) * 4,
        scratch_shapes=reduce_scratch(2, PIECE, width, jnp.float32) + reduce_scratch(1, W_ROWS, width, jnp.float32) + gather_sems() + gather_sems() + sems + [pltpu.VMEM((2, 2, 2, W_ROWS, width), jnp.float32), pltpu.VMEM((8, 8, 128), jnp.float32)],
        compiler_params=pltpu.CompilerParams(vmem_limit_bytes=60 * 1024 * 1024, collective_id=2, has_side_effects=True),
        name="back_rows",
    )(d_part, loss_part, *rest)


def solution(mesh):
    num_dev = mesh.shape["dp"]

    def local_step(tokens, w_one, w_two, wi_one, wi_two, table_loc, cand_ids, log_q, targ_loc):
        my_index = lax.axis_index("dp")
        rows_loc, width = table_loc.shape
        n_cand = cand_ids.shape[0]
        tok_total = tokens.shape[0] * num_dev
        targ_all = share_ids(targ_loc).reshape(-1)
        local_ids = jnp.concatenate([cand_ids, targ_all]) - my_index * rows_loc
        ids_two = 2 * jnp.where((local_ids >= 0) & (local_ids < rows_loc), local_ids, rows_loc)
        data_c, data_t = pick_rows(ids_two, table_loc, n_cand)
        data_c = data_c.reshape(2, 2, 2, n_cand // 8, width)
        data_t = data_t.reshape(2, 2, 2, tokens.shape[0], width)
        cand_mine, c_pre, c_hid, cand_vec, targ_raw, t_pre, t_hid, targ_vec, q_pre, q_hid, query = fetch_rows(data_c, data_t, wi_one, wi_two, tokens, w_one, w_two)
        cand_vec = cand_vec.reshape(n_cand, width)
        loss_part, d_query, d_targ_vec, d_part = softmax_grads(query, targ_vec, cand_vec, log_q, targ_loc, cand_ids, tok_total)
        back_t, back_c, w_mine, loss = back_rows(d_part.reshape(2, 2, 2, n_cand // 8, width), loss_part, d_query, d_targ_vec, tokens, q_pre, q_hid, w_two, targ_raw, t_pre, t_hid, cand_mine, c_pre, c_hid, wi_one, wi_two)
        w_all = lax.all_gather(w_mine, "dp", axis=0)
        d_table = scatter_rows(ids_two, back_c.reshape(-1, width), back_t.reshape(-1, width), rows_loc)

        def pair(first, n):
            return jnp.concatenate([w_all[:, first : first + n].reshape(8 * n, width), w_all[:, first + n : first + 2 * n].reshape(8 * n, width)], axis=1)

        dw_one = pair(0, 128)
        dw_two = w_all[:, 256:320].reshape(-1, width)
        dwi_one = pair(320, 32)
        dwi_two = w_all[:, 384:448].reshape(-1, width)
        return loss[0, 0] / tok_total, d_table, dw_one, dw_two, dwi_one, dwi_two

    return jax.shard_map(local_step, mesh=mesh, in_specs=(P("dp", None), P(), P(), P(), P(), P("dp", None), P(), P(), P("dp")), out_specs=(P(), P("dp", None), P(), P(), P(), P()), check_vma=False)
```

```python
import functools
import math
import jax
import jax.numpy as jnp
from jax import lax
from jax.experimental import pallas as pl
from jax.experimental.pallas import tpu as pltpu
from jax.sharding import PartitionSpec as P

SCORE_GAIN = 3.0
HIT_VALUE = -1e9


def tower_fwd(row_block, w_in, w_out):
    pre_act = jnp.dot(row_block, w_in, preferred_element_type=jnp.float32)
    hidden = jax.nn.gelu(pre_act).astype(jnp.bfloat16)
    tower_out = jnp.dot(hidden, w_out, preferred_element_type=jnp.float32).astype(jnp.bfloat16)
    return pre_act, hidden, tower_out


def over_rows(a, b):
    return lax.dot_general(a, b, (((0,), (0,)), ((), ())), preferred_element_type=jnp.float32)


def by_transpose(a, b):
    return lax.dot_general(a, b, (((1,), (1,)), ((), ())), preferred_element_type=jnp.float32)


def grad_through(grad_out, w_out, pre_act):
    grad_hidden = by_transpose(grad_out, w_out)
    gelu_back = jax.vjp(jax.nn.gelu, pre_act)[1]
    return gelu_back(grad_hidden)[0].astype(jnp.bfloat16)


def tower_back(row_block, w_out, pre_act, hidden, grad_out):
    dw_out = over_rows(hidden, grad_out)
    grad_pre = grad_through(grad_out, w_out, pre_act)
    dw_in = over_rows(row_block, grad_pre)
    return grad_pre, dw_in, dw_out


GROUP = 16
BATCH = 128
SPARE = 256
STAGE_ROWS = 2048
OUT_ROWS = 1024


def pick_body(ids_s, table, cand_out, targ_out, wide, stage, rows_f, stage_sem):
    rows_loc, width = table.shape
    lane = width // 2
    n_stage = rows_loc // STAGE_ROWS

    def stage_copy(i, slot):
        return pltpu.make_async_copy(table.at[pl.ds(i * STAGE_ROWS, STAGE_ROWS)], stage.at[slot], stage_sem.at[slot])

    for i in range(3):
        stage_copy(i, i).start()
    wide[pl.ds(2 * rows_loc, 2 * SPARE), :] = jnp.zeros((2 * SPARE, lane), jnp.float32)

    @pl.loop(0, n_stage)
    def _(i):
        slot = i % 4

        @pl.when(i + 3 < n_stage)
        def _():
            stage_copy(i + 3, (i + 3) % 4).start()

        stage_copy(i, slot).wait()

        @pl.loop(0, STAGE_ROWS // 128)
        def _(j):
            block = stage[slot, pl.ds(pl.multiple_of(j * 128, 128), 128), :].astype(jnp.float32)
            base = pl.multiple_of((i * STAGE_ROWS + j * 128) * 2, 256)
            wide[pl.ds(base, 128, 2), :] = block[:, :lane]
            wide[pl.ds(base + 1, 128, 2), :] = block[:, lane:]

    def fill(out, first):
        @pl.loop(0, out.shape[0] // BATCH)
        def _(b):
            for r in range(BATCH):
                at = pl.multiple_of(ids_s[first + b * BATCH + r], 2)
                rows_f[pl.ds(2 * r, 2), :] = wide[pl.ds(at, 2), :]
            rows = pl.ds(pl.multiple_of(b * BATCH, BATCH), BATCH)
            out[rows, :lane] = rows_f[pl.ds(0, BATCH, 2), :].astype(jnp.bfloat16)
            out[rows, lane:] = rows_f[pl.ds(1, BATCH, 2), :].astype(jnp.bfloat16)

    fill(cand_out, 0)
    fill(targ_out, cand_out.shape[0])


def pick_rows(ids_two, table_loc, n_cand):
    rows_loc, width = table_loc.shape
    n_targ = ids_two.shape[0] - n_cand
    vmem = pl.BlockSpec(memory_space=pltpu.VMEM)
    return pl.pallas_call(
        pick_body,
        out_shape=(jax.ShapeDtypeStruct((n_cand, width), jnp.bfloat16), jax.ShapeDtypeStruct((n_targ, width), jnp.bfloat16)),
        in_specs=[pl.BlockSpec(memory_space=pltpu.SMEM), pl.BlockSpec(memory_space=pl.ANY)],
        out_specs=(vmem, vmem),
        scratch_shapes=[
            pltpu.VMEM((2 * (rows_loc + SPARE), width // 2), jnp.float32),
            pltpu.VMEM((4, STAGE_ROWS, width), jnp.bfloat16),
            pltpu.VMEM((2 * BATCH, width // 2), jnp.float32),
            pltpu.SemaphoreType.DMA((4,)),
        ],
        compiler_params=pltpu.CompilerParams(vmem_limit_bytes=50 * 1024 * 1024),
        name="pick_rows",
    )(ids_two, table_loc)


def scatter_body(ids_s, ids_v, cand_ref, targ_ref, out_ref, acc, g2, out_stage, sem):
    rows, width = out_ref.shape
    lane = width // 2
    n_cand = cand_ref.shape[0]
    n_all = n_cand + targ_ref.shape[0]

    @pl.loop(0, 2 * rows // 512)
    def _(i):
        acc[pl.ds(pl.multiple_of(i * 512, 512), 512), :] = jnp.zeros((512, lane), jnp.float32)

    row_i = lax.broadcasted_iota(jnp.int32, (BATCH, BATCH), 0) // GROUP
    col_i = lax.broadcasted_iota(jnp.int32, (BATCH, BATCH), 1) // GROUP
    same_group = row_i == col_i

    def one_batch(b, src, src_base):
        idr = jnp.broadcast_to(ids_v[pl.ds(b, 1), :], (BATCH, BATCH))
        same = jnp.where((idr == idr.T) & same_group, 1.0, 0.0).astype(jnp.bfloat16)
        part = jnp.dot(same, src[pl.ds(pl.multiple_of(b * BATCH - src_base, BATCH), BATCH), :], preferred_element_type=jnp.float32)
        g2[pl.ds(0, BATCH, 2), :] = part[:, :lane]
        g2[pl.ds(1, BATCH, 2), :] = part[:, lane:]
        for g in range(BATCH // GROUP):
            idx = [pl.multiple_of(ids_s[b * BATCH + g * GROUP + r], 2) for r in range(GROUP)]
            new = [acc[pl.ds(idx[r], 2), :] + g2[pl.ds(2 * (g * GROUP + r), 2), :] for r in range(GROUP)]
            for r in range(GROUP):
                acc[pl.ds(idx[r], 2), :] = new[r]

    @pl.loop(0, n_cand // BATCH)
    def _(b):
        one_batch(b, cand_ref, 0)

    @pl.loop(n_cand // BATCH, n_all // BATCH)
    def _(b):
        one_batch(b, targ_ref, n_cand)

    n_out = rows // OUT_ROWS

    def out_copy(i, slot):
        return pltpu.make_async_copy(out_stage.at[slot], out_ref.at[pl.ds(i * OUT_ROWS, OUT_ROWS)], sem.at[slot])

    @pl.loop(0, n_out)
    def _(i):
        slot = i % 4

        @pl.when(i >= 4)
        def _():
            out_copy(i - 4, slot).wait()

        @pl.loop(0, OUT_ROWS // 128)
        def _(j):
            base = pl.multiple_of((i * OUT_ROWS + j * 128) * 2, 256)
            here = pl.ds(pl.multiple_of(j * 128, 128), 128)
            out_stage[slot, here, :lane] = acc[pl.ds(base, 128, 2), :]
            out_stage[slot, here, lane:] = acc[pl.ds(base + 1, 128, 2), :]

        out_copy(i, slot).start()

    for i in range(n_out - 4, n_out):
        out_copy(i, i % 4).wait()


def scatter_rows(ids_two, back_cand, back_targ, rows_loc):
    n_all = ids_two.shape[0]
    width = back_cand.shape[1]
    vmem = pl.BlockSpec(memory_space=pltpu.VMEM)
    return pl.pallas_call(
        scatter_body,
        out_shape=jax.ShapeDtypeStruct((rows_loc, width), jnp.float32),
        in_specs=[pl.BlockSpec(memory_space=pltpu.SMEM), vmem, vmem, vmem],
        out_specs=pl.BlockSpec(memory_space=pl.ANY),
        scratch_shapes=[
            pltpu.VMEM((2 * (rows_loc + SPARE), width // 2), jnp.float32),
            pltpu.VMEM((2 * BATCH, width // 2), jnp.float32),
            pltpu.VMEM((4, OUT_ROWS, width), jnp.float32),
            pltpu.SemaphoreType.DMA((4,)),
        ],
        compiler_params=pltpu.CompilerParams(vmem_limit_bytes=52 * 1024 * 1024),
        cost_estimate=pl.CostEstimate(flops=60_000_000_000, bytes_accessed=40 << 20, transcendentals=0),
        name="scatter_rows",
    )(ids_two, ids_two.reshape(n_all // BATCH, BATCH), back_cand, back_targ)


TOK_BLK = 256
CHUNK = 256
SUB = 64
BACK_CHUNK = 512


def softmax_body(tok_total, h_ref, v_ref, u_ref, lq_ref, cid_ref, tid_ref, loss_ref, dh_ref, dv_ref, du_ref, e_s, m_s, ut_s):
    step = pl.program_id(0)
    n_cand, width = u_ref.shape
    scale = SCORE_GAIN / math.sqrt(width)

    @pl.when(step == 0)
    def _():
        loss_ref[...] = jnp.zeros_like(loss_ref)
        du_ref[...] = jnp.zeros_like(du_ref)
        for i in range(n_cand // 512):
            ut_s[:, i * 512 : (i + 1) * 512] = u_ref[i * 512 : (i + 1) * 512, :].T

    h = h_ref[...]
    hf = h.astype(jnp.float32)
    vf = v_ref[...].astype(jnp.float32)
    ht = h.T
    zt = jnp.sum(hf * vf, axis=1, keepdims=True) * scale
    zt = jnp.broadcast_to(zt, (TOK_BLK, 128)).T[0:1, :]
    tid = tid_ref[0]
    lanes = TOK_BLK // 128

    def forward(i, carry):
        m8, s8 = carry
        off = pl.multiple_of(i * CHUNK, CHUNK)
        z_all = jnp.dot(u_ref[pl.ds(off, CHUNK), :], ht, preferred_element_type=jnp.float32)
        for k in range(CHUNK // SUB):
            rows = pl.ds(pl.multiple_of(off + k * SUB, SUB), SUB)
            lq = jnp.concatenate([lq_ref[rows, :]] * lanes, axis=1)
            cid = jnp.concatenate([cid_ref[rows, :]] * lanes, axis=1)
            z = z_all[k * SUB : (k + 1) * SUB] * scale - lq
            z = jnp.where(cid == tid, HIT_VALUE, z).reshape(SUB // 8, 8, TOK_BLK)
            m_new = jnp.maximum(m8, jnp.max(z, axis=0))
            e = jnp.exp(z - m_new[None])
            s8 = s8 * jnp.exp(m8 - m_new) + jnp.sum(e, axis=0)
            m8 = m_new
            e_s[rows, :] = e.reshape(SUB, TOK_BLK)
            m_s[pl.ds(pl.multiple_of(i * (8 * CHUNK // SUB) + 8 * k, 8), 8), :] = m8
        return m8, s8

    m8, s8 = lax.fori_loop(0, n_cand // CHUNK, forward, (jnp.broadcast_to(zt, (8, TOK_BLK)), jnp.zeros((8, TOK_BLK), jnp.float32)))
    m = jnp.max(m8, axis=0, keepdims=True)
    et = jnp.exp(zt - m)
    den = et + jnp.sum(s8 * jnp.exp(m8 - m), axis=0, keepdims=True)
    part = jnp.sum(jnp.log(den) + m - zt, axis=1, keepdims=True)
    dzt = ((et / den - 1.0) / tok_total).astype(jnp.bfloat16).astype(jnp.float32)
    inv = 1.0 / den / tok_total
    loss_ref[...] += jnp.broadcast_to(part, loss_ref.shape)

    def backward(i, dht):
        off = pl.multiple_of(i * BACK_CHUNK, BACK_CHUNK)
        pieces = []
        for k in range(BACK_CHUNK // SUB):
            rows = pl.ds(pl.multiple_of(off + k * SUB, SUB), SUB)
            m_k = m_s[pl.ds(pl.multiple_of(i * (8 * BACK_CHUNK // SUB) + 8 * k, 8), 8), :]
            fac = jnp.exp(m_k - m) * inv
            pieces.append((e_s[rows, :].reshape(SUB // 8, 8, TOK_BLK) * fac[None]).reshape(SUB, TOK_BLK).astype(jnp.bfloat16))
        dz = jnp.concatenate(pieces, axis=0)
        du_ref[pl.ds(off, BACK_CHUNK), :] += jnp.dot(dz, h, preferred_element_type=jnp.float32)
        return dht + jnp.dot(ut_s[:, pl.ds(off, BACK_CHUNK)], dz, preferred_element_type=jnp.float32)

    dht = lax.fori_loop(0, n_cand // BACK_CHUNK, backward, jnp.zeros((width, TOK_BLK), jnp.float32))
    dzt_c = jnp.broadcast_to(dzt, (128, TOK_BLK)).T[:, 0:1]
    dh_ref[...] = ((dzt_c * vf + dht.T) * scale).astype(jnp.bfloat16)
    dv_ref[...] = (scale * dzt_c * hf).astype(jnp.bfloat16)


def softmax_grads(query, targ_vec, cand_vec, lq_b, cid_b, targ_ids, tok_total):
    n_tok, width = query.shape
    n_cand = cand_vec.shape[0]
    steps = n_tok // TOK_BLK
    whole = lambda s: (0, 0)
    return pl.pallas_call(
        functools.partial(softmax_body, tok_total),
        grid=(steps,),
        out_shape=(jax.ShapeDtypeStruct((8, 128), jnp.float32), jax.ShapeDtypeStruct((n_tok, width), jnp.bfloat16), jax.ShapeDtypeStruct((n_tok, width), jnp.bfloat16), jax.ShapeDtypeStruct((n_cand, width), jnp.float32)),
        in_specs=[
            pl.BlockSpec((TOK_BLK, width), lambda s: (s, 0)),
            pl.BlockSpec((TOK_BLK, width), lambda s: (s, 0)),
            pl.BlockSpec((n_cand, width), whole),
            pl.BlockSpec((n_cand, 128), whole),
            pl.BlockSpec((n_cand, 128), whole),
            pl.BlockSpec((1, 1, TOK_BLK), lambda s: (s, 0, 0)),
        ],
        out_specs=(
            pl.BlockSpec((8, 128), whole),
            pl.BlockSpec((TOK_BLK, width), lambda s: (s, 0)),
            pl.BlockSpec((TOK_BLK, width), lambda s: (s, 0)),
            pl.BlockSpec((n_cand, width), whole),
        ),
        scratch_shapes=[pltpu.VMEM((n_cand, TOK_BLK), jnp.float32), pltpu.VMEM((8 * n_cand // SUB, TOK_BLK), jnp.float32), pltpu.VMEM((width, n_cand), jnp.bfloat16)],
        compiler_params=pltpu.CompilerParams(vmem_limit_bytes=48 * 1024 * 1024, dimension_semantics=("arbitrary",)),
        cost_estimate=pl.CostEstimate(flops=6 * n_tok * n_cand * width, bytes_accessed=16 << 20, transcendentals=n_tok * n_cand),
        name="softmax_grads",
    )(query, targ_vec, cand_vec, lq_b, cid_b, targ_ids.reshape(steps, 1, TOK_BLK))


MESH = pl.DeviceIdType.MESH


def my_place():
    me = lax.axis_index("dp")
    return me, me // 4, (me // 2) % 2, me % 2


def peer_of(place, dy, dx, dc):
    me, y, x, c = place
    return me + dy * (4 - 8 * y) + dx * (2 - 4 * x) + dc * (1 - 2 * c)


def greet(place):
    barrier = pltpu.get_barrier_semaphore()
    for k in range(1, 8):
        pl.semaphore_signal(barrier, inc=1, device_id=(peer_of(place, k // 4, (k // 2) % 2, k % 2),), device_id_type=MESH)


def meet(place):
    greet(place)
    pl.semaphore_wait(pltpu.get_barrier_semaphore(), 7)


def push(src, dst, send_sem, recv_sem, peer):
    copy = pltpu.make_async_remote_copy(src_ref=src, dst_ref=dst, send_sem=send_sem, recv_sem=recv_sem, device_id=(peer,), device_id_type=MESH)
    copy.start()
    return copy


class Reduce:
    def __init__(self, place, data, in_one, mid, in_xa, in_yb, part_a, part_b, in_ya, in_xb, send_sem, recv_sem):
        self.place, self.data = place, data
        self.in_one, self.mid, self.in_xa, self.in_yb = in_one, mid, in_xa, in_yb
        self.part_a, self.part_b, self.in_ya, self.in_xb = part_a, part_b, in_ya, in_xb
        self.send_sem, self.recv_sem = send_sem, recv_sem
        self.half = data.shape[3] // 2
        self.copies = []

    def push(self, k, src, dst, dy, dx, dc):
        copy = push(src, dst, self.send_sem.at[k], self.recv_sem.at[k], peer_of(self.place, dy, dx, dc))
        self.copies.append(copy)

    def one(self):
        c = self.place[3]
        self.push(0, self.data.at[:, :, 1 - c], self.in_one, 0, 0, 1)

    def two(self):
        _, y, x, c = self.place
        half = self.half
        self.copies[0].wait_recv()
        for i in range(2):
            for j in range(2):
                self.mid[i, j] = self.data[i, j, c] + self.in_one[i, j]
        self.push(1, self.mid.at[:, 1 - x, pl.ds(0, half)], self.in_xa, 0, 1, 0)
        self.push(2, self.mid.at[1 - y, :, pl.ds(half, half)], self.in_yb, 1, 0, 0)

    def three(self):
        _, y, x, c = self.place
        half = self.half
        self.copies[1].wait_recv()
        for i in range(2):
            self.part_a[i] = self.mid[i, x, 0:half] + self.in_xa[i]
        self.push(3, self.part_a.at[1 - y], self.in_ya, 1, 0, 0)
        self.copies[2].wait_recv()
        for i in range(2):
            self.part_b[i] = self.mid[y, i, half : 2 * half] + self.in_yb[i]
        self.push(4, self.part_b.at[1 - x], self.in_xb, 0, 1, 0)

    def last(self):
        _, y, x, c = self.place
        self.copies[3].wait_recv()
        first = self.part_a[y] + self.in_ya[...]
        self.copies[4].wait_recv()
        return first, self.part_b[x] + self.in_xb[...]

    def drain(self):
        for copy in self.copies:
            copy.wait_send()


def reduce_scratch(n, rows, width, dtype):
    half = rows // 2
    return [
        pltpu.VMEM((n, 2, 2, rows, width), dtype),
        pltpu.VMEM((n, 2, 2, rows, width), dtype),
        pltpu.VMEM((n, 2, half, width), dtype),
        pltpu.VMEM((n, 2, half, width), dtype),
        pltpu.VMEM((n, 2, half, width), dtype),
        pltpu.VMEM((n, 2, half, width), dtype),
        pltpu.VMEM((n, half, width), dtype),
        pltpu.VMEM((n, half, width), dtype),
        pltpu.SemaphoreType.DMA((n, 5)),
        pltpu.SemaphoreType.DMA((n, 5)),
    ]


class Gather:
    def __init__(self, place, full, send_sem, recv_sem):
        self.place, self.full = place, full
        self.send_sem, self.recv_sem = send_sem, recv_sem
        self.half = full.shape[3] // 2
        self.copies = []

    def push(self, k, ref, dy, dx, dc):
        copy = push(ref, ref, self.send_sem.at[k], self.recv_sem.at[k], peer_of(self.place, dy, dx, dc))
        self.copies.append(copy)

    def one(self):
        _, y, x, c = self.place
        half = self.half
        self.push(0, self.full.at[y, x, c, pl.ds(0, half)], 0, 1, 0)
        self.push(1, self.full.at[y, x, c, pl.ds(half, half)], 1, 0, 0)

    def two(self):
        _, y, x, c = self.place
        half = self.half
        self.copies[0].wait_recv()
        self.push(2, self.full.at[y, :, c, pl.ds(0, half)], 1, 0, 0)
        self.copies[1].wait_recv()
        self.push(3, self.full.at[:, x, c, pl.ds(half, half)], 0, 1, 0)

    def three(self):
        c = self.place[3]
        self.copies[2].wait_recv()
        self.copies[3].wait_recv()
        self.push(4, self.full.at[:, :, c], 0, 0, 1)

    def last(self):
        self.copies[4].wait_recv()

    def drain(self):
        for copy in self.copies:
            copy.wait_send()


def gather_sems():
    return [pltpu.SemaphoreType.DMA((5,)), pltpu.SemaphoreType.DMA((5,))]


def prepare_body(mine, lq_ref, cid_ref, tokens, w_one, w_two, full, lq_out, cid_out, q_pre, q_hid, query, send_sem, recv_sem):
    place = my_place()
    greet(place)
    for i in range(tokens.shape[0] // 256):
        at = slice(i * 256, i * 256 + 256)
        pre, hid, vec = tower_fwd(tokens[at, :], w_one[...], w_two[...])
        q_pre[at, :] = pre
        q_hid[at, :] = hid
        query[at, :] = vec
    pl.semaphore_wait(pltpu.get_barrier_semaphore(), 7)
    full[place[0]] = mine[...]
    copies = []
    for k in range(1, 8):
        copies.append(push(mine, full.at[place[0]], send_sem.at[k], recv_sem.at[k], peer_of(place, k // 4, (k // 2) % 2, k % 2)))

    @pl.loop(0, lq_ref.shape[0])
    def _(i):
        rows = pl.ds(pl.multiple_of(i * 128, 128), 128)
        lq_out[rows, :] = jnp.broadcast_to(lq_ref[pl.ds(i, 1), :], (128, 128)).T
        cid_out[rows, :] = jnp.broadcast_to(cid_ref[pl.ds(i, 1), :], (128, 128)).T

    for copy in copies:
        copy.wait()


def prepare(targ_loc, log_q, cand_ids, tokens, w_one, w_two):
    n_cand = cand_ids.shape[0]
    n_tok = tokens.shape[0]
    ff, width = w_two.shape
    vmem = pl.BlockSpec(memory_space=pltpu.VMEM)
    return pl.pallas_call(
        prepare_body,
        out_shape=(
            jax.ShapeDtypeStruct((8, 8, 128), jnp.int32),
            jax.ShapeDtypeStruct((n_cand, 128), jnp.float32),
            jax.ShapeDtypeStruct((n_cand, 128), jnp.int32),
            jax.ShapeDtypeStruct((n_tok, ff), jnp.float32),
            jax.ShapeDtypeStruct((n_tok, ff), jnp.bfloat16),
            jax.ShapeDtypeStruct((n_tok, width), jnp.bfloat16),
        ),
        in_specs=[vmem] * 6,
        out_specs=(vmem,) * 6,
        scratch_shapes=[pltpu.SemaphoreType.DMA((8,)), pltpu.SemaphoreType.DMA((8,))],
        compiler_params=pltpu.CompilerParams(vmem_limit_bytes=40 * 1024 * 1024, collective_id=0, has_side_effects=True),
        name="prepare",
    )(targ_loc.reshape(8, 128), log_q.reshape(-1, 128), cand_ids.reshape(-1, 128), tokens, w_one, w_two)


PIECE = 256


def fetch_body(data_c, data_t, wi_one, wi_two, cand_raw, c_pre, c_hid, cand_vec, targ_raw, t_pre, t_hid, targ_vec, in_one, mid, in_xa, in_yb, part_a, part_b, in_ya, in_xb, rs_send, rs_recv, ag_send, ag_recv):
    place = my_place()
    me, y, x, c = place
    half = PIECE // 2
    meet(place)
    reduces = []
    for k in range(6):
        data = data_c.at[:, :, :, pl.ds(k * PIECE, PIECE)] if k < 2 else data_t.at[:, :, :, pl.ds((k - 2) * PIECE, PIECE)]
        reduces.append(Reduce(place, data, in_one.at[k], mid.at[k], in_xa.at[k], in_yb.at[k], part_a.at[k], part_b.at[k], in_ya.at[k], in_xb.at[k], rs_send.at[k], rs_recv.at[k]))
    ag = Gather(place, cand_vec, ag_send, ag_recv)

    def close(k, out, base):
        first, second = reduces[k].last()
        out[base : base + half, :] = first
        out[base + half : base + PIECE, :] = second

    def tower(rows_ref, at, w_in, w_out, pre_ref, hid_ref):
        pre, hid, vec = tower_fwd(rows_ref[at, :], w_in[...], w_out[...])
        pre_ref[at, :] = pre
        hid_ref[at, :] = hid
        return vec

    def targ_tower(k):
        close(k + 2, targ_raw, k * PIECE)
        at = slice(k * PIECE, (k + 1) * PIECE)
        targ_vec[at, :] = tower(targ_raw, at, wi_one, wi_two, t_pre, t_hid)

    for k in range(6):
        reduces[k].one()
    reduces[0].two()
    reduces[1].two()
    reduces[2].two()
    reduces[0].three()
    reduces[1].three()
    reduces[3].two()
    reduces[4].two()
    close(0, cand_raw, 0)
    close(1, cand_raw, PIECE)
    cand_vec[y, x, c] = tower(cand_raw, slice(0, 512), wi_one, wi_two, c_pre, c_hid)
    ag.one()
    reduces[5].two()
    reduces[2].three()
    ag.two()
    reduces[3].three()
    reduces[4].three()
    targ_tower(0)
    reduces[5].three()
    targ_tower(1)
    ag.three()
    targ_tower(2)
    targ_tower(3)
    ag.last()
    for red in reduces:
        red.drain()
    ag.drain()


def fetch_rows(data_c, data_t, wi_one, wi_two):
    n_mine, width = data_c.shape[3:]
    n_tok = data_t.shape[3]
    ff = wi_one.shape[1]
    vmem = pl.BlockSpec(memory_space=pltpu.VMEM)

    def outs(n):
        return [jax.ShapeDtypeStruct((n, ff), jnp.float32), jax.ShapeDtypeStruct((n, ff), jnp.bfloat16)]

    def rows(n):
        return [jax.ShapeDtypeStruct((n, width), jnp.bfloat16)]

    full = [jax.ShapeDtypeStruct((2, 2, 2, n_mine, width), jnp.bfloat16)]
    return pl.pallas_call(
        fetch_body,
        out_shape=tuple(rows(n_mine) + outs(n_mine) + full + rows(n_tok) + outs(n_tok) + rows(n_tok)),
        in_specs=[vmem] * 4,
        out_specs=(vmem,) * 8,
        scratch_shapes=reduce_scratch(6, PIECE, width, jnp.bfloat16) + gather_sems(),
        compiler_params=pltpu.CompilerParams(vmem_limit_bytes=56 * 1024 * 1024, collective_id=1, has_side_effects=True),
        name="fetch_rows",
    )(data_c, data_t, wi_one, wi_two)


def back_body(d_part, loss_in, d_query, d_targ, tokens, q_pre, q_hid, w_two, targ_raw, t_pre, t_hid, cand_raw, c_pre, c_hid, wi_one, wi_two, back_t, back_c, w_mine, loss_out, *scratch):
    place = my_place()
    me, y, x, c = place
    rs_u, rs_w = scratch[0:10], scratch[10:20]
    at_send, at_recv, ac_send, ac_recv, l_send, l_recv, w_data, l_all = scratch[20:28]
    width = d_query.shape[1]
    scale = SCORE_GAIN / math.sqrt(width)
    meet(place)
    red_u = []
    for k in range(2):
        red_u.append(Reduce(place, d_part.at[:, :, :, pl.ds(k * PIECE, PIECE)], *[s.at[k] for s in rs_u]))
    red_w = Reduce(place, w_data, *[s.at[0] for s in rs_w])
    ag_t = Gather(place, back_t, at_send, at_recv)
    ag_c = Gather(place, back_c, ac_send, ac_recv)
    red_u[0].one()
    red_u[1].one()
    l_all[me] = loss_in[...]
    l_copies = []
    for k in range(1, 8):
        l_copies.append(push(loss_in, l_all.at[me], l_send.at[k], l_recv.at[k], peer_of(place, k // 4, (k // 2) % 2, k % 2)))

    def put(first, value):
        n = value.shape[0] // 8
        for b in range(8):
            w_data[b // 4, (b // 2) % 2, b % 2, first : first + n, :] = value[b * n : (b + 1) * n, :]

    dwi_two = over_rows(t_hid[...], d_targ[...])
    red_u[0].two()
    red_u[1].two()
    t_q = grad_through(d_targ[...], wi_two[...], t_pre[...])
    back_t[y, x, c] = by_transpose(t_q, wi_one[...]).astype(jnp.bfloat16)
    ag_t.one()
    dwi_one = over_rows(targ_raw[...], t_q)
    _, dw_one, dw_two = tower_back(tokens[...], w_two[...], q_pre[...], q_hid[...], d_query[...])
    put(0, dw_one[:, :width])
    put(128, dw_one[:, width:])
    put(256, dw_two)
    red_u[0].three()
    red_u[1].three()
    ag_t.two()
    parts = []
    for k in range(2):
        first, second = red_u[k].last()
        parts += [first, second]
    d_cand = (jnp.concatenate(parts, axis=0) * scale).astype(jnp.bfloat16)
    c_q, dwi_one_c, dwi_two_c = tower_back(cand_raw[...], wi_two[...], c_pre[...], c_hid[...], d_cand)
    back_c[y, x, c] = by_transpose(c_q, wi_one[...]).astype(jnp.bfloat16)
    ag_c.one()
    dwi_one = dwi_one + dwi_one_c
    put(320, dwi_one[:, :width])
    put(352, dwi_one[:, width:])
    put(384, dwi_two + dwi_two_c)
    red_w.one()
    for copy in l_copies:
        copy.wait()
    loss_out[...] = jnp.sum(l_all[...], axis=0)
    ag_c.two()
    red_w.two()
    ag_t.three()
    red_w.three()
    ag_c.three()
    first, second = red_w.last()
    half = first.shape[0]
    w_mine[0:half, :] = first
    w_mine[half : 2 * half, :] = second
    ag_t.last()
    ag_c.last()
    for part in red_u + [red_w, ag_t, ag_c]:
        part.drain()


W_ROWS = 448


def back_rows(d_part, loss_part, *rest):
    n_mine, width = d_part.shape[3:]
    n_tok = rest[0].shape[0]
    vmem = pl.BlockSpec(memory_space=pltpu.VMEM)
    sems = [pltpu.SemaphoreType.DMA((8,)), pltpu.SemaphoreType.DMA((8,))]
    return pl.pallas_call(
        back_body,
        out_shape=(
            jax.ShapeDtypeStruct((2, 2, 2, n_tok, width), jnp.bfloat16),
            jax.ShapeDtypeStruct((2, 2, 2, n_mine, width), jnp.bfloat16),
            jax.ShapeDtypeStruct((W_ROWS, width), jnp.float32),
            jax.ShapeDtypeStruct((8, 128), jnp.float32),
        ),
        in_specs=[vmem] * 16,
        out_specs=(vmem,) * 4,
        scratch_shapes=reduce_scratch(2, PIECE, width, jnp.float32) + reduce_scratch(1, W_ROWS, width, jnp.float32) + gather_sems() + gather_sems() + sems + [pltpu.VMEM((2, 2, 2, W_ROWS, width), jnp.float32), pltpu.VMEM((8, 8, 128), jnp.float32)],
        compiler_params=pltpu.CompilerParams(vmem_limit_bytes=60 * 1024 * 1024, collective_id=2, has_side_effects=True),
        name="back_rows",
    )(d_part, loss_part, *rest)


def solution(mesh):
    num_dev = mesh.shape["dp"]

    def local_step(tokens, w_one, w_two, wi_one, wi_two, table_loc, cand_ids, log_q, targ_loc):
        my_index = lax.axis_index("dp")
        rows_loc, width = table_loc.shape
        n_cand = cand_ids.shape[0]
        tok_total = tokens.shape[0] * num_dev
        targ_all, lq_b, cid_b, q_pre, q_hid, query = prepare(targ_loc, log_q, cand_ids, tokens, w_one, w_two)
        targ_all = targ_all.reshape(-1)
        local_ids = jnp.concatenate([cand_ids, targ_all]) - my_index * rows_loc
        spare = rows_loc + jnp.arange(local_ids.shape[0], dtype=jnp.int32) % SPARE
        ids_two = 2 * jnp.where((local_ids >= 0) & (local_ids < rows_loc), local_ids, spare)
        data_c, data_t = pick_rows(ids_two, table_loc, n_cand)
        data_c = data_c.reshape(2, 2, 2, n_cand // 8, width)
        data_t = data_t.reshape(2, 2, 2, tokens.shape[0], width)
        cand_mine, c_pre, c_hid, cand_vec, targ_raw, t_pre, t_hid, targ_vec = fetch_rows(data_c, data_t, wi_one, wi_two)
        cand_vec = cand_vec.reshape(n_cand, width)
        loss_part, d_query, d_targ_vec, d_part = softmax_grads(query, targ_vec, cand_vec, lq_b, cid_b, targ_loc, tok_total)
        back_t, back_c, w_mine, loss = back_rows(d_part.reshape(2, 2, 2, n_cand // 8, width), loss_part, d_query, d_targ_vec, tokens, q_pre, q_hid, w_two, targ_raw, t_pre, t_hid, cand_mine, c_pre, c_hid, wi_one, wi_two)
        w_all = lax.all_gather(w_mine, "dp", axis=0)
        d_table = scatter_rows(ids_two, back_c.reshape(-1, width), back_t.reshape(-1, width), rows_loc)

        def pair(first, n):
            return jnp.concatenate([w_all[:, first : first + n].reshape(8 * n, width), w_all[:, first + n : first + 2 * n].reshape(8 * n, width)], axis=1)

        dw_one = pair(0, 128)
        dw_two = w_all[:, 256:320].reshape(-1, width)
        dwi_one = pair(320, 32)
        dwi_two = w_all[:, 384:448].reshape(-1, width)
        return loss[0, 0] / tok_total, d_table, dw_one, dw_two, dwi_one, dwi_two

    return jax.shard_map(local_step, mesh=mesh, in_specs=(P("dp", None), P(), P(), P(), P(), P("dp", None), P(), P(), P("dp")), out_specs=(P(), P("dp", None), P(), P(), P(), P()), check_vma=False)
```

```python
import functools
import math
import jax
import jax.numpy as jnp
from jax import lax
from jax.experimental import pallas as pl
from jax.experimental.pallas import tpu as pltpu
from jax.sharding import PartitionSpec as P

SCORE_GAIN = 3.0
HIT_VALUE = -1e9


def tower_fwd(row_block, w_in, w_out):
    pre_act = jnp.dot(row_block, w_in, preferred_element_type=jnp.float32)
    hidden = jax.nn.gelu(pre_act).astype(jnp.bfloat16)
    tower_out = jnp.dot(hidden, w_out, preferred_element_type=jnp.float32).astype(jnp.bfloat16)
    return pre_act, hidden, tower_out


def over_rows(a, b):
    return lax.dot_general(a, b, (((0,), (0,)), ((), ())), preferred_element_type=jnp.float32)


def by_transpose(a, b):
    return lax.dot_general(a, b, (((1,), (1,)), ((), ())), preferred_element_type=jnp.float32)


def grad_through(grad_out, w_out, pre_act):
    grad_hidden = by_transpose(grad_out, w_out)
    gelu_back = jax.vjp(jax.nn.gelu, pre_act)[1]
    return gelu_back(grad_hidden)[0].astype(jnp.bfloat16)


def tower_back(row_block, w_out, pre_act, hidden, grad_out):
    dw_out = over_rows(hidden, grad_out)
    grad_pre = grad_through(grad_out, w_out, pre_act)
    dw_in = over_rows(row_block, grad_pre)
    return grad_pre, dw_in, dw_out


VMEM_LIMIT = 63 * 1024 * 1024
BATCH = 128
SPARE = 256
STAGE_ROWS = 2048
OUT_ROWS = 1024


def pick_body(ids_s, table, cand_out, targ_out, wide, stage, rows_f, stage_sem):
    rows_loc, width = table.shape
    lane = width // 2
    n_stage = rows_loc // STAGE_ROWS

    def stage_copy(i, slot):
        return pltpu.make_async_copy(table.at[pl.ds(i * STAGE_ROWS, STAGE_ROWS)], stage.at[slot], stage_sem.at[slot])

    for i in range(3):
        stage_copy(i, i).start()
    wide[pl.ds(2 * rows_loc, 2 * SPARE), :] = jnp.zeros((2 * SPARE, lane), jnp.float32)

    @pl.loop(0, n_stage)
    def _(i):
        slot = i % 4

        @pl.when(i + 3 < n_stage)
        def _():
            stage_copy(i + 3, (i + 3) % 4).start()

        stage_copy(i, slot).wait()

        @pl.loop(0, STAGE_ROWS // 128)
        def _(j):
            block = stage[slot, pl.ds(pl.multiple_of(j * 128, 128), 128), :].astype(jnp.float32)
            base = pl.multiple_of((i * STAGE_ROWS + j * 128) * 2, 256)
            wide[pl.ds(base, 128, 2), :] = block[:, :lane]
            wide[pl.ds(base + 1, 128, 2), :] = block[:, lane:]

    def fill(out, first):
        @pl.loop(0, out.shape[0] // BATCH)
        def _(b):
            for r in range(BATCH):
                at = pl.multiple_of(ids_s[first + b * BATCH + r], 2)
                rows_f[pl.ds(2 * r, 2), :] = wide[pl.ds(at, 2), :]
            rows = pl.ds(pl.multiple_of(b * BATCH, BATCH), BATCH)
            out[rows, :lane] = rows_f[pl.ds(0, BATCH, 2), :].astype(jnp.bfloat16)
            out[rows, lane:] = rows_f[pl.ds(1, BATCH, 2), :].astype(jnp.bfloat16)

    fill(cand_out, 0)
    fill(targ_out, cand_out.shape[0])


def pick_rows(ids_two, table_loc, n_cand):
    rows_loc, width = table_loc.shape
    n_targ = ids_two.shape[0] - n_cand
    vmem = pl.BlockSpec(memory_space=pltpu.VMEM)
    return pl.pallas_call(
        pick_body,
        out_shape=(jax.ShapeDtypeStruct((n_cand, width), jnp.bfloat16), jax.ShapeDtypeStruct((n_targ, width), jnp.bfloat16)),
        in_specs=[pl.BlockSpec(memory_space=pltpu.SMEM), pl.BlockSpec(memory_space=pl.ANY)],
        out_specs=(vmem, vmem),
        scratch_shapes=[
            pltpu.VMEM((2 * (rows_loc + SPARE), width // 2), jnp.float32),
            pltpu.VMEM((4, STAGE_ROWS, width), jnp.bfloat16),
            pltpu.VMEM((2 * BATCH, width // 2), jnp.float32),
            pltpu.SemaphoreType.DMA((4,)),
        ],
        compiler_params=pltpu.CompilerParams(vmem_limit_bytes=VMEM_LIMIT),
        name="pick_rows",
    )(ids_two, table_loc)


def scatter_body(ids_s, ids_v, cand_ref, targ_ref, out_ref, acc, g2, new, out_stage, sem):
    rows, width = out_ref.shape
    lane = width // 2
    n_cand = cand_ref.shape[0]
    n_all = n_cand + targ_ref.shape[0]

    @pl.loop(0, 2 * rows // 512)
    def _(i):
        acc[pl.ds(pl.multiple_of(i * 512, 512), 512), :] = jnp.zeros((512, lane), jnp.float32)

    def one_batch(b, src, src_base):
        idr = jnp.broadcast_to(ids_v[pl.ds(b, 1), :], (BATCH, BATCH))
        same = jnp.where(idr == idr.T, 1.0, 0.0).astype(jnp.bfloat16)
        part = jnp.dot(same, src[pl.ds(pl.multiple_of(b * BATCH - src_base, BATCH), BATCH), :], preferred_element_type=jnp.float32)
        g2[pl.ds(0, BATCH, 2), :] = part[:, :lane]
        g2[pl.ds(1, BATCH, 2), :] = part[:, lane:]
        for r in range(BATCH):
            at = pl.multiple_of(ids_s[b * BATCH + r], 2)
            new[pl.ds(2 * r, 2), :] = acc[pl.ds(at, 2), :] + g2[pl.ds(2 * r, 2), :]
        for r in range(BATCH):
            at = pl.multiple_of(ids_s[b * BATCH + r], 2)
            acc[pl.ds(at, 2), :] = new[pl.ds(2 * r, 2), :]

    @pl.loop(0, n_cand // BATCH)
    def _(b):
        one_batch(b, cand_ref, 0)

    @pl.loop(n_cand // BATCH, n_all // BATCH)
    def _(b):
        one_batch(b, targ_ref, n_cand)

    n_out = rows // OUT_ROWS

    def out_copy(i, slot):
        return pltpu.make_async_copy(out_stage.at[slot], out_ref.at[pl.ds(i * OUT_ROWS, OUT_ROWS)], sem.at[slot])

    @pl.loop(0, n_out)
    def _(i):
        slot = i % 4

        @pl.when(i >= 4)
        def _():
            out_copy(i - 4, slot).wait()

        @pl.loop(0, OUT_ROWS // 128)
        def _(j):
            base = pl.multiple_of((i * OUT_ROWS + j * 128) * 2, 256)
            here = pl.ds(pl.multiple_of(j * 128, 128), 128)
            out_stage[slot, here, :lane] = acc[pl.ds(base, 128, 2), :]
            out_stage[slot, here, lane:] = acc[pl.ds(base + 1, 128, 2), :]

        out_copy(i, slot).start()

    for i in range(n_out - 4, n_out):
        out_copy(i, i % 4).wait()


def scatter_rows(ids_two, back_cand, back_targ, rows_loc):
    n_all = ids_two.shape[0]
    width = back_cand.shape[1]
    vmem = pl.BlockSpec(memory_space=pltpu.VMEM)
    return pl.pallas_call(
        scatter_body,
        out_shape=jax.ShapeDtypeStruct((rows_loc, width), jnp.float32),
        in_specs=[pl.BlockSpec(memory_space=pltpu.SMEM), vmem, vmem, vmem],
        out_specs=pl.BlockSpec(memory_space=pl.ANY),
        scratch_shapes=[
            pltpu.VMEM((2 * (rows_loc + SPARE), width // 2), jnp.float32),
            pltpu.VMEM((2 * BATCH, width // 2), jnp.float32),
            pltpu.VMEM((2 * BATCH, width // 2), jnp.float32),
            pltpu.VMEM((4, OUT_ROWS, width), jnp.float32),
            pltpu.SemaphoreType.DMA((4,)),
        ],
        compiler_params=pltpu.CompilerParams(vmem_limit_bytes=VMEM_LIMIT),
        cost_estimate=pl.CostEstimate(flops=60_000_000_000, bytes_accessed=40 << 20, transcendentals=0),
        name="scatter_rows",
    )(ids_two, ids_two.reshape(n_all // BATCH, BATCH), back_cand, back_targ)


CHUNK = 512
SUB = 64
COLS = 256


def logits_pass(u_ref, h, lq_ref, cid_ref, tid, z_a, z_b, e_s, m_s, s_s):
    n_cand, width = u_ref.shape
    n_tok = h.shape[0]
    scale = SCORE_GAIN / math.sqrt(width)
    ht = h.T
    n_chunk = n_cand // CHUNK

    def multiply(i, z_ref):
        off = pl.multiple_of(jnp.minimum(i, n_chunk - 1) * CHUNK, CHUNK)
        z_ref[...] = jnp.dot(u_ref[pl.ds(off, CHUNK), :], ht, preferred_element_type=jnp.float32)

    def absorb(i, z_ref, first):
        off = pl.multiple_of(i * CHUNK, CHUNK)
        for col in range(0, n_tok, COLS):
            cols = slice(col, col + COLS)
            m8 = m_s[0, :, cols]
            s8 = s_s[:, cols]
            for k in range(CHUNK // SUB):
                rows = pl.ds(pl.multiple_of(off + k * SUB, SUB), SUB)
                lq = jnp.concatenate([lq_ref[rows, :]] * (COLS // 128), axis=1)
                cid = jnp.concatenate([cid_ref[rows, :]] * (COLS // 128), axis=1)
                z = z_ref[k * SUB : (k + 1) * SUB, cols] * scale - lq
                z = jnp.where(cid == tid[:, cols], HIT_VALUE, z).reshape(SUB // 8, 8, COLS)
                m_new = jnp.maximum(m8, jnp.max(z, axis=0))
                e = jnp.exp(z - m_new[None])
                s8 = s8 * jnp.exp(m8 - m_new) + jnp.sum(e, axis=0)
                m8 = m_new
                e_s[rows, cols] = e.reshape(SUB, COLS)
                m_s[1 + i * (CHUNK // SUB) + k, :, cols] = m8
            m_s[0, :, cols] = m8
            s_s[:, cols] = s8

    m_s[0] = jnp.full((8, n_tok), jnp.finfo(jnp.float32).min, jnp.float32)
    s_s[...] = jnp.zeros_like(s_s)
    multiply(0, z_a)

    @pl.loop(0, n_chunk // 2)
    def _(i):
        multiply(2 * i + 1, z_b)
        absorb(2 * i, z_a, 0)
        multiply(2 * i + 2, z_a)
        absorb(2 * i + 1, z_b, 0)


def loss_pass(tok_total, u_ref, ut_s, h, v, e_s, m_s, s_s, fac_s, dz_a, dz_b, dht_s, loss_ref, dh_ref, dv_ref, du_ref):
    n_cand, width = u_ref.shape
    n_tok = h.shape[0]
    scale = SCORE_GAIN / math.sqrt(width)
    n_chunk = n_cand // CHUNK
    hf = h.astype(jnp.float32)
    vf = v.astype(jnp.float32)
    zt = jnp.sum(hf * vf, axis=1, keepdims=True) * scale
    zt = jnp.broadcast_to(zt, (n_tok, 128)).T[0:1, :]
    m8 = m_s[0]
    m = jnp.maximum(zt, jnp.max(m8, axis=0, keepdims=True))
    et = jnp.exp(zt - m)
    den = et + jnp.sum(s_s[...] * jnp.exp(m8 - m), axis=0, keepdims=True)
    part = jnp.sum(jnp.log(den) + m - zt, axis=1, keepdims=True)
    loss_ref[...] = jnp.broadcast_to(part, loss_ref.shape)
    dzt = ((et / den - 1.0) / tok_total).astype(jnp.bfloat16).astype(jnp.float32)
    inv = 1.0 / den / tok_total
    fac_s[0:8, :] = jnp.broadcast_to(m, (8, n_tok))
    fac_s[8:16, :] = jnp.broadcast_to(inv, (8, n_tok))
    for i in range(n_cand // 512):
        ut_s[:, i * 512 : (i + 1) * 512] = u_ref[i * 512 : (i + 1) * 512, :].T

    def gradient(i, dz_ref):
        i = jnp.minimum(i, n_chunk - 1)
        off = pl.multiple_of(i * CHUNK, CHUNK)
        for col in range(0, n_tok, COLS):
            cols = slice(col, col + COLS)
            for k in range(CHUNK // SUB):
                rows = pl.ds(pl.multiple_of(off + k * SUB, SUB), SUB)
                fac = jnp.exp(m_s[1 + i * (CHUNK // SUB) + k, :, cols] - fac_s[0:8, cols]) * fac_s[8:16, cols]
                dz_ref[k * SUB : (k + 1) * SUB, cols] = (e_s[rows, cols].reshape(SUB // 8, 8, COLS) * fac[None]).reshape(SUB, COLS).astype(jnp.bfloat16)

    def spread(i, dz_ref):
        off = pl.multiple_of(i * CHUNK, CHUNK)
        du_ref[pl.ds(off, CHUNK), :] = jnp.dot(dz_ref[...], h, preferred_element_type=jnp.float32)
        dht_s[...] += jnp.dot(ut_s[:, pl.ds(off, CHUNK)], dz_ref[...], preferred_element_type=jnp.float32)

    dht_s[...] = jnp.zeros_like(dht_s)
    gradient(0, dz_a)

    @pl.loop(0, n_chunk // 2)
    def _(i):
        gradient(2 * i + 1, dz_b)
        spread(2 * i, dz_a)
        gradient(2 * i + 2, dz_a)
        spread(2 * i + 1, dz_b)

    dzt_c = jnp.broadcast_to(dzt, (128, n_tok)).T[:, 0:1]
    dh_ref[...] = ((dzt_c * vf + dht_s[...].T) * scale).astype(jnp.bfloat16)
    dv_ref[...] = (scale * dzt_c * hf).astype(jnp.bfloat16)


def softmax_scratch(n_cand, n_tok, width):
    return [
        pltpu.VMEM((CHUNK, n_tok), jnp.float32),
        pltpu.VMEM((CHUNK, n_tok), jnp.float32),
        pltpu.VMEM((n_cand, n_tok), jnp.float32),
        pltpu.VMEM((1 + n_cand // SUB, 8, n_tok), jnp.float32),
        pltpu.VMEM((8, n_tok), jnp.float32),
        pltpu.VMEM((width, n_cand), jnp.bfloat16),
        pltpu.VMEM((16, n_tok), jnp.float32),
        pltpu.VMEM((CHUNK, n_tok), jnp.bfloat16),
        pltpu.VMEM((CHUNK, n_tok), jnp.bfloat16),
        pltpu.VMEM((width, n_tok), jnp.float32),
    ]


def softmax_body(tok_total, h_ref, v_ref, u_ref, lq_ref, cid_ref, tid_ref, loss_ref, dh_ref, dv_ref, du_ref, z_a, z_b, e_s, m_s, s_s, ut_s, fac_s, dz_a, dz_b, dht_s):
    h = h_ref[...]
    logits_pass(u_ref, h, lq_ref, cid_ref, tid_ref[...], z_a, z_b, e_s, m_s, s_s)
    loss_pass(tok_total, u_ref, ut_s, h, v_ref[...], e_s, m_s, s_s, fac_s, dz_a, dz_b, dht_s, loss_ref, dh_ref, dv_ref, du_ref)


def softmax_grads(query, targ_vec, cand_vec, lq_b, cid_b, targ_ids, tok_total):
    n_tok, width = query.shape
    n_cand = cand_vec.shape[0]
    vmem = pl.BlockSpec(memory_space=pltpu.VMEM)
    return pl.pallas_call(
        functools.partial(softmax_body, tok_total),
        out_shape=(jax.ShapeDtypeStruct((8, 128), jnp.float32), jax.ShapeDtypeStruct((n_tok, width), jnp.bfloat16), jax.ShapeDtypeStruct((n_tok, width), jnp.bfloat16), jax.ShapeDtypeStruct((n_cand, width), jnp.float32)),
        in_specs=[vmem] * 6,
        out_specs=(vmem,) * 4,
        scratch_shapes=softmax_scratch(n_cand, n_tok, width),
        compiler_params=pltpu.CompilerParams(vmem_limit_bytes=VMEM_LIMIT),
        cost_estimate=pl.CostEstimate(flops=6 * n_tok * n_cand * width, bytes_accessed=16 << 20, transcendentals=n_tok * n_cand),
        name="softmax_grads",
    )(query, targ_vec, cand_vec, lq_b, cid_b, targ_ids.reshape(1, n_tok))


MESH = pl.DeviceIdType.MESH


def my_place():
    me = lax.axis_index("dp")
    return me, me // 4, (me // 2) % 2, me % 2


def peer_of(place, dy, dx, dc):
    me, y, x, c = place
    return me + dy * (4 - 8 * y) + dx * (2 - 4 * x) + dc * (1 - 2 * c)


def greet(place):
    barrier = pltpu.get_barrier_semaphore()
    for k in range(1, 8):
        pl.semaphore_signal(barrier, inc=1, device_id=(peer_of(place, k // 4, (k // 2) % 2, k % 2),), device_id_type=MESH)


def meet(place):
    greet(place)
    pl.semaphore_wait(pltpu.get_barrier_semaphore(), 7)


def push(src, dst, send_sem, recv_sem, peer):
    copy = pltpu.make_async_remote_copy(src_ref=src, dst_ref=dst, send_sem=send_sem, recv_sem=recv_sem, device_id=(peer,), device_id_type=MESH)
    copy.start()
    return copy


class Reduce:
    def __init__(self, place, data, in_one, mid, in_xa, in_yb, part_a, part_b, in_ya, in_xb, send_sem, recv_sem):
        self.place, self.data = place, data
        self.in_one, self.mid, self.in_xa, self.in_yb = in_one, mid, in_xa, in_yb
        self.part_a, self.part_b, self.in_ya, self.in_xb = part_a, part_b, in_ya, in_xb
        self.send_sem, self.recv_sem = send_sem, recv_sem
        self.half = data.shape[3] // 2
        self.copies = []

    def push(self, k, src, dst, dy, dx, dc):
        copy = push(src, dst, self.send_sem.at[k], self.recv_sem.at[k], peer_of(self.place, dy, dx, dc))
        self.copies.append(copy)

    def one(self):
        c = self.place[3]
        self.push(0, self.data.at[:, :, 1 - c], self.in_one, 0, 0, 1)

    def two(self):
        _, y, x, c = self.place
        half = self.half
        self.copies[0].wait_recv()
        for i in range(2):
            for j in range(2):
                self.mid[i, j] = self.data[i, j, c] + self.in_one[i, j]
        self.push(1, self.mid.at[:, 1 - x, pl.ds(0, half)], self.in_xa, 0, 1, 0)
        self.push(2, self.mid.at[1 - y, :, pl.ds(half, half)], self.in_yb, 1, 0, 0)

    def three(self):
        _, y, x, c = self.place
        half = self.half
        self.copies[1].wait_recv()
        for i in range(2):
            self.part_a[i] = self.mid[i, x, 0:half] + self.in_xa[i]
        self.push(3, self.part_a.at[1 - y], self.in_ya, 1, 0, 0)
        self.copies[2].wait_recv()
        for i in range(2):
            self.part_b[i] = self.mid[y, i, half : 2 * half] + self.in_yb[i]
        self.push(4, self.part_b.at[1 - x], self.in_xb, 0, 1, 0)

    def last(self):
        _, y, x, c = self.place
        self.copies[3].wait_recv()
        first = self.part_a[y] + self.in_ya[...]
        self.copies[4].wait_recv()
        return first, self.part_b[x] + self.in_xb[...]

    def drain(self):
        for copy in self.copies:
            copy.wait_send()


def reduce_scratch(n, rows, width, dtype):
    half = rows // 2
    return [
        pltpu.VMEM((n, 2, 2, rows, width), dtype),
        pltpu.VMEM((n, 2, 2, rows, width), dtype),
        pltpu.VMEM((n, 2, half, width), dtype),
        pltpu.VMEM((n, 2, half, width), dtype),
        pltpu.VMEM((n, 2, half, width), dtype),
        pltpu.VMEM((n, 2, half, width), dtype),
        pltpu.VMEM((n, half, width), dtype),
        pltpu.VMEM((n, half, width), dtype),
        pltpu.SemaphoreType.DMA((n, 5)),
        pltpu.SemaphoreType.DMA((n, 5)),
    ]


class Gather:
    def __init__(self, place, full, send_sem, recv_sem):
        self.place, self.full = place, full
        self.send_sem, self.recv_sem = send_sem, recv_sem
        self.half = full.shape[3] // 2
        self.copies = []

    def push(self, k, ref, dy, dx, dc):
        copy = push(ref, ref, self.send_sem.at[k], self.recv_sem.at[k], peer_of(self.place, dy, dx, dc))
        self.copies.append(copy)

    def one(self):
        _, y, x, c = self.place
        half = self.half
        self.push(0, self.full.at[y, x, c, pl.ds(0, half)], 0, 1, 0)
        self.push(1, self.full.at[y, x, c, pl.ds(half, half)], 1, 0, 0)

    def two(self):
        _, y, x, c = self.place
        half = self.half
        self.copies[0].wait_recv()
        self.push(2, self.full.at[y, :, c, pl.ds(0, half)], 1, 0, 0)
        self.copies[1].wait_recv()
        self.push(3, self.full.at[:, x, c, pl.ds(half, half)], 0, 1, 0)

    def three(self):
        c = self.place[3]
        self.copies[2].wait_recv()
        self.copies[3].wait_recv()
        self.push(4, self.full.at[:, :, c], 0, 0, 1)

    def last(self):
        self.copies[4].wait_recv()

    def drain(self):
        for copy in self.copies:
            copy.wait_send()


def gather_sems():
    return [pltpu.SemaphoreType.DMA((5,)), pltpu.SemaphoreType.DMA((5,))]


def prepare_body(mine, lq_ref, cid_ref, tokens, w_one, w_two, full, lq_out, cid_out, q_pre, q_hid, query, send_sem, recv_sem):
    place = my_place()
    greet(place)
    for i in range(tokens.shape[0] // 256):
        at = slice(i * 256, i * 256 + 256)
        pre, hid, vec = tower_fwd(tokens[at, :], w_one[...], w_two[...])
        q_pre[at, :] = pre
        q_hid[at, :] = hid
        query[at, :] = vec
    pl.semaphore_wait(pltpu.get_barrier_semaphore(), 7)
    full[place[0]] = mine[...]
    copies = []
    for k in range(1, 8):
        copies.append(push(mine, full.at[place[0]], send_sem.at[k], recv_sem.at[k], peer_of(place, k // 4, (k // 2) % 2, k % 2)))

    @pl.loop(0, lq_ref.shape[0])
    def _(i):
        rows = pl.ds(pl.multiple_of(i * 128, 128), 128)
        lq_out[rows, :] = jnp.broadcast_to(lq_ref[pl.ds(i, 1), :], (128, 128)).T
        cid_out[rows, :] = jnp.broadcast_to(cid_ref[pl.ds(i, 1), :], (128, 128)).T

    for copy in copies:
        copy.wait()


def prepare(targ_loc, log_q, cand_ids, tokens, w_one, w_two):
    n_cand = cand_ids.shape[0]
    n_tok = tokens.shape[0]
    ff, width = w_two.shape
    vmem = pl.BlockSpec(memory_space=pltpu.VMEM)
    return pl.pallas_call(
        prepare_body,
        out_shape=(
            jax.ShapeDtypeStruct((8, 8, 128), jnp.int32),
            jax.ShapeDtypeStruct((n_cand, 128), jnp.float32),
            jax.ShapeDtypeStruct((n_cand, 128), jnp.int32),
            jax.ShapeDtypeStruct((n_tok, ff), jnp.float32),
            jax.ShapeDtypeStruct((n_tok, ff), jnp.bfloat16),
            jax.ShapeDtypeStruct((n_tok, width), jnp.bfloat16),
        ),
        in_specs=[vmem] * 6,
        out_specs=(vmem,) * 6,
        scratch_shapes=[pltpu.SemaphoreType.DMA((8,)), pltpu.SemaphoreType.DMA((8,))],
        compiler_params=pltpu.CompilerParams(vmem_limit_bytes=VMEM_LIMIT, collective_id=0, has_side_effects=True),
        name="prepare",
    )(targ_loc.reshape(8, 128), log_q.reshape(-1, 128), cand_ids.reshape(-1, 128), tokens, w_one, w_two)


PIECE = 256


def fetch_body(data_c, data_t, wi_one, wi_two, cand_raw, c_pre, c_hid, cand_vec, targ_raw, t_pre, t_hid, targ_vec, in_one, mid, in_xa, in_yb, part_a, part_b, in_ya, in_xb, rs_send, rs_recv, ag_send, ag_recv):
    place = my_place()
    me, y, x, c = place
    half = PIECE // 2
    meet(place)
    reduces = []
    for k in range(6):
        data = data_c.at[:, :, :, pl.ds(k * PIECE, PIECE)] if k < 2 else data_t.at[:, :, :, pl.ds((k - 2) * PIECE, PIECE)]
        reduces.append(Reduce(place, data, in_one.at[k], mid.at[k], in_xa.at[k], in_yb.at[k], part_a.at[k], part_b.at[k], in_ya.at[k], in_xb.at[k], rs_send.at[k], rs_recv.at[k]))
    ag = Gather(place, cand_vec, ag_send, ag_recv)

    def close(k, out, base):
        first, second = reduces[k].last()
        out[base : base + half, :] = first
        out[base + half : base + PIECE, :] = second

    def tower(rows_ref, at, w_in, w_out, pre_ref, hid_ref):
        pre, hid, vec = tower_fwd(rows_ref[at, :], w_in[...], w_out[...])
        pre_ref[at, :] = pre
        hid_ref[at, :] = hid
        return vec

    def targ_tower(k):
        close(k + 2, targ_raw, k * PIECE)
        at = slice(k * PIECE, (k + 1) * PIECE)
        targ_vec[at, :] = tower(targ_raw, at, wi_one, wi_two, t_pre, t_hid)

    for k in range(6):
        reduces[k].one()
    reduces[0].two()
    reduces[1].two()
    reduces[2].two()
    reduces[0].three()
    reduces[1].three()
    reduces[3].two()
    reduces[4].two()
    close(0, cand_raw, 0)
    close(1, cand_raw, PIECE)
    cand_vec[y, x, c] = tower(cand_raw, slice(0, 512), wi_one, wi_two, c_pre, c_hid)
    ag.one()
    reduces[5].two()
    reduces[2].three()
    ag.two()
    reduces[3].three()
    reduces[4].three()
    targ_tower(0)
    reduces[5].three()
    targ_tower(1)
    ag.three()
    targ_tower(2)
    targ_tower(3)
    ag.last()
    for red in reduces:
        red.drain()
    ag.drain()


def fetch_rows(data_c, data_t, wi_one, wi_two):
    n_mine, width = data_c.shape[3:]
    n_tok = data_t.shape[3]
    ff = wi_one.shape[1]
    vmem = pl.BlockSpec(memory_space=pltpu.VMEM)

    def outs(n):
        return [jax.ShapeDtypeStruct((n, ff), jnp.float32), jax.ShapeDtypeStruct((n, ff), jnp.bfloat16)]

    def rows(n):
        return [jax.ShapeDtypeStruct((n, width), jnp.bfloat16)]

    full = [jax.ShapeDtypeStruct((2, 2, 2, n_mine, width), jnp.bfloat16)]
    return pl.pallas_call(
        fetch_body,
        out_shape=tuple(rows(n_mine) + outs(n_mine) + full + rows(n_tok) + outs(n_tok) + rows(n_tok)),
        in_specs=[vmem] * 4,
        out_specs=(vmem,) * 8,
        scratch_shapes=reduce_scratch(6, PIECE, width, jnp.bfloat16) + gather_sems(),
        compiler_params=pltpu.CompilerParams(vmem_limit_bytes=VMEM_LIMIT, collective_id=1, has_side_effects=True),
        name="fetch_rows",
    )(data_c, data_t, wi_one, wi_two)


def back_body(d_part, loss_in, d_query, d_targ, tokens, q_pre, q_hid, w_two, targ_raw, t_pre, t_hid, cand_raw, c_pre, c_hid, wi_one, wi_two, back_t, back_c, dw_one_out, dw_two_out, dwi_one_out, dwi_two_out, loss_out, *scratch):
    place = my_place()
    me, y, x, c = place
    rs_u, rs_w = scratch[0:10], scratch[10:20]
    at_send, at_recv, ac_send, ac_recv, aw_send, aw_recv, l_send, l_recv, w_data, w_full, l_all = scratch[20:31]
    width = d_query.shape[1]
    scale = SCORE_GAIN / math.sqrt(width)
    meet(place)
    red_u = []
    for k in range(2):
        red_u.append(Reduce(place, d_part.at[:, :, :, pl.ds(k * PIECE, PIECE)], *[s.at[k] for s in rs_u]))
    red_w = Reduce(place, w_data, *[s.at[0] for s in rs_w])
    ag_t = Gather(place, back_t, at_send, at_recv)
    ag_c = Gather(place, back_c, ac_send, ac_recv)
    ag_w = Gather(place, w_full, aw_send, aw_recv)
    red_u[0].one()
    red_u[1].one()
    l_all[me] = loss_in[...]
    l_copies = []
    for k in range(1, 8):
        l_copies.append(push(loss_in, l_all.at[me], l_send.at[k], l_recv.at[k], peer_of(place, k // 4, (k // 2) % 2, k % 2)))

    def put(first, value):
        n = value.shape[0] // 8
        for b in range(8):
            w_data[b // 4, (b // 2) % 2, b % 2, first : first + n, :] = value[b * n : (b + 1) * n, :]

    dwi_two = over_rows(t_hid[...], d_targ[...])
    red_u[0].two()
    red_u[1].two()
    t_q = grad_through(d_targ[...], wi_two[...], t_pre[...])
    back_t[y, x, c] = by_transpose(t_q, wi_one[...]).astype(jnp.bfloat16)
    ag_t.one()
    dwi_one = over_rows(targ_raw[...], t_q)
    _, dw_one, dw_two = tower_back(tokens[...], w_two[...], q_pre[...], q_hid[...], d_query[...])
    dw_one_out[...] = dw_one
    dw_two_out[...] = dw_two
    red_u[0].three()
    red_u[1].three()
    ag_t.two()
    parts = []
    for k in range(2):
        first, second = red_u[k].last()
        parts += [first, second]
    d_cand = (jnp.concatenate(parts, axis=0) * scale).astype(jnp.bfloat16)
    c_q, dwi_one_c, dwi_two_c = tower_back(cand_raw[...], wi_two[...], c_pre[...], c_hid[...], d_cand)
    back_c[y, x, c] = by_transpose(c_q, wi_one[...]).astype(jnp.bfloat16)
    ag_c.one()
    dwi_one = dwi_one + dwi_one_c
    put(0, dwi_one[:, :width])
    put(32, dwi_one[:, width:])
    put(64, dwi_two + dwi_two_c)
    red_w.one()
    for copy in l_copies:
        copy.wait()
    loss_out[...] = jnp.sum(l_all[...], axis=0)
    red_w.two()
    red_w.three()
    ag_c.two()
    first, second = red_w.last()
    half = first.shape[0]
    w_full[y, x, c, 0:half, :] = first
    w_full[y, x, c, half : 2 * half, :] = second
    ag_w.one()
    ag_t.three()
    ag_w.two()
    ag_c.three()
    ag_w.three()
    ag_t.last()
    ag_c.last()
    ag_w.last()
    for b in range(8):
        block = w_full.at[b // 4, (b // 2) % 2, b % 2]
        dwi_one_out[b * 32 : (b + 1) * 32, :width] = block[0:32, :]
        dwi_one_out[b * 32 : (b + 1) * 32, width:] = block[32:64, :]
        dwi_two_out[b * 64 : (b + 1) * 64, :] = block[64:128, :]
    for part in red_u + [red_w, ag_t, ag_c, ag_w]:
        part.drain()


W_ROWS = 128


def back_rows(d_part, loss_part, *rest):
    n_mine, width = d_part.shape[3:]
    n_tok = rest[0].shape[0]
    vmem = pl.BlockSpec(memory_space=pltpu.VMEM)
    sems = [pltpu.SemaphoreType.DMA((8,)), pltpu.SemaphoreType.DMA((8,))]
    return pl.pallas_call(
        back_body,
        out_shape=(
            jax.ShapeDtypeStruct((2, 2, 2, n_tok, width), jnp.bfloat16),
            jax.ShapeDtypeStruct((2, 2, 2, n_mine, width), jnp.bfloat16),
            jax.ShapeDtypeStruct((rest[2].shape[1], rest[3].shape[1]), jnp.float32),
            jax.ShapeDtypeStruct(rest[5].shape, jnp.float32),
            jax.ShapeDtypeStruct(rest[12].shape, jnp.float32),
            jax.ShapeDtypeStruct(rest[13].shape, jnp.float32),
            jax.ShapeDtypeStruct((8, 128), jnp.float32),
        ),
        in_specs=[vmem] * 16,
        out_specs=(vmem,) * 7,
        scratch_shapes=reduce_scratch(2, PIECE, width, jnp.float32) + reduce_scratch(1, W_ROWS, width, jnp.float32) + gather_sems() + gather_sems() + gather_sems() + sems + [pltpu.VMEM((2, 2, 2, W_ROWS, width), jnp.float32), pltpu.VMEM((2, 2, 2, W_ROWS, width), jnp.float32), pltpu.VMEM((8, 8, 128), jnp.float32)],
        compiler_params=pltpu.CompilerParams(vmem_limit_bytes=VMEM_LIMIT, collective_id=2, has_side_effects=True),
        name="back_rows",
    )(d_part, loss_part, *rest)


def solution(mesh):
    num_dev = mesh.shape["dp"]

    def local_step(tokens, w_one, w_two, wi_one, wi_two, table_loc, cand_ids, log_q, targ_loc):
        my_index = lax.axis_index("dp")
        rows_loc, width = table_loc.shape
        n_cand = cand_ids.shape[0]
        tok_total = tokens.shape[0] * num_dev
        targ_all, lq_b, cid_b, q_pre, q_hid, query = prepare(targ_loc, log_q, cand_ids, tokens, w_one, w_two)
        targ_all = targ_all.reshape(-1)
        local_ids = jnp.concatenate([cand_ids, targ_all]) - my_index * rows_loc
        spare = rows_loc + jnp.arange(local_ids.shape[0], dtype=jnp.int32) % SPARE
        ids_two = 2 * jnp.where((local_ids >= 0) & (local_ids < rows_loc), local_ids, spare)
        data_c, data_t = pick_rows(ids_two, table_loc, n_cand)
        data_c = data_c.reshape(2, 2, 2, n_cand // 8, width)
        data_t = data_t.reshape(2, 2, 2, tokens.shape[0], width)
        cand_mine, c_pre, c_hid, cand_vec, targ_raw, t_pre, t_hid, targ_vec = fetch_rows(data_c, data_t, wi_one, wi_two)
        cand_vec = cand_vec.reshape(n_cand, width)
        loss_part, d_query, d_targ_vec, d_part = softmax_grads(query, targ_vec, cand_vec, lq_b, cid_b, targ_loc, tok_total)
        back_t, back_c, dw_one, dw_two, dwi_one, dwi_two, loss = back_rows(d_part.reshape(2, 2, 2, n_cand // 8, width), loss_part, d_query, d_targ_vec, tokens, q_pre, q_hid, w_two, targ_raw, t_pre, t_hid, cand_mine, c_pre, c_hid, wi_one, wi_two)
        dw_one, dw_two = lax.psum((dw_one, dw_two), "dp")
        d_table = scatter_rows(ids_two, back_c.reshape(-1, width), back_t.reshape(-1, width), rows_loc)
        return loss[0, 0] / tok_total, d_table, dw_one, dw_two, dwi_one, dwi_two

    return jax.shard_map(local_step, mesh=mesh, in_specs=(P("dp", None), P(), P(), P(), P(), P("dp", None), P(), P(), P("dp")), out_specs=(P(), P("dp", None), P(), P(), P(), P()), check_vma=False)
```

```python
import functools
import math
import jax
import jax.numpy as jnp
from jax import lax
from jax.experimental import pallas as pl
from jax.experimental.pallas import tpu as pltpu
from jax.sharding import PartitionSpec as P

SCORE_GAIN = 3.0
HIT_VALUE = -1e9


def tower_fwd(row_block, w_in, w_out):
    pre_act = jnp.dot(row_block, w_in, preferred_element_type=jnp.float32)
    hidden = jax.nn.gelu(pre_act).astype(jnp.bfloat16)
    tower_out = jnp.dot(hidden, w_out, preferred_element_type=jnp.float32).astype(jnp.bfloat16)
    return tower_out


def over_rows(a, b):
    return lax.dot_general(a, b, (((0,), (0,)), ((), ())), preferred_element_type=jnp.float32)


def by_transpose(a, b):
    return lax.dot_general(a, b, (((1,), (1,)), ((), ())), preferred_element_type=jnp.float32)


def tower_back(row_block, w_in, w_out, grad_out):
    pre_act = jnp.dot(row_block, w_in, preferred_element_type=jnp.float32)
    hidden, gelu_back = jax.vjp(jax.nn.gelu, pre_act)
    grad_hidden = by_transpose(grad_out, w_out)
    return gelu_back(grad_hidden)[0].astype(jnp.bfloat16), hidden.astype(jnp.bfloat16)


VMEM_LIMIT = 63 * 1024 * 1024
BATCH = 128
SPARE = 256
GROUP = 16
STAGE_ROWS = 2048
OUT_ROWS = 1024
IN_SLOTS = 12
OUT_SLOTS = 12


def pick_body(ids_s, table, cand_out, targ_out, wide, stage, rows_f, stage_sem):
    rows_loc, width = table.shape
    lane = width // 2
    n_stage = rows_loc // STAGE_ROWS

    def stage_copy(i, slot):
        return pltpu.make_async_copy(table.at[pl.ds(i * STAGE_ROWS, STAGE_ROWS)], stage.at[slot], stage_sem.at[slot])

    for i in range(IN_SLOTS - 1):
        stage_copy(i, i).start()
    wide[pl.ds(2 * rows_loc, 2 * SPARE), :] = jnp.zeros((2 * SPARE, lane), jnp.float32)

    @pl.loop(0, n_stage)
    def _(i):
        slot = i % IN_SLOTS

        @pl.when(i + IN_SLOTS - 1 < n_stage)
        def _():
            stage_copy(i + IN_SLOTS - 1, (i + IN_SLOTS - 1) % IN_SLOTS).start()

        stage_copy(i, slot).wait()

        @pl.loop(0, STAGE_ROWS // 128)
        def _(j):
            block = stage[slot, pl.ds(pl.multiple_of(j * 128, 128), 128), :].astype(jnp.float32)
            base = pl.multiple_of((i * STAGE_ROWS + j * 128) * 2, 256)
            wide[pl.ds(base, 128, 2), :] = block[:, :lane]
            wide[pl.ds(base + 1, 128, 2), :] = block[:, lane:]

    def fill(out, first):
        @pl.loop(0, out.shape[0] // BATCH)
        def _(b):
            for r in range(BATCH):
                at = pl.multiple_of(ids_s[first + b * BATCH + r], 2)
                rows_f[pl.ds(2 * r, 2), :] = wide[pl.ds(at, 2), :]
            rows = pl.ds(pl.multiple_of(b * BATCH, BATCH), BATCH)
            out[rows, :lane] = rows_f[pl.ds(0, BATCH, 2), :].astype(jnp.bfloat16)
            out[rows, lane:] = rows_f[pl.ds(1, BATCH, 2), :].astype(jnp.bfloat16)

    fill(cand_out, 0)
    fill(targ_out, cand_out.shape[0])


def pick_rows(ids_two, table_loc, n_cand):
    rows_loc, width = table_loc.shape
    n_targ = ids_two.shape[0] - n_cand
    vmem = pl.BlockSpec(memory_space=pltpu.VMEM)
    return pl.pallas_call(
        pick_body,
        out_shape=(jax.ShapeDtypeStruct((n_cand, width), jnp.bfloat16), jax.ShapeDtypeStruct((n_targ, width), jnp.bfloat16)),
        in_specs=[pl.BlockSpec(memory_space=pltpu.SMEM), pl.BlockSpec(memory_space=pl.ANY)],
        out_specs=(vmem, vmem),
        scratch_shapes=[
            pltpu.VMEM((2 * (rows_loc + SPARE), width // 2), jnp.float32),
            pltpu.VMEM((IN_SLOTS, STAGE_ROWS, width), jnp.bfloat16),
            pltpu.VMEM((2 * BATCH, width // 2), jnp.float32),
            pltpu.SemaphoreType.DMA((IN_SLOTS,)),
        ],
        compiler_params=pltpu.CompilerParams(vmem_limit_bytes=VMEM_LIMIT),
        name="pick_rows",
    )(ids_two, table_loc)


def scatter_body(ids_s, ids_v, cand_hbm, targ_hbm, out_ref, acc, g2, cand_ref, targ_ref, out_stage, sem, in_sem):
    rows, width = out_ref.shape
    lane = width // 2
    n_cand = cand_ref.shape[0]
    n_all = n_cand + targ_ref.shape[0]
    in_copies = [pltpu.make_async_copy(cand_hbm, cand_ref, in_sem.at[0]), pltpu.make_async_copy(targ_hbm, targ_ref, in_sem.at[1])]
    for copy in in_copies:
        copy.start()

    @pl.loop(0, 2 * rows // 512)
    def _(i):
        acc[pl.ds(pl.multiple_of(i * 512, 512), 512), :] = jnp.zeros((512, lane), jnp.float32)

    row_i = lax.broadcasted_iota(jnp.int32, (BATCH, BATCH), 0) // GROUP
    col_i = lax.broadcasted_iota(jnp.int32, (BATCH, BATCH), 1) // GROUP
    same_group = row_i == col_i

    def one_batch(b, src, src_base):
        idr = jnp.broadcast_to(ids_v[pl.ds(b, 1), :], (BATCH, BATCH))
        same = jnp.where((idr == idr.T) & same_group, 1.0, 0.0).astype(jnp.bfloat16)
        part = jnp.dot(same, src[pl.ds(pl.multiple_of(b * BATCH - src_base, BATCH), BATCH), :], preferred_element_type=jnp.float32)
        g2[pl.ds(0, BATCH, 2), :] = part[:, :lane]
        g2[pl.ds(1, BATCH, 2), :] = part[:, lane:]
        for g in range(BATCH // GROUP):
            at = [pl.multiple_of(ids_s[b * BATCH + g * GROUP + r], 2) for r in range(GROUP)]
            new = [acc[pl.ds(at[r], 2), :] + g2[pl.ds(2 * (g * GROUP + r), 2), :] for r in range(GROUP)]
            for r in range(GROUP):
                acc[pl.ds(at[r], 2), :] = new[r]

    for copy in in_copies:
        copy.wait()

    @pl.loop(0, n_cand // BATCH)
    def _(b):
        one_batch(b, cand_ref, 0)

    @pl.loop(n_cand // BATCH, n_all // BATCH)
    def _(b):
        one_batch(b, targ_ref, n_cand)

    n_out = rows // OUT_ROWS

    def out_copy(i, slot):
        return pltpu.make_async_copy(out_stage.at[slot], out_ref.at[pl.ds(i * OUT_ROWS, OUT_ROWS)], sem.at[slot])

    @pl.loop(0, n_out)
    def _(i):
        slot = i % OUT_SLOTS

        @pl.when(i >= OUT_SLOTS)
        def _():
            out_copy(i - OUT_SLOTS, slot).wait()

        @pl.loop(0, OUT_ROWS // 128)
        def _(j):
            base = pl.multiple_of((i * OUT_ROWS + j * 128) * 2, 256)
            here = pl.ds(pl.multiple_of(j * 128, 128), 128)
            out_stage[slot, here, :lane] = acc[pl.ds(base, 128, 2), :]
            out_stage[slot, here, lane:] = acc[pl.ds(base + 1, 128, 2), :]

        out_copy(i, slot).start()

    for i in range(n_out - OUT_SLOTS, n_out):
        out_copy(i, i % OUT_SLOTS).wait()


def scatter_rows(ids_two, back_cand, back_targ, rows_loc):
    n_all = ids_two.shape[0]
    width = back_cand.shape[1]
    vmem = pl.BlockSpec(memory_space=pltpu.VMEM)
    return pl.pallas_call(
        scatter_body,
        out_shape=jax.ShapeDtypeStruct((rows_loc, width), jnp.float32),
        in_specs=[pl.BlockSpec(memory_space=pltpu.SMEM), vmem, pl.BlockSpec(memory_space=pl.ANY), pl.BlockSpec(memory_space=pl.ANY)],
        out_specs=pl.BlockSpec(memory_space=pl.ANY),
        scratch_shapes=[
            pltpu.VMEM((2 * (rows_loc + SPARE), width // 2), jnp.float32),
            pltpu.VMEM((2 * BATCH, width // 2), jnp.float32),
            pltpu.VMEM(back_cand.shape, jnp.bfloat16),
            pltpu.VMEM(back_targ.shape, jnp.bfloat16),
            pltpu.VMEM((OUT_SLOTS, OUT_ROWS, width), jnp.float32),
            pltpu.SemaphoreType.DMA((OUT_SLOTS,)),
            pltpu.SemaphoreType.DMA((2,)),
        ],
        compiler_params=pltpu.CompilerParams(vmem_limit_bytes=VMEM_LIMIT),
        cost_estimate=pl.CostEstimate(flops=60_000_000_000, bytes_accessed=40 << 20, transcendentals=0),
        name="scatter_rows",
    )(ids_two, ids_two.reshape(n_all // BATCH, BATCH), back_cand, back_targ)


CHUNK = 512
SUB = 64
COLS = 256


def logits_pass(u_ref, h, lq_ref, cid_ref, tid, z_a, z_b, e_s, m_s, s_s):
    n_cand, width = u_ref.shape
    n_tok = h.shape[0]
    scale = SCORE_GAIN / math.sqrt(width)
    ht = h.T
    n_chunk = n_cand // CHUNK

    def multiply(i, z_ref):
        off = pl.multiple_of(jnp.minimum(i, n_chunk - 1) * CHUNK, CHUNK)
        z_ref[...] = jnp.dot(u_ref[pl.ds(off, CHUNK), :], ht, preferred_element_type=jnp.float32)

    def absorb(i, z_ref, first):
        off = pl.multiple_of(i * CHUNK, CHUNK)
        for col in range(0, n_tok, COLS):
            cols = slice(col, col + COLS)
            m8 = m_s[0, :, cols]
            s8 = s_s[:, cols]
            for k in range(CHUNK // SUB):
                rows = pl.ds(pl.multiple_of(off + k * SUB, SUB), SUB)
                lq = jnp.concatenate([lq_ref[rows, :]] * (COLS // 128), axis=1)
                cid = jnp.concatenate([cid_ref[rows, :]] * (COLS // 128), axis=1)
                z = z_ref[k * SUB : (k + 1) * SUB, cols] * scale - lq
                z = jnp.where(cid == tid[:, cols], HIT_VALUE, z).reshape(SUB // 8, 8, COLS)
                m_new = jnp.maximum(m8, jnp.max(z, axis=0))
                e = jnp.exp(z - m_new[None])
                s8 = s8 * jnp.exp(m8 - m_new) + jnp.sum(e, axis=0)
                m8 = m_new
                e_s[rows, cols] = e.reshape(SUB, COLS)
                m_s[1 + i * (CHUNK // SUB) + k, :, cols] = m8
            m_s[0, :, cols] = m8
            s_s[:, cols] = s8

    m_s[0] = jnp.full((8, n_tok), jnp.finfo(jnp.float32).min, jnp.float32)
    s_s[...] = jnp.zeros_like(s_s)
    multiply(0, z_a)

    @pl.loop(0, n_chunk // 2)
    def _(i):
        multiply(2 * i + 1, z_b)
        absorb(2 * i, z_a, 0)
        multiply(2 * i + 2, z_a)
        absorb(2 * i + 1, z_b, 0)


def loss_pass(tok_total, u_ref, ut_s, h, v, e_s, m_s, s_s, fac_s, dz_a, dz_b, dht_s, loss_ref, dh_ref, dv_ref, du_ref):
    n_cand, width = u_ref.shape
    n_tok = h.shape[0]
    scale = SCORE_GAIN / math.sqrt(width)
    n_chunk = n_cand // CHUNK
    hf = h.astype(jnp.float32)
    vf = v.astype(jnp.float32)
    zt = jnp.sum(hf * vf, axis=1, keepdims=True) * scale
    zt = jnp.broadcast_to(zt, (n_tok, 128)).T[0:1, :]
    m8 = m_s[0]
    m = jnp.maximum(zt, jnp.max(m8, axis=0, keepdims=True))
    et = jnp.exp(zt - m)
    den = et + jnp.sum(s_s[...] * jnp.exp(m8 - m), axis=0, keepdims=True)
    part = jnp.sum(jnp.log(den) + m - zt, axis=1, keepdims=True)
    loss_ref[...] = jnp.broadcast_to(part, loss_ref.shape)
    dzt = ((et / den - 1.0) / tok_total).astype(jnp.bfloat16).astype(jnp.float32)
    inv = 1.0 / den / tok_total
    fac_s[0:8, :] = jnp.broadcast_to(m, (8, n_tok))
    fac_s[8:16, :] = jnp.broadcast_to(inv, (8, n_tok))
    for i in range(n_cand // 512):
        ut_s[:, i * 512 : (i + 1) * 512] = u_ref[i * 512 : (i + 1) * 512, :].T

    def gradient(i, dz_ref):
        i = jnp.minimum(i, n_chunk - 1)
        off = pl.multiple_of(i * CHUNK, CHUNK)
        for col in range(0, n_tok, COLS):
            cols = slice(col, col + COLS)
            for k in range(CHUNK // SUB):
                rows = pl.ds(pl.multiple_of(off + k * SUB, SUB), SUB)
                fac = jnp.exp(m_s[1 + i * (CHUNK // SUB) + k, :, cols] - fac_s[0:8, cols]) * fac_s[8:16, cols]
                dz_ref[k * SUB : (k + 1) * SUB, cols] = (e_s[rows, cols].reshape(SUB // 8, 8, COLS) * fac[None]).reshape(SUB, COLS).astype(jnp.bfloat16)

    def spread(i, dz_ref):
        off = pl.multiple_of(i * CHUNK, CHUNK)
        du_ref[pl.ds(off, CHUNK), :] = jnp.dot(dz_ref[...], h, preferred_element_type=jnp.float32)
        dht_s[...] += jnp.dot(ut_s[:, pl.ds(off, CHUNK)], dz_ref[...], preferred_element_type=jnp.float32)

    dht_s[...] = jnp.zeros_like(dht_s)
    gradient(0, dz_a)

    @pl.loop(0, n_chunk // 2)
    def _(i):
        gradient(2 * i + 1, dz_b)
        spread(2 * i, dz_a)
        gradient(2 * i + 2, dz_a)
        spread(2 * i + 1, dz_b)

    dzt_c = jnp.broadcast_to(dzt, (128, n_tok)).T[:, 0:1]
    dh_ref[...] = ((dzt_c * vf + dht_s[...].T) * scale).astype(jnp.bfloat16)
    dv_ref[...] = (scale * dzt_c * hf).astype(jnp.bfloat16)


def softmax_scratch(n_cand, n_tok, width):
    return [
        pltpu.VMEM((CHUNK, n_tok), jnp.float32),
        pltpu.VMEM((CHUNK, n_tok), jnp.float32),
        pltpu.VMEM((n_cand, n_tok), jnp.float32),
        pltpu.VMEM((1 + n_cand // SUB, 8, n_tok), jnp.float32),
        pltpu.VMEM((8, n_tok), jnp.float32),
        pltpu.VMEM((width, n_cand), jnp.bfloat16),
        pltpu.VMEM((16, n_tok), jnp.float32),
        pltpu.VMEM((CHUNK, n_tok), jnp.bfloat16),
        pltpu.VMEM((CHUNK, n_tok), jnp.bfloat16),
        pltpu.VMEM((width, n_tok), jnp.float32),
    ]


MESH = pl.DeviceIdType.MESH


def my_place():
    me = lax.axis_index("dp")
    return me, me // 4, (me // 2) % 2, me % 2


def peer_of(place, dy, dx, dc):
    me, y, x, c = place
    return me + dy * (4 - 8 * y) + dx * (2 - 4 * x) + dc * (1 - 2 * c)


def greet(place):
    barrier = pltpu.get_barrier_semaphore()
    for k in range(1, 8):
        pl.semaphore_signal(barrier, inc=1, device_id=(peer_of(place, k // 4, (k // 2) % 2, k % 2),), device_id_type=MESH)


def meet(place):
    greet(place)
    pl.semaphore_wait(pltpu.get_barrier_semaphore(), 7)


def push(src, dst, send_sem, recv_sem, peer):
    copy = pltpu.make_async_remote_copy(src_ref=src, dst_ref=dst, send_sem=send_sem, recv_sem=recv_sem, device_id=(peer,), device_id_type=MESH)
    copy.start()
    return copy


class Reduce:
    def __init__(self, place, data, in_one, mid, in_xa, in_yb, part_a, part_b, in_ya, in_xb, send_sem, recv_sem):
        self.place, self.data = place, data
        self.in_one, self.mid, self.in_xa, self.in_yb = in_one, mid, in_xa, in_yb
        self.part_a, self.part_b, self.in_ya, self.in_xb = part_a, part_b, in_ya, in_xb
        self.send_sem, self.recv_sem = send_sem, recv_sem
        self.half = data.shape[3] // 2
        self.copies = []

    def push(self, k, src, dst, dy, dx, dc):
        copy = push(src, dst, self.send_sem.at[k], self.recv_sem.at[k], peer_of(self.place, dy, dx, dc))
        self.copies.append(copy)

    def one(self):
        c = self.place[3]
        self.push(0, self.data.at[:, :, 1 - c], self.in_one, 0, 0, 1)

    def two(self):
        _, y, x, c = self.place
        half = self.half
        self.copies[0].wait_recv()
        for i in range(2):
            for j in range(2):
                self.mid[i, j] = self.data[i, j, c] + self.in_one[i, j]
        self.push(1, self.mid.at[:, 1 - x, pl.ds(0, half)], self.in_xa, 0, 1, 0)
        self.push(2, self.mid.at[1 - y, :, pl.ds(half, half)], self.in_yb, 1, 0, 0)

    def three(self):
        _, y, x, c = self.place
        half = self.half
        self.copies[1].wait_recv()
        for i in range(2):
            self.part_a[i] = self.mid[i, x, 0:half] + self.in_xa[i]
        self.push(3, self.part_a.at[1 - y], self.in_ya, 1, 0, 0)
        self.copies[2].wait_recv()
        for i in range(2):
            self.part_b[i] = self.mid[y, i, half : 2 * half] + self.in_yb[i]
        self.push(4, self.part_b.at[1 - x], self.in_xb, 0, 1, 0)

    def last(self):
        _, y, x, c = self.place
        self.copies[3].wait_recv()
        first = self.part_a[y] + self.in_ya[...]
        self.copies[4].wait_recv()
        return first, self.part_b[x] + self.in_xb[...]

    def drain(self):
        for copy in self.copies:
            copy.wait_send()


def reduce_scratch(n, rows, width, dtype):
    half = rows // 2
    return [
        pltpu.VMEM((n, 2, 2, rows, width), dtype),
        pltpu.VMEM((n, 2, 2, rows, width), dtype),
        pltpu.VMEM((n, 2, half, width), dtype),
        pltpu.VMEM((n, 2, half, width), dtype),
        pltpu.VMEM((n, 2, half, width), dtype),
        pltpu.VMEM((n, 2, half, width), dtype),
        pltpu.VMEM((n, half, width), dtype),
        pltpu.VMEM((n, half, width), dtype),
        pltpu.SemaphoreType.DMA((n, 5)),
        pltpu.SemaphoreType.DMA((n, 5)),
    ]


class Gather:
    def __init__(self, place, full, send_sem, recv_sem):
        self.place, self.full = place, full
        self.send_sem, self.recv_sem = send_sem, recv_sem
        self.half = full.shape[3] // 2
        self.copies = []

    def push(self, k, ref, dy, dx, dc):
        copy = push(ref, ref, self.send_sem.at[k], self.recv_sem.at[k], peer_of(self.place, dy, dx, dc))
        self.copies.append(copy)

    def one(self):
        _, y, x, c = self.place
        half = self.half
        self.push(0, self.full.at[y, x, c, pl.ds(0, half)], 0, 1, 0)
        self.push(1, self.full.at[y, x, c, pl.ds(half, half)], 1, 0, 0)

    def two(self):
        _, y, x, c = self.place
        half = self.half
        self.copies[0].wait_recv()
        self.push(2, self.full.at[y, :, c, pl.ds(0, half)], 1, 0, 0)
        self.copies[1].wait_recv()
        self.push(3, self.full.at[:, x, c, pl.ds(half, half)], 0, 1, 0)

    def three(self):
        c = self.place[3]
        self.copies[2].wait_recv()
        self.copies[3].wait_recv()
        self.push(4, self.full.at[:, :, c], 0, 0, 1)

    def last(self):
        self.copies[4].wait_recv()

    def drain(self):
        for copy in self.copies:
            copy.wait_send()


def gather_sems():
    return [pltpu.SemaphoreType.DMA((5,)), pltpu.SemaphoreType.DMA((5,))]


def prepare_body(mine, tokens, w_one, w_two, full, query, send_sem, recv_sem):
    place = my_place()
    greet(place)
    for i in range(tokens.shape[0] // 256):
        at = slice(i * 256, i * 256 + 256)
        query[at, :] = tower_fwd(tokens[at, :], w_one[...], w_two[...])
    pl.semaphore_wait(pltpu.get_barrier_semaphore(), 7)
    full[place[0]] = mine[...]
    copies = []
    for k in range(1, 8):
        copies.append(push(mine, full.at[place[0]], send_sem.at[k], recv_sem.at[k], peer_of(place, k // 4, (k // 2) % 2, k % 2)))

    for copy in copies:
        copy.wait()


def prepare(targ_loc, tokens, w_one, w_two):
    n_tok = tokens.shape[0]
    vmem = pl.BlockSpec(memory_space=pltpu.VMEM)
    return pl.pallas_call(
        prepare_body,
        out_shape=(jax.ShapeDtypeStruct((8, 8, 128), jnp.int32), jax.ShapeDtypeStruct((n_tok, w_two.shape[1]), jnp.bfloat16)),
        in_specs=[vmem] * 4,
        out_specs=(vmem,) * 2,
        scratch_shapes=[pltpu.SemaphoreType.DMA((8,)), pltpu.SemaphoreType.DMA((8,))],
        compiler_params=pltpu.CompilerParams(vmem_limit_bytes=VMEM_LIMIT, collective_id=0, has_side_effects=True),
        name="prepare",
    )(targ_loc.reshape(8, 128), tokens, w_one, w_two)


PIECE = 256


def score_body(tok_total, c_hbm, t_hbm, wi_one, wi_two, h_ref, lq_ref, cid_ref, tid_ref, cand_raw, targ_raw, loss_ref, dh_ref, dv_ref, du_ref, *scratch):
    place = my_place()
    me, y, x, c = place
    half = PIECE // 2
    data_c, data_t, in_sem, cand_vec, lq_b, cid_b, rs, ag_send, ag_recv = scratch[0:6] + (scratch[6:16],) + scratch[16:18]
    z_a, z_b, e_s, m_s, s_s, ut_s, fac_s, dz_a, dz_b, dht_s, u_s = scratch[18:29]
    n_cand, width = du_ref.shape
    in_copies = [pltpu.make_async_copy(c_hbm, data_c, in_sem.at[0]), pltpu.make_async_copy(t_hbm, data_t, in_sem.at[1])]
    for copy in in_copies:
        copy.start()
    meet(place)
    reduces = []
    for k in range(6):
        data = data_c.at[:, :, :, pl.ds(k * PIECE, PIECE)] if k < 2 else data_t.at[:, :, :, pl.ds((k - 2) * PIECE, PIECE)]
        reduces.append(Reduce(place, data, *[r.at[k] for r in rs]))
    ag = Gather(place, cand_vec, ag_send, ag_recv)

    def close(k, out, base):
        first, second = reduces[k].last()
        out[base : base + half, :] = first
        out[base + half : base + PIECE, :] = second

    in_copies[0].wait()
    reduces[0].one()
    reduces[1].one()
    in_copies[1].wait()
    for k in range(2, 6):
        reduces[k].one()
    reduces[0].two()
    reduces[1].two()
    reduces[2].two()
    reduces[0].three()
    reduces[1].three()
    reduces[3].two()

    @pl.loop(0, n_cand // 128)
    def _(i):
        rows = pl.ds(pl.multiple_of(i * 128, 128), 128)
        lq_b[rows, :] = jnp.broadcast_to(lq_ref[pl.ds(i, 1), :], (128, 128)).T
        cid_b[rows, :] = jnp.broadcast_to(cid_ref[pl.ds(i, 1), :], (128, 128)).T

    close(0, cand_raw, 0)
    close(1, cand_raw, PIECE)
    cand_vec[y, x, c] = tower_fwd(cand_raw[...], wi_one[...], wi_two[...])
    ag.one()
    reduces[4].two()
    reduces[5].two()
    reduces[2].three()
    ag.two()
    reduces[3].three()
    reduces[4].three()
    ag.three()
    reduces[5].three()
    ag.last()
    n_mine = n_cand // 8
    for b in range(8):
        u_s[b * n_mine : (b + 1) * n_mine, :] = cand_vec[b // 4, (b // 2) % 2, b % 2]
    h = h_ref[...]
    logits_pass(u_s, h, lq_b, cid_b, tid_ref[...], z_a, z_b, e_s, m_s, s_s)
    for k in range(4):
        close(k + 2, targ_raw, k * PIECE)
    v = tower_fwd(targ_raw[...], wi_one[...], wi_two[...])
    loss_pass(tok_total, u_s, ut_s, h, v, e_s, m_s, s_s, fac_s, dz_a, dz_b, dht_s, loss_ref, dh_ref, dv_ref, du_ref)
    for red in reduces:
        red.drain()
    ag.drain()


def score(tok_total, data_c, data_t, wi_one, wi_two, query, log_q, cand_ids, targ_loc):
    n_mine, width = data_c.shape[3:]
    n_tok = data_t.shape[3]
    n_cand = 8 * n_mine
    vmem = pl.BlockSpec(memory_space=pltpu.VMEM)
    hbm = pl.BlockSpec(memory_space=pl.ANY)
    scratch = [pltpu.VMEM(data_c.shape, jnp.bfloat16), pltpu.VMEM(data_t.shape, jnp.bfloat16), pltpu.SemaphoreType.DMA((2,))]
    scratch += [pltpu.VMEM(data_c.shape, jnp.bfloat16), pltpu.VMEM((n_cand, 128), jnp.float32), pltpu.VMEM((n_cand, 128), jnp.int32)]
    scratch += reduce_scratch(6, PIECE, width, jnp.bfloat16) + gather_sems() + softmax_scratch(n_cand, n_tok, width)
    scratch += [pltpu.VMEM((n_cand, width), jnp.bfloat16)]
    rows = [jax.ShapeDtypeStruct((n, width), jnp.bfloat16) for n in (n_mine, n_tok, n_tok, n_tok)]
    return pl.pallas_call(
        functools.partial(score_body, tok_total),
        out_shape=(rows[0], rows[1], jax.ShapeDtypeStruct((8, 128), jnp.float32), rows[2], rows[3], jax.ShapeDtypeStruct((n_cand, width), jnp.float32)),
        in_specs=[hbm, hbm] + [vmem] * 6,
        out_specs=(vmem,) * 6,
        scratch_shapes=scratch,
        compiler_params=pltpu.CompilerParams(vmem_limit_bytes=VMEM_LIMIT, collective_id=1, has_side_effects=True),
        name="score",
    )(data_c, data_t, wi_one, wi_two, query, log_q.reshape(-1, 128), cand_ids.reshape(-1, 128), targ_loc.reshape(1, n_tok))


W_ROWS = 448


def back_body(part_hbm, tok_hbm, loss_in, d_query, d_targ, w_one, w_two, targ_raw, cand_raw, wi_one, wi_two, back_t, back_c, w_first, w_rest, loss_out, *scratch):
    place = my_place()
    me, y, x, c = place
    rs_u, rs_w = scratch[0:10], scratch[10:20]
    at_send, at_recv, ac_send, ac_recv, l_send, l_recv, w_data, l_all, d_part, tokens, in_sem = scratch[20:31]
    width = d_query.shape[1]
    scale = SCORE_GAIN / math.sqrt(width)
    in_copies = [pltpu.make_async_copy(part_hbm, d_part, in_sem.at[0]), pltpu.make_async_copy(tok_hbm, tokens, in_sem.at[1])]
    for copy in in_copies:
        copy.start()
    meet(place)
    red_u = []
    for k in range(2):
        red_u.append(Reduce(place, d_part.at[:, :, :, pl.ds(k * PIECE, PIECE)], *[r.at[k] for r in rs_u]))
    red_w = Reduce(place, w_data, *[r.at[0] for r in rs_w])
    ag_t = Gather(place, back_t, at_send, at_recv)
    ag_c = Gather(place, back_c, ac_send, ac_recv)
    in_copies[0].wait()
    red_u[0].one()
    red_u[1].one()
    l_all[me] = loss_in[...]
    l_copies = []
    for k in range(1, 8):
        l_copies.append(push(loss_in, l_all.at[me], l_send.at[k], l_recv.at[k], peer_of(place, k // 4, (k // 2) % 2, k % 2)))

    def put(first, value):
        n = value.shape[0] // 8
        for b in range(8):
            w_data[b // 4, (b // 2) % 2, b % 2, first : first + n, :] = value[b * n : (b + 1) * n, :]

    t_q, t_hid = tower_back(targ_raw[...], wi_one[...], wi_two[...], d_targ[...])
    red_u[0].two()
    red_u[1].two()
    back_t[y, x, c] = by_transpose(t_q, wi_one[...]).astype(jnp.bfloat16)
    ag_t.one()
    in_copies[1].wait()
    q_q, q_hid = tower_back(tokens[...], w_one[...], w_two[...], d_query[...])
    red_u[0].three()
    red_u[1].three()
    ag_t.two()
    dw_one = over_rows(tokens[...], q_q)
    put(0, dw_one[:, :width])
    put(128, dw_one[:, width:])
    put(256, over_rows(q_hid, d_query[...]))
    parts = []
    for k in range(2):
        first, second = red_u[k].last()
        parts += [first, second]
    d_cand = (jnp.concatenate(parts, axis=0) * scale).astype(jnp.bfloat16)
    c_q, c_hid = tower_back(cand_raw[...], wi_one[...], wi_two[...], d_cand)
    back_c[y, x, c] = by_transpose(c_q, wi_one[...]).astype(jnp.bfloat16)
    ag_c.one()
    dwi_one = over_rows(targ_raw[...], t_q) + over_rows(cand_raw[...], c_q)
    put(320, dwi_one[:, :width])
    put(352, dwi_one[:, width:])
    put(384, over_rows(t_hid, d_targ[...]) + over_rows(c_hid, d_cand))
    red_w.one()
    for copy in l_copies:
        copy.wait()
    loss_out[...] = jnp.sum(l_all[...], axis=0)
    ag_c.two()
    red_w.two()
    ag_t.three()
    red_w.three()
    ag_c.three()
    first, second = red_w.last()
    w_mine = jnp.concatenate([first, second], axis=0)
    w_first[:, :width] = w_mine[0:128]
    w_first[:, width:] = w_mine[128:256]
    w_rest[...] = w_mine[256:W_ROWS]
    ag_t.last()
    ag_c.last()
    for part in red_u + [red_w, ag_t, ag_c]:
        part.drain()


def back_rows(d_part, tokens, loss_part, d_query, d_targ, w_one, w_two, targ_raw, cand_raw, wi_one, wi_two):
    n_mine, width = d_part.shape[3:]
    n_tok = d_query.shape[0]
    vmem = pl.BlockSpec(memory_space=pltpu.VMEM)
    hbm = pl.BlockSpec(memory_space=pl.ANY)
    scratch = reduce_scratch(2, PIECE, width, jnp.float32) + reduce_scratch(1, W_ROWS, width, jnp.float32) + gather_sems() + gather_sems()
    scratch += [pltpu.SemaphoreType.DMA((8,)), pltpu.SemaphoreType.DMA((8,))]
    scratch += [pltpu.VMEM((2, 2, 2, W_ROWS, width), jnp.float32), pltpu.VMEM((8, 8, 128), jnp.float32)]
    scratch += [pltpu.VMEM(d_part.shape, jnp.float32), pltpu.VMEM(tokens.shape, jnp.bfloat16), pltpu.SemaphoreType.DMA((2,))]
    return pl.pallas_call(
        back_body,
        out_shape=(
            jax.ShapeDtypeStruct((2, 2, 2, n_tok, width), jnp.bfloat16),
            jax.ShapeDtypeStruct((2, 2, 2, n_mine, width), jnp.bfloat16),
            jax.ShapeDtypeStruct((128, 2 * width), jnp.float32),
            jax.ShapeDtypeStruct((W_ROWS - 256, width), jnp.float32),
            jax.ShapeDtypeStruct((8, 128), jnp.float32),
        ),
        in_specs=[hbm, hbm] + [vmem] * 9,
        out_specs=(vmem,) * 5,
        scratch_shapes=scratch,
        compiler_params=pltpu.CompilerParams(vmem_limit_bytes=VMEM_LIMIT, collective_id=2, has_side_effects=True),
        name="back_rows",
    )(d_part, tokens, loss_part, d_query, d_targ, w_one, w_two, targ_raw, cand_raw, wi_one, wi_two)


def solution(mesh):
    num_dev = mesh.shape["dp"]

    def local_step(tokens, w_one, w_two, wi_one, wi_two, table_loc, cand_ids, log_q, targ_loc):
        my_index = lax.axis_index("dp")
        rows_loc, width = table_loc.shape
        n_cand = cand_ids.shape[0]
        tok_total = tokens.shape[0] * num_dev
        targ_all, query = prepare(targ_loc, tokens, w_one, w_two)
        targ_all = targ_all.reshape(-1)
        local_ids = jnp.concatenate([cand_ids, targ_all]) - my_index * rows_loc
        spare = rows_loc + jnp.arange(local_ids.shape[0], dtype=jnp.int32) % SPARE
        ids_two = 2 * jnp.where((local_ids >= 0) & (local_ids < rows_loc), local_ids, spare)
        data_c, data_t = pick_rows(ids_two, table_loc, n_cand)
        data_c = data_c.reshape(2, 2, 2, n_cand // 8, width)
        data_t = data_t.reshape(2, 2, 2, tokens.shape[0], width)
        cand_raw, targ_raw, loss_part, d_query, d_targ, d_part = score(tok_total, data_c, data_t, wi_one, wi_two, query, log_q, cand_ids, targ_loc)
        back_t, back_c, w_first, w_rest, loss = back_rows(d_part.reshape(2, 2, 2, n_cand // 8, width), tokens, loss_part, d_query, d_targ, w_one, w_two, targ_raw, cand_raw, wi_one, wi_two)
        dw_one = lax.all_gather(w_first, "dp", axis=0, tiled=True)
        w_all = lax.all_gather(w_rest, "dp", axis=0)
        d_table = scatter_rows(ids_two, back_c.reshape(-1, width), back_t.reshape(-1, width), rows_loc)
        dw_two = w_all[:, 0:64].reshape(-1, width)
        dwi_one = jnp.concatenate([w_all[:, 64:96].reshape(-1, width), w_all[:, 96:128].reshape(-1, width)], axis=1)
        dwi_two = w_all[:, 128:192].reshape(-1, width)
        return loss[0, 0] / tok_total, d_table, dw_one, dw_two, dwi_one, dwi_two

    return jax.shard_map(local_step, mesh=mesh, in_specs=(P("dp", None), P(), P(), P(), P(), P("dp", None), P(), P(), P("dp")), out_specs=(P(), P("dp", None), P(), P(), P(), P()), check_vma=False)
```

```python
import functools
import math
import jax
import jax.numpy as jnp
from jax import lax
from jax.experimental import pallas as pl
from jax.experimental.pallas import tpu as pltpu
from jax.sharding import PartitionSpec as P

SCORE_GAIN = 3.0
HIT_VALUE = -1e9


def tower_fwd(row_block, w_in, w_out):
    pre_act = jnp.dot(row_block, w_in, preferred_element_type=jnp.float32)
    hidden = jax.nn.gelu(pre_act).astype(jnp.bfloat16)
    tower_out = jnp.dot(hidden, w_out, preferred_element_type=jnp.float32).astype(jnp.bfloat16)
    return tower_out


def over_rows(a, b):
    return lax.dot_general(a, b, (((0,), (0,)), ((), ())), preferred_element_type=jnp.float32)


def by_transpose(a, b):
    return lax.dot_general(a, b, (((1,), (1,)), ((), ())), preferred_element_type=jnp.float32)


def tower_back(row_block, w_in, w_out, grad_out):
    pre_act = jnp.dot(row_block, w_in, preferred_element_type=jnp.float32)
    hidden, gelu_back = jax.vjp(jax.nn.gelu, pre_act)
    grad_hidden = by_transpose(grad_out, w_out)
    return gelu_back(grad_hidden)[0].astype(jnp.bfloat16), hidden.astype(jnp.bfloat16)


VMEM_LIMIT = 63 * 1024 * 1024
BATCH = 128
SPARE = 256
GROUP = 16
STAGE_ROWS = 2048
OUT_ROWS = 1024
IN_SLOTS = 12
OUT_SLOTS = 8


def pick_body(ids_s, table, cand_out, targ_out, wide, stage, rows_f, stage_sem):
    rows_loc, width = table.shape
    lane = width // 2
    n_stage = rows_loc // STAGE_ROWS

    def stage_copy(i, slot):
        return pltpu.make_async_copy(table.at[pl.ds(i * STAGE_ROWS, STAGE_ROWS)], stage.at[slot], stage_sem.at[slot])

    for i in range(IN_SLOTS - 1):
        stage_copy(i, i).start()
    wide[pl.ds(2 * rows_loc, 2 * SPARE), :] = jnp.zeros((2 * SPARE, lane), jnp.float32)

    @pl.loop(0, n_stage)
    def _(i):
        slot = i % IN_SLOTS

        @pl.when(i + IN_SLOTS - 1 < n_stage)
        def _():
            stage_copy(i + IN_SLOTS - 1, (i + IN_SLOTS - 1) % IN_SLOTS).start()

        stage_copy(i, slot).wait()

        @pl.loop(0, STAGE_ROWS // 128)
        def _(j):
            block = stage[slot, pl.ds(pl.multiple_of(j * 128, 128), 128), :].astype(jnp.float32)
            base = pl.multiple_of((i * STAGE_ROWS + j * 128) * 2, 256)
            wide[pl.ds(base, 128, 2), :] = block[:, :lane]
            wide[pl.ds(base + 1, 128, 2), :] = block[:, lane:]

    def fill(out, first):
        @pl.loop(0, out.shape[0] // BATCH)
        def _(b):
            for r in range(BATCH):
                at = pl.multiple_of(ids_s[first + b * BATCH + r], 2)
                rows_f[pl.ds(2 * r, 2), :] = wide[pl.ds(at, 2), :]
            rows = pl.ds(pl.multiple_of(b * BATCH, BATCH), BATCH)
            out[rows, :lane] = rows_f[pl.ds(0, BATCH, 2), :].astype(jnp.bfloat16)
            out[rows, lane:] = rows_f[pl.ds(1, BATCH, 2), :].astype(jnp.bfloat16)

    fill(cand_out, 0)
    fill(targ_out, cand_out.shape[0])


def pick_rows(ids_two, table_loc, n_cand):
    rows_loc, width = table_loc.shape
    n_targ = ids_two.shape[0] - n_cand
    vmem = pl.BlockSpec(memory_space=pltpu.VMEM)
    return pl.pallas_call(
        pick_body,
        out_shape=(jax.ShapeDtypeStruct((n_cand, width), jnp.bfloat16), jax.ShapeDtypeStruct((n_targ, width), jnp.bfloat16)),
        in_specs=[pl.BlockSpec(memory_space=pltpu.SMEM), pl.BlockSpec(memory_space=pl.ANY)],
        out_specs=(vmem, vmem),
        scratch_shapes=[
            pltpu.VMEM((2 * (rows_loc + SPARE), width // 2), jnp.float32),
            pltpu.VMEM((IN_SLOTS, STAGE_ROWS, width), jnp.bfloat16),
            pltpu.VMEM((2 * BATCH, width // 2), jnp.float32),
            pltpu.SemaphoreType.DMA((IN_SLOTS,)),
        ],
        compiler_params=pltpu.CompilerParams(vmem_limit_bytes=VMEM_LIMIT),
        name="pick_rows",
    )(ids_two, table_loc)


def scatter_body(ids_s, ids_v, cand_hbm, targ_hbm, wa_hbm, wb_hbm, out_ref, dw_one, dw_two, dwi_one, dwi_two, acc, g2, cand_ref, targ_ref, wa, wb, flag_v, flag_s, out_stage, sem, in_sem, flag_sem, w_sem):
    rows, width = out_ref.shape
    lane = width // 2
    n_cand = cand_ref.shape[0]
    n_all = n_cand + targ_ref.shape[0]
    in_copies = [pltpu.make_async_copy(src, dst, in_sem.at[k]) for k, (src, dst) in enumerate([(cand_hbm, cand_ref), (targ_hbm, targ_ref), (wa_hbm, wa), (wb_hbm, wb)])]
    for copy in in_copies:
        copy.start()

    ids = ids_v[...]
    place = lax.broadcasted_iota(jnp.int32, ids.shape, 1) % GROUP
    twice = jnp.zeros(ids.shape, jnp.int32)
    for k in range(1, GROUP):
        twice = jnp.where((ids == pltpu.roll(ids, k, 1)) & (place >= k), 1, twice)
    flag_v[...] = jnp.broadcast_to(jnp.max(twice, axis=1, keepdims=True), ids.shape)
    flag_copy = pltpu.make_async_copy(flag_v, flag_s, flag_sem)
    flag_copy.start()

    @pl.loop(0, 2 * rows // 512)
    def _(i):
        acc[pl.ds(pl.multiple_of(i * 512, 512), 512), :] = jnp.zeros((512, lane), jnp.float32)

    def one_batch(b, src, src_base):
        rows_b = pl.ds(pl.multiple_of(b * BATCH - src_base, BATCH), BATCH)
        repeated = flag_s[b, 0]

        @pl.when(repeated == 0)
        def _():
            part = src[rows_b, :].astype(jnp.float32)
            g2[pl.ds(0, BATCH, 2), :] = part[:, :lane]
            g2[pl.ds(1, BATCH, 2), :] = part[:, lane:]

        @pl.when(repeated != 0)
        def _():
            row_i = lax.broadcasted_iota(jnp.int32, (BATCH, BATCH), 0) // GROUP
            col_i = lax.broadcasted_iota(jnp.int32, (BATCH, BATCH), 1) // GROUP
            idr = jnp.broadcast_to(ids_v[pl.ds(b, 1), :], (BATCH, BATCH))
            same = jnp.where((idr == idr.T) & (row_i == col_i), 1.0, 0.0).astype(jnp.bfloat16)
            part = jnp.dot(same, src[rows_b, :], preferred_element_type=jnp.float32)
            g2[pl.ds(0, BATCH, 2), :] = part[:, :lane]
            g2[pl.ds(1, BATCH, 2), :] = part[:, lane:]

        for g in range(BATCH // GROUP):
            at = [pl.multiple_of(ids_s[b * BATCH + g * GROUP + r], 2) for r in range(GROUP)]
            new = [acc[pl.ds(at[r], 2), :] + g2[pl.ds(2 * (g * GROUP + r), 2), :] for r in range(GROUP)]
            for r in range(GROUP):
                acc[pl.ds(at[r], 2), :] = new[r]

    for copy in in_copies:
        copy.wait()
    w_copies = []

    def place_block(src, dst):
        copy = pltpu.make_async_copy(src, dst, w_sem)
        copy.start()
        w_copies.append(copy)

    for b in range(8):
        place_block(wa.at[b, pl.ds(0, 128)], dw_one.at[pl.ds(b * 128, 128), pl.ds(0, width)])
        place_block(wa.at[b, pl.ds(128, 128)], dw_one.at[pl.ds(b * 128, 128), pl.ds(width, width)])
        place_block(wa.at[b, pl.ds(256, 64)], dw_two.at[pl.ds(b * 64, 64)])
        place_block(wb.at[b, pl.ds(0, 32)], dwi_one.at[pl.ds(b * 32, 32), pl.ds(0, width)])
        place_block(wb.at[b, pl.ds(32, 32)], dwi_one.at[pl.ds(b * 32, 32), pl.ds(width, width)])
        place_block(wb.at[b, pl.ds(64, 64)], dwi_two.at[pl.ds(b * 64, 64)])
    flag_copy.wait()

    @pl.loop(0, n_cand // BATCH)
    def _(b):
        one_batch(b, cand_ref, 0)

    @pl.loop(n_cand // BATCH, n_all // BATCH)
    def _(b):
        one_batch(b, targ_ref, n_cand)

    n_out = rows // OUT_ROWS

    def out_copy(i, slot):
        return pltpu.make_async_copy(out_stage.at[slot], out_ref.at[pl.ds(i * OUT_ROWS, OUT_ROWS)], sem.at[slot])

    @pl.loop(0, n_out)
    def _(i):
        slot = i % OUT_SLOTS

        @pl.when(i >= OUT_SLOTS)
        def _():
            out_copy(i - OUT_SLOTS, slot).wait()

        @pl.loop(0, OUT_ROWS // 128)
        def _(j):
            base = pl.multiple_of((i * OUT_ROWS + j * 128) * 2, 256)
            here = pl.ds(pl.multiple_of(j * 128, 128), 128)
            out_stage[slot, here, :lane] = acc[pl.ds(base, 128, 2), :]
            out_stage[slot, here, lane:] = acc[pl.ds(base + 1, 128, 2), :]

        out_copy(i, slot).start()

    for i in range(n_out - OUT_SLOTS, n_out):
        out_copy(i, i % OUT_SLOTS).wait()
    for copy in w_copies:
        copy.wait()


def scatter_rows(ids_two, back_cand, back_targ, wa, wb, rows_loc, din):
    n_all = ids_two.shape[0]
    width = back_cand.shape[1]
    n_batch = n_all // BATCH
    vmem = pl.BlockSpec(memory_space=pltpu.VMEM)
    hbm = pl.BlockSpec(memory_space=pl.ANY)
    shapes = [(rows_loc, width), (din, 2 * width), (2 * width, width), (width, 2 * width), (2 * width, width)]
    return pl.pallas_call(
        scatter_body,
        out_shape=tuple(jax.ShapeDtypeStruct(shape, jnp.float32) for shape in shapes),
        in_specs=[pl.BlockSpec(memory_space=pltpu.SMEM), vmem] + [hbm] * 4,
        out_specs=(hbm,) * 5,
        scratch_shapes=[
            pltpu.VMEM((2 * (rows_loc + SPARE), width // 2), jnp.float32),
            pltpu.VMEM((2 * BATCH, width // 2), jnp.float32),
            pltpu.VMEM(back_cand.shape, jnp.bfloat16),
            pltpu.VMEM(back_targ.shape, jnp.bfloat16),
            pltpu.VMEM(wa.shape, jnp.float32),
            pltpu.VMEM(wb.shape, jnp.float32),
            pltpu.VMEM((n_batch, BATCH), jnp.int32),
            pltpu.SMEM((n_batch, BATCH), jnp.int32),
            pltpu.VMEM((OUT_SLOTS, OUT_ROWS, width), jnp.float32),
            pltpu.SemaphoreType.DMA((OUT_SLOTS,)),
            pltpu.SemaphoreType.DMA((4,)),
            pltpu.SemaphoreType.DMA,
            pltpu.SemaphoreType.DMA,
        ],
        compiler_params=pltpu.CompilerParams(vmem_limit_bytes=VMEM_LIMIT),
        cost_estimate=pl.CostEstimate(flops=60_000_000_000, bytes_accessed=40 << 20, transcendentals=0),
        name="scatter_rows",
    )(ids_two, ids_two.reshape(n_batch, BATCH), back_cand, back_targ, wa, wb)


CHUNK = 512
SUB = 64
COLS = 256


def logits_pass(u_ref, h, lq_ref, cid_ref, tid, z_a, z_b, e_s, m_s, s_s):
    n_cand, width = u_ref.shape
    n_tok = h.shape[0]
    scale = SCORE_GAIN / math.sqrt(width)
    ht = h.T
    n_chunk = n_cand // CHUNK

    def multiply(i, z_ref):
        off = pl.multiple_of(jnp.minimum(i, n_chunk - 1) * CHUNK, CHUNK)
        z_ref[...] = jnp.dot(u_ref[pl.ds(off, CHUNK), :], ht, preferred_element_type=jnp.float32)

    def absorb(i, z_ref, first):
        off = pl.multiple_of(i * CHUNK, CHUNK)
        for col in range(0, n_tok, COLS):
            cols = slice(col, col + COLS)
            m8 = m_s[0, :, cols]
            s8 = s_s[:, cols]
            for k in range(CHUNK // SUB):
                rows = pl.ds(pl.multiple_of(off + k * SUB, SUB), SUB)
                lq = jnp.concatenate([lq_ref[rows, :]] * (COLS // 128), axis=1)
                cid = jnp.concatenate([cid_ref[rows, :]] * (COLS // 128), axis=1)
                z = z_ref[k * SUB : (k + 1) * SUB, cols] * scale - lq
                z = jnp.where(cid == tid[:, cols], HIT_VALUE, z).reshape(SUB // 8, 8, COLS)
                m_new = jnp.maximum(m8, jnp.max(z, axis=0))
                e = jnp.exp(z - m_new[None])
                s8 = s8 * jnp.exp(m8 - m_new) + jnp.sum(e, axis=0)
                m8 = m_new
                e_s[rows, cols] = e.reshape(SUB, COLS)
                m_s[1 + i * (CHUNK // SUB) + k, :, cols] = m8
            m_s[0, :, cols] = m8
            s_s[:, cols] = s8

    m_s[0] = jnp.full((8, n_tok), jnp.finfo(jnp.float32).min, jnp.float32)
    s_s[...] = jnp.zeros_like(s_s)
    multiply(0, z_a)

    @pl.loop(0, n_chunk // 2)
    def _(i):
        multiply(2 * i + 1, z_b)
        absorb(2 * i, z_a, 0)
        multiply(2 * i + 2, z_a)
        absorb(2 * i + 1, z_b, 0)


def loss_pass(tok_total, u_ref, ut_s, h, v, e_s, m_s, s_s, fac_s, dz_a, dz_b, dht_s, loss_ref, dh_ref, dv_ref, du_ref):
    n_cand, width = u_ref.shape
    n_tok = h.shape[0]
    scale = SCORE_GAIN / math.sqrt(width)
    n_chunk = n_cand // CHUNK
    hf = h.astype(jnp.float32)
    vf = v.astype(jnp.float32)
    zt = jnp.sum(hf * vf, axis=1, keepdims=True) * scale
    zt = jnp.broadcast_to(zt, (n_tok, 128)).T[0:1, :]
    m8 = m_s[0]
    m = jnp.maximum(zt, jnp.max(m8, axis=0, keepdims=True))
    et = jnp.exp(zt - m)
    den = et + jnp.sum(s_s[...] * jnp.exp(m8 - m), axis=0, keepdims=True)
    part = jnp.sum(jnp.log(den) + m - zt, axis=1, keepdims=True)
    loss_ref[...] = jnp.broadcast_to(part, loss_ref.shape)
    dzt = ((et / den - 1.0) / tok_total).astype(jnp.bfloat16).astype(jnp.float32)
    inv = 1.0 / den / tok_total
    fac_s[0:8, :] = jnp.broadcast_to(m, (8, n_tok))
    fac_s[8:16, :] = jnp.broadcast_to(inv, (8, n_tok))
    for i in range(n_cand // 512):
        ut_s[:, i * 512 : (i + 1) * 512] = u_ref[i * 512 : (i + 1) * 512, :].T

    def gradient(i, dz_ref):
        i = jnp.minimum(i, n_chunk - 1)
        off = pl.multiple_of(i * CHUNK, CHUNK)
        for col in range(0, n_tok, COLS):
            cols = slice(col, col + COLS)
            for k in range(CHUNK // SUB):
                rows = pl.ds(pl.multiple_of(off + k * SUB, SUB), SUB)
                fac = jnp.exp(m_s[1 + i * (CHUNK // SUB) + k, :, cols] - fac_s[0:8, cols]) * fac_s[8:16, cols]
                dz_ref[k * SUB : (k + 1) * SUB, cols] = (e_s[rows, cols].reshape(SUB // 8, 8, COLS) * fac[None]).reshape(SUB, COLS).astype(jnp.bfloat16)

    def spread(i, dz_ref):
        off = pl.multiple_of(i * CHUNK, CHUNK)
        du_ref[pl.ds(off, CHUNK), :] = jnp.dot(dz_ref[...], h, preferred_element_type=jnp.float32)
        dht_s[...] += jnp.dot(ut_s[:, pl.ds(off, CHUNK)], dz_ref[...], preferred_element_type=jnp.float32)

    dht_s[...] = jnp.zeros_like(dht_s)
    gradient(0, dz_a)

    @pl.loop(0, n_chunk // 2)
    def _(i):
        gradient(2 * i + 1, dz_b)
        spread(2 * i, dz_a)
        gradient(2 * i + 2, dz_a)
        spread(2 * i + 1, dz_b)

    dzt_c = jnp.broadcast_to(dzt, (128, n_tok)).T[:, 0:1]
    dh_ref[...] = ((dzt_c * vf + dht_s[...].T) * scale).astype(jnp.bfloat16)
    dv_ref[...] = (scale * dzt_c * hf).astype(jnp.bfloat16)


def softmax_scratch(n_cand, n_tok, width):
    return [
        pltpu.VMEM((CHUNK, n_tok), jnp.float32),
        pltpu.VMEM((CHUNK, n_tok), jnp.float32),
        pltpu.VMEM((n_cand, n_tok), jnp.float32),
        pltpu.VMEM((1 + n_cand // SUB, 8, n_tok), jnp.float32),
        pltpu.VMEM((8, n_tok), jnp.float32),
        pltpu.VMEM((width, n_cand), jnp.bfloat16),
        pltpu.VMEM((16, n_tok), jnp.float32),
        pltpu.VMEM((CHUNK, n_tok), jnp.bfloat16),
        pltpu.VMEM((CHUNK, n_tok), jnp.bfloat16),
        pltpu.VMEM((width, n_tok), jnp.float32),
    ]


MESH = pl.DeviceIdType.MESH


def my_place():
    me = lax.axis_index("dp")
    return me, me // 4, (me // 2) % 2, me % 2


def peer_of(place, dy, dx, dc):
    me, y, x, c = place
    return me + dy * (4 - 8 * y) + dx * (2 - 4 * x) + dc * (1 - 2 * c)


def greet(place):
    barrier = pltpu.get_barrier_semaphore()
    for k in range(1, 8):
        pl.semaphore_signal(barrier, inc=1, device_id=(peer_of(place, k // 4, (k // 2) % 2, k % 2),), device_id_type=MESH)


def meet(place):
    greet(place)
    pl.semaphore_wait(pltpu.get_barrier_semaphore(), 7)


def push(src, dst, send_sem, recv_sem, peer):
    copy = pltpu.make_async_remote_copy(src_ref=src, dst_ref=dst, send_sem=send_sem, recv_sem=recv_sem, device_id=(peer,), device_id_type=MESH)
    copy.start()
    return copy


class Reduce:
    def __init__(self, place, data, in_one, mid, in_xa, in_yb, part_a, part_b, in_ya, in_xb, send_sem, recv_sem):
        self.place, self.data = place, data
        self.in_one, self.mid, self.in_xa, self.in_yb = in_one, mid, in_xa, in_yb
        self.part_a, self.part_b, self.in_ya, self.in_xb = part_a, part_b, in_ya, in_xb
        self.send_sem, self.recv_sem = send_sem, recv_sem
        self.half = data.shape[3] // 2
        self.copies = []

    def push(self, k, src, dst, dy, dx, dc):
        copy = push(src, dst, self.send_sem.at[k], self.recv_sem.at[k], peer_of(self.place, dy, dx, dc))
        self.copies.append(copy)

    def one(self):
        c = self.place[3]
        self.push(0, self.data.at[:, :, 1 - c], self.in_one, 0, 0, 1)

    def two(self):
        _, y, x, c = self.place
        half = self.half
        self.copies[0].wait_recv()
        for i in range(2):
            for j in range(2):
                self.mid[i, j] = self.data[i, j, c] + self.in_one[i, j]
        self.push(1, self.mid.at[:, 1 - x, pl.ds(0, half)], self.in_xa, 0, 1, 0)
        self.push(2, self.mid.at[1 - y, :, pl.ds(half, half)], self.in_yb, 1, 0, 0)

    def three(self):
        _, y, x, c = self.place
        half = self.half
        self.copies[1].wait_recv()
        for i in range(2):
            self.part_a[i] = self.mid[i, x, 0:half] + self.in_xa[i]
        self.push(3, self.part_a.at[1 - y], self.in_ya, 1, 0, 0)
        self.copies[2].wait_recv()
        for i in range(2):
            self.part_b[i] = self.mid[y, i, half : 2 * half] + self.in_yb[i]
        self.push(4, self.part_b.at[1 - x], self.in_xb, 0, 1, 0)

    def last(self):
        _, y, x, c = self.place
        self.copies[3].wait_recv()
        first = self.part_a[y] + self.in_ya[...]
        self.copies[4].wait_recv()
        return first, self.part_b[x] + self.in_xb[...]

    def drain(self):
        for copy in self.copies:
            copy.wait_send()


def reduce_scratch(n, rows, width, dtype):
    half = rows // 2
    return [
        pltpu.VMEM((n, 2, 2, rows, width), dtype),
        pltpu.VMEM((n, 2, 2, rows, width), dtype),
        pltpu.VMEM((n, 2, half, width), dtype),
        pltpu.VMEM((n, 2, half, width), dtype),
        pltpu.VMEM((n, 2, half, width), dtype),
        pltpu.VMEM((n, 2, half, width), dtype),
        pltpu.VMEM((n, half, width), dtype),
        pltpu.VMEM((n, half, width), dtype),
        pltpu.SemaphoreType.DMA((n, 5)),
        pltpu.SemaphoreType.DMA((n, 5)),
    ]


class Gather:
    def __init__(self, place, full, send_sem, recv_sem):
        self.place, self.full = place, full
        self.send_sem, self.recv_sem = send_sem, recv_sem
        self.half = full.shape[3] // 2
        self.copies = []

    def push(self, k, ref, dy, dx, dc):
        copy = push(ref, ref, self.send_sem.at[k], self.recv_sem.at[k], peer_of(self.place, dy, dx, dc))
        self.copies.append(copy)

    def one(self):
        _, y, x, c = self.place
        half = self.half
        self.push(0, self.full.at[y, x, c, pl.ds(0, half)], 0, 1, 0)
        self.push(1, self.full.at[y, x, c, pl.ds(half, half)], 1, 0, 0)

    def two(self):
        _, y, x, c = self.place
        half = self.half
        self.copies[0].wait_recv()
        self.push(2, self.full.at[y, :, c, pl.ds(0, half)], 1, 0, 0)
        self.copies[1].wait_recv()
        self.push(3, self.full.at[:, x, c, pl.ds(half, half)], 0, 1, 0)

    def three(self):
        c = self.place[3]
        self.copies[2].wait_recv()
        self.copies[3].wait_recv()
        self.push(4, self.full.at[:, :, c], 0, 0, 1)

    def last(self):
        self.copies[4].wait_recv()

    def drain(self):
        for copy in self.copies:
            copy.wait_send()


def gather_sems():
    return [pltpu.SemaphoreType.DMA((5,)), pltpu.SemaphoreType.DMA((5,))]


def prepare_body(mine, tokens, w_one, w_two, full, query, send_sem, recv_sem):
    place = my_place()
    greet(place)
    for i in range(tokens.shape[0] // 256):
        at = slice(i * 256, i * 256 + 256)
        query[at, :] = tower_fwd(tokens[at, :], w_one[...], w_two[...])
    pl.semaphore_wait(pltpu.get_barrier_semaphore(), 7)
    full[place[0]] = mine[...]
    copies = []
    for k in range(1, 8):
        copies.append(push(mine, full.at[place[0]], send_sem.at[k], recv_sem.at[k], peer_of(place, k // 4, (k // 2) % 2, k % 2)))

    for copy in copies:
        copy.wait()


def prepare(targ_loc, tokens, w_one, w_two):
    n_tok = tokens.shape[0]
    vmem = pl.BlockSpec(memory_space=pltpu.VMEM)
    return pl.pallas_call(
        prepare_body,
        out_shape=(jax.ShapeDtypeStruct((8, 8, 128), jnp.int32), jax.ShapeDtypeStruct((n_tok, w_two.shape[1]), jnp.bfloat16)),
        in_specs=[vmem] * 4,
        out_specs=(vmem,) * 2,
        scratch_shapes=[pltpu.SemaphoreType.DMA((8,)), pltpu.SemaphoreType.DMA((8,))],
        compiler_params=pltpu.CompilerParams(vmem_limit_bytes=VMEM_LIMIT, collective_id=0, has_side_effects=True),
        name="prepare",
    )(targ_loc.reshape(8, 128), tokens, w_one, w_two)


PIECE = 256


def score_body(tok_total, c_hbm, t_hbm, wi_one, wi_two, h_ref, lq_ref, cid_ref, tid_ref, cand_raw, targ_raw, loss_ref, dh_ref, dv_ref, du_ref, *scratch):
    place = my_place()
    me, y, x, c = place
    half = PIECE // 2
    data_c, data_t, in_sem, cand_vec, lq_b, cid_b, rs, ag_send, ag_recv = scratch[0:6] + (scratch[6:16],) + scratch[16:18]
    z_a, z_b, e_s, m_s, s_s, ut_s, fac_s, dz_a, dz_b, dht_s, u_s = scratch[18:29]
    n_cand, width = du_ref.shape
    in_copies = [pltpu.make_async_copy(c_hbm, data_c, in_sem.at[0]), pltpu.make_async_copy(t_hbm, data_t, in_sem.at[1])]
    for copy in in_copies:
        copy.start()
    meet(place)
    reduces = []
    for k in range(6):
        data = data_c.at[:, :, :, pl.ds(k * PIECE, PIECE)] if k < 2 else data_t.at[:, :, :, pl.ds((k - 2) * PIECE, PIECE)]
        reduces.append(Reduce(place, data, *[r.at[k] for r in rs]))
    ag = Gather(place, cand_vec, ag_send, ag_recv)

    def close(k, out, base):
        first, second = reduces[k].last()
        out[base : base + half, :] = first
        out[base + half : base + PIECE, :] = second

    in_copies[0].wait()
    reduces[0].one()
    reduces[1].one()
    in_copies[1].wait()
    for k in range(2, 6):
        reduces[k].one()
    reduces[0].two()
    reduces[1].two()
    reduces[2].two()
    reduces[0].three()
    reduces[1].three()
    reduces[3].two()

    @pl.loop(0, n_cand // 128)
    def _(i):
        rows = pl.ds(pl.multiple_of(i * 128, 128), 128)
        lq_b[rows, :] = jnp.broadcast_to(lq_ref[pl.ds(i, 1), :], (128, 128)).T
        cid_b[rows, :] = jnp.broadcast_to(cid_ref[pl.ds(i, 1), :], (128, 128)).T

    close(0, cand_raw, 0)
    close(1, cand_raw, PIECE)
    cand_vec[y, x, c] = tower_fwd(cand_raw[...], wi_one[...], wi_two[...])
    ag.one()
    reduces[4].two()
    reduces[5].two()
    reduces[2].three()
    ag.two()
    reduces[3].three()
    reduces[4].three()
    ag.three()
    reduces[5].three()
    ag.last()
    n_mine = n_cand // 8
    for b in range(8):
        u_s[b * n_mine : (b + 1) * n_mine, :] = cand_vec[b // 4, (b // 2) % 2, b % 2]
    h = h_ref[...]
    logits_pass(u_s, h, lq_b, cid_b, tid_ref[...], z_a, z_b, e_s, m_s, s_s)
    for k in range(4):
        close(k + 2, targ_raw, k * PIECE)
    v = tower_fwd(targ_raw[...], wi_one[...], wi_two[...])
    loss_pass(tok_total, u_s, ut_s, h, v, e_s, m_s, s_s, fac_s, dz_a, dz_b, dht_s, loss_ref, dh_ref, dv_ref, du_ref)
    for red in reduces:
        red.drain()
    ag.drain()


def score(tok_total, data_c, data_t, wi_one, wi_two, query, log_q, cand_ids, targ_loc):
    n_mine, width = data_c.shape[3:]
    n_tok = data_t.shape[3]
    n_cand = 8 * n_mine
    vmem = pl.BlockSpec(memory_space=pltpu.VMEM)
    hbm = pl.BlockSpec(memory_space=pl.ANY)
    scratch = [pltpu.VMEM(data_c.shape, jnp.bfloat16), pltpu.VMEM(data_t.shape, jnp.bfloat16), pltpu.SemaphoreType.DMA((2,))]
    scratch += [pltpu.VMEM(data_c.shape, jnp.bfloat16), pltpu.VMEM((n_cand, 128), jnp.float32), pltpu.VMEM((n_cand, 128), jnp.int32)]
    scratch += reduce_scratch(6, PIECE, width, jnp.bfloat16) + gather_sems() + softmax_scratch(n_cand, n_tok, width)
    scratch += [pltpu.VMEM((n_cand, width), jnp.bfloat16)]
    rows = [jax.ShapeDtypeStruct((n, width), jnp.bfloat16) for n in (n_mine, n_tok, n_tok, n_tok)]
    return pl.pallas_call(
        functools.partial(score_body, tok_total),
        out_shape=(rows[0], rows[1], jax.ShapeDtypeStruct((8, 128), jnp.float32), rows[2], rows[3], jax.ShapeDtypeStruct((n_cand, width), jnp.float32)),
        in_specs=[hbm, hbm] + [vmem] * 6,
        out_specs=(vmem,) * 6,
        scratch_shapes=scratch,
        compiler_params=pltpu.CompilerParams(vmem_limit_bytes=VMEM_LIMIT, collective_id=1, has_side_effects=True),
        name="score",
    )(data_c, data_t, wi_one, wi_two, query, log_q.reshape(-1, 128), cand_ids.reshape(-1, 128), targ_loc.reshape(1, n_tok))


WA_ROWS = 320
WB_ROWS = 128


def back_body(part_hbm, tok_hbm, loss_in, d_query, d_targ, w_one, w_two, targ_raw, cand_raw, wi_one, wi_two, back_t, back_c, wa_full, wb_full, loss_out, *scratch):
    place = my_place()
    me, y, x, c = place
    rs_u, rs_a, rs_b = scratch[0:10], scratch[10:20], scratch[20:30]
    at_send, at_recv, ac_send, ac_recv, aa_send, aa_recv, ab_send, ab_recv, l_send, l_recv, wa_data, wb_data, l_all, d_part, tokens, in_sem = scratch[30:46]
    width = d_query.shape[1]
    scale = SCORE_GAIN / math.sqrt(width)
    in_copies = [pltpu.make_async_copy(part_hbm, d_part, in_sem.at[0]), pltpu.make_async_copy(tok_hbm, tokens, in_sem.at[1])]
    for copy in in_copies:
        copy.start()
    meet(place)
    red_u = []
    for k in range(2):
        red_u.append(Reduce(place, d_part.at[:, :, :, pl.ds(k * PIECE, PIECE)], *[r.at[k] for r in rs_u]))
    red_a = Reduce(place, wa_data, *[r.at[0] for r in rs_a])
    red_b = Reduce(place, wb_data, *[r.at[0] for r in rs_b])
    ag_a = Gather(place, wa_full, aa_send, aa_recv)
    ag_b = Gather(place, wb_full, ab_send, ab_recv)
    ag_t = Gather(place, back_t, at_send, at_recv)
    ag_c = Gather(place, back_c, ac_send, ac_recv)
    in_copies[0].wait()
    red_u[0].one()
    red_u[1].one()
    l_all[me] = loss_in[...]
    l_copies = []
    for k in range(1, 8):
        l_copies.append(push(loss_in, l_all.at[me], l_send.at[k], l_recv.at[k], peer_of(place, k // 4, (k // 2) % 2, k % 2)))

    def put(data, first, value):
        n = value.shape[0] // 8
        for b in range(8):
            data[b // 4, (b // 2) % 2, b % 2, first : first + n, :] = value[b * n : (b + 1) * n, :]

    def own(red, full):
        first, second = red.last()
        half = first.shape[0]
        full[y, x, c, 0:half, :] = first
        full[y, x, c, half : 2 * half, :] = second

    t_q, t_hid = tower_back(targ_raw[...], wi_one[...], wi_two[...], d_targ[...])
    red_u[0].two()
    red_u[1].two()
    back_t[y, x, c] = by_transpose(t_q, wi_one[...]).astype(jnp.bfloat16)
    ag_t.one()
    in_copies[1].wait()
    q_q, q_hid = tower_back(tokens[...], w_one[...], w_two[...], d_query[...])
    dw_one = over_rows(tokens[...], q_q)
    put(wa_data, 0, dw_one[:, :width])
    put(wa_data, 128, dw_one[:, width:])
    put(wa_data, 256, over_rows(q_hid, d_query[...]))
    red_a.one()
    red_u[0].three()
    red_u[1].three()
    red_a.two()
    ag_t.two()
    parts = []
    for k in range(2):
        first, second = red_u[k].last()
        parts += [first, second]
    d_cand = (jnp.concatenate(parts, axis=0) * scale).astype(jnp.bfloat16)
    c_q, c_hid = tower_back(cand_raw[...], wi_one[...], wi_two[...], d_cand)
    back_c[y, x, c] = by_transpose(c_q, wi_one[...]).astype(jnp.bfloat16)
    ag_c.one()
    dwi_one = over_rows(targ_raw[...], t_q) + over_rows(cand_raw[...], c_q)
    put(wb_data, 0, dwi_one[:, :width])
    put(wb_data, 32, dwi_one[:, width:])
    put(wb_data, 64, over_rows(t_hid, d_targ[...]) + over_rows(c_hid, d_cand))
    red_b.one()
    red_a.three()
    red_b.two()
    ag_c.two()
    own(red_a, wa_full)
    ag_a.one()
    red_b.three()
    ag_t.three()
    ag_a.two()
    own(red_b, wb_full)
    ag_b.one()
    ag_c.three()
    ag_b.two()
    for copy in l_copies:
        copy.wait()
    loss_out[...] = jnp.sum(l_all[...], axis=0)
    ag_a.three()
    ag_b.three()
    for part in (ag_t, ag_c, ag_a, ag_b):
        part.last()
    for part in red_u + [red_a, red_b, ag_t, ag_c, ag_a, ag_b]:
        part.drain()


def back_rows(d_part, tokens, loss_part, d_query, d_targ, w_one, w_two, targ_raw, cand_raw, wi_one, wi_two):
    n_mine, width = d_part.shape[3:]
    n_tok = d_query.shape[0]
    vmem = pl.BlockSpec(memory_space=pltpu.VMEM)
    hbm = pl.BlockSpec(memory_space=pl.ANY)
    scratch = reduce_scratch(2, PIECE, width, jnp.float32) + reduce_scratch(1, WA_ROWS, width, jnp.float32) + reduce_scratch(1, WB_ROWS, width, jnp.float32)
    scratch += gather_sems() + gather_sems() + gather_sems() + gather_sems()
    scratch += [pltpu.SemaphoreType.DMA((8,)), pltpu.SemaphoreType.DMA((8,))]
    scratch += [pltpu.VMEM((2, 2, 2, WA_ROWS, width), jnp.float32), pltpu.VMEM((2, 2, 2, WB_ROWS, width), jnp.float32), pltpu.VMEM((8, 8, 128), jnp.float32)]
    scratch += [pltpu.VMEM(d_part.shape, jnp.float32), pltpu.VMEM(tokens.shape, jnp.bfloat16), pltpu.SemaphoreType.DMA((2,))]
    return pl.pallas_call(
        back_body,
        out_shape=(
            jax.ShapeDtypeStruct((2, 2, 2, n_tok, width), jnp.bfloat16),
            jax.ShapeDtypeStruct((2, 2, 2, n_mine, width), jnp.bfloat16),
            jax.ShapeDtypeStruct((2, 2, 2, WA_ROWS, width), jnp.float32),
            jax.ShapeDtypeStruct((2, 2, 2, WB_ROWS, width), jnp.float32),
            jax.ShapeDtypeStruct((8, 128), jnp.float32),
        ),
        in_specs=[hbm, hbm] + [vmem] * 9,
        out_specs=(vmem,) * 5,
        scratch_shapes=scratch,
        compiler_params=pltpu.CompilerParams(vmem_limit_bytes=VMEM_LIMIT, collective_id=2, has_side_effects=True),
        name="back_rows",
    )(d_part, tokens, loss_part, d_query, d_targ, w_one, w_two, targ_raw, cand_raw, wi_one, wi_two)


def solution(mesh):
    num_dev = mesh.shape["dp"]

    def local_step(tokens, w_one, w_two, wi_one, wi_two, table_loc, cand_ids, log_q, targ_loc):
        my_index = lax.axis_index("dp")
        rows_loc, width = table_loc.shape
        n_cand = cand_ids.shape[0]
        tok_total = tokens.shape[0] * num_dev
        targ_all, query = prepare(targ_loc, tokens, w_one, w_two)
        targ_all = targ_all.reshape(-1)
        local_ids = jnp.concatenate([cand_ids, targ_all]) - my_index * rows_loc
        spare = rows_loc + jnp.arange(local_ids.shape[0], dtype=jnp.int32) % SPARE
        ids_two = 2 * jnp.where((local_ids >= 0) & (local_ids < rows_loc), local_ids, spare)
        data_c, data_t = pick_rows(ids_two, table_loc, n_cand)
        data_c = data_c.reshape(2, 2, 2, n_cand // 8, width)
        data_t = data_t.reshape(2, 2, 2, tokens.shape[0], width)
        cand_raw, targ_raw, loss_part, d_query, d_targ, d_part = score(tok_total, data_c, data_t, wi_one, wi_two, query, log_q, cand_ids, targ_loc)
        back_t, back_c, wa, wb, loss = back_rows(d_part.reshape(2, 2, 2, n_cand // 8, width), tokens, loss_part, d_query, d_targ, w_one, w_two, targ_raw, cand_raw, wi_one, wi_two)
        d_table, dw_one, dw_two, dwi_one, dwi_two = scatter_rows(ids_two, back_c.reshape(-1, width), back_t.reshape(-1, width), wa.reshape(8, WA_ROWS, width), wb.reshape(8, WB_ROWS, width), rows_loc, tokens.shape[1])
        return loss[0, 0] / tok_total, d_table, dw_one, dw_two, dwi_one, dwi_two

    return jax.shard_map(local_step, mesh=mesh, in_specs=(P("dp", None), P(), P(), P(), P(), P("dp", None), P(), P(), P("dp")), out_specs=(P(), P("dp", None), P(), P(), P(), P()), check_vma=False)
```

```python
import functools
import math
import jax
import jax.numpy as jnp
from jax import lax
from jax.experimental import pallas as pl
from jax.experimental.pallas import tpu as pltpu
from jax.sharding import PartitionSpec as P

SCORE_GAIN = 3.0
HIT_VALUE = -1e9


def tower_fwd(row_block, w_in, w_out):
    pre_act = jnp.dot(row_block, w_in, preferred_element_type=jnp.float32)
    hidden = jax.nn.gelu(pre_act).astype(jnp.bfloat16)
    tower_out = jnp.dot(hidden, w_out, preferred_element_type=jnp.float32).astype(jnp.bfloat16)
    return tower_out


def over_rows(a, b):
    return lax.dot_general(a, b, (((0,), (0,)), ((), ())), preferred_element_type=jnp.float32)


def by_transpose(a, b):
    return lax.dot_general(a, b, (((1,), (1,)), ((), ())), preferred_element_type=jnp.float32)


def tower_back(row_block, w_in, w_out, grad_out):
    pre_act = jnp.dot(row_block, w_in, preferred_element_type=jnp.float32)
    hidden, gelu_back = jax.vjp(jax.nn.gelu, pre_act)
    grad_hidden = by_transpose(grad_out, w_out)
    return gelu_back(grad_hidden)[0].astype(jnp.bfloat16), hidden.astype(jnp.bfloat16)


VMEM_LIMIT = 63 * 1024 * 1024
BATCH = 128
SPARE = 256
GROUP = 16
STAGE_ROWS = 2048
OUT_ROWS = 1024
IN_SLOTS = 12
OUT_SLOTS = 8


def pick_body(ids_s, table, cand_out, targ_out, wide, stage, rows_f, stage_sem):
    rows_loc, width = table.shape
    lane = width // 2
    n_stage = rows_loc // STAGE_ROWS

    def stage_copy(i, slot):
        return pltpu.make_async_copy(table.at[pl.ds(i * STAGE_ROWS, STAGE_ROWS)], stage.at[slot], stage_sem.at[slot])

    for i in range(IN_SLOTS - 1):
        stage_copy(i, i).start()
    wide[pl.ds(2 * rows_loc, 2 * SPARE), :] = jnp.zeros((2 * SPARE, lane), jnp.float32)

    @pl.loop(0, n_stage)
    def _(i):
        slot = i % IN_SLOTS

        @pl.when(i + IN_SLOTS - 1 < n_stage)
        def _():
            stage_copy(i + IN_SLOTS - 1, (i + IN_SLOTS - 1) % IN_SLOTS).start()

        stage_copy(i, slot).wait()

        @pl.loop(0, STAGE_ROWS // 128)
        def _(j):
            block = stage[slot, pl.ds(pl.multiple_of(j * 128, 128), 128), :].astype(jnp.float32)
            base = pl.multiple_of((i * STAGE_ROWS + j * 128) * 2, 256)
            wide[pl.ds(base, 128, 2), :] = block[:, :lane]
            wide[pl.ds(base + 1, 128, 2), :] = block[:, lane:]

    def fill(out, first):
        @pl.loop(0, out.shape[0] // BATCH)
        def _(b):
            for r in range(BATCH):
                at = pl.multiple_of(ids_s[first + b, r], 2)
                rows_f[pl.ds(2 * r, 2), :] = wide[pl.ds(at, 2), :]
            rows = pl.ds(pl.multiple_of(b * BATCH, BATCH), BATCH)
            out[rows, :lane] = rows_f[pl.ds(0, BATCH, 2), :].astype(jnp.bfloat16)
            out[rows, lane:] = rows_f[pl.ds(1, BATCH, 2), :].astype(jnp.bfloat16)

    fill(cand_out, 0)
    fill(targ_out, cand_out.shape[0] // BATCH)


def pick_rows(ids_two, table_loc, n_cand):
    rows_loc, width = table_loc.shape
    n_targ = ids_two.size - n_cand
    vmem = pl.BlockSpec(memory_space=pltpu.VMEM)
    return pl.pallas_call(
        pick_body,
        out_shape=(jax.ShapeDtypeStruct((n_cand, width), jnp.bfloat16), jax.ShapeDtypeStruct((n_targ, width), jnp.bfloat16)),
        in_specs=[pl.BlockSpec(memory_space=pltpu.SMEM), pl.BlockSpec(memory_space=pl.ANY)],
        out_specs=(vmem, vmem),
        scratch_shapes=[
            pltpu.VMEM((2 * (rows_loc + SPARE), width // 2), jnp.float32),
            pltpu.VMEM((IN_SLOTS, STAGE_ROWS, width), jnp.bfloat16),
            pltpu.VMEM((2 * BATCH, width // 2), jnp.float32),
            pltpu.SemaphoreType.DMA((IN_SLOTS,)),
        ],
        compiler_params=pltpu.CompilerParams(vmem_limit_bytes=VMEM_LIMIT),
        name="pick_rows",
    )(ids_two, table_loc)


def scatter_body(ids_s, ids_v, cand_hbm, targ_hbm, wa_hbm, wb_hbm, out_ref, dw_one, dw_two, dwi_one, dwi_two, acc, g2, cand_ref, targ_ref, wa, wb, flag_v, flag_s, out_stage, sem, in_sem, flag_sem, w_sem):
    rows, width = out_ref.shape
    lane = width // 2
    n_cand = cand_ref.shape[0]
    n_all = n_cand + targ_ref.shape[0]
    in_copies = [pltpu.make_async_copy(src, dst, in_sem.at[k]) for k, (src, dst) in enumerate([(cand_hbm, cand_ref), (targ_hbm, targ_ref), (wa_hbm, wa), (wb_hbm, wb)])]
    for copy in in_copies:
        copy.start()

    ids = ids_v[...]
    place = lax.broadcasted_iota(jnp.int32, ids.shape, 1) % GROUP
    twice = jnp.zeros(ids.shape, jnp.int32)
    for k in range(1, GROUP):
        twice = jnp.where((ids == pltpu.roll(ids, k, 1)) & (place >= k), 1, twice)
    flag_v[...] = jnp.broadcast_to(jnp.max(twice, axis=1, keepdims=True), ids.shape)
    flag_copy = pltpu.make_async_copy(flag_v, flag_s, flag_sem)
    flag_copy.start()

    @pl.loop(0, 2 * rows // 512)
    def _(i):
        acc[pl.ds(pl.multiple_of(i * 512, 512), 512), :] = jnp.zeros((512, lane), jnp.float32)

    def one_batch(b, src, src_base):
        rows_b = pl.ds(pl.multiple_of(b * BATCH - src_base, BATCH), BATCH)
        repeated = flag_s[b, 0]

        @pl.when(repeated == 0)
        def _():
            part = src[rows_b, :].astype(jnp.float32)
            g2[pl.ds(0, BATCH, 2), :] = part[:, :lane]
            g2[pl.ds(1, BATCH, 2), :] = part[:, lane:]

        @pl.when(repeated != 0)
        def _():
            row_i = lax.broadcasted_iota(jnp.int32, (BATCH, BATCH), 0) // GROUP
            col_i = lax.broadcasted_iota(jnp.int32, (BATCH, BATCH), 1) // GROUP
            idr = jnp.broadcast_to(ids_v[pl.ds(b, 1), :], (BATCH, BATCH))
            same = jnp.where((idr == idr.T) & (row_i == col_i), 1.0, 0.0).astype(jnp.bfloat16)
            part = jnp.dot(same, src[rows_b, :], preferred_element_type=jnp.float32)
            g2[pl.ds(0, BATCH, 2), :] = part[:, :lane]
            g2[pl.ds(1, BATCH, 2), :] = part[:, lane:]

        for g in range(BATCH // GROUP):
            at = [pl.multiple_of(ids_s[b, g * GROUP + r], 2) for r in range(GROUP)]
            new = [acc[pl.ds(at[r], 2), :] + g2[pl.ds(2 * (g * GROUP + r), 2), :] for r in range(GROUP)]
            for r in range(GROUP):
                acc[pl.ds(at[r], 2), :] = new[r]

    for copy in in_copies:
        copy.wait()
    w_copies = []

    def place_block(src, dst):
        copy = pltpu.make_async_copy(src, dst, w_sem)
        copy.start()
        w_copies.append(copy)

    for b in range(8):
        place_block(wa.at[b, pl.ds(0, 128)], dw_one.at[pl.ds(b * 128, 128), pl.ds(0, width)])
        place_block(wa.at[b, pl.ds(128, 128)], dw_one.at[pl.ds(b * 128, 128), pl.ds(width, width)])
        place_block(wa.at[b, pl.ds(256, 64)], dw_two.at[pl.ds(b * 64, 64)])
        place_block(wb.at[b, pl.ds(0, 32)], dwi_one.at[pl.ds(b * 32, 32), pl.ds(0, width)])
        place_block(wb.at[b, pl.ds(32, 32)], dwi_one.at[pl.ds(b * 32, 32), pl.ds(width, width)])
        place_block(wb.at[b, pl.ds(64, 64)], dwi_two.at[pl.ds(b * 64, 64)])
    flag_copy.wait()

    @pl.loop(0, n_cand // BATCH)
    def _(b):
        one_batch(b, cand_ref, 0)

    @pl.loop(n_cand // BATCH, n_all // BATCH)
    def _(b):
        one_batch(b, targ_ref, n_cand)

    n_out = rows // OUT_ROWS

    def out_copy(i, slot):
        return pltpu.make_async_copy(out_stage.at[slot], out_ref.at[pl.ds(i * OUT_ROWS, OUT_ROWS)], sem.at[slot])

    @pl.loop(0, n_out)
    def _(i):
        slot = i % OUT_SLOTS

        @pl.when(i >= OUT_SLOTS)
        def _():
            out_copy(i - OUT_SLOTS, slot).wait()

        @pl.loop(0, OUT_ROWS // 128)
        def _(j):
            base = pl.multiple_of((i * OUT_ROWS + j * 128) * 2, 256)
            here = pl.ds(pl.multiple_of(j * 128, 128), 128)
            out_stage[slot, here, :lane] = acc[pl.ds(base, 128, 2), :]
            out_stage[slot, here, lane:] = acc[pl.ds(base + 1, 128, 2), :]

        out_copy(i, slot).start()

    for i in range(n_out - OUT_SLOTS, n_out):
        out_copy(i, i % OUT_SLOTS).wait()
    for copy in w_copies:
        copy.wait()


def scatter_rows(ids_two, back_cand, back_targ, wa, wb, rows_loc, din):
    width = back_cand.shape[1]
    n_batch = ids_two.shape[0]
    vmem = pl.BlockSpec(memory_space=pltpu.VMEM)
    hbm = pl.BlockSpec(memory_space=pl.ANY)
    shapes = [(rows_loc, width), (din, 2 * width), (2 * width, width), (width, 2 * width), (2 * width, width)]
    return pl.pallas_call(
        scatter_body,
        out_shape=tuple(jax.ShapeDtypeStruct(shape, jnp.float32) for shape in shapes),
        in_specs=[pl.BlockSpec(memory_space=pltpu.SMEM), vmem] + [hbm] * 4,
        out_specs=(hbm,) * 5,
        scratch_shapes=[
            pltpu.VMEM((2 * (rows_loc + SPARE), width // 2), jnp.float32),
            pltpu.VMEM((2 * BATCH, width // 2), jnp.float32),
            pltpu.VMEM(back_cand.shape, jnp.bfloat16),
            pltpu.VMEM(back_targ.shape, jnp.bfloat16),
            pltpu.VMEM(wa.shape, jnp.float32),
            pltpu.VMEM(wb.shape, jnp.float32),
            pltpu.VMEM((n_batch, BATCH), jnp.int32),
            pltpu.SMEM((n_batch, BATCH), jnp.int32),
            pltpu.VMEM((OUT_SLOTS, OUT_ROWS, width), jnp.float32),
            pltpu.SemaphoreType.DMA((OUT_SLOTS,)),
            pltpu.SemaphoreType.DMA((4,)),
            pltpu.SemaphoreType.DMA,
            pltpu.SemaphoreType.DMA,
        ],
        compiler_params=pltpu.CompilerParams(vmem_limit_bytes=VMEM_LIMIT),
        cost_estimate=pl.CostEstimate(flops=60_000_000_000, bytes_accessed=40 << 20, transcendentals=0),
        name="scatter_rows",
    )(ids_two, ids_two, back_cand, back_targ, wa, wb)


CHUNK = 512
SUB = 128
COLS = 256


def logits_pass(u_at, n_cand, h, lq_ref, cid_ref, tid, z_a, z_b, e_s, m_s, s_s, between):
    n_tok, width = h.shape
    scale = SCORE_GAIN / math.sqrt(width)
    ht = h.T
    n_chunk = n_cand // CHUNK

    def multiply(i, z_ref):
        z_ref[...] = jnp.dot(u_at(jnp.minimum(i, n_chunk - 1)), ht, preferred_element_type=jnp.float32)

    def absorb(i, z_ref):
        off = pl.multiple_of(i * CHUNK, CHUNK)
        for col in range(0, n_tok, COLS):
            cols = slice(col, col + COLS)
            m8 = m_s[0, :, cols]
            s8 = s_s[:, cols]
            for k in range(CHUNK // SUB):
                rows = pl.ds(pl.multiple_of(off + k * SUB, SUB), SUB)
                lq = jnp.concatenate([lq_ref[rows, :]] * (COLS // 128), axis=1)
                cid = jnp.concatenate([cid_ref[rows, :]] * (COLS // 128), axis=1)
                z = z_ref[k * SUB : (k + 1) * SUB, cols] * scale - lq
                z = jnp.where(cid == tid[:, cols], HIT_VALUE, z).reshape(SUB // 8, 8, COLS)
                m_new = jnp.maximum(m8, jnp.max(z, axis=0))
                e = jnp.exp(z - m_new[None])
                s8 = s8 * jnp.exp(m8 - m_new) + jnp.sum(e, axis=0)
                m8 = m_new
                e_s[rows, cols] = e.reshape(SUB, COLS)
                m_s[1 + i * (CHUNK // SUB) + k, :, cols] = m8
            m_s[0, :, cols] = m8
            s_s[:, cols] = s8

    m_s[0] = jnp.full((8, n_tok), jnp.finfo(jnp.float32).min, jnp.float32)
    s_s[...] = jnp.zeros_like(s_s)
    multiply(0, z_a)

    def two_chunks(i):
        multiply(2 * i + 1, z_b)
        absorb(2 * i, z_a)
        multiply(2 * i + 2, z_a)
        absorb(2 * i + 1, z_b)

    pl.loop(0, n_chunk // 4)(two_chunks)
    between()
    pl.loop(n_chunk // 4, n_chunk // 2)(two_chunks)


def loss_pass(tok_total, u_at, ut_s, h, v, e_s, m_s, s_s, fac_s, dz_a, dz_b, dht_s, loss_ref, dh_ref, dv_ref, du_ref, dz_ref):
    n_cand, width = du_ref.shape
    n_tok = h.shape[0]
    scale = SCORE_GAIN / math.sqrt(width)
    n_chunk = n_cand // CHUNK
    hf = h.astype(jnp.float32)
    vf = v.astype(jnp.float32)
    zt = jnp.sum(hf * vf, axis=1, keepdims=True) * scale
    zt = jnp.broadcast_to(zt, (n_tok, 128)).T[0:1, :]
    m8 = m_s[0]
    m = jnp.maximum(zt, jnp.max(m8, axis=0, keepdims=True))
    et = jnp.exp(zt - m)
    den = et + jnp.sum(s_s[...] * jnp.exp(m8 - m), axis=0, keepdims=True)
    part = jnp.sum(jnp.log(den) + m - zt, axis=1, keepdims=True)
    loss_ref[...] = jnp.broadcast_to(part, loss_ref.shape)
    dzt = ((et / den - 1.0) / tok_total).astype(jnp.bfloat16).astype(jnp.float32)
    inv = 1.0 / den / tok_total
    fac_s[0:8, :] = jnp.broadcast_to(m, (8, n_tok))
    fac_s[8:16, :] = jnp.broadcast_to(inv, (8, n_tok))
    for i in range(n_chunk):
        ut_s[:, i * CHUNK : (i + 1) * CHUNK] = u_at(i).T
    for i in range(8):
        dz_ref[i : i + 1, :] = dzt[:, i * 128 : (i + 1) * 128]

    def gradient(i, out):
        i = jnp.minimum(i, n_chunk - 1)
        off = pl.multiple_of(i * CHUNK, CHUNK)
        for col in range(0, n_tok, COLS):
            cols = slice(col, col + COLS)
            for k in range(CHUNK // SUB):
                rows = pl.ds(pl.multiple_of(off + k * SUB, SUB), SUB)
                fac = jnp.exp(m_s[1 + i * (CHUNK // SUB) + k, :, cols] - fac_s[0:8, cols]) * fac_s[8:16, cols]
                out[k * SUB : (k + 1) * SUB, cols] = (e_s[rows, cols].reshape(SUB // 8, 8, COLS) * fac[None]).reshape(SUB, COLS).astype(jnp.bfloat16)

    def spread(i, dz_c):
        off = pl.multiple_of(i * CHUNK, CHUNK)
        du_ref[pl.ds(off, CHUNK), :] = jnp.dot(dz_c[...], h, preferred_element_type=jnp.float32)
        dht_s[...] += jnp.dot(ut_s[:, pl.ds(off, CHUNK)], dz_c[...], preferred_element_type=jnp.float32)

    dht_s[...] = jnp.zeros_like(dht_s)
    gradient(0, dz_a)

    @pl.loop(0, n_chunk // 2)
    def _(i):
        gradient(2 * i + 1, dz_b)
        spread(2 * i, dz_a)
        gradient(2 * i + 2, dz_a)
        spread(2 * i + 1, dz_b)

    dzt_c = jnp.broadcast_to(dzt, (128, n_tok)).T[:, 0:1]
    dh_ref[...] = ((dzt_c * vf + dht_s[...].T) * scale).astype(jnp.bfloat16)
    dv_ref[...] = (scale * dzt_c * hf).astype(jnp.bfloat16)


def softmax_scratch(n_cand, n_tok, width):
    return [
        pltpu.VMEM((CHUNK, n_tok), jnp.float32),
        pltpu.VMEM((CHUNK, n_tok), jnp.float32),
        pltpu.VMEM((n_cand, n_tok), jnp.float32),
        pltpu.VMEM((1 + n_cand // SUB, 8, n_tok), jnp.float32),
        pltpu.VMEM((8, n_tok), jnp.float32),
        pltpu.VMEM((width, n_cand), jnp.bfloat16),
        pltpu.VMEM((16, n_tok), jnp.float32),
        pltpu.VMEM((CHUNK, n_tok), jnp.bfloat16),
        pltpu.VMEM((CHUNK, n_tok), jnp.bfloat16),
        pltpu.VMEM((width, n_tok), jnp.float32),
    ]


MESH = pl.DeviceIdType.MESH


def my_place():
    me = lax.axis_index("dp")
    return me, me // 4, (me // 2) % 2, me % 2


def peer_of(place, dy, dx, dc):
    me, y, x, c = place
    return me + dy * (4 - 8 * y) + dx * (2 - 4 * x) + dc * (1 - 2 * c)


def greet(place):
    barrier = pltpu.get_barrier_semaphore()
    for k in range(1, 8):
        pl.semaphore_signal(barrier, inc=1, device_id=(peer_of(place, k // 4, (k // 2) % 2, k % 2),), device_id_type=MESH)


def meet(place):
    greet(place)
    pl.semaphore_wait(pltpu.get_barrier_semaphore(), 7)


def push(src, dst, send_sem, recv_sem, peer):
    copy = pltpu.make_async_remote_copy(src_ref=src, dst_ref=dst, send_sem=send_sem, recv_sem=recv_sem, device_id=(peer,), device_id_type=MESH)
    copy.start()
    return copy


class Reduce:
    def __init__(self, place, data, in_one, mid, in_xa, in_yb, part_a, part_b, in_ya, in_xb, send_sem, recv_sem):
        self.place, self.data = place, data
        self.in_one, self.mid, self.in_xa, self.in_yb = in_one, mid, in_xa, in_yb
        self.part_a, self.part_b, self.in_ya, self.in_xb = part_a, part_b, in_ya, in_xb
        self.send_sem, self.recv_sem = send_sem, recv_sem
        self.half = data.shape[3] // 2
        self.copies = []

    def push(self, k, src, dst, dy, dx, dc):
        copy = push(src, dst, self.send_sem.at[k], self.recv_sem.at[k], peer_of(self.place, dy, dx, dc))
        self.copies.append(copy)

    def one(self):
        c = self.place[3]
        self.push(0, self.data.at[:, :, 1 - c], self.in_one, 0, 0, 1)

    def two(self):
        _, y, x, c = self.place
        half = self.half
        self.copies[0].wait_recv()
        for i in range(2):
            for j in range(2):
                self.mid[i, j] = self.data[i, j, c] + self.in_one[i, j]
        self.push(1, self.mid.at[:, 1 - x, pl.ds(0, half)], self.in_xa, 0, 1, 0)
        self.push(2, self.mid.at[1 - y, :, pl.ds(half, half)], self.in_yb, 1, 0, 0)

    def three(self):
        _, y, x, c = self.place
        half = self.half
        self.copies[1].wait_recv()
        for i in range(2):
            self.part_a[i] = self.mid[i, x, 0:half] + self.in_xa[i]
        self.push(3, self.part_a.at[1 - y], self.in_ya, 1, 0, 0)
        self.copies[2].wait_recv()
        for i in range(2):
            self.part_b[i] = self.mid[y, i, half : 2 * half] + self.in_yb[i]
        self.push(4, self.part_b.at[1 - x], self.in_xb, 0, 1, 0)

    def last(self):
        _, y, x, c = self.place
        self.copies[3].wait_recv()
        first = self.part_a[y] + self.in_ya[...]
        self.copies[4].wait_recv()
        return first, self.part_b[x] + self.in_xb[...]

    def drain(self):
        for copy in self.copies:
            copy.wait_send()


def reduce_scratch(n, rows, width, dtype):
    half = rows // 2
    return [
        pltpu.VMEM((n, 2, 2, rows, width), dtype),
        pltpu.VMEM((n, 2, 2, rows, width), dtype),
        pltpu.VMEM((n, 2, half, width), dtype),
        pltpu.VMEM((n, 2, half, width), dtype),
        pltpu.VMEM((n, 2, half, width), dtype),
        pltpu.VMEM((n, 2, half, width), dtype),
        pltpu.VMEM((n, half, width), dtype),
        pltpu.VMEM((n, half, width), dtype),
        pltpu.SemaphoreType.DMA((n, 5)),
        pltpu.SemaphoreType.DMA((n, 5)),
    ]


class Gather:
    def __init__(self, place, full, send_sem, recv_sem):
        self.place, self.full = place, full
        self.send_sem, self.recv_sem = send_sem, recv_sem
        self.half = full.shape[3] // 2
        self.copies = []

    def push(self, k, ref, dy, dx, dc):
        copy = push(ref, ref, self.send_sem.at[k], self.recv_sem.at[k], peer_of(self.place, dy, dx, dc))
        self.copies.append(copy)

    def one(self):
        _, y, x, c = self.place
        half = self.half
        self.push(0, self.full.at[y, x, c, pl.ds(0, half)], 0, 1, 0)
        self.push(1, self.full.at[y, x, c, pl.ds(half, half)], 1, 0, 0)

    def two(self):
        _, y, x, c = self.place
        half = self.half
        self.copies[0].wait_recv()
        self.push(2, self.full.at[y, :, c, pl.ds(0, half)], 1, 0, 0)
        self.copies[1].wait_recv()
        self.push(3, self.full.at[:, x, c, pl.ds(half, half)], 0, 1, 0)

    def three(self):
        c = self.place[3]
        self.copies[2].wait_recv()
        self.copies[3].wait_recv()
        self.push(4, self.full.at[:, :, c], 0, 0, 1)

    def last(self):
        self.copies[4].wait_recv()

    def drain(self):
        for copy in self.copies:
            copy.wait_send()


def gather_sems():
    return [pltpu.SemaphoreType.DMA((5,)), pltpu.SemaphoreType.DMA((5,))]


def prepare_body(rows_loc, mine, cand_ids, tokens, w_one, w_two, ids_two, query, full, send_sem, recv_sem):
    place = my_place()
    me = place[0]
    greet(place)
    for i in range(tokens.shape[0] // 256):
        at = slice(i * 256, i * 256 + 256)
        query[at, :] = tower_fwd(tokens[at, :], w_one[...], w_two[...])
    pl.semaphore_wait(pltpu.get_barrier_semaphore(), 7)
    full[me] = mine[...]
    copies = []
    for k in range(1, 8):
        copies.append(push(mine, full.at[me], send_sem.at[k], recv_sem.at[k], peer_of(place, k // 4, (k // 2) % 2, k % 2)))

    def owned(ids):
        local = ids - me * rows_loc
        spare = rows_loc + (lax.broadcasted_iota(jnp.int32, ids.shape, 0) % 2) * 128 + lax.broadcasted_iota(jnp.int32, ids.shape, 1)
        return 2 * jnp.where((local >= 0) & (local < rows_loc), local, spare)

    n_c = cand_ids.shape[0]
    ids_two[0:n_c, :] = owned(cand_ids[...])
    for copy in copies:
        copy.wait()
    ids_two[n_c : n_c + 64, :] = owned(full[...].reshape(64, 128))


def prepare(targ_loc, cand_ids, tokens, w_one, w_two, rows_loc):
    n_tok = tokens.shape[0]
    n_c = cand_ids.shape[0] // 128
    vmem = pl.BlockSpec(memory_space=pltpu.VMEM)
    return pl.pallas_call(
        functools.partial(prepare_body, rows_loc),
        out_shape=(jax.ShapeDtypeStruct((n_c + 64, 128), jnp.int32), jax.ShapeDtypeStruct((n_tok, w_two.shape[1]), jnp.bfloat16)),
        in_specs=[vmem] * 5,
        out_specs=(vmem,) * 2,
        scratch_shapes=[pltpu.VMEM((8, 8, 128), jnp.int32), pltpu.SemaphoreType.DMA((8,)), pltpu.SemaphoreType.DMA((8,))],
        compiler_params=pltpu.CompilerParams(vmem_limit_bytes=VMEM_LIMIT, collective_id=0, has_side_effects=True),
        name="prepare",
    )(targ_loc.reshape(8, 128), cand_ids.reshape(n_c, 128), tokens, w_one, w_two)


PIECE = 256


def score_body(tok_total, c_hbm, t_hbm, wi_one, wi_two, h_ref, lq_ref, cid_ref, tid_ref, cand_raw, targ_raw, loss_ref, dh_ref, dv_ref, du_ref, dz_ref, h_part, *scratch):
    place = my_place()
    me, y, x, c = place
    half = PIECE // 2
    data_c, data_t, in_sem, cand_vec, lq_b, cid_b, rs, ag_send, ag_recv = scratch[0:6] + (scratch[6:16],) + scratch[16:18]
    z_a, z_b, e_s, m_s, s_s, ut_s, fac_s, dz_a, dz_b, dht_s, h_send, h_recv = scratch[18:30]
    n_cand, width = du_ref.shape
    in_copies = [pltpu.make_async_copy(c_hbm, data_c, in_sem.at[0]), pltpu.make_async_copy(t_hbm, data_t, in_sem.at[1])]
    for copy in in_copies:
        copy.start()
    meet(place)
    reduces = []
    for k in range(6):
        data = data_c.at[:, :, :, pl.ds(k * PIECE, PIECE)] if k < 2 else data_t.at[:, :, :, pl.ds((k - 2) * PIECE, PIECE)]
        reduces.append(Reduce(place, data, *[r.at[k] for r in rs]))
    ag = Gather(place, cand_vec, ag_send, ag_recv)
    ag_h = Gather((me, y, x, 0), h_part, h_send, h_recv)
    h_part[y, x, 0] = h_ref[...]

    def close(k, out, base):
        first, second = reduces[k].last()
        out[base : base + half, :] = first
        out[base + half : base + PIECE, :] = second

    in_copies[0].wait()
    reduces[0].one()
    reduces[1].one()
    in_copies[1].wait()
    for k in range(2, 6):
        reduces[k].one()
    reduces[0].two()
    reduces[1].two()
    reduces[2].two()
    reduces[0].three()
    reduces[1].three()
    reduces[3].two()

    @pl.loop(0, n_cand // 128)
    def _(i):
        rows = pl.ds(pl.multiple_of(i * 128, 128), 128)
        lq_b[rows, :] = jnp.broadcast_to(lq_ref[pl.ds(i, 1), :], (128, 128)).T
        cid_b[rows, :] = jnp.broadcast_to(cid_ref[pl.ds(i, 1), :], (128, 128)).T

    close(0, cand_raw, 0)
    close(1, cand_raw, PIECE)
    cand_vec[y, x, c] = tower_fwd(cand_raw[...], wi_one[...], wi_two[...])
    ag.one()
    reduces[4].two()
    reduces[5].two()
    reduces[2].three()
    ag.two()
    ag_h.one()
    reduces[3].three()
    reduces[4].three()
    ag.three()
    reduces[5].three()
    ag.last()

    def u_at(i):
        return cand_vec[i // 4, (i // 2) % 2, i % 2]

    h = h_ref[...]
    logits_pass(u_at, n_cand, h, lq_b, cid_b, tid_ref[...], z_a, z_b, e_s, m_s, s_s, ag_h.two)
    for k in range(4):
        close(k + 2, targ_raw, k * PIECE)
    v = tower_fwd(targ_raw[...], wi_one[...], wi_two[...])
    loss_pass(tok_total, u_at, ut_s, h, v, e_s, m_s, s_s, fac_s, dz_a, dz_b, dht_s, loss_ref, dh_ref, dv_ref, du_ref, dz_ref)
    ag_h.copies[2].wait_recv()
    ag_h.copies[3].wait_recv()
    for red in reduces:
        red.drain()
    ag.drain()
    ag_h.drain()


def score(tok_total, data_c, data_t, wi_one, wi_two, query, log_q, cand_ids, targ_loc):
    n_mine, width = data_c.shape[3:]
    n_tok = data_t.shape[3]
    n_cand = 8 * n_mine
    vmem = pl.BlockSpec(memory_space=pltpu.VMEM)
    hbm = pl.BlockSpec(memory_space=pl.ANY)
    scratch = [pltpu.VMEM(data_c.shape, jnp.bfloat16), pltpu.VMEM(data_t.shape, jnp.bfloat16), pltpu.SemaphoreType.DMA((2,))]
    scratch += [pltpu.VMEM(data_c.shape, jnp.bfloat16), pltpu.VMEM((n_cand, 128), jnp.float32), pltpu.VMEM((n_cand, 128), jnp.int32)]
    scratch += reduce_scratch(6, PIECE, width, jnp.bfloat16) + gather_sems() + softmax_scratch(n_cand, n_tok, width)
    scratch += gather_sems()
    rows = [jax.ShapeDtypeStruct((n, width), jnp.bfloat16) for n in (n_mine, n_tok, n_tok, n_tok)]
    return pl.pallas_call(
        functools.partial(score_body, tok_total),
        out_shape=(rows[0], rows[1], jax.ShapeDtypeStruct((8, 128), jnp.float32), rows[2], rows[3], jax.ShapeDtypeStruct((n_cand, width), jnp.float32), jax.ShapeDtypeStruct((8, 128), jnp.float32), jax.ShapeDtypeStruct((2, 2, 1, n_tok, width), jnp.bfloat16)),
        in_specs=[hbm, hbm] + [vmem] * 6,
        out_specs=(vmem,) * 8,
        scratch_shapes=scratch,
        compiler_params=pltpu.CompilerParams(vmem_limit_bytes=VMEM_LIMIT, collective_id=1, has_side_effects=True),
        name="score",
    )(data_c, data_t, wi_one, wi_two, query, log_q.reshape(-1, 128), cand_ids.reshape(-1, 128), targ_loc.reshape(1, n_tok))


WA_ROWS = 320
WB_ROWS = 128


ROWS_BLK = 512


def back_body(part_hbm, tok_hbm, raw_hbm, h_hbm, loss_in, dz_in, d_query, d_targ, w_one, w_two, targ_raw, cand_raw, wi_one, wi_two, rows_t, back_c, wa_full, wb_full, loss_out, *scratch):
    place = my_place()
    me, y, x, c = place
    rs_u, rs_a, rs_b = scratch[0:10], scratch[10:20], scratch[20:30]
    ac_send, ac_recv, aa_send, aa_recv, ab_send, ab_recv, l_send, l_recv, z_send, z_recv, h_sem, wa_data, wb_data, l_all, dz_all, d_part, tokens, raw_all, h_all, in_sem = scratch[30:50]
    width = d_query.shape[1]
    scale = SCORE_GAIN / math.sqrt(width)
    in_copies = [pltpu.make_async_copy(src, dst, in_sem.at[k]) for k, (src, dst) in enumerate([(part_hbm, d_part), (h_hbm.at[:, :, 0], h_all.at[:, :, c]), (tok_hbm, tokens), (raw_hbm, raw_all)])]
    for copy in in_copies:
        copy.start()
    meet(place)
    red_u = []
    for k in range(2):
        red_u.append(Reduce(place, d_part.at[:, :, :, pl.ds(k * PIECE, PIECE)], *[r.at[k] for r in rs_u]))
    red_a = Reduce(place, wa_data, *[r.at[0] for r in rs_a])
    red_b = Reduce(place, wb_data, *[r.at[0] for r in rs_b])
    ag_a = Gather(place, wa_full, aa_send, aa_recv)
    ag_b = Gather(place, wb_full, ab_send, ab_recv)
    ag_c = Gather(place, back_c, ac_send, ac_recv)
    in_copies[0].wait()
    red_u[0].one()
    red_u[1].one()
    l_all[me] = loss_in[...]
    dz_all[me] = dz_in[...]
    l_copies = []
    for k in range(1, 8):
        peer = peer_of(place, k // 4, (k // 2) % 2, k % 2)
        l_copies.append(push(loss_in, l_all.at[me], l_send.at[k], l_recv.at[k], peer))
        l_copies.append(push(dz_in, dz_all.at[me], z_send.at[k], z_recv.at[k], peer))
    in_copies[1].wait()
    h_copy = push(h_all.at[:, :, c], h_all.at[:, :, c], h_sem.at[0], h_sem.at[1], peer_of(place, 0, 0, 1))

    def rows_pass(first, last):
        per = rows_t.shape[3] // ROWS_BLK

        @pl.loop(first, last)
        def _(i):
            b = i // per
            by, bx, bc = b // 4, (b // 2) % 2, b % 2
            rows = pl.ds(pl.multiple_of((i % per) * ROWS_BLK, ROWS_BLK), ROWS_BLK)
            columns = []
            for k in range(ROWS_BLK // 128):
                line = dz_all[b, pl.ds((i % per) * (ROWS_BLK // 128) + k, 1), :]
                columns.append(jnp.broadcast_to(line, (128, 128)).T)
            column = jnp.concatenate(columns, axis=0)
            column = jnp.concatenate([column] * (width // 128), axis=1)
            grad = (scale * column * h_all[by, bx, bc, rows, :].astype(jnp.float32)).astype(jnp.bfloat16)
            q = tower_back(raw_all[by, bx, bc, rows, :], wi_one[...], wi_two[...], grad)[0]
            rows_t[by, bx, bc, rows, :] = by_transpose(q, wi_one[...]).astype(jnp.bfloat16)

    def put(data, first, value):
        n = value.shape[0] // 8
        for b in range(8):
            data[b // 4, (b // 2) % 2, b % 2, first : first + n, :] = value[b * n : (b + 1) * n, :]

    def own(red, full):
        first, second = red.last()
        half = first.shape[0]
        full[y, x, c, 0:half, :] = first
        full[y, x, c, half : 2 * half, :] = second

    t_q, t_hid = tower_back(targ_raw[...], wi_one[...], wi_two[...], d_targ[...])
    red_u[0].two()
    red_u[1].two()
    in_copies[2].wait()
    q_q, q_hid = tower_back(tokens[...], w_one[...], w_two[...], d_query[...])
    dw_one = over_rows(tokens[...], q_q)
    put(wa_data, 0, dw_one[:, :width])
    put(wa_data, 128, dw_one[:, width:])
    put(wa_data, 256, over_rows(q_hid, d_query[...]))
    red_a.one()
    red_u[0].three()
    red_u[1].three()
    red_a.two()
    in_copies[3].wait()
    for copy in l_copies:
        copy.wait()
    h_copy.wait()
    loss_out[...] = jnp.sum(l_all[...], axis=0)
    rows_pass(0, 5)
    parts = []
    for k in range(2):
        first, second = red_u[k].last()
        parts += [first, second]
    d_cand = (jnp.concatenate(parts, axis=0) * scale).astype(jnp.bfloat16)
    c_q, c_hid = tower_back(cand_raw[...], wi_one[...], wi_two[...], d_cand)
    back_c[y, x, c] = by_transpose(c_q, wi_one[...]).astype(jnp.bfloat16)
    ag_c.one()
    dwi_one = over_rows(targ_raw[...], t_q) + over_rows(cand_raw[...], c_q)
    put(wb_data, 0, dwi_one[:, :width])
    put(wb_data, 32, dwi_one[:, width:])
    put(wb_data, 64, over_rows(t_hid, d_targ[...]) + over_rows(c_hid, d_cand))
    red_b.one()
    red_a.three()
    red_b.two()
    ag_c.two()
    rows_pass(5, 7)
    own(red_a, wa_full)
    ag_a.one()
    red_b.three()
    rows_pass(7, 10)
    ag_a.two()
    own(red_b, wb_full)
    ag_b.one()
    ag_c.three()
    rows_pass(10, 12)
    ag_b.two()
    rows_pass(12, 16)
    ag_a.three()
    ag_b.three()
    for part in (ag_c, ag_a, ag_b):
        part.last()
    for part in red_u + [red_a, red_b, ag_c, ag_a, ag_b]:
        part.drain()


def back_rows(d_part, tokens, raw_all, h_part, loss_part, dz, d_query, d_targ, w_one, w_two, targ_raw, cand_raw, wi_one, wi_two):
    n_mine, width = d_part.shape[3:]
    vmem = pl.BlockSpec(memory_space=pltpu.VMEM)
    hbm = pl.BlockSpec(memory_space=pl.ANY)
    eight = pltpu.SemaphoreType.DMA((8,))
    scratch = reduce_scratch(2, PIECE, width, jnp.float32) + reduce_scratch(1, WA_ROWS, width, jnp.float32) + reduce_scratch(1, WB_ROWS, width, jnp.float32)
    scratch += gather_sems() + gather_sems() + gather_sems() + [eight] * 4 + [pltpu.SemaphoreType.DMA((2,))]
    scratch += [pltpu.VMEM((2, 2, 2, WA_ROWS, width), jnp.float32), pltpu.VMEM((2, 2, 2, WB_ROWS, width), jnp.float32), pltpu.VMEM((8, 8, 128), jnp.float32), pltpu.VMEM((8, 8, 128), jnp.float32)]
    scratch += [pltpu.VMEM(d_part.shape, jnp.float32), pltpu.VMEM(tokens.shape, jnp.bfloat16), pltpu.VMEM(raw_all.shape, jnp.bfloat16), pltpu.VMEM(raw_all.shape, jnp.bfloat16), pltpu.SemaphoreType.DMA((4,))]
    return pl.pallas_call(
        back_body,
        out_shape=(
            jax.ShapeDtypeStruct(raw_all.shape, jnp.bfloat16),
            jax.ShapeDtypeStruct((2, 2, 2, n_mine, width), jnp.bfloat16),
            jax.ShapeDtypeStruct((2, 2, 2, WA_ROWS, width), jnp.float32),
            jax.ShapeDtypeStruct((2, 2, 2, WB_ROWS, width), jnp.float32),
            jax.ShapeDtypeStruct((8, 128), jnp.float32),
        ),
        in_specs=[hbm] * 4 + [vmem] * 10,
        out_specs=(vmem,) * 5,
        scratch_shapes=scratch,
        compiler_params=pltpu.CompilerParams(vmem_limit_bytes=VMEM_LIMIT, collective_id=2, has_side_effects=True),
        name="back_rows",
    )(d_part, tokens, raw_all, h_part, loss_part, dz, d_query, d_targ, w_one, w_two, targ_raw, cand_raw, wi_one, wi_two)


def solution(mesh):
    num_dev = mesh.shape["dp"]

    def local_step(tokens, w_one, w_two, wi_one, wi_two, table_loc, cand_ids, log_q, targ_loc):
        rows_loc, width = table_loc.shape
        n_cand = cand_ids.shape[0]
        n_tok = tokens.shape[0]
        tok_total = n_tok * num_dev
        ids_two, query = prepare(targ_loc, cand_ids, tokens, w_one, w_two, rows_loc)
        data_c, data_t = pick_rows(ids_two, table_loc, n_cand)
        data_c = data_c.reshape(2, 2, 2, n_cand // 8, width)
        data_t = data_t.reshape(2, 2, 2, n_tok, width)
        cand_raw, targ_raw, loss_part, d_query, d_targ, d_part, dz, h_part = score(tok_total, data_c, data_t, wi_one, wi_two, query, log_q, cand_ids, targ_loc)
        rows_t, back_c, wa, wb, loss = back_rows(d_part.reshape(2, 2, 2, n_cand // 8, width), tokens, data_t, h_part, loss_part, dz, d_query, d_targ, w_one, w_two, targ_raw, cand_raw, wi_one, wi_two)
        d_table, dw_one, dw_two, dwi_one, dwi_two = scatter_rows(ids_two, back_c.reshape(-1, width), rows_t.reshape(-1, width), wa.reshape(8, WA_ROWS, width), wb.reshape(8, WB_ROWS, width), rows_loc, tokens.shape[1])
        return loss[0, 0] / tok_total, d_table, dw_one, dw_two, dwi_one, dwi_two

    return jax.shard_map(local_step, mesh=mesh, in_specs=(P("dp", None), P(), P(), P(), P(), P("dp", None), P(), P(), P("dp")), out_specs=(P(), P("dp", None), P(), P(), P(), P()), check_vma=False)
```

```python
import functools
import math
import jax
import jax.numpy as jnp
from jax import lax
from jax.experimental import pallas as pl
from jax.experimental.pallas import tpu as pltpu
from jax.sharding import PartitionSpec as P

SCORE_GAIN = 3.0
HIT_VALUE = -1e9


def tower_fwd(row_block, w_in, w_out):
    pre_act = jnp.dot(row_block, w_in, preferred_element_type=jnp.float32)
    hidden = jax.nn.gelu(pre_act).astype(jnp.bfloat16)
    tower_out = jnp.dot(hidden, w_out, preferred_element_type=jnp.float32).astype(jnp.bfloat16)
    return tower_out


def over_rows(a, b):
    return lax.dot_general(a, b, (((0,), (0,)), ((), ())), preferred_element_type=jnp.float32)


def by_transpose(a, b):
    return lax.dot_general(a, b, (((1,), (1,)), ((), ())), preferred_element_type=jnp.float32)


def tower_back(row_block, w_in, w_out, grad_out):
    pre_act = jnp.dot(row_block, w_in, preferred_element_type=jnp.float32)
    hidden, gelu_back = jax.vjp(jax.nn.gelu, pre_act)
    grad_hidden = by_transpose(grad_out, w_out)
    return gelu_back(grad_hidden)[0].astype(jnp.bfloat16), hidden.astype(jnp.bfloat16)


VMEM_LIMIT = 63 * 1024 * 1024
BATCH = 128
SPARE = 256
GROUP = 16
STAGE_ROWS = 2048
OUT_ROWS = 1024
IN_SLOTS = 12
OUT_SLOTS = 8


def pick_body(ids_s, table, cand_hbm, targ_hbm, wide, stage, rows_f, cand_out, targ_out, stage_sem, out_sem):
    rows_loc, width = table.shape
    lane = width // 2
    n_stage = rows_loc // STAGE_ROWS

    def stage_copy(i, slot):
        return pltpu.make_async_copy(table.at[pl.ds(i * STAGE_ROWS, STAGE_ROWS)], stage.at[slot], stage_sem.at[slot])

    for i in range(IN_SLOTS - 1):
        stage_copy(i, i).start()
    wide[pl.ds(2 * rows_loc, 2 * SPARE), :] = jnp.zeros((2 * SPARE, lane), jnp.float32)

    @pl.loop(0, n_stage)
    def _(i):
        slot = i % IN_SLOTS

        @pl.when(i + IN_SLOTS - 1 < n_stage)
        def _():
            stage_copy(i + IN_SLOTS - 1, (i + IN_SLOTS - 1) % IN_SLOTS).start()

        stage_copy(i, slot).wait()

        @pl.loop(0, STAGE_ROWS // 128)
        def _(j):
            block = stage[slot, pl.ds(pl.multiple_of(j * 128, 128), 128), :].astype(jnp.float32)
            base = pl.multiple_of((i * STAGE_ROWS + j * 128) * 2, 256)
            wide[pl.ds(base, 128, 2), :] = block[:, :lane]
            wide[pl.ds(base + 1, 128, 2), :] = block[:, lane:]

    copies = []

    def fill(out, hbm, first, count, ids_row):
        @pl.loop(0, count // BATCH)
        def _(b):
            for r in range(BATCH):
                at = pl.multiple_of(ids_s[ids_row + b, r], 2)
                rows_f[pl.ds(2 * r, 2), :] = wide[pl.ds(at, 2), :]
            rows = pl.ds(pl.multiple_of(first + b * BATCH, BATCH), BATCH)
            out[rows, :lane] = rows_f[pl.ds(0, BATCH, 2), :].astype(jnp.bfloat16)
            out[rows, lane:] = rows_f[pl.ds(1, BATCH, 2), :].astype(jnp.bfloat16)

        copy = pltpu.make_async_copy(out.at[pl.ds(first, count)], hbm.at[pl.ds(first, count)], out_sem.at[len(copies)])
        copy.start()
        copies.append(copy)

    n_cand = cand_out.shape[0]
    part = targ_out.shape[0] // 4
    fill(cand_out, cand_hbm, 0, n_cand, 0)
    for k in range(4):
        fill(targ_out, targ_hbm, k * part, part, (n_cand + k * part) // BATCH)
    for copy in copies:
        copy.wait()


def pick_rows(ids_two, table_loc, n_cand):
    rows_loc, width = table_loc.shape
    n_targ = ids_two.size - n_cand
    hbm = pl.BlockSpec(memory_space=pl.ANY)
    return pl.pallas_call(
        pick_body,
        out_shape=(jax.ShapeDtypeStruct((n_cand, width), jnp.bfloat16), jax.ShapeDtypeStruct((n_targ, width), jnp.bfloat16)),
        in_specs=[pl.BlockSpec(memory_space=pltpu.SMEM), hbm],
        out_specs=(hbm, hbm),
        scratch_shapes=[
            pltpu.VMEM((2 * (rows_loc + SPARE), width // 2), jnp.float32),
            pltpu.VMEM((IN_SLOTS, STAGE_ROWS, width), jnp.bfloat16),
            pltpu.VMEM((2 * BATCH, width // 2), jnp.float32),
            pltpu.VMEM((n_cand, width), jnp.bfloat16),
            pltpu.VMEM((n_targ, width), jnp.bfloat16),
            pltpu.SemaphoreType.DMA((IN_SLOTS,)),
            pltpu.SemaphoreType.DMA((5,)),
        ],
        compiler_params=pltpu.CompilerParams(vmem_limit_bytes=VMEM_LIMIT),
        name="pick_rows",
    )(ids_two, table_loc)


def scatter_body(tok_total, ids_s, ids_v, loss_s, cand_hbm, targ_hbm, wa_hbm, wb_hbm, out_ref, dw_one, dw_two, dwi_one, dwi_two, loss_out, acc, g2, cand_ref, targ_ref, wa, wb, flag_v, flag_s, out_stage, sem, in_sem, flag_sem, w_sem):
    rows, width = out_ref.shape
    lane = width // 2
    n_cand = cand_ref.shape[0]
    loss_out[0, 0] = loss_s[0, 0] * (1.0 / tok_total)
    n_all = n_cand + targ_ref.shape[0]
    in_copies = [pltpu.make_async_copy(src, dst, in_sem.at[k]) for k, (src, dst) in enumerate([(cand_hbm, cand_ref), (targ_hbm, targ_ref), (wa_hbm, wa), (wb_hbm, wb)])]
    for copy in in_copies:
        copy.start()

    ids = ids_v[...]
    place = lax.broadcasted_iota(jnp.int32, ids.shape, 1) % GROUP
    twice = jnp.zeros(ids.shape, jnp.int32)
    for k in range(1, GROUP):
        twice = jnp.where((ids == pltpu.roll(ids, k, 1)) & (place >= k), 1, twice)
    flag_v[...] = jnp.broadcast_to(jnp.max(twice, axis=1, keepdims=True), ids.shape)
    flag_copy = pltpu.make_async_copy(flag_v, flag_s, flag_sem)
    flag_copy.start()

    @pl.loop(0, 2 * rows // 512)
    def _(i):
        acc[pl.ds(pl.multiple_of(i * 512, 512), 512), :] = jnp.zeros((512, lane), jnp.float32)

    def one_batch(b, src, src_base):
        rows_b = pl.ds(pl.multiple_of(b * BATCH - src_base, BATCH), BATCH)
        repeated = flag_s[b, 0]

        @pl.when(repeated == 0)
        def _():
            part = src[rows_b, :].astype(jnp.float32)
            g2[pl.ds(0, BATCH, 2), :] = part[:, :lane]
            g2[pl.ds(1, BATCH, 2), :] = part[:, lane:]

        @pl.when(repeated != 0)
        def _():
            row_i = lax.broadcasted_iota(jnp.int32, (BATCH, BATCH), 0) // GROUP
            col_i = lax.broadcasted_iota(jnp.int32, (BATCH, BATCH), 1) // GROUP
            idr = jnp.broadcast_to(ids_v[pl.ds(b, 1), :], (BATCH, BATCH))
            same = jnp.where((idr == idr.T) & (row_i == col_i), 1.0, 0.0).astype(jnp.bfloat16)
            part = jnp.dot(same, src[rows_b, :], preferred_element_type=jnp.float32)
            g2[pl.ds(0, BATCH, 2), :] = part[:, :lane]
            g2[pl.ds(1, BATCH, 2), :] = part[:, lane:]

        for g in range(BATCH // GROUP):
            at = [pl.multiple_of(ids_s[b, g * GROUP + r], 2) for r in range(GROUP)]
            new = [acc[pl.ds(at[r], 2), :] + g2[pl.ds(2 * (g * GROUP + r), 2), :] for r in range(GROUP)]
            for r in range(GROUP):
                acc[pl.ds(at[r], 2), :] = new[r]

    for copy in in_copies:
        copy.wait()
    w_copies = []

    def place_block(src, dst):
        copy = pltpu.make_async_copy(src, dst, w_sem)
        copy.start()
        w_copies.append(copy)

    for b in range(8):
        place_block(wa.at[b, pl.ds(0, 128)], dw_one.at[pl.ds(b * 128, 128), pl.ds(0, width)])
        place_block(wa.at[b, pl.ds(128, 128)], dw_one.at[pl.ds(b * 128, 128), pl.ds(width, width)])
        place_block(wa.at[b, pl.ds(256, 64)], dw_two.at[pl.ds(b * 64, 64)])
        place_block(wb.at[b, pl.ds(0, 32)], dwi_one.at[pl.ds(b * 32, 32), pl.ds(0, width)])
        place_block(wb.at[b, pl.ds(32, 32)], dwi_one.at[pl.ds(b * 32, 32), pl.ds(width, width)])
        place_block(wb.at[b, pl.ds(64, 64)], dwi_two.at[pl.ds(b * 64, 64)])
    flag_copy.wait()

    @pl.loop(0, n_cand // BATCH)
    def _(b):
        one_batch(b, cand_ref, 0)

    @pl.loop(n_cand // BATCH, n_all // BATCH)
    def _(b):
        one_batch(b, targ_ref, n_cand)

    n_out = rows // OUT_ROWS

    def out_copy(i, slot):
        return pltpu.make_async_copy(out_stage.at[slot], out_ref.at[pl.ds(i * OUT_ROWS, OUT_ROWS)], sem.at[slot])

    @pl.loop(0, n_out)
    def _(i):
        slot = i % OUT_SLOTS

        @pl.when(i >= OUT_SLOTS)
        def _():
            out_copy(i - OUT_SLOTS, slot).wait()

        @pl.loop(0, OUT_ROWS // 128)
        def _(j):
            base = pl.multiple_of((i * OUT_ROWS + j * 128) * 2, 256)
            here = pl.ds(pl.multiple_of(j * 128, 128), 128)
            out_stage[slot, here, :lane] = acc[pl.ds(base, 128, 2), :]
            out_stage[slot, here, lane:] = acc[pl.ds(base + 1, 128, 2), :]

        out_copy(i, slot).start()

    for i in range(n_out - OUT_SLOTS, n_out):
        out_copy(i, i % OUT_SLOTS).wait()
    for copy in w_copies:
        copy.wait()


def scatter_rows(tok_total, ids_two, loss, back_cand, back_targ, wa, wb, rows_loc, din):
    width = back_cand.shape[1]
    n_batch = ids_two.shape[0]
    vmem = pl.BlockSpec(memory_space=pltpu.VMEM)
    hbm = pl.BlockSpec(memory_space=pl.ANY)
    smem = pl.BlockSpec(memory_space=pltpu.SMEM)
    shapes = [(rows_loc, width), (din, 2 * width), (2 * width, width), (width, 2 * width), (2 * width, width), (1, 1)]
    return pl.pallas_call(
        functools.partial(scatter_body, tok_total),
        out_shape=tuple(jax.ShapeDtypeStruct(shape, jnp.float32) for shape in shapes),
        in_specs=[smem, vmem, smem] + [hbm] * 4,
        out_specs=(hbm,) * 5 + (smem,),
        scratch_shapes=[
            pltpu.VMEM((2 * (rows_loc + SPARE), width // 2), jnp.float32),
            pltpu.VMEM((2 * BATCH, width // 2), jnp.float32),
            pltpu.VMEM(back_cand.shape, jnp.bfloat16),
            pltpu.VMEM(back_targ.shape, jnp.bfloat16),
            pltpu.VMEM(wa.shape, jnp.float32),
            pltpu.VMEM(wb.shape, jnp.float32),
            pltpu.VMEM((n_batch, BATCH), jnp.int32),
            pltpu.SMEM((n_batch, BATCH), jnp.int32),
            pltpu.VMEM((OUT_SLOTS, OUT_ROWS, width), jnp.float32),
            pltpu.SemaphoreType.DMA((OUT_SLOTS,)),
            pltpu.SemaphoreType.DMA((4,)),
            pltpu.SemaphoreType.DMA,
            pltpu.SemaphoreType.DMA,
        ],
        compiler_params=pltpu.CompilerParams(vmem_limit_bytes=VMEM_LIMIT),
        cost_estimate=pl.CostEstimate(flops=60_000_000_000, bytes_accessed=40 << 20, transcendentals=0),
        name="scatter_rows",
    )(ids_two, ids_two, loss, back_cand, back_targ, wa, wb)


CHUNK = 512
SUB = 128
COLS = 256


def logits_pass(u_at, n_cand, h, lq_ref, cid_ref, tid, z_a, z_b, e_s, m_s, s_s, between):
    n_tok, width = h.shape
    scale = SCORE_GAIN / math.sqrt(width)
    ht = h.T
    n_chunk = n_cand // CHUNK

    def multiply(i, z_ref):
        z_ref[...] = jnp.dot(u_at(jnp.minimum(i, n_chunk - 1)), ht, preferred_element_type=jnp.float32)

    def absorb(i, z_ref):
        off = pl.multiple_of(i * CHUNK, CHUNK)
        for col in range(0, n_tok, COLS):
            cols = slice(col, col + COLS)
            m8 = m_s[0, :, cols]
            s8 = s_s[:, cols]
            for k in range(CHUNK // SUB):
                rows = pl.ds(pl.multiple_of(off + k * SUB, SUB), SUB)
                lq = jnp.concatenate([lq_ref[rows, :]] * (COLS // 128), axis=1)
                cid = jnp.concatenate([cid_ref[rows, :]] * (COLS // 128), axis=1)
                z = z_ref[k * SUB : (k + 1) * SUB, cols] * scale - lq
                z = jnp.where(cid == tid[:, cols], HIT_VALUE, z).reshape(SUB // 8, 8, COLS)
                m_new = jnp.maximum(m8, jnp.max(z, axis=0))
                e = jnp.exp(z - m_new[None])
                s8 = s8 * jnp.exp(m8 - m_new) + jnp.sum(e, axis=0)
                m8 = m_new
                e_s[rows, cols] = e.reshape(SUB, COLS)
                m_s[1 + i * (CHUNK // SUB) + k, :, cols] = m8
            m_s[0, :, cols] = m8
            s_s[:, cols] = s8

    m_s[0] = jnp.full((8, n_tok), jnp.finfo(jnp.float32).min, jnp.float32)
    s_s[...] = jnp.zeros_like(s_s)
    multiply(0, z_a)

    def two_chunks(i):
        multiply(2 * i + 1, z_b)
        absorb(2 * i, z_a)
        multiply(2 * i + 2, z_a)
        absorb(2 * i + 1, z_b)

    pl.loop(0, n_chunk // 4)(two_chunks)
    between()
    pl.loop(n_chunk // 4, n_chunk // 2)(two_chunks)


def loss_pass(tok_total, u_at, ut_s, h, v, e_s, m_s, s_s, fac_s, dz_a, dz_b, dht_s, loss_ref, dh_ref, dv_ref, du_ref, dz_ref):
    n_cand, width = du_ref.shape
    n_tok = h.shape[0]
    scale = SCORE_GAIN / math.sqrt(width)
    n_chunk = n_cand // CHUNK
    hf = h.astype(jnp.float32)
    vf = v.astype(jnp.float32)
    zt = jnp.sum(hf * vf, axis=1, keepdims=True) * scale
    zt = jnp.broadcast_to(zt, (n_tok, 128)).T[0:1, :]
    m8 = m_s[0]
    m = jnp.maximum(zt, jnp.max(m8, axis=0, keepdims=True))
    et = jnp.exp(zt - m)
    den = et + jnp.sum(s_s[...] * jnp.exp(m8 - m), axis=0, keepdims=True)
    part = jnp.sum(jnp.log(den) + m - zt, axis=1, keepdims=True)
    loss_ref[...] = jnp.broadcast_to(part, loss_ref.shape)
    dzt = ((et / den - 1.0) / tok_total).astype(jnp.bfloat16).astype(jnp.float32)
    inv = 1.0 / den / tok_total
    fac_s[0:8, :] = jnp.broadcast_to(m, (8, n_tok))
    fac_s[8:16, :] = jnp.broadcast_to(inv, (8, n_tok))
    for i in range(n_chunk):
        ut_s[:, i * CHUNK : (i + 1) * CHUNK] = u_at(i).T
    for i in range(8):
        dz_ref[i : i + 1, :] = dzt[:, i * 128 : (i + 1) * 128]

    def gradient(i, out):
        i = jnp.minimum(i, n_chunk - 1)
        off = pl.multiple_of(i * CHUNK, CHUNK)
        for col in range(0, n_tok, COLS):
            cols = slice(col, col + COLS)
            for k in range(CHUNK // SUB):
                rows = pl.ds(pl.multiple_of(off + k * SUB, SUB), SUB)
                fac = jnp.exp(m_s[1 + i * (CHUNK // SUB) + k, :, cols] - fac_s[0:8, cols]) * fac_s[8:16, cols]
                out[k * SUB : (k + 1) * SUB, cols] = (e_s[rows, cols].reshape(SUB // 8, 8, COLS) * fac[None]).reshape(SUB, COLS).astype(jnp.bfloat16)

    def spread(i, dz_c):
        off = pl.multiple_of(i * CHUNK, CHUNK)
        du_ref[pl.ds(off, CHUNK), :] = jnp.dot(dz_c[...], h, preferred_element_type=jnp.float32)
        dht_s[...] += jnp.dot(ut_s[:, pl.ds(off, CHUNK)], dz_c[...], preferred_element_type=jnp.float32)

    dht_s[...] = jnp.zeros_like(dht_s)
    gradient(0, dz_a)

    @pl.loop(0, n_chunk // 2)
    def _(i):
        gradient(2 * i + 1, dz_b)
        spread(2 * i, dz_a)
        gradient(2 * i + 2, dz_a)
        spread(2 * i + 1, dz_b)

    dzt_c = jnp.broadcast_to(dzt, (128, n_tok)).T[:, 0:1]
    dh_ref[...] = ((dzt_c * vf + dht_s[...].T) * scale).astype(jnp.bfloat16)
    dv_ref[...] = (scale * dzt_c * hf).astype(jnp.bfloat16)


def softmax_scratch(n_cand, n_tok, width):
    return [
        pltpu.VMEM((CHUNK, n_tok), jnp.float32),
        pltpu.VMEM((CHUNK, n_tok), jnp.float32),
        pltpu.VMEM((n_cand, n_tok), jnp.float32),
        pltpu.VMEM((1 + n_cand // SUB, 8, n_tok), jnp.float32),
        pltpu.VMEM((8, n_tok), jnp.float32),
        pltpu.VMEM((width, n_cand), jnp.bfloat16),
        pltpu.VMEM((16, n_tok), jnp.float32),
        pltpu.VMEM((CHUNK, n_tok), jnp.bfloat16),
        pltpu.VMEM((CHUNK, n_tok), jnp.bfloat16),
        pltpu.VMEM((width, n_tok), jnp.float32),
    ]


MESH = pl.DeviceIdType.MESH


def my_place():
    me = lax.axis_index("dp")
    return me, me // 4, (me // 2) % 2, me % 2


def peer_of(place, dy, dx, dc):
    me, y, x, c = place
    return me + dy * (4 - 8 * y) + dx * (2 - 4 * x) + dc * (1 - 2 * c)


def greet(place):
    barrier = pltpu.get_barrier_semaphore()
    for k in range(1, 8):
        pl.semaphore_signal(barrier, inc=1, device_id=(peer_of(place, k // 4, (k // 2) % 2, k % 2),), device_id_type=MESH)


def meet(place):
    greet(place)
    pl.semaphore_wait(pltpu.get_barrier_semaphore(), 7)


def push(src, dst, send_sem, recv_sem, peer):
    copy = pltpu.make_async_remote_copy(src_ref=src, dst_ref=dst, send_sem=send_sem, recv_sem=recv_sem, device_id=(peer,), device_id_type=MESH)
    copy.start()
    return copy


class Reduce:
    def __init__(self, place, data, in_one, mid, in_xa, in_yb, part_a, part_b, in_ya, in_xb, send_sem, recv_sem):
        self.place, self.data = place, data
        self.in_one, self.mid, self.in_xa, self.in_yb = in_one, mid, in_xa, in_yb
        self.part_a, self.part_b, self.in_ya, self.in_xb = part_a, part_b, in_ya, in_xb
        self.send_sem, self.recv_sem = send_sem, recv_sem
        self.half = data.shape[3] // 2
        self.copies = []

    def push(self, k, src, dst, dy, dx, dc):
        copy = push(src, dst, self.send_sem.at[k], self.recv_sem.at[k], peer_of(self.place, dy, dx, dc))
        self.copies.append(copy)

    def one(self):
        c = self.place[3]
        self.push(0, self.data.at[:, :, 1 - c], self.in_one, 0, 0, 1)

    def two(self):
        _, y, x, c = self.place
        half = self.half
        self.copies[0].wait_recv()
        for i in range(2):
            for j in range(2):
                self.mid[i, j] = self.data[i, j, c] + self.in_one[i, j]
        self.push(1, self.mid.at[:, 1 - x, pl.ds(0, half)], self.in_xa, 0, 1, 0)
        self.push(2, self.mid.at[1 - y, :, pl.ds(half, half)], self.in_yb, 1, 0, 0)

    def three(self):
        _, y, x, c = self.place
        half = self.half
        self.copies[1].wait_recv()
        for i in range(2):
            self.part_a[i] = self.mid[i, x, 0:half] + self.in_xa[i]
        self.push(3, self.part_a.at[1 - y], self.in_ya, 1, 0, 0)
        self.copies[2].wait_recv()
        for i in range(2):
            self.part_b[i] = self.mid[y, i, half : 2 * half] + self.in_yb[i]
        self.push(4, self.part_b.at[1 - x], self.in_xb, 0, 1, 0)

    def last(self):
        _, y, x, c = self.place
        self.copies[3].wait_recv()
        first = self.part_a[y] + self.in_ya[...]
        self.copies[4].wait_recv()
        return first, self.part_b[x] + self.in_xb[...]

    def drain(self):
        for copy in self.copies:
            copy.wait_send()


def reduce_scratch(n, rows, width, dtype):
    half = rows // 2
    return [
        pltpu.VMEM((n, 2, 2, rows, width), dtype),
        pltpu.VMEM((n, 2, 2, rows, width), dtype),
        pltpu.VMEM((n, 2, half, width), dtype),
        pltpu.VMEM((n, 2, half, width), dtype),
        pltpu.VMEM((n, 2, half, width), dtype),
        pltpu.VMEM((n, 2, half, width), dtype),
        pltpu.VMEM((n, half, width), dtype),
        pltpu.VMEM((n, half, width), dtype),
        pltpu.SemaphoreType.DMA((n, 5)),
        pltpu.SemaphoreType.DMA((n, 5)),
    ]


class Gather:
    def __init__(self, place, full, send_sem, recv_sem):
        self.place, self.full = place, full
        self.send_sem, self.recv_sem = send_sem, recv_sem
        self.half = full.shape[3] // 2
        self.copies = []

    def push(self, k, ref, dy, dx, dc):
        copy = push(ref, ref, self.send_sem.at[k], self.recv_sem.at[k], peer_of(self.place, dy, dx, dc))
        self.copies.append(copy)

    def one(self):
        _, y, x, c = self.place
        half = self.half
        self.push(0, self.full.at[y, x, c, pl.ds(0, half)], 0, 1, 0)
        self.push(1, self.full.at[y, x, c, pl.ds(half, half)], 1, 0, 0)

    def two(self):
        _, y, x, c = self.place
        half = self.half
        self.copies[0].wait_recv()
        self.push(2, self.full.at[y, :, c, pl.ds(0, half)], 1, 0, 0)
        self.copies[1].wait_recv()
        self.push(3, self.full.at[:, x, c, pl.ds(half, half)], 0, 1, 0)

    def three(self):
        c = self.place[3]
        self.copies[2].wait_recv()
        self.copies[3].wait_recv()
        self.push(4, self.full.at[:, :, c], 0, 0, 1)

    def last(self):
        self.copies[4].wait_recv()

    def drain(self):
        for copy in self.copies:
            copy.wait_send()


def gather_sems():
    return [pltpu.SemaphoreType.DMA((5,)), pltpu.SemaphoreType.DMA((5,))]


def prepare_body(rows_loc, mine, cand_ids, tokens, w_one, w_two, ids_two, query, full, send_sem, recv_sem):
    place = my_place()
    me = place[0]
    greet(place)
    half = tokens.shape[0] // 2
    query[0:half, :] = tower_fwd(tokens[0:half, :], w_one[...], w_two[...])
    pl.semaphore_wait(pltpu.get_barrier_semaphore(), 7)
    full[me] = mine[...]
    copies = []
    for k in range(1, 8):
        copies.append(push(mine, full.at[me], send_sem.at[k], recv_sem.at[k], peer_of(place, k // 4, (k // 2) % 2, k % 2)))

    def owned(ids):
        local = ids - me * rows_loc
        spare = rows_loc + (lax.broadcasted_iota(jnp.int32, ids.shape, 0) % 2) * 128 + lax.broadcasted_iota(jnp.int32, ids.shape, 1)
        return 2 * jnp.where((local >= 0) & (local < rows_loc), local, spare)

    n_c = cand_ids.shape[0]
    ids_two[0:n_c, :] = owned(cand_ids[...])
    query[half : 2 * half, :] = tower_fwd(tokens[half : 2 * half, :], w_one[...], w_two[...])
    for copy in copies:
        copy.wait()
    ids_two[n_c : n_c + 64, :] = owned(full[...].reshape(64, 128))


def prepare(targ_loc, cand_ids, tokens, w_one, w_two, rows_loc):
    n_tok = tokens.shape[0]
    n_c = cand_ids.shape[0] // 128
    vmem = pl.BlockSpec(memory_space=pltpu.VMEM)
    return pl.pallas_call(
        functools.partial(prepare_body, rows_loc),
        out_shape=(jax.ShapeDtypeStruct((n_c + 64, 128), jnp.int32), jax.ShapeDtypeStruct((n_tok, w_two.shape[1]), jnp.bfloat16)),
        in_specs=[vmem] * 5,
        out_specs=(vmem,) * 2,
        scratch_shapes=[pltpu.VMEM((8, 8, 128), jnp.int32), pltpu.SemaphoreType.DMA((8,)), pltpu.SemaphoreType.DMA((8,))],
        compiler_params=pltpu.CompilerParams(vmem_limit_bytes=VMEM_LIMIT, collective_id=0, has_side_effects=True),
        name="prepare",
    )(targ_loc.reshape(8, 128), cand_ids.reshape(n_c, 128), tokens, w_one, w_two)


PIECE = 256


def score_body(tok_total, c_hbm, t_hbm, wi_one, wi_two, h_ref, lq_ref, cid_ref, tid_ref, cand_raw, targ_raw, loss_ref, dh_ref, dv_ref, du_ref, dz_ref, h_part, *scratch):
    place = my_place()
    me, y, x, c = place
    half = PIECE // 2
    data_c, data_t, in_sem, cand_vec, lq_b, cid_b, rs, ag_send, ag_recv = scratch[0:6] + (scratch[6:16],) + scratch[16:18]
    z_a, z_b, e_s, m_s, s_s, ut_s, fac_s, dz_a, dz_b, dht_s, h_send, h_recv = scratch[18:30]
    n_cand, width = du_ref.shape
    in_copies = [pltpu.make_async_copy(c_hbm, data_c, in_sem.at[0]), pltpu.make_async_copy(t_hbm, data_t, in_sem.at[1])]
    for copy in in_copies:
        copy.start()
    meet(place)
    reduces = []
    for k in range(6):
        data = data_c.at[:, :, :, pl.ds(k * PIECE, PIECE)] if k < 2 else data_t.at[:, :, :, pl.ds((k - 2) * PIECE, PIECE)]
        reduces.append(Reduce(place, data, *[r.at[k] for r in rs]))
    ag = Gather(place, cand_vec, ag_send, ag_recv)
    ag_h = Gather((me, y, x, 0), h_part, h_send, h_recv)
    h_part[y, x, 0] = h_ref[...]

    def close(k, out, base):
        first, second = reduces[k].last()
        out[base : base + half, :] = first
        out[base + half : base + PIECE, :] = second

    in_copies[0].wait()
    reduces[0].one()
    reduces[1].one()
    in_copies[1].wait()
    for k in range(2, 6):
        reduces[k].one()
    reduces[0].two()
    reduces[1].two()
    reduces[2].two()
    reduces[0].three()
    reduces[1].three()
    reduces[3].two()

    @pl.loop(0, n_cand // 128)
    def _(i):
        rows = pl.ds(pl.multiple_of(i * 128, 128), 128)
        lq_b[rows, :] = jnp.broadcast_to(lq_ref[pl.ds(i, 1), :], (128, 128)).T
        cid_b[rows, :] = jnp.broadcast_to(cid_ref[pl.ds(i, 1), :], (128, 128)).T

    close(0, cand_raw, 0)
    close(1, cand_raw, PIECE)
    cand_vec[y, x, c] = tower_fwd(cand_raw[...], wi_one[...], wi_two[...])
    ag.one()
    reduces[4].two()
    reduces[5].two()
    reduces[2].three()
    ag.two()
    ag_h.one()
    reduces[3].three()
    reduces[4].three()
    ag.three()
    reduces[5].three()
    ag.last()

    def u_at(i):
        return cand_vec[i // 4, (i // 2) % 2, i % 2]

    h = h_ref[...]
    logits_pass(u_at, n_cand, h, lq_b, cid_b, tid_ref[...], z_a, z_b, e_s, m_s, s_s, ag_h.two)
    for k in range(4):
        close(k + 2, targ_raw, k * PIECE)
    v = tower_fwd(targ_raw[...], wi_one[...], wi_two[...])
    loss_pass(tok_total, u_at, ut_s, h, v, e_s, m_s, s_s, fac_s, dz_a, dz_b, dht_s, loss_ref, dh_ref, dv_ref, du_ref, dz_ref)
    ag_h.copies[2].wait_recv()
    ag_h.copies[3].wait_recv()
    for red in reduces:
        red.drain()
    ag.drain()
    ag_h.drain()


def score(tok_total, data_c, data_t, wi_one, wi_two, query, log_q, cand_ids, targ_loc):
    n_mine, width = data_c.shape[3:]
    n_tok = data_t.shape[3]
    n_cand = 8 * n_mine
    vmem = pl.BlockSpec(memory_space=pltpu.VMEM)
    hbm = pl.BlockSpec(memory_space=pl.ANY)
    scratch = [pltpu.VMEM(data_c.shape, jnp.bfloat16), pltpu.VMEM(data_t.shape, jnp.bfloat16), pltpu.SemaphoreType.DMA((2,))]
    scratch += [pltpu.VMEM(data_c.shape, jnp.bfloat16), pltpu.VMEM((n_cand, 128), jnp.float32), pltpu.VMEM((n_cand, 128), jnp.int32)]
    scratch += reduce_scratch(6, PIECE, width, jnp.bfloat16) + gather_sems() + softmax_scratch(n_cand, n_tok, width)
    scratch += gather_sems()
    rows = [jax.ShapeDtypeStruct((n, width), jnp.bfloat16) for n in (n_mine, n_tok, n_tok, n_tok)]
    return pl.pallas_call(
        functools.partial(score_body, tok_total),
        out_shape=(rows[0], rows[1], jax.ShapeDtypeStruct((8, 128), jnp.float32), rows[2], rows[3], jax.ShapeDtypeStruct((n_cand, width), jnp.float32), jax.ShapeDtypeStruct((8, 128), jnp.float32), jax.ShapeDtypeStruct((2, 2, 1, n_tok, width), jnp.bfloat16)),
        in_specs=[hbm, hbm] + [vmem] * 6,
        out_specs=(vmem,) * 8,
        scratch_shapes=scratch,
        compiler_params=pltpu.CompilerParams(vmem_limit_bytes=VMEM_LIMIT, collective_id=1, has_side_effects=True),
        name="score",
    )(data_c, data_t, wi_one, wi_two, query, log_q.reshape(-1, 128), cand_ids.reshape(-1, 128), targ_loc.reshape(1, n_tok))


WA_ROWS = 320
WB_ROWS = 128


ROWS_BLK = 512


def back_body(part_hbm, tok_hbm, raw_hbm, h_hbm, loss_in, dz_in, d_query, d_targ, w_one, w_two, targ_raw, cand_raw, wi_one, wi_two, rows_out, cand_out, wa_out, wb_out, loss_out, *scratch):
    place = my_place()
    me, y, x, c = place
    rs_u, rs_a, rs_b = scratch[0:10], scratch[10:20], scratch[20:30]
    ac_send, ac_recv, aa_send, aa_recv, ab_send, ab_recv, l_send, l_recv, z_send, z_recv, h_sem, wa_data, wb_data, l_all, dz_all, d_part, tokens, raw_all, h_all, in_sem, rows_t, back_c, wa_full, wb_full, rows_sem, out_sem = scratch[30:56]
    width = d_query.shape[1]
    scale = SCORE_GAIN / math.sqrt(width)
    in_copies = [pltpu.make_async_copy(src, dst, in_sem.at[k]) for k, (src, dst) in enumerate([(part_hbm, d_part), (h_hbm.at[:, :, 0], h_all.at[:, :, c]), (tok_hbm, tokens), (raw_hbm, raw_all)])]
    for copy in in_copies:
        copy.start()
    meet(place)
    red_u = []
    for k in range(2):
        red_u.append(Reduce(place, d_part.at[:, :, :, pl.ds(k * PIECE, PIECE)], *[r.at[k] for r in rs_u]))
    red_a = Reduce(place, wa_data, *[r.at[0] for r in rs_a])
    red_b = Reduce(place, wb_data, *[r.at[0] for r in rs_b])
    ag_a = Gather(place, wa_full, aa_send, aa_recv)
    ag_b = Gather(place, wb_full, ab_send, ab_recv)
    ag_c = Gather(place, back_c, ac_send, ac_recv)
    in_copies[0].wait()
    red_u[0].one()
    red_u[1].one()
    l_all[me] = loss_in[...]
    dz_all[me] = dz_in[...]
    l_copies = []
    for k in range(1, 8):
        peer = peer_of(place, k // 4, (k // 2) % 2, k % 2)
        l_copies.append(push(loss_in, l_all.at[me], l_send.at[k], l_recv.at[k], peer))
        l_copies.append(push(dz_in, dz_all.at[me], z_send.at[k], z_recv.at[k], peer))
    in_copies[1].wait()
    h_copy = push(h_all.at[:, :, c], h_all.at[:, :, c], h_sem.at[0], h_sem.at[1], peer_of(place, 0, 0, 1))

    per = rows_t.shape[3] // ROWS_BLK

    def rows_copy(i):
        b = i // per
        here = (b // 4, (b // 2) % 2, b % 2, pl.ds(pl.multiple_of((i % per) * ROWS_BLK, ROWS_BLK), ROWS_BLK))
        return pltpu.make_async_copy(rows_t.at[here], rows_out.at[here], rows_sem.at[i])

    def rows_pass(first, last):

        @pl.loop(first, last)
        def _(i):
            b = i // per
            by, bx, bc = b // 4, (b // 2) % 2, b % 2
            rows = pl.ds(pl.multiple_of((i % per) * ROWS_BLK, ROWS_BLK), ROWS_BLK)
            columns = []
            for k in range(ROWS_BLK // 128):
                line = dz_all[b, pl.ds((i % per) * (ROWS_BLK // 128) + k, 1), :]
                columns.append(jnp.broadcast_to(line, (128, 128)).T)
            column = jnp.concatenate(columns, axis=0)
            column = jnp.concatenate([column] * (width // 128), axis=1)
            grad = (scale * column * h_all[by, bx, bc, rows, :].astype(jnp.float32)).astype(jnp.bfloat16)
            q = tower_back(raw_all[by, bx, bc, rows, :], wi_one[...], wi_two[...], grad)[0]
            rows_t[by, bx, bc, rows, :] = by_transpose(q, wi_one[...]).astype(jnp.bfloat16)
            rows_copy(i).start()

    def put(data, first, value):
        n = value.shape[0] // 8
        for b in range(8):
            data[b // 4, (b // 2) % 2, b % 2, first : first + n, :] = value[b * n : (b + 1) * n, :]

    def own(red, full):
        first, second = red.last()
        half = first.shape[0]
        full[y, x, c, 0:half, :] = first
        full[y, x, c, half : 2 * half, :] = second

    t_q, t_hid = tower_back(targ_raw[...], wi_one[...], wi_two[...], d_targ[...])
    red_u[0].two()
    red_u[1].two()
    in_copies[2].wait()
    q_q, q_hid = tower_back(tokens[...], w_one[...], w_two[...], d_query[...])
    dw_one = over_rows(tokens[...], q_q)
    put(wa_data, 0, dw_one[:, :width])
    put(wa_data, 128, dw_one[:, width:])
    put(wa_data, 256, over_rows(q_hid, d_query[...]))
    red_a.one()
    in_copies[3].wait()
    for copy in l_copies:
        copy.wait()
    h_copy.wait()
    loss_out[...] = jnp.sum(l_all[...], axis=0)
    rows_pass(0, 3)
    red_u[0].three()
    red_u[1].three()
    red_a.two()
    rows_pass(3, 6)
    parts = []
    for k in range(2):
        first, second = red_u[k].last()
        parts += [first, second]
    d_cand = (jnp.concatenate(parts, axis=0) * scale).astype(jnp.bfloat16)
    c_q, c_hid = tower_back(cand_raw[...], wi_one[...], wi_two[...], d_cand)
    back_c[y, x, c] = by_transpose(c_q, wi_one[...]).astype(jnp.bfloat16)
    ag_c.one()
    dwi_one = over_rows(targ_raw[...], t_q) + over_rows(cand_raw[...], c_q)
    put(wb_data, 0, dwi_one[:, :width])
    put(wb_data, 32, dwi_one[:, width:])
    put(wb_data, 64, over_rows(t_hid, d_targ[...]) + over_rows(c_hid, d_cand))
    red_b.one()
    red_a.three()
    red_b.two()
    ag_c.two()
    rows_pass(6, 8)
    own(red_a, wa_full)
    ag_a.one()
    red_b.three()
    rows_pass(8, 13)
    ag_a.two()
    own(red_b, wb_full)
    ag_b.one()
    ag_c.three()
    rows_pass(13, 16)
    ag_b.two()
    ag_c.last()
    out_copies = [pltpu.make_async_copy(back_c, cand_out, out_sem.at[0])]
    out_copies[0].start()
    ag_a.three()
    ag_b.three()
    ag_a.last()
    out_copies.append(pltpu.make_async_copy(wa_full, wa_out, out_sem.at[1]))
    out_copies[1].start()
    ag_b.last()
    out_copies.append(pltpu.make_async_copy(wb_full, wb_out, out_sem.at[2]))
    out_copies[2].start()
    for part in red_u + [red_a, red_b, ag_c, ag_a, ag_b]:
        part.drain()
    for i in range(rows_sem.shape[0]):
        rows_copy(i).wait()
    for copy in out_copies:
        copy.wait()


def back_rows(d_part, tokens, raw_all, h_part, loss_part, dz, d_query, d_targ, w_one, w_two, targ_raw, cand_raw, wi_one, wi_two):
    n_mine, width = d_part.shape[3:]
    vmem = pl.BlockSpec(memory_space=pltpu.VMEM)
    hbm = pl.BlockSpec(memory_space=pl.ANY)
    eight = pltpu.SemaphoreType.DMA((8,))
    scratch = reduce_scratch(2, PIECE, width, jnp.float32) + reduce_scratch(1, WA_ROWS, width, jnp.float32) + reduce_scratch(1, WB_ROWS, width, jnp.float32)
    scratch += gather_sems() + gather_sems() + gather_sems() + [eight] * 4 + [pltpu.SemaphoreType.DMA((2,))]
    scratch += [pltpu.VMEM((2, 2, 2, WA_ROWS, width), jnp.float32), pltpu.VMEM((2, 2, 2, WB_ROWS, width), jnp.float32), pltpu.VMEM((8, 8, 128), jnp.float32), pltpu.VMEM((8, 8, 128), jnp.float32)]
    scratch += [pltpu.VMEM(d_part.shape, jnp.float32), pltpu.VMEM(tokens.shape, jnp.bfloat16), pltpu.VMEM(raw_all.shape, jnp.bfloat16), pltpu.VMEM(raw_all.shape, jnp.bfloat16), pltpu.SemaphoreType.DMA((4,))]
    scratch += [pltpu.VMEM(raw_all.shape, jnp.bfloat16), pltpu.VMEM((2, 2, 2, n_mine, width), jnp.bfloat16), pltpu.VMEM((2, 2, 2, WA_ROWS, width), jnp.float32), pltpu.VMEM((2, 2, 2, WB_ROWS, width), jnp.float32)]
    scratch += [pltpu.SemaphoreType.DMA((8 * raw_all.shape[3] // ROWS_BLK,)), pltpu.SemaphoreType.DMA((3,))]
    return pl.pallas_call(
        back_body,
        out_shape=(
            jax.ShapeDtypeStruct(raw_all.shape, jnp.bfloat16),
            jax.ShapeDtypeStruct((2, 2, 2, n_mine, width), jnp.bfloat16),
            jax.ShapeDtypeStruct((2, 2, 2, WA_ROWS, width), jnp.float32),
            jax.ShapeDtypeStruct((2, 2, 2, WB_ROWS, width), jnp.float32),
            jax.ShapeDtypeStruct((8, 128), jnp.float32),
        ),
        in_specs=[hbm] * 4 + [vmem] * 10,
        out_specs=(hbm,) * 4 + (vmem,),
        scratch_shapes=scratch,
        compiler_params=pltpu.CompilerParams(vmem_limit_bytes=VMEM_LIMIT, collective_id=2, has_side_effects=True),
        name="back_rows",
    )(d_part, tokens, raw_all, h_part, loss_part, dz, d_query, d_targ, w_one, w_two, targ_raw, cand_raw, wi_one, wi_two)


def solution(mesh):
    num_dev = mesh.shape["dp"]

    def local_step(tokens, w_one, w_two, wi_one, wi_two, table_loc, cand_ids, log_q, targ_loc):
        rows_loc, width = table_loc.shape
        n_cand = cand_ids.shape[0]
        n_tok = tokens.shape[0]
        tok_total = n_tok * num_dev
        ids_two, query = prepare(targ_loc, cand_ids, tokens, w_one, w_two, rows_loc)
        data_c, data_t = pick_rows(ids_two, table_loc, n_cand)
        data_c = data_c.reshape(2, 2, 2, n_cand // 8, width)
        data_t = data_t.reshape(2, 2, 2, n_tok, width)
        cand_raw, targ_raw, loss_part, d_query, d_targ, d_part, dz, h_part = score(tok_total, data_c, data_t, wi_one, wi_two, query, log_q, cand_ids, targ_loc)
        rows_t, back_c, wa, wb, loss = back_rows(d_part.reshape(2, 2, 2, n_cand // 8, width), tokens, data_t, h_part, loss_part, dz, d_query, d_targ, w_one, w_two, targ_raw, cand_raw, wi_one, wi_two)
        d_table, dw_one, dw_two, dwi_one, dwi_two, loss = scatter_rows(tok_total, ids_two, loss, back_c.reshape(-1, width), rows_t.reshape(-1, width), wa.reshape(8, WA_ROWS, width), wb.reshape(8, WB_ROWS, width), rows_loc, tokens.shape[1])
        return loss.reshape(()), d_table, dw_one, dw_two, dwi_one, dwi_two

    return jax.shard_map(local_step, mesh=mesh, in_specs=(P("dp", None), P(), P(), P(), P(), P("dp", None), P(), P(), P("dp")), out_specs=(P(), P("dp", None), P(), P(), P(), P()), check_vma=False)
```

```python
import functools
import math
import jax
import jax.numpy as jnp
from jax import lax
from jax.experimental import pallas as pl
from jax.experimental.pallas import tpu as pltpu
from jax.sharding import PartitionSpec as P

SCORE_GAIN = 3.0
HIT_VALUE = -1e9


def tower_fwd(row_block, w_in, w_out):
    pre_act = jnp.dot(row_block, w_in, preferred_element_type=jnp.float32)
    hidden = jax.nn.gelu(pre_act).astype(jnp.bfloat16)
    tower_out = jnp.dot(hidden, w_out, preferred_element_type=jnp.float32).astype(jnp.bfloat16)
    return tower_out


def over_rows(a, b):
    return lax.dot_general(a, b, (((0,), (0,)), ((), ())), preferred_element_type=jnp.float32)


def by_transpose(a, b):
    return lax.dot_general(a, b, (((1,), (1,)), ((), ())), preferred_element_type=jnp.float32)


def tower_back(row_block, w_in, w_out, grad_out):
    pre_act = jnp.dot(row_block, w_in, preferred_element_type=jnp.float32)
    hidden, gelu_back = jax.vjp(jax.nn.gelu, pre_act)
    grad_hidden = by_transpose(grad_out, w_out)
    return gelu_back(grad_hidden)[0].astype(jnp.bfloat16), hidden.astype(jnp.bfloat16)


VMEM_LIMIT = 63 * 1024 * 1024
BATCH = 128
SPARE = 256
GROUP = 16
STAGE_ROWS = 2048
OUT_ROWS = 1024
IN_SLOTS = 12
OUT_SLOTS = 8


def pick_body(ids_s, table, cand_hbm, targ_hbm, wide, stage, rows_f, cand_out, targ_out, stage_sem, out_sem):
    rows_loc, width = table.shape
    lane = width // 2
    n_stage = rows_loc // STAGE_ROWS

    def stage_copy(i, slot):
        return pltpu.make_async_copy(table.at[pl.ds(i * STAGE_ROWS, STAGE_ROWS)], stage.at[slot], stage_sem.at[slot])

    for i in range(IN_SLOTS - 1):
        stage_copy(i, i).start()
    wide[pl.ds(2 * rows_loc, 2 * SPARE), :] = jnp.zeros((2 * SPARE, lane), jnp.float32)

    @pl.loop(0, n_stage)
    def _(i):
        slot = i % IN_SLOTS

        @pl.when(i + IN_SLOTS - 1 < n_stage)
        def _():
            stage_copy(i + IN_SLOTS - 1, (i + IN_SLOTS - 1) % IN_SLOTS).start()

        stage_copy(i, slot).wait()

        @pl.loop(0, STAGE_ROWS // 128)
        def _(j):
            block = stage[slot, pl.ds(pl.multiple_of(j * 128, 128), 128), :].astype(jnp.float32)
            base = pl.multiple_of((i * STAGE_ROWS + j * 128) * 2, 256)
            wide[pl.ds(base, 128, 2), :] = block[:, :lane]
            wide[pl.ds(base + 1, 128, 2), :] = block[:, lane:]

    copies = []

    def fill(out, hbm, first, count, ids_row):
        @pl.loop(0, count // BATCH)
        def _(b):
            for r in range(BATCH):
                at = pl.multiple_of(ids_s[ids_row + b, r], 2)
                rows_f[pl.ds(2 * r, 2), :] = wide[pl.ds(at, 2), :]
            rows = pl.ds(pl.multiple_of(first + b * BATCH, BATCH), BATCH)
            out[rows, :lane] = rows_f[pl.ds(0, BATCH, 2), :].astype(jnp.bfloat16)
            out[rows, lane:] = rows_f[pl.ds(1, BATCH, 2), :].astype(jnp.bfloat16)

        copy = pltpu.make_async_copy(out.at[pl.ds(first, count)], hbm.at[pl.ds(first, count)], out_sem.at[len(copies)])
        copy.start()
        copies.append(copy)

    n_cand = cand_out.shape[0]
    part = targ_out.shape[0] // 4
    fill(cand_out, cand_hbm, 0, n_cand, 0)
    for k in range(4):
        fill(targ_out, targ_hbm, k * part, part, (n_cand + k * part) // BATCH)
    for copy in copies:
        copy.wait()


def pick_rows(ids_two, table_loc, n_cand):
    rows_loc, width = table_loc.shape
    n_targ = ids_two.size - n_cand
    hbm = pl.BlockSpec(memory_space=pl.ANY)
    return pl.pallas_call(
        pick_body,
        out_shape=(jax.ShapeDtypeStruct((n_cand, width), jnp.bfloat16), jax.ShapeDtypeStruct((n_targ, width), jnp.bfloat16)),
        in_specs=[pl.BlockSpec(memory_space=pltpu.SMEM), hbm],
        out_specs=(hbm, hbm),
        scratch_shapes=[
            pltpu.VMEM((2 * (rows_loc + SPARE), width // 2), jnp.float32),
            pltpu.VMEM((IN_SLOTS, STAGE_ROWS, width), jnp.bfloat16),
            pltpu.VMEM((2 * BATCH, width // 2), jnp.float32),
            pltpu.VMEM((n_cand, width), jnp.bfloat16),
            pltpu.VMEM((n_targ, width), jnp.bfloat16),
            pltpu.SemaphoreType.DMA((IN_SLOTS,)),
            pltpu.SemaphoreType.DMA((5,)),
        ],
        compiler_params=pltpu.CompilerParams(vmem_limit_bytes=VMEM_LIMIT),
        name="pick_rows",
    )(ids_two, table_loc)


def scatter_body(tok_total, ids_s, ids_v, loss_s, cand_hbm, targ_hbm, wa_hbm, wb_hbm, out_ref, dw_one, dw_two, dwi_one, dwi_two, loss_out, acc, g2, cand_ref, targ_ref, wa, wb, flag_v, flag_s, out_stage, sem, in_sem, flag_sem, w_sem):
    rows, width = out_ref.shape
    lane = width // 2
    n_cand = cand_ref.shape[0]
    loss_out[0, 0] = loss_s[0, 0] * (1.0 / tok_total)
    n_all = n_cand + targ_ref.shape[0]
    in_copies = [pltpu.make_async_copy(src, dst, in_sem.at[k]) for k, (src, dst) in enumerate([(cand_hbm, cand_ref), (targ_hbm, targ_ref), (wa_hbm, wa), (wb_hbm, wb)])]
    for copy in in_copies:
        copy.start()

    ids = ids_v[...]
    place = lax.broadcasted_iota(jnp.int32, ids.shape, 1) % GROUP
    twice = jnp.zeros(ids.shape, jnp.int32)
    for k in range(1, GROUP):
        twice = jnp.where((ids == pltpu.roll(ids, k, 1)) & (place >= k), 1, twice)
    flag_v[...] = jnp.broadcast_to(jnp.max(twice, axis=1, keepdims=True), ids.shape)
    flag_copy = pltpu.make_async_copy(flag_v, flag_s, flag_sem)
    flag_copy.start()

    @pl.loop(0, 2 * rows // 512)
    def _(i):
        acc[pl.ds(pl.multiple_of(i * 512, 512), 512), :] = jnp.zeros((512, lane), jnp.float32)

    def one_batch(b, src, src_base):
        rows_b = pl.ds(pl.multiple_of(b * BATCH - src_base, BATCH), BATCH)
        repeated = flag_s[b, 0]

        @pl.when(repeated == 0)
        def _():
            part = src[rows_b, :].astype(jnp.float32)
            g2[pl.ds(0, BATCH, 2), :] = part[:, :lane]
            g2[pl.ds(1, BATCH, 2), :] = part[:, lane:]

        @pl.when(repeated != 0)
        def _():
            row_i = lax.broadcasted_iota(jnp.int32, (BATCH, BATCH), 0) // GROUP
            col_i = lax.broadcasted_iota(jnp.int32, (BATCH, BATCH), 1) // GROUP
            idr = jnp.broadcast_to(ids_v[pl.ds(b, 1), :], (BATCH, BATCH))
            same = jnp.where((idr == idr.T) & (row_i == col_i), 1.0, 0.0).astype(jnp.bfloat16)
            part = jnp.dot(same, src[rows_b, :], preferred_element_type=jnp.float32)
            g2[pl.ds(0, BATCH, 2), :] = part[:, :lane]
            g2[pl.ds(1, BATCH, 2), :] = part[:, lane:]

        for g in range(BATCH // GROUP):
            at = [pl.multiple_of(ids_s[b, g * GROUP + r], 2) for r in range(GROUP)]
            new = [acc[pl.ds(at[r], 2), :] + g2[pl.ds(2 * (g * GROUP + r), 2), :] for r in range(GROUP)]
            for r in range(GROUP):
                acc[pl.ds(at[r], 2), :] = new[r]

    for copy in in_copies:
        copy.wait()
    w_copies = []

    def place_block(src, dst):
        copy = pltpu.make_async_copy(src, dst, w_sem)
        copy.start()
        w_copies.append(copy)

    for b in range(8):
        place_block(wa.at[b, pl.ds(0, 128)], dw_one.at[pl.ds(b * 128, 128), pl.ds(0, width)])
        place_block(wa.at[b, pl.ds(128, 128)], dw_one.at[pl.ds(b * 128, 128), pl.ds(width, width)])
        place_block(wa.at[b, pl.ds(256, 64)], dw_two.at[pl.ds(b * 64, 64)])
        place_block(wb.at[b, pl.ds(0, 32)], dwi_one.at[pl.ds(b * 32, 32), pl.ds(0, width)])
        place_block(wb.at[b, pl.ds(32, 32)], dwi_one.at[pl.ds(b * 32, 32), pl.ds(width, width)])
        place_block(wb.at[b, pl.ds(64, 64)], dwi_two.at[pl.ds(b * 64, 64)])
    flag_copy.wait()

    @pl.loop(0, n_cand // BATCH)
    def _(b):
        one_batch(b, cand_ref, 0)

    @pl.loop(n_cand // BATCH, n_all // BATCH)
    def _(b):
        one_batch(b, targ_ref, n_cand)

    n_out = rows // OUT_ROWS

    def out_copy(i, slot):
        return pltpu.make_async_copy(out_stage.at[slot], out_ref.at[pl.ds(i * OUT_ROWS, OUT_ROWS)], sem.at[slot])

    @pl.loop(0, n_out)
    def _(i):
        slot = i % OUT_SLOTS

        @pl.when(i >= OUT_SLOTS)
        def _():
            out_copy(i - OUT_SLOTS, slot).wait()

        @pl.loop(0, OUT_ROWS // 128)
        def _(j):
            base = pl.multiple_of((i * OUT_ROWS + j * 128) * 2, 256)
            here = pl.ds(pl.multiple_of(j * 128, 128), 128)
            out_stage[slot, here, :lane] = acc[pl.ds(base, 128, 2), :]
            out_stage[slot, here, lane:] = acc[pl.ds(base + 1, 128, 2), :]

        out_copy(i, slot).start()

    for i in range(n_out - OUT_SLOTS, n_out):
        out_copy(i, i % OUT_SLOTS).wait()
    for copy in w_copies:
        copy.wait()


def scatter_rows(tok_total, ids_two, loss, back_cand, back_targ, wa, wb, rows_loc, din):
    width = back_cand.shape[1]
    n_batch = ids_two.shape[0]
    vmem = pl.BlockSpec(memory_space=pltpu.VMEM)
    hbm = pl.BlockSpec(memory_space=pl.ANY)
    smem = pl.BlockSpec(memory_space=pltpu.SMEM)
    shapes = [(rows_loc, width), (din, 2 * width), (2 * width, width), (width, 2 * width), (2 * width, width), (1, 1)]
    return pl.pallas_call(
        functools.partial(scatter_body, tok_total),
        out_shape=tuple(jax.ShapeDtypeStruct(shape, jnp.float32) for shape in shapes),
        in_specs=[smem, vmem, smem] + [hbm] * 4,
        out_specs=(hbm,) * 5 + (smem,),
        scratch_shapes=[
            pltpu.VMEM((2 * (rows_loc + SPARE), width // 2), jnp.float32),
            pltpu.VMEM((2 * BATCH, width // 2), jnp.float32),
            pltpu.VMEM(back_cand.shape, jnp.bfloat16),
            pltpu.VMEM(back_targ.shape, jnp.bfloat16),
            pltpu.VMEM(wa.shape, jnp.float32),
            pltpu.VMEM(wb.shape, jnp.float32),
            pltpu.VMEM((n_batch, BATCH), jnp.int32),
            pltpu.SMEM((n_batch, BATCH), jnp.int32),
            pltpu.VMEM((OUT_SLOTS, OUT_ROWS, width), jnp.float32),
            pltpu.SemaphoreType.DMA((OUT_SLOTS,)),
            pltpu.SemaphoreType.DMA((4,)),
            pltpu.SemaphoreType.DMA,
            pltpu.SemaphoreType.DMA,
        ],
        compiler_params=pltpu.CompilerParams(vmem_limit_bytes=VMEM_LIMIT),
        cost_estimate=pl.CostEstimate(flops=60_000_000_000, bytes_accessed=40 << 20, transcendentals=0),
        name="scatter_rows",
    )(ids_two, ids_two, loss, back_cand, back_targ, wa, wb)


CHUNK = 512
SUB = 128
COLS = 256


def logits_pass(u_at, n_cand, h, lq_ref, cid_ref, tid, z_a, z_b, e_s, m_s, s_s):
    n_tok, width = h.shape
    scale = SCORE_GAIN / math.sqrt(width)
    ht = h.T
    n_chunk = n_cand // CHUNK

    def multiply(i, z_ref):
        z_ref[...] = jnp.dot(u_at(jnp.minimum(i, n_chunk - 1)), ht, preferred_element_type=jnp.float32)

    def absorb(i, z_ref):
        off = pl.multiple_of(i * CHUNK, CHUNK)
        for col in range(0, n_tok, COLS):
            cols = slice(col, col + COLS)
            m8 = m_s[0, :, cols]
            s8 = s_s[:, cols]
            for k in range(CHUNK // SUB):
                rows = pl.ds(pl.multiple_of(off + k * SUB, SUB), SUB)
                lq = jnp.concatenate([lq_ref[rows, :]] * (COLS // 128), axis=1)
                cid = jnp.concatenate([cid_ref[rows, :]] * (COLS // 128), axis=1)
                z = z_ref[k * SUB : (k + 1) * SUB, cols] * scale - lq
                z = jnp.where(cid == tid[:, cols], HIT_VALUE, z).reshape(SUB // 8, 8, COLS)
                m_new = jnp.maximum(m8, jnp.max(z, axis=0))
                e = jnp.exp(z - m_new[None])
                s8 = s8 * jnp.exp(m8 - m_new) + jnp.sum(e, axis=0)
                m8 = m_new
                e_s[rows, cols] = e.reshape(SUB, COLS)
                m_s[1 + i * (CHUNK // SUB) + k, :, cols] = m8
            m_s[0, :, cols] = m8
            s_s[:, cols] = s8

    m_s[0] = jnp.full((8, n_tok), jnp.finfo(jnp.float32).min, jnp.float32)
    s_s[...] = jnp.zeros_like(s_s)
    multiply(0, z_a)

    def two_chunks(i):
        multiply(2 * i + 1, z_b)
        absorb(2 * i, z_a)
        multiply(2 * i + 2, z_a)
        absorb(2 * i + 1, z_b)

    pl.loop(0, n_chunk // 2)(two_chunks)


def loss_pass(tok_total, u_at, ut_s, h, v, e_s, m_s, s_s, fac_s, dz_a, dz_b, dht_s, loss_ref, dh_ref, dv_ref, du_ref, dz_ref, du_copy):
    n_cand, width = du_ref.shape
    n_tok = h.shape[0]
    scale = SCORE_GAIN / math.sqrt(width)
    n_chunk = n_cand // CHUNK
    hf = h.astype(jnp.float32)
    vf = v.astype(jnp.float32)
    zt = jnp.sum(hf * vf, axis=1, keepdims=True) * scale
    zt = jnp.broadcast_to(zt, (n_tok, 128)).T[0:1, :]
    m8 = m_s[0]
    m = jnp.maximum(zt, jnp.max(m8, axis=0, keepdims=True))
    et = jnp.exp(zt - m)
    den = et + jnp.sum(s_s[...] * jnp.exp(m8 - m), axis=0, keepdims=True)
    part = jnp.sum(jnp.log(den) + m - zt, axis=1, keepdims=True)
    loss_ref[...] = jnp.broadcast_to(part, loss_ref.shape)
    dzt = ((et / den - 1.0) / tok_total).astype(jnp.bfloat16).astype(jnp.float32)
    inv = 1.0 / den / tok_total
    fac_s[0:8, :] = jnp.broadcast_to(m, (8, n_tok))
    fac_s[8:16, :] = jnp.broadcast_to(inv, (8, n_tok))
    for i in range(n_chunk):
        ut_s[:, i * CHUNK : (i + 1) * CHUNK] = u_at(i).T
    for i in range(8):
        dz_ref[i : i + 1, :] = dzt[:, i * 128 : (i + 1) * 128]

    def gradient(i, out):
        i = jnp.minimum(i, n_chunk - 1)
        off = pl.multiple_of(i * CHUNK, CHUNK)
        for col in range(0, n_tok, COLS):
            cols = slice(col, col + COLS)
            for k in range(CHUNK // SUB):
                rows = pl.ds(pl.multiple_of(off + k * SUB, SUB), SUB)
                fac = jnp.exp(m_s[1 + i * (CHUNK // SUB) + k, :, cols] - fac_s[0:8, cols]) * fac_s[8:16, cols]
                out[k * SUB : (k + 1) * SUB, cols] = (e_s[rows, cols].reshape(SUB // 8, 8, COLS) * fac[None]).reshape(SUB, COLS).astype(jnp.bfloat16)

    def spread(i, dz_c):
        off = pl.multiple_of(i * CHUNK, CHUNK)
        du_ref[pl.ds(off, CHUNK), :] = jnp.dot(dz_c[...], h, preferred_element_type=jnp.float32)
        du_copy(i).start()
        dht_s[...] += jnp.dot(ut_s[:, pl.ds(off, CHUNK)], dz_c[...], preferred_element_type=jnp.float32)

    dht_s[...] = jnp.zeros_like(dht_s)
    gradient(0, dz_a)

    @pl.loop(0, n_chunk // 2)
    def _(i):
        gradient(2 * i + 1, dz_b)
        spread(2 * i, dz_a)
        gradient(2 * i + 2, dz_a)
        spread(2 * i + 1, dz_b)

    dzt_c = jnp.broadcast_to(dzt, (128, n_tok)).T[:, 0:1]
    dh_ref[...] = ((dzt_c * vf + dht_s[...].T) * scale).astype(jnp.bfloat16)
    dv_ref[...] = (scale * dzt_c * hf).astype(jnp.bfloat16)


def softmax_scratch(n_cand, n_tok, width):
    return [
        pltpu.VMEM((CHUNK, n_tok), jnp.float32),
        pltpu.VMEM((CHUNK, n_tok), jnp.float32),
        pltpu.VMEM((n_cand, n_tok), jnp.float32),
        pltpu.VMEM((1 + n_cand // SUB, 8, n_tok), jnp.float32),
        pltpu.VMEM((8, n_tok), jnp.float32),
        pltpu.VMEM((width, n_cand), jnp.bfloat16),
        pltpu.VMEM((16, n_tok), jnp.float32),
        pltpu.VMEM((CHUNK, n_tok), jnp.bfloat16),
        pltpu.VMEM((CHUNK, n_tok), jnp.bfloat16),
        pltpu.VMEM((width, n_tok), jnp.float32),
    ]


MESH = pl.DeviceIdType.MESH


def my_place():
    me = lax.axis_index("dp")
    return me, me // 4, (me // 2) % 2, me % 2


def peer_of(place, dy, dx, dc):
    me, y, x, c = place
    return me + dy * (4 - 8 * y) + dx * (2 - 4 * x) + dc * (1 - 2 * c)


def greet(place):
    barrier = pltpu.get_barrier_semaphore()
    for k in range(1, 8):
        pl.semaphore_signal(barrier, inc=1, device_id=(peer_of(place, k // 4, (k // 2) % 2, k % 2),), device_id_type=MESH)


def meet(place):
    greet(place)
    pl.semaphore_wait(pltpu.get_barrier_semaphore(), 7)


def push(src, dst, send_sem, recv_sem, peer):
    copy = pltpu.make_async_remote_copy(src_ref=src, dst_ref=dst, send_sem=send_sem, recv_sem=recv_sem, device_id=(peer,), device_id_type=MESH)
    copy.start()
    return copy


class Reduce:
    def __init__(self, place, data, in_one, mid, in_xa, in_yb, part_a, part_b, in_ya, in_xb, send_sem, recv_sem):
        self.place, self.data = place, data
        self.in_one, self.mid, self.in_xa, self.in_yb = in_one, mid, in_xa, in_yb
        self.part_a, self.part_b, self.in_ya, self.in_xb = part_a, part_b, in_ya, in_xb
        self.send_sem, self.recv_sem = send_sem, recv_sem
        self.half = data.shape[3] // 2
        self.copies = []

    def push(self, k, src, dst, dy, dx, dc):
        copy = push(src, dst, self.send_sem.at[k], self.recv_sem.at[k], peer_of(self.place, dy, dx, dc))
        self.copies.append(copy)

    def one(self):
        c = self.place[3]
        self.push(0, self.data.at[:, :, 1 - c], self.in_one, 0, 0, 1)

    def two(self):
        _, y, x, c = self.place
        half = self.half
        self.copies[0].wait_recv()
        for i in range(2):
            for j in range(2):
                self.mid[i, j] = self.data[i, j, c] + self.in_one[i, j]
        self.push(1, self.mid.at[:, 1 - x, pl.ds(0, half)], self.in_xa, 0, 1, 0)
        self.push(2, self.mid.at[1 - y, :, pl.ds(half, half)], self.in_yb, 1, 0, 0)

    def three(self):
        _, y, x, c = self.place
        half = self.half
        self.copies[1].wait_recv()
        for i in range(2):
            self.part_a[i] = self.mid[i, x, 0:half] + self.in_xa[i]
        self.push(3, self.part_a.at[1 - y], self.in_ya, 1, 0, 0)
        self.copies[2].wait_recv()
        for i in range(2):
            self.part_b[i] = self.mid[y, i, half : 2 * half] + self.in_yb[i]
        self.push(4, self.part_b.at[1 - x], self.in_xb, 0, 1, 0)

    def last(self):
        _, y, x, c = self.place
        self.copies[3].wait_recv()
        first = self.part_a[y] + self.in_ya[...]
        self.copies[4].wait_recv()
        return first, self.part_b[x] + self.in_xb[...]

    def drain(self):
        for copy in self.copies:
            copy.wait_send()


def reduce_scratch(n, rows, width, dtype):
    half = rows // 2
    return [
        pltpu.VMEM((n, 2, 2, rows, width), dtype),
        pltpu.VMEM((n, 2, 2, rows, width), dtype),
        pltpu.VMEM((n, 2, half, width), dtype),
        pltpu.VMEM((n, 2, half, width), dtype),
        pltpu.VMEM((n, 2, half, width), dtype),
        pltpu.VMEM((n, 2, half, width), dtype),
        pltpu.VMEM((n, half, width), dtype),
        pltpu.VMEM((n, half, width), dtype),
        pltpu.SemaphoreType.DMA((n, 5)),
        pltpu.SemaphoreType.DMA((n, 5)),
    ]


class Gather:
    def __init__(self, place, full, send_sem, recv_sem):
        self.place, self.full = place, full
        self.send_sem, self.recv_sem = send_sem, recv_sem
        self.half = full.shape[3] // 2
        self.copies = []

    def push(self, k, ref, dy, dx, dc):
        copy = push(ref, ref, self.send_sem.at[k], self.recv_sem.at[k], peer_of(self.place, dy, dx, dc))
        self.copies.append(copy)

    def one(self):
        _, y, x, c = self.place
        half = self.half
        self.push(0, self.full.at[y, x, c, pl.ds(0, half)], 0, 1, 0)
        self.push(1, self.full.at[y, x, c, pl.ds(half, half)], 1, 0, 0)

    def two(self):
        _, y, x, c = self.place
        half = self.half
        self.copies[0].wait_recv()
        self.push(2, self.full.at[y, :, c, pl.ds(0, half)], 1, 0, 0)
        self.copies[1].wait_recv()
        self.push(3, self.full.at[:, x, c, pl.ds(half, half)], 0, 1, 0)

    def three(self):
        c = self.place[3]
        self.copies[2].wait_recv()
        self.copies[3].wait_recv()
        self.push(4, self.full.at[:, :, c], 0, 0, 1)

    def last(self):
        self.copies[4].wait_recv()

    def drain(self):
        for copy in self.copies:
            copy.wait_send()


def gather_sems():
    return [pltpu.SemaphoreType.DMA((5,)), pltpu.SemaphoreType.DMA((5,))]


def prepare_body(rows_loc, mine, cand_ids, tokens, w_one, w_two, ids_two, query, full, send_sem, recv_sem):
    place = my_place()
    me = place[0]
    greet(place)
    half = tokens.shape[0] // 2
    query[0:half, :] = tower_fwd(tokens[0:half, :], w_one[...], w_two[...])
    pl.semaphore_wait(pltpu.get_barrier_semaphore(), 7)
    full[me] = mine[...]
    copies = []
    for k in range(1, 8):
        copies.append(push(mine, full.at[me], send_sem.at[k], recv_sem.at[k], peer_of(place, k // 4, (k // 2) % 2, k % 2)))

    def owned(ids):
        local = ids - me * rows_loc
        spare = rows_loc + (lax.broadcasted_iota(jnp.int32, ids.shape, 0) % 2) * 128 + lax.broadcasted_iota(jnp.int32, ids.shape, 1)
        return 2 * jnp.where((local >= 0) & (local < rows_loc), local, spare)

    n_c = cand_ids.shape[0]
    ids_two[0:n_c, :] = owned(cand_ids[...])
    query[half : 2 * half, :] = tower_fwd(tokens[half : 2 * half, :], w_one[...], w_two[...])
    for copy in copies:
        copy.wait()
    ids_two[n_c : n_c + 64, :] = owned(full[...].reshape(64, 128))


def prepare(targ_loc, cand_ids, tokens, w_one, w_two, rows_loc):
    n_tok = tokens.shape[0]
    n_c = cand_ids.shape[0] // 128
    vmem = pl.BlockSpec(memory_space=pltpu.VMEM)
    return pl.pallas_call(
        functools.partial(prepare_body, rows_loc),
        out_shape=(jax.ShapeDtypeStruct((n_c + 64, 128), jnp.int32), jax.ShapeDtypeStruct((n_tok, w_two.shape[1]), jnp.bfloat16)),
        in_specs=[vmem] * 5,
        out_specs=(vmem,) * 2,
        scratch_shapes=[pltpu.VMEM((8, 8, 128), jnp.int32), pltpu.SemaphoreType.DMA((8,)), pltpu.SemaphoreType.DMA((8,))],
        compiler_params=pltpu.CompilerParams(vmem_limit_bytes=VMEM_LIMIT, collective_id=0, has_side_effects=True),
        name="prepare",
    )(targ_loc.reshape(8, 128), cand_ids.reshape(n_c, 128), tokens, w_one, w_two)


PIECE = 256


def score_body(tok_total, c_hbm, t_hbm, wi_one, wi_two, h_ref, lq_ref, cid_ref, tid_ref, cand_raw, targ_raw, loss_ref, dh_ref, dv_ref, du_hbm, dz_ref, h_part, *scratch):
    place = my_place()
    me, y, x, c = place
    half = PIECE // 2
    data_c, data_t, in_sem, cand_vec, lq_b, cid_b, rs, ag_send, ag_recv = scratch[0:6] + (scratch[6:16],) + scratch[16:18]
    z_a, z_b, e_s, m_s, s_s, ut_s, fac_s, dz_a, dz_b, dht_s, h_send, h_recv, du_ref, du_sem = scratch[18:32]
    n_cand, width = du_ref.shape
    in_copies = [pltpu.make_async_copy(c_hbm, data_c, in_sem.at[0]), pltpu.make_async_copy(t_hbm, data_t, in_sem.at[1])]
    for copy in in_copies:
        copy.start()
    ag_h = Gather((me, y, x, 0), h_part, h_send, h_recv)
    h_part[y, x, 0] = h_ref[...]
    meet(place)
    ag_h.one()
    reduces = []
    for k in range(6):
        data = data_c.at[:, :, :, pl.ds(k * PIECE, PIECE)] if k < 2 else data_t.at[:, :, :, pl.ds((k - 2) * PIECE, PIECE)]
        reduces.append(Reduce(place, data, *[r.at[k] for r in rs]))
    ag = Gather(place, cand_vec, ag_send, ag_recv)

    def close(k, out, base):
        first, second = reduces[k].last()
        out[base : base + half, :] = first
        out[base + half : base + PIECE, :] = second

    in_copies[0].wait()
    reduces[0].one()
    reduces[1].one()
    in_copies[1].wait()
    for k in range(2, 6):
        reduces[k].one()
    reduces[0].two()
    reduces[1].two()
    reduces[2].two()
    reduces[0].three()
    reduces[1].three()
    reduces[3].two()

    @pl.loop(0, n_cand // 128)
    def _(i):
        rows = pl.ds(pl.multiple_of(i * 128, 128), 128)
        lq_b[rows, :] = jnp.broadcast_to(lq_ref[pl.ds(i, 1), :], (128, 128)).T
        cid_b[rows, :] = jnp.broadcast_to(cid_ref[pl.ds(i, 1), :], (128, 128)).T

    close(0, cand_raw, 0)
    close(1, cand_raw, PIECE)
    cand_vec[y, x, c] = tower_fwd(cand_raw[...], wi_one[...], wi_two[...])
    ag.one()
    reduces[4].two()
    reduces[5].two()
    reduces[2].three()
    ag.two()
    reduces[3].three()
    reduces[4].three()
    ag.three()
    reduces[5].three()
    ag_h.two()
    ag.last()

    def du_copy(i):
        rows = pl.ds(pl.multiple_of(i * CHUNK, CHUNK), CHUNK)
        return pltpu.make_async_copy(du_ref.at[rows], du_hbm.at[rows], du_sem.at[i])

    def u_at(i):
        return cand_vec[i // 4, (i // 2) % 2, i % 2]

    h = h_ref[...]
    logits_pass(u_at, n_cand, h, lq_b, cid_b, tid_ref[...], z_a, z_b, e_s, m_s, s_s)
    for k in range(4):
        close(k + 2, targ_raw, k * PIECE)
    v = tower_fwd(targ_raw[...], wi_one[...], wi_two[...])
    loss_pass(tok_total, u_at, ut_s, h, v, e_s, m_s, s_s, fac_s, dz_a, dz_b, dht_s, loss_ref, dh_ref, dv_ref, du_ref, dz_ref, du_copy)
    for i in range(n_cand // CHUNK):
        du_copy(i).wait()
    ag_h.copies[2].wait_recv()
    ag_h.copies[3].wait_recv()
    for red in reduces:
        red.drain()
    ag.drain()
    ag_h.drain()


def score(tok_total, data_c, data_t, wi_one, wi_two, query, log_q, cand_ids, targ_loc):
    n_mine, width = data_c.shape[3:]
    n_tok = data_t.shape[3]
    n_cand = 8 * n_mine
    vmem = pl.BlockSpec(memory_space=pltpu.VMEM)
    hbm = pl.BlockSpec(memory_space=pl.ANY)
    scratch = [pltpu.VMEM(data_c.shape, jnp.bfloat16), pltpu.VMEM(data_t.shape, jnp.bfloat16), pltpu.SemaphoreType.DMA((2,))]
    scratch += [pltpu.VMEM(data_c.shape, jnp.bfloat16), pltpu.VMEM((n_cand, 128), jnp.float32), pltpu.VMEM((n_cand, 128), jnp.int32)]
    scratch += reduce_scratch(6, PIECE, width, jnp.bfloat16) + gather_sems() + softmax_scratch(n_cand, n_tok, width)
    scratch += gather_sems() + [pltpu.VMEM((n_cand, width), jnp.float32), pltpu.SemaphoreType.DMA((n_cand // CHUNK,))]
    rows = [jax.ShapeDtypeStruct((n, width), jnp.bfloat16) for n in (n_mine, n_tok, n_tok, n_tok)]
    return pl.pallas_call(
        functools.partial(score_body, tok_total),
        out_shape=(rows[0], rows[1], jax.ShapeDtypeStruct((8, 128), jnp.float32), rows[2], rows[3], jax.ShapeDtypeStruct((n_cand, width), jnp.float32), jax.ShapeDtypeStruct((8, 128), jnp.float32), jax.ShapeDtypeStruct((2, 2, 1, n_tok, width), jnp.bfloat16)),
        in_specs=[hbm, hbm] + [vmem] * 6,
        out_specs=(vmem,) * 5 + (hbm,) + (vmem,) * 2,
        scratch_shapes=scratch,
        compiler_params=pltpu.CompilerParams(vmem_limit_bytes=VMEM_LIMIT, collective_id=1, has_side_effects=True),
        name="score",
    )(data_c, data_t, wi_one, wi_two, query, log_q.reshape(-1, 128), cand_ids.reshape(-1, 128), targ_loc.reshape(1, n_tok))


WA_ROWS = 320
WB_ROWS = 128


ROWS_BLK = 512


def back_body(part_hbm, tok_hbm, raw_hbm, h_hbm, *rest):
    operands, (loss_in, dz_in, rows_out, cand_out, wa_out, wb_out, loss_out), scratch = rest[0:8], rest[8:15], rest[15:]
    place = my_place()
    me, y, x, c = place
    rs_u, rs_a, rs_b = scratch[0:10], scratch[10:20], scratch[20:30]
    ac_send, ac_recv, aa_send, aa_recv, ab_send, ab_recv, l_send, l_recv, z_send, z_recv, h_sem, wa_data, wb_data, l_all, dz_all, d_part, tokens, raw_all, h_all, in_sem, rows_t, back_c, wa_full, wb_full, rows_sem, out_sem = scratch[30:56]
    d_targ, targ_raw, wi_one, wi_two, d_query, w_one, w_two, cand_raw = scratch[56:64]
    width = d_query.shape[1]
    scale = SCORE_GAIN / math.sqrt(width)
    pairs = [(part_hbm, d_part), (h_hbm.at[:, :, 0], h_all.at[:, :, c]), (tok_hbm, tokens), (raw_hbm, raw_all)] + list(zip(operands, scratch[56:64]))
    in_copies = [pltpu.make_async_copy(src, dst, in_sem.at[k]) for k, (src, dst) in enumerate(pairs)]
    in_copies[0].start()
    for copy in in_copies[4:]:
        copy.start()
    meet(place)
    for copy in in_copies[1:4]:
        copy.start()
    red_u = []
    for k in range(2):
        red_u.append(Reduce(place, d_part.at[:, :, :, pl.ds(k * PIECE, PIECE)], *[r.at[k] for r in rs_u]))
    red_a = Reduce(place, wa_data, *[r.at[0] for r in rs_a])
    red_b = Reduce(place, wb_data, *[r.at[0] for r in rs_b])
    ag_a = Gather(place, wa_full, aa_send, aa_recv)
    ag_b = Gather(place, wb_full, ab_send, ab_recv)
    ag_c = Gather(place, back_c, ac_send, ac_recv)
    in_copies[0].wait()
    red_u[0].one()
    red_u[1].one()
    l_all[me] = loss_in[...]
    dz_all[me] = dz_in[...]
    l_copies = []
    for k in range(1, 8):
        peer = peer_of(place, k // 4, (k // 2) % 2, k % 2)
        l_copies.append(push(loss_in, l_all.at[me], l_send.at[k], l_recv.at[k], peer))
        l_copies.append(push(dz_in, dz_all.at[me], z_send.at[k], z_recv.at[k], peer))
    in_copies[1].wait()
    h_copy = push(h_all.at[:, :, c], h_all.at[:, :, c], h_sem.at[0], h_sem.at[1], peer_of(place, 0, 0, 1))

    per = rows_t.shape[3] // ROWS_BLK

    def rows_copy(i):
        b = i // per
        here = (b // 4, (b // 2) % 2, b % 2, pl.ds(pl.multiple_of((i % per) * ROWS_BLK, ROWS_BLK), ROWS_BLK))
        return pltpu.make_async_copy(rows_t.at[here], rows_out.at[here], rows_sem.at[i])

    def rows_pass(first, last):

        @pl.loop(first, last)
        def _(i):
            b = i // per
            by, bx, bc = b // 4, (b // 2) % 2, b % 2
            rows = pl.ds(pl.multiple_of((i % per) * ROWS_BLK, ROWS_BLK), ROWS_BLK)
            columns = []
            for k in range(ROWS_BLK // 128):
                line = dz_all[b, pl.ds((i % per) * (ROWS_BLK // 128) + k, 1), :]
                columns.append(jnp.broadcast_to(line, (128, 128)).T)
            column = jnp.concatenate(columns, axis=0)
            column = jnp.concatenate([column] * (width // 128), axis=1)
            grad = (scale * column * h_all[by, bx, bc, rows, :].astype(jnp.float32)).astype(jnp.bfloat16)
            q = tower_back(raw_all[by, bx, bc, rows, :], wi_one[...], wi_two[...], grad)[0]
            rows_t[by, bx, bc, rows, :] = by_transpose(q, wi_one[...]).astype(jnp.bfloat16)
            rows_copy(i).start()

    def put(data, first, value):
        n = value.shape[0] // 8
        for b in range(8):
            data[b // 4, (b // 2) % 2, b % 2, first : first + n, :] = value[b * n : (b + 1) * n, :]

    def own(red, full):
        first, second = red.last()
        half = first.shape[0]
        full[y, x, c, 0:half, :] = first
        full[y, x, c, half : 2 * half, :] = second

    for copy in in_copies[4:]:
        copy.wait()
    t_q, t_hid = tower_back(targ_raw[...], wi_one[...], wi_two[...], d_targ[...])
    red_u[0].two()
    red_u[1].two()
    in_copies[2].wait()
    q_q, q_hid = tower_back(tokens[...], w_one[...], w_two[...], d_query[...])
    dw_one = over_rows(tokens[...], q_q)
    put(wa_data, 0, dw_one[:, :width])
    put(wa_data, 128, dw_one[:, width:])
    put(wa_data, 256, over_rows(q_hid, d_query[...]))
    red_a.one()
    in_copies[3].wait()
    for copy in l_copies:
        copy.wait()
    h_copy.wait()
    loss_out[...] = jnp.sum(l_all[...], axis=0)
    rows_pass(0, 3)
    red_u[0].three()
    red_u[1].three()
    red_a.two()
    rows_pass(3, 6)
    parts = []
    for k in range(2):
        first, second = red_u[k].last()
        parts += [first, second]
    d_cand = (jnp.concatenate(parts, axis=0) * scale).astype(jnp.bfloat16)
    c_q, c_hid = tower_back(cand_raw[...], wi_one[...], wi_two[...], d_cand)
    back_c[y, x, c] = by_transpose(c_q, wi_one[...]).astype(jnp.bfloat16)
    ag_c.one()
    dwi_one = over_rows(targ_raw[...], t_q) + over_rows(cand_raw[...], c_q)
    put(wb_data, 0, dwi_one[:, :width])
    put(wb_data, 32, dwi_one[:, width:])
    put(wb_data, 64, over_rows(t_hid, d_targ[...]) + over_rows(c_hid, d_cand))
    red_b.one()
    red_a.three()
    red_b.two()
    ag_c.two()
    rows_pass(6, 8)
    own(red_a, wa_full)
    ag_a.one()
    red_b.three()
    rows_pass(8, 13)
    ag_a.two()
    own(red_b, wb_full)
    ag_b.one()
    ag_c.three()
    rows_pass(13, 16)
    ag_b.two()
    ag_c.last()
    out_copies = [pltpu.make_async_copy(back_c, cand_out, out_sem.at[0])]
    out_copies[0].start()
    ag_a.three()
    ag_b.three()
    ag_a.last()
    out_copies.append(pltpu.make_async_copy(wa_full, wa_out, out_sem.at[1]))
    out_copies[1].start()
    ag_b.last()
    out_copies.append(pltpu.make_async_copy(wb_full, wb_out, out_sem.at[2]))
    out_copies[2].start()
    for part in red_u + [red_a, red_b, ag_c, ag_a, ag_b]:
        part.drain()
    for i in range(rows_sem.shape[0]):
        rows_copy(i).wait()
    for copy in out_copies:
        copy.wait()


def back_rows(d_part, tokens, raw_all, h_part, operands, loss_part, dz):
    n_mine, width = d_part.shape[3:]
    vmem = pl.BlockSpec(memory_space=pltpu.VMEM)
    hbm = pl.BlockSpec(memory_space=pl.ANY)
    eight = pltpu.SemaphoreType.DMA((8,))
    scratch = reduce_scratch(2, PIECE, width, jnp.float32) + reduce_scratch(1, WA_ROWS, width, jnp.float32) + reduce_scratch(1, WB_ROWS, width, jnp.float32)
    scratch += gather_sems() + gather_sems() + gather_sems() + [eight] * 4 + [pltpu.SemaphoreType.DMA((2,))]
    scratch += [pltpu.VMEM((2, 2, 2, WA_ROWS, width), jnp.float32), pltpu.VMEM((2, 2, 2, WB_ROWS, width), jnp.float32), pltpu.VMEM((8, 8, 128), jnp.float32), pltpu.VMEM((8, 8, 128), jnp.float32)]
    scratch += [pltpu.VMEM(d_part.shape, jnp.float32), pltpu.VMEM(tokens.shape, jnp.bfloat16), pltpu.VMEM(raw_all.shape, jnp.bfloat16), pltpu.VMEM(raw_all.shape, jnp.bfloat16), pltpu.SemaphoreType.DMA((4 + len(operands),))]
    scratch += [pltpu.VMEM(raw_all.shape, jnp.bfloat16), pltpu.VMEM((2, 2, 2, n_mine, width), jnp.bfloat16), pltpu.VMEM((2, 2, 2, WA_ROWS, width), jnp.float32), pltpu.VMEM((2, 2, 2, WB_ROWS, width), jnp.float32)]
    scratch += [pltpu.SemaphoreType.DMA((8 * raw_all.shape[3] // ROWS_BLK,)), pltpu.SemaphoreType.DMA((3,))]
    scratch += [pltpu.VMEM(operand.shape, operand.dtype) for operand in operands]
    return pl.pallas_call(
        back_body,
        out_shape=(
            jax.ShapeDtypeStruct(raw_all.shape, jnp.bfloat16),
            jax.ShapeDtypeStruct((2, 2, 2, n_mine, width), jnp.bfloat16),
            jax.ShapeDtypeStruct((2, 2, 2, WA_ROWS, width), jnp.float32),
            jax.ShapeDtypeStruct((2, 2, 2, WB_ROWS, width), jnp.float32),
            jax.ShapeDtypeStruct((8, 128), jnp.float32),
        ),
        in_specs=[hbm] * 12 + [vmem] * 2,
        out_specs=(hbm,) * 4 + (vmem,),
        scratch_shapes=scratch,
        compiler_params=pltpu.CompilerParams(vmem_limit_bytes=VMEM_LIMIT, collective_id=2, has_side_effects=True),
        name="back_rows",
    )(d_part, tokens, raw_all, h_part, *operands, loss_part, dz)


def solution(mesh):
    num_dev = mesh.shape["dp"]

    def local_step(tokens, w_one, w_two, wi_one, wi_two, table_loc, cand_ids, log_q, targ_loc):
        rows_loc, width = table_loc.shape
        n_cand = cand_ids.shape[0]
        n_tok = tokens.shape[0]
        tok_total = n_tok * num_dev
        ids_two, query = prepare(targ_loc, cand_ids, tokens, w_one, w_two, rows_loc)
        data_c, data_t = pick_rows(ids_two, table_loc, n_cand)
        data_c = data_c.reshape(2, 2, 2, n_cand // 8, width)
        data_t = data_t.reshape(2, 2, 2, n_tok, width)
        cand_raw, targ_raw, loss_part, d_query, d_targ, d_part, dz, h_part = score(tok_total, data_c, data_t, wi_one, wi_two, query, log_q, cand_ids, targ_loc)
        rows_t, back_c, wa, wb, loss = back_rows(d_part.reshape(2, 2, 2, n_cand // 8, width), tokens, data_t, h_part, (d_targ, targ_raw, wi_one, wi_two, d_query, w_one, w_two, cand_raw), loss_part, dz)
        d_table, dw_one, dw_two, dwi_one, dwi_two, loss = scatter_rows(tok_total, ids_two, loss, back_c.reshape(-1, width), rows_t.reshape(-1, width), wa.reshape(8, WA_ROWS, width), wb.reshape(8, WB_ROWS, width), rows_loc, tokens.shape[1])
        return loss.reshape(()), d_table, dw_one, dw_two, dwi_one, dwi_two

    return jax.shard_map(local_step, mesh=mesh, in_specs=(P("dp", None), P(), P(), P(), P(), P("dp", None), P(), P(), P("dp")), out_specs=(P(), P("dp", None), P(), P(), P(), P()), check_vma=False)
```

```python
import functools
import math
import jax
import jax.numpy as jnp
from jax import lax
from jax.experimental import pallas as pl
from jax.experimental.pallas import tpu as pltpu
from jax.sharding import PartitionSpec as P

SCORE_GAIN = 3.0
HIT_VALUE = -1e9


def tower_fwd(row_block, w_in, w_out):
    pre_act = jnp.dot(row_block, w_in, preferred_element_type=jnp.float32)
    hidden = jax.nn.gelu(pre_act).astype(jnp.bfloat16)
    tower_out = jnp.dot(hidden, w_out, preferred_element_type=jnp.float32).astype(jnp.bfloat16)
    return tower_out


def over_rows(a, b):
    return lax.dot_general(a, b, (((0,), (0,)), ((), ())), preferred_element_type=jnp.float32)


def by_transpose(a, b):
    return lax.dot_general(a, b, (((1,), (1,)), ((), ())), preferred_element_type=jnp.float32)


def tower_back(row_block, w_in, w_out, grad_out):
    pre_act = jnp.dot(row_block, w_in, preferred_element_type=jnp.float32)
    hidden, gelu_back = jax.vjp(jax.nn.gelu, pre_act)
    grad_hidden = by_transpose(grad_out, w_out)
    return gelu_back(grad_hidden)[0].astype(jnp.bfloat16), hidden.astype(jnp.bfloat16)


VMEM_LIMIT = 63 * 1024 * 1024
BATCH = 128
SPARE = 256
GROUP = 16
STAGE_ROWS = 2048
OUT_ROWS = 1024
IN_SLOTS = 12
OUT_SLOTS = 8


def pick_body(ids_s, table, cand_hbm, targ_hbm, wide, stage, rows_f, cand_out, targ_out, stage_sem, out_sem):
    rows_loc, width = table.shape
    lane = width // 2
    n_stage = rows_loc // STAGE_ROWS

    def stage_copy(i, slot):
        return pltpu.make_async_copy(table.at[pl.ds(i * STAGE_ROWS, STAGE_ROWS)], stage.at[slot], stage_sem.at[slot])

    for i in range(IN_SLOTS - 1):
        stage_copy(i, i).start()
    wide[pl.ds(2 * rows_loc, 2 * SPARE), :] = jnp.zeros((2 * SPARE, lane), jnp.float32)

    @pl.loop(0, n_stage)
    def _(i):
        slot = i % IN_SLOTS

        @pl.when(i + IN_SLOTS - 1 < n_stage)
        def _():
            stage_copy(i + IN_SLOTS - 1, (i + IN_SLOTS - 1) % IN_SLOTS).start()

        stage_copy(i, slot).wait()

        @pl.loop(0, STAGE_ROWS // 128)
        def _(j):
            block = stage[slot, pl.ds(pl.multiple_of(j * 128, 128), 128), :].astype(jnp.float32)
            base = pl.multiple_of((i * STAGE_ROWS + j * 128) * 2, 256)
            wide[pl.ds(base, 128, 2), :] = block[:, :lane]
            wide[pl.ds(base + 1, 128, 2), :] = block[:, lane:]

    copies = []

    def fill(out, hbm, first, count, ids_row):
        @pl.loop(0, count // BATCH)
        def _(b):
            for r in range(BATCH):
                at = pl.multiple_of(ids_s[ids_row + b, r], 2)
                rows_f[pl.ds(2 * r, 2), :] = wide[pl.ds(at, 2), :]
            rows = pl.ds(pl.multiple_of(first + b * BATCH, BATCH), BATCH)
            out[rows, :lane] = rows_f[pl.ds(0, BATCH, 2), :].astype(jnp.bfloat16)
            out[rows, lane:] = rows_f[pl.ds(1, BATCH, 2), :].astype(jnp.bfloat16)

        copy = pltpu.make_async_copy(out.at[pl.ds(first, count)], hbm.at[pl.ds(first, count)], out_sem.at[len(copies)])
        copy.start()
        copies.append(copy)

    n_cand = cand_out.shape[0]
    part = targ_out.shape[0] // 4
    fill(cand_out, cand_hbm, 0, n_cand, 0)
    for k in range(4):
        fill(targ_out, targ_hbm, k * part, part, (n_cand + k * part) // BATCH)
    for copy in copies:
        copy.wait()


def pick_rows(ids_two, table_loc, n_cand):
    rows_loc, width = table_loc.shape
    n_targ = ids_two.size - n_cand
    hbm = pl.BlockSpec(memory_space=pl.ANY)
    return pl.pallas_call(
        pick_body,
        out_shape=(jax.ShapeDtypeStruct((n_cand, width), jnp.bfloat16), jax.ShapeDtypeStruct((n_targ, width), jnp.bfloat16)),
        in_specs=[pl.BlockSpec(memory_space=pltpu.SMEM), hbm],
        out_specs=(hbm, hbm),
        scratch_shapes=[
            pltpu.VMEM((2 * (rows_loc + SPARE), width // 2), jnp.float32),
            pltpu.VMEM((IN_SLOTS, STAGE_ROWS, width), jnp.bfloat16),
            pltpu.VMEM((2 * BATCH, width // 2), jnp.float32),
            pltpu.VMEM((n_cand, width), jnp.bfloat16),
            pltpu.VMEM((n_targ, width), jnp.bfloat16),
            pltpu.SemaphoreType.DMA((IN_SLOTS,)),
            pltpu.SemaphoreType.DMA((5,)),
        ],
        compiler_params=pltpu.CompilerParams(vmem_limit_bytes=VMEM_LIMIT),
        name="pick_rows",
    )(ids_two, table_loc)


def scatter_body(tok_total, ids_s, ids_v, loss_s, cand_hbm, targ_hbm, wa_hbm, wb_hbm, out_ref, dw_one, dw_two, dwi_one, dwi_two, loss_out, acc, g2, cand_ref, targ_ref, wa, wb, flag_v, flag_s, out_stage, sem, in_sem, flag_sem, w_sem):
    rows, width = out_ref.shape
    lane = width // 2
    n_cand = cand_ref.shape[0]
    loss_out[0, 0] = loss_s[0, 0] * (1.0 / tok_total)
    n_all = n_cand + targ_ref.shape[0]
    in_copies = [pltpu.make_async_copy(src, dst, in_sem.at[k]) for k, (src, dst) in enumerate([(cand_hbm, cand_ref), (targ_hbm, targ_ref), (wa_hbm, wa), (wb_hbm, wb)])]
    for copy in in_copies:
        copy.start()

    ids = ids_v[...]
    place = lax.broadcasted_iota(jnp.int32, ids.shape, 1) % GROUP
    twice = jnp.zeros(ids.shape, jnp.int32)
    for k in range(1, GROUP):
        twice = jnp.where((ids == pltpu.roll(ids, k, 1)) & (place >= k), 1, twice)
    flag_v[...] = jnp.broadcast_to(jnp.max(twice, axis=1, keepdims=True), ids.shape)
    flag_copy = pltpu.make_async_copy(flag_v, flag_s, flag_sem)
    flag_copy.start()

    @pl.loop(0, 2 * rows // 512)
    def _(i):
        acc[pl.ds(pl.multiple_of(i * 512, 512), 512), :] = jnp.zeros((512, lane), jnp.float32)

    def one_batch(b, src, src_base):
        rows_b = pl.ds(pl.multiple_of(b * BATCH - src_base, BATCH), BATCH)
        repeated = flag_s[b, 0]

        @pl.when(repeated == 0)
        def _():
            part = src[rows_b, :].astype(jnp.float32)
            g2[pl.ds(0, BATCH, 2), :] = part[:, :lane]
            g2[pl.ds(1, BATCH, 2), :] = part[:, lane:]

        @pl.when(repeated != 0)
        def _():
            row_i = lax.broadcasted_iota(jnp.int32, (BATCH, BATCH), 0) // GROUP
            col_i = lax.broadcasted_iota(jnp.int32, (BATCH, BATCH), 1) // GROUP
            idr = jnp.broadcast_to(ids_v[pl.ds(b, 1), :], (BATCH, BATCH))
            same = jnp.where((idr == idr.T) & (row_i == col_i), 1.0, 0.0).astype(jnp.bfloat16)
            part = jnp.dot(same, src[rows_b, :], preferred_element_type=jnp.float32)
            g2[pl.ds(0, BATCH, 2), :] = part[:, :lane]
            g2[pl.ds(1, BATCH, 2), :] = part[:, lane:]

        for g in range(BATCH // GROUP):
            at = [pl.multiple_of(ids_s[b, g * GROUP + r], 2) for r in range(GROUP)]
            new = [acc[pl.ds(at[r], 2), :] + g2[pl.ds(2 * (g * GROUP + r), 2), :] for r in range(GROUP)]
            for r in range(GROUP):
                acc[pl.ds(at[r], 2), :] = new[r]

    for copy in in_copies:
        copy.wait()
    w_copies = []

    def place_block(src, dst):
        copy = pltpu.make_async_copy(src, dst, w_sem)
        copy.start()
        w_copies.append(copy)

    for b in range(8):
        place_block(wa.at[b, pl.ds(0, 128)], dw_one.at[pl.ds(b * 128, 128), pl.ds(0, width)])
        place_block(wa.at[b, pl.ds(128, 128)], dw_one.at[pl.ds(b * 128, 128), pl.ds(width, width)])
        place_block(wa.at[b, pl.ds(256, 64)], dw_two.at[pl.ds(b * 64, 64)])
        place_block(wb.at[b, pl.ds(0, 32)], dwi_one.at[pl.ds(b * 32, 32), pl.ds(0, width)])
        place_block(wb.at[b, pl.ds(32, 32)], dwi_one.at[pl.ds(b * 32, 32), pl.ds(width, width)])
        place_block(wb.at[b, pl.ds(64, 64)], dwi_two.at[pl.ds(b * 64, 64)])
    flag_copy.wait()

    @pl.loop(0, n_cand // BATCH)
    def _(b):
        one_batch(b, cand_ref, 0)

    @pl.loop(n_cand // BATCH, n_all // BATCH)
    def _(b):
        one_batch(b, targ_ref, n_cand)

    n_out = rows // OUT_ROWS

    def out_copy(i, slot):
        return pltpu.make_async_copy(out_stage.at[slot], out_ref.at[pl.ds(i * OUT_ROWS, OUT_ROWS)], sem.at[slot])

    @pl.loop(0, n_out)
    def _(i):
        slot = i % OUT_SLOTS

        @pl.when(i >= OUT_SLOTS)
        def _():
            out_copy(i - OUT_SLOTS, slot).wait()

        @pl.loop(0, OUT_ROWS // 128)
        def _(j):
            base = pl.multiple_of((i * OUT_ROWS + j * 128) * 2, 256)
            here = pl.ds(pl.multiple_of(j * 128, 128), 128)
            out_stage[slot, here, :lane] = acc[pl.ds(base, 128, 2), :]
            out_stage[slot, here, lane:] = acc[pl.ds(base + 1, 128, 2), :]

        out_copy(i, slot).start()

    for i in range(n_out - OUT_SLOTS, n_out):
        out_copy(i, i % OUT_SLOTS).wait()
    for copy in w_copies:
        copy.wait()


def scatter_rows(tok_total, ids_two, loss, back_cand, back_targ, wa, wb, rows_loc, din):
    width = back_cand.shape[1]
    n_batch = ids_two.shape[0]
    vmem = pl.BlockSpec(memory_space=pltpu.VMEM)
    hbm = pl.BlockSpec(memory_space=pl.ANY)
    smem = pl.BlockSpec(memory_space=pltpu.SMEM)
    shapes = [(rows_loc, width), (din, 2 * width), (2 * width, width), (width, 2 * width), (2 * width, width), (1, 1)]
    return pl.pallas_call(
        functools.partial(scatter_body, tok_total),
        out_shape=tuple(jax.ShapeDtypeStruct(shape, jnp.float32) for shape in shapes),
        in_specs=[smem, vmem, smem] + [hbm] * 4,
        out_specs=(hbm,) * 5 + (smem,),
        scratch_shapes=[
            pltpu.VMEM((2 * (rows_loc + SPARE), width // 2), jnp.float32),
            pltpu.VMEM((2 * BATCH, width // 2), jnp.float32),
            pltpu.VMEM(back_cand.shape, jnp.bfloat16),
            pltpu.VMEM(back_targ.shape, jnp.bfloat16),
            pltpu.VMEM(wa.shape, jnp.float32),
            pltpu.VMEM(wb.shape, jnp.float32),
            pltpu.VMEM((n_batch, BATCH), jnp.int32),
            pltpu.SMEM((n_batch, BATCH), jnp.int32),
            pltpu.VMEM((OUT_SLOTS, OUT_ROWS, width), jnp.float32),
            pltpu.SemaphoreType.DMA((OUT_SLOTS,)),
            pltpu.SemaphoreType.DMA((4,)),
            pltpu.SemaphoreType.DMA,
            pltpu.SemaphoreType.DMA,
        ],
        compiler_params=pltpu.CompilerParams(vmem_limit_bytes=VMEM_LIMIT),
        cost_estimate=pl.CostEstimate(flops=60_000_000_000, bytes_accessed=40 << 20, transcendentals=0),
        name="scatter_rows",
    )(ids_two, ids_two, loss, back_cand, back_targ, wa, wb)


CHUNK = 512
SUB = 128
COLS = 256


def logits_pass(u_at, n_cand, h, lq_ref, cid_ref, tid, z_a, z_b, e_s, m_s, s_s):
    n_tok, width = h.shape
    scale = SCORE_GAIN / math.sqrt(width)
    ht = h.T
    n_chunk = n_cand // CHUNK

    def multiply(i, z_ref):
        z_ref[...] = jnp.dot(u_at(jnp.minimum(i, n_chunk - 1)), ht, preferred_element_type=jnp.float32)

    def absorb(i, z_ref):
        off = pl.multiple_of(i * CHUNK, CHUNK)
        for col in range(0, n_tok, COLS):
            cols = slice(col, col + COLS)
            m8 = m_s[0, :, cols]
            s8 = s_s[:, cols]
            for k in range(CHUNK // SUB):
                rows = pl.ds(pl.multiple_of(off + k * SUB, SUB), SUB)
                lq = jnp.concatenate([lq_ref[rows, :]] * (COLS // 128), axis=1)
                cid = jnp.concatenate([cid_ref[rows, :]] * (COLS // 128), axis=1)
                z = z_ref[k * SUB : (k + 1) * SUB, cols] * scale - lq
                z = jnp.where(cid == tid[:, cols], HIT_VALUE, z).reshape(SUB // 8, 8, COLS)
                m_new = jnp.maximum(m8, jnp.max(z, axis=0))
                e = jnp.exp(z - m_new[None])
                s8 = s8 * jnp.exp(m8 - m_new) + jnp.sum(e, axis=0)
                m8 = m_new
                e_s[rows, cols] = e.reshape(SUB, COLS)
                m_s[1 + i * (CHUNK // SUB) + k, :, cols] = m8
            m_s[0, :, cols] = m8
            s_s[:, cols] = s8

    m_s[0] = jnp.full((8, n_tok), jnp.finfo(jnp.float32).min, jnp.float32)
    s_s[...] = jnp.zeros_like(s_s)
    multiply(0, z_a)

    def two_chunks(i):
        multiply(2 * i + 1, z_b)
        absorb(2 * i, z_a)
        multiply(2 * i + 2, z_a)
        absorb(2 * i + 1, z_b)

    pl.loop(0, n_chunk // 2)(two_chunks)


def loss_pass(tok_total, u_at, ut_s, h, v, e_s, m_s, s_s, fac_s, dz_a, dz_b, dht_s, loss_ref, dh_ref, dv_ref, du_ref, dz_ref, du_copy):
    n_cand, width = du_ref.shape
    n_tok = h.shape[0]
    scale = SCORE_GAIN / math.sqrt(width)
    n_chunk = n_cand // CHUNK
    hf = h.astype(jnp.float32)
    vf = v.astype(jnp.float32)
    zt = jnp.sum(hf * vf, axis=1, keepdims=True) * scale
    zt = jnp.broadcast_to(zt, (n_tok, 128)).T[0:1, :]
    m8 = m_s[0]
    m = jnp.maximum(zt, jnp.max(m8, axis=0, keepdims=True))
    et = jnp.exp(zt - m)
    den = et + jnp.sum(s_s[...] * jnp.exp(m8 - m), axis=0, keepdims=True)
    part = jnp.sum(jnp.log(den) + m - zt, axis=1, keepdims=True)
    loss_ref[...] = jnp.broadcast_to(part, loss_ref.shape)
    dzt = ((et / den - 1.0) / tok_total).astype(jnp.bfloat16).astype(jnp.float32)
    inv = 1.0 / den / tok_total
    fac_s[0:8, :] = jnp.broadcast_to(m, (8, n_tok))
    fac_s[8:16, :] = jnp.broadcast_to(inv, (8, n_tok))
    for i in range(n_chunk):
        ut_s[:, i * CHUNK : (i + 1) * CHUNK] = u_at(i).T
    for i in range(8):
        dz_ref[i : i + 1, :] = dzt[:, i * 128 : (i + 1) * 128]

    def gradient(i, out):
        i = jnp.minimum(i, n_chunk - 1)
        off = pl.multiple_of(i * CHUNK, CHUNK)
        for col in range(0, n_tok, COLS):
            cols = slice(col, col + COLS)
            for k in range(CHUNK // SUB):
                rows = pl.ds(pl.multiple_of(off + k * SUB, SUB), SUB)
                fac = jnp.exp(m_s[1 + i * (CHUNK // SUB) + k, :, cols] - fac_s[0:8, cols]) * fac_s[8:16, cols]
                out[k * SUB : (k + 1) * SUB, cols] = (e_s[rows, cols].reshape(SUB // 8, 8, COLS) * fac[None]).reshape(SUB, COLS).astype(jnp.bfloat16)

    def spread(i, dz_c):
        off = pl.multiple_of(i * CHUNK, CHUNK)
        du_ref[pl.ds(off, CHUNK), :] = jnp.dot(dz_c[...], h, preferred_element_type=jnp.float32)
        du_copy(i).start()
        dht_s[...] += jnp.dot(ut_s[:, pl.ds(off, CHUNK)], dz_c[...], preferred_element_type=jnp.float32)

    dht_s[...] = jnp.zeros_like(dht_s)
    gradient(0, dz_a)

    @pl.loop(0, n_chunk // 2)
    def _(i):
        gradient(2 * i + 1, dz_b)
        spread(2 * i, dz_a)
        gradient(2 * i + 2, dz_a)
        spread(2 * i + 1, dz_b)

    dzt_c = jnp.broadcast_to(dzt, (128, n_tok)).T[:, 0:1]
    dh_ref[...] = ((dzt_c * vf + dht_s[...].T) * scale).astype(jnp.bfloat16)
    dv_ref[...] = (scale * dzt_c * hf).astype(jnp.bfloat16)


def softmax_scratch(n_cand, n_tok, width):
    return [
        pltpu.VMEM((CHUNK, n_tok), jnp.float32),
        pltpu.VMEM((CHUNK, n_tok), jnp.float32),
        pltpu.VMEM((n_cand, n_tok), jnp.float32),
        pltpu.VMEM((1 + n_cand // SUB, 8, n_tok), jnp.float32),
        pltpu.VMEM((8, n_tok), jnp.float32),
        pltpu.VMEM((width, n_cand), jnp.bfloat16),
        pltpu.VMEM((16, n_tok), jnp.float32),
        pltpu.VMEM((CHUNK, n_tok), jnp.bfloat16),
        pltpu.VMEM((CHUNK, n_tok), jnp.bfloat16),
        pltpu.VMEM((width, n_tok), jnp.float32),
    ]


MESH = pl.DeviceIdType.MESH


def my_place():
    me = lax.axis_index("dp")
    return me, me // 4, (me // 2) % 2, me % 2


def peer_of(place, dy, dx, dc):
    me, y, x, c = place
    return me + dy * (4 - 8 * y) + dx * (2 - 4 * x) + dc * (1 - 2 * c)


def greet(place):
    barrier = pltpu.get_barrier_semaphore()
    for k in range(1, 8):
        pl.semaphore_signal(barrier, inc=1, device_id=(peer_of(place, k // 4, (k // 2) % 2, k % 2),), device_id_type=MESH)


def meet(place):
    greet(place)
    pl.semaphore_wait(pltpu.get_barrier_semaphore(), 7)


def push(src, dst, send_sem, recv_sem, peer):
    copy = pltpu.make_async_remote_copy(src_ref=src, dst_ref=dst, send_sem=send_sem, recv_sem=recv_sem, device_id=(peer,), device_id_type=MESH)
    copy.start()
    return copy


class Reduce:
    def __init__(self, place, data, in_one, mid, in_xa, in_yb, part_a, part_b, in_ya, in_xb, send_sem, recv_sem):
        self.place, self.data = place, data
        self.in_one, self.mid, self.in_xa, self.in_yb = in_one, mid, in_xa, in_yb
        self.part_a, self.part_b, self.in_ya, self.in_xb = part_a, part_b, in_ya, in_xb
        self.send_sem, self.recv_sem = send_sem, recv_sem
        self.half = data.shape[3] // 2
        self.copies = []

    def push(self, k, src, dst, dy, dx, dc):
        copy = push(src, dst, self.send_sem.at[k], self.recv_sem.at[k], peer_of(self.place, dy, dx, dc))
        self.copies.append(copy)

    def one(self):
        c = self.place[3]
        self.push(0, self.data.at[:, :, 1 - c], self.in_one, 0, 0, 1)

    def two(self):
        _, y, x, c = self.place
        half = self.half
        self.copies[0].wait_recv()
        for i in range(2):
            for j in range(2):
                self.mid[i, j] = self.data[i, j, c] + self.in_one[i, j]
        self.push(1, self.mid.at[:, 1 - x, pl.ds(0, half)], self.in_xa, 0, 1, 0)
        self.push(2, self.mid.at[1 - y, :, pl.ds(half, half)], self.in_yb, 1, 0, 0)

    def three(self):
        _, y, x, c = self.place
        half = self.half
        self.copies[1].wait_recv()
        for i in range(2):
            self.part_a[i] = self.mid[i, x, 0:half] + self.in_xa[i]
        self.push(3, self.part_a.at[1 - y], self.in_ya, 1, 0, 0)
        self.copies[2].wait_recv()
        for i in range(2):
            self.part_b[i] = self.mid[y, i, half : 2 * half] + self.in_yb[i]
        self.push(4, self.part_b.at[1 - x], self.in_xb, 0, 1, 0)

    def last(self):
        _, y, x, c = self.place
        self.copies[3].wait_recv()
        first = self.part_a[y] + self.in_ya[...]
        self.copies[4].wait_recv()
        return first, self.part_b[x] + self.in_xb[...]

    def drain(self):
        for copy in self.copies:
            copy.wait_send()


def reduce_scratch(n, rows, width, dtype):
    half = rows // 2
    return [
        pltpu.VMEM((n, 2, 2, rows, width), dtype),
        pltpu.VMEM((n, 2, 2, rows, width), dtype),
        pltpu.VMEM((n, 2, half, width), dtype),
        pltpu.VMEM((n, 2, half, width), dtype),
        pltpu.VMEM((n, 2, half, width), dtype),
        pltpu.VMEM((n, 2, half, width), dtype),
        pltpu.VMEM((n, half, width), dtype),
        pltpu.VMEM((n, half, width), dtype),
        pltpu.SemaphoreType.DMA((n, 5)),
        pltpu.SemaphoreType.DMA((n, 5)),
    ]


class Gather:
    def __init__(self, place, full, send_sem, recv_sem):
        self.place, self.full = place, full
        self.send_sem, self.recv_sem = send_sem, recv_sem
        self.half = full.shape[3] // 2
        self.copies = []

    def push(self, k, ref, dy, dx, dc):
        copy = push(ref, ref, self.send_sem.at[k], self.recv_sem.at[k], peer_of(self.place, dy, dx, dc))
        self.copies.append(copy)

    def one(self):
        _, y, x, c = self.place
        half = self.half
        self.push(0, self.full.at[y, x, c, pl.ds(0, half)], 0, 1, 0)
        self.push(1, self.full.at[y, x, c, pl.ds(half, half)], 1, 0, 0)

    def two(self):
        _, y, x, c = self.place
        half = self.half
        self.copies[0].wait_recv()
        self.push(2, self.full.at[y, :, c, pl.ds(0, half)], 1, 0, 0)
        self.copies[1].wait_recv()
        self.push(3, self.full.at[:, x, c, pl.ds(half, half)], 0, 1, 0)

    def three(self):
        c = self.place[3]
        self.copies[2].wait_recv()
        self.copies[3].wait_recv()
        self.push(4, self.full.at[:, :, c], 0, 0, 1)

    def last(self):
        self.copies[4].wait_recv()

    def drain(self):
        for copy in self.copies:
            copy.wait_send()


def gather_sems():
    return [pltpu.SemaphoreType.DMA((5,)), pltpu.SemaphoreType.DMA((5,))]


def prepare_body(rows_loc, mine, cand_ids, tokens, w_one, w_two, ids_two, query, full, send_sem, recv_sem):
    place = my_place()
    me = place[0]
    greet(place)
    half = tokens.shape[0] // 2
    query[0:half, :] = tower_fwd(tokens[0:half, :], w_one[...], w_two[...])
    pl.semaphore_wait(pltpu.get_barrier_semaphore(), 7)
    full[me] = mine[...]
    copies = []
    for k in range(1, 8):
        copies.append(push(mine, full.at[me], send_sem.at[k], recv_sem.at[k], peer_of(place, k // 4, (k // 2) % 2, k % 2)))

    def owned(ids):
        local = ids - me * rows_loc
        spare = rows_loc + (lax.broadcasted_iota(jnp.int32, ids.shape, 0) % 2) * 128 + lax.broadcasted_iota(jnp.int32, ids.shape, 1)
        return 2 * jnp.where((local >= 0) & (local < rows_loc), local, spare)

    n_c = cand_ids.shape[0]
    ids_two[0:n_c, :] = owned(cand_ids[...])
    query[half : 2 * half, :] = tower_fwd(tokens[half : 2 * half, :], w_one[...], w_two[...])
    for copy in copies:
        copy.wait()
    ids_two[n_c : n_c + 64, :] = owned(full[...].reshape(64, 128))


def prepare(targ_loc, cand_ids, tokens, w_one, w_two, rows_loc):
    n_tok = tokens.shape[0]
    n_c = cand_ids.shape[0] // 128
    vmem = pl.BlockSpec(memory_space=pltpu.VMEM)
    return pl.pallas_call(
        functools.partial(prepare_body, rows_loc),
        out_shape=(jax.ShapeDtypeStruct((n_c + 64, 128), jnp.int32), jax.ShapeDtypeStruct((n_tok, w_two.shape[1]), jnp.bfloat16)),
        in_specs=[vmem] * 5,
        out_specs=(vmem,) * 2,
        scratch_shapes=[pltpu.VMEM((8, 8, 128), jnp.int32), pltpu.SemaphoreType.DMA((8,)), pltpu.SemaphoreType.DMA((8,))],
        compiler_params=pltpu.CompilerParams(vmem_limit_bytes=VMEM_LIMIT, collective_id=0, has_side_effects=True),
        name="prepare",
    )(targ_loc.reshape(8, 128), cand_ids.reshape(n_c, 128), tokens, w_one, w_two)


PIECE = 256


def score_body(tok_total, c_hbm, t_hbm, wi_one, wi_two, h_ref, lq_ref, cid_ref, tid_ref, cand_raw, targ_raw, loss_ref, dh_ref, dv_ref, du_hbm, dz_ref, h_part, *scratch):
    place = my_place()
    me, y, x, c = place
    half = PIECE // 2
    data_c, data_t, in_sem, cand_vec, lq_b, cid_b, rs, ag_send, ag_recv = scratch[0:6] + (scratch[6:16],) + scratch[16:18]
    z_a, z_b, e_s, m_s, s_s, ut_s, fac_s, dz_a, dz_b, dht_s, h_send, h_recv, du_ref, du_sem = scratch[18:32]
    n_cand, width = du_ref.shape
    in_copies = [pltpu.make_async_copy(c_hbm, data_c, in_sem.at[0]), pltpu.make_async_copy(t_hbm, data_t, in_sem.at[1])]
    for copy in in_copies:
        copy.start()
    ag_h = Gather((me, y, x, 0), h_part, h_send, h_recv)
    h_part[y, x, 0] = h_ref[...]
    meet(place)
    ag_h.one()
    reduces = []
    for k in range(6):
        data = data_c.at[:, :, :, pl.ds(k * PIECE, PIECE)] if k < 2 else data_t.at[:, :, :, pl.ds((k - 2) * PIECE, PIECE)]
        reduces.append(Reduce(place, data, *[r.at[k] for r in rs]))
    ag = Gather(place, cand_vec, ag_send, ag_recv)

    def close(k, out, base):
        first, second = reduces[k].last()
        out[base : base + half, :] = first
        out[base + half : base + PIECE, :] = second

    in_copies[0].wait()
    reduces[0].one()
    reduces[1].one()
    in_copies[1].wait()
    for k in range(2, 6):
        reduces[k].one()
    reduces[0].two()
    reduces[1].two()
    reduces[2].two()
    reduces[0].three()
    reduces[1].three()
    reduces[3].two()

    @pl.loop(0, n_cand // 128)
    def _(i):
        rows = pl.ds(pl.multiple_of(i * 128, 128), 128)
        lq_b[rows, :] = jnp.broadcast_to(lq_ref[pl.ds(i, 1), :], (128, 128)).T
        cid_b[rows, :] = jnp.broadcast_to(cid_ref[pl.ds(i, 1), :], (128, 128)).T

    close(0, cand_raw, 0)
    close(1, cand_raw, PIECE)
    cand_vec[y, x, c] = tower_fwd(cand_raw[...], wi_one[...], wi_two[...])
    ag.one()
    reduces[4].two()
    ag.two()
    reduces[5].two()
    reduces[2].three()
    reduces[3].three()
    reduces[4].three()
    ag.three()
    reduces[5].three()
    ag_h.two()
    ag.last()

    def du_copy(i):
        rows = pl.ds(pl.multiple_of(i * CHUNK, CHUNK), CHUNK)
        return pltpu.make_async_copy(du_ref.at[rows], du_hbm.at[rows], du_sem.at[i])

    def u_at(i):
        return cand_vec[i // 4, (i // 2) % 2, i % 2]

    h = h_ref[...]
    logits_pass(u_at, n_cand, h, lq_b, cid_b, tid_ref[...], z_a, z_b, e_s, m_s, s_s)
    for k in range(4):
        close(k + 2, targ_raw, k * PIECE)
    v = tower_fwd(targ_raw[...], wi_one[...], wi_two[...])
    loss_pass(tok_total, u_at, ut_s, h, v, e_s, m_s, s_s, fac_s, dz_a, dz_b, dht_s, loss_ref, dh_ref, dv_ref, du_ref, dz_ref, du_copy)
    for i in range(n_cand // CHUNK):
        du_copy(i).wait()
    ag_h.copies[2].wait_recv()
    ag_h.copies[3].wait_recv()
    for red in reduces:
        red.drain()
    ag.drain()
    ag_h.drain()


def score(tok_total, data_c, data_t, wi_one, wi_two, query, log_q, cand_ids, targ_loc):
    n_mine, width = data_c.shape[3:]
    n_tok = data_t.shape[3]
    n_cand = 8 * n_mine
    vmem = pl.BlockSpec(memory_space=pltpu.VMEM)
    hbm = pl.BlockSpec(memory_space=pl.ANY)
    scratch = [pltpu.VMEM(data_c.shape, jnp.bfloat16), pltpu.VMEM(data_t.shape, jnp.bfloat16), pltpu.SemaphoreType.DMA((2,))]
    scratch += [pltpu.VMEM(data_c.shape, jnp.bfloat16), pltpu.VMEM((n_cand, 128), jnp.float32), pltpu.VMEM((n_cand, 128), jnp.int32)]
    scratch += reduce_scratch(6, PIECE, width, jnp.bfloat16) + gather_sems() + softmax_scratch(n_cand, n_tok, width)
    scratch += gather_sems() + [pltpu.VMEM((n_cand, width), jnp.float32), pltpu.SemaphoreType.DMA((n_cand // CHUNK,))]
    rows = [jax.ShapeDtypeStruct((n, width), jnp.bfloat16) for n in (n_mine, n_tok, n_tok, n_tok)]
    return pl.pallas_call(
        functools.partial(score_body, tok_total),
        out_shape=(rows[0], rows[1], jax.ShapeDtypeStruct((8, 128), jnp.float32), rows[2], rows[3], jax.ShapeDtypeStruct((n_cand, width), jnp.float32), jax.ShapeDtypeStruct((8, 128), jnp.float32), jax.ShapeDtypeStruct((2, 2, 1, n_tok, width), jnp.bfloat16)),
        in_specs=[hbm, hbm] + [vmem] * 6,
        out_specs=(vmem,) * 5 + (hbm,) + (vmem,) * 2,
        scratch_shapes=scratch,
        compiler_params=pltpu.CompilerParams(vmem_limit_bytes=VMEM_LIMIT, collective_id=1, has_side_effects=True),
        name="score",
    )(data_c, data_t, wi_one, wi_two, query, log_q.reshape(-1, 128), cand_ids.reshape(-1, 128), targ_loc.reshape(1, n_tok))


WA_ROWS = 320
WB_ROWS = 128


ROWS_BLK = 512


def back_body(part_hbm, tok_hbm, raw_hbm, h_hbm, *rest):
    operands, (loss_in, dz_in, rows_out, cand_out, wa_out, wb_out, loss_out), scratch = rest[0:8], rest[8:15], rest[15:]
    place = my_place()
    me, y, x, c = place
    rs_u, rs_a, rs_b = scratch[0:10], scratch[10:20], scratch[20:30]
    ac_send, ac_recv, aa_send, aa_recv, ab_send, ab_recv, l_send, l_recv, z_send, z_recv, h_sem, wa_data, wb_data, l_all, dz_all, d_part, tokens, raw_all, h_all, in_sem, rows_t, back_c, wa_full, wb_full, rows_sem, out_sem = scratch[30:56]
    d_targ, targ_raw, wi_one, wi_two, d_query, w_one, w_two, cand_raw = scratch[56:64]
    width = d_query.shape[1]
    scale = SCORE_GAIN / math.sqrt(width)
    pairs = [(part_hbm, d_part), (h_hbm.at[:, :, 0], h_all.at[:, :, c]), (tok_hbm, tokens), (raw_hbm, raw_all)] + list(zip(operands, scratch[56:64]))
    in_copies = [pltpu.make_async_copy(src, dst, in_sem.at[k]) for k, (src, dst) in enumerate(pairs)]
    in_copies[0].start()
    for copy in in_copies[4:]:
        copy.start()
    meet(place)
    for copy in in_copies[1:4]:
        copy.start()
    red_u = []
    for k in range(2):
        red_u.append(Reduce(place, d_part.at[:, :, :, pl.ds(k * PIECE, PIECE)], *[r.at[k] for r in rs_u]))
    red_a = Reduce(place, wa_data, *[r.at[0] for r in rs_a])
    red_b = Reduce(place, wb_data, *[r.at[0] for r in rs_b])
    ag_a = Gather(place, wa_full, aa_send, aa_recv)
    ag_b = Gather(place, wb_full, ab_send, ab_recv)
    ag_c = Gather(place, back_c, ac_send, ac_recv)
    in_copies[0].wait()
    red_u[0].one()
    red_u[1].one()
    l_all[me] = loss_in[...]
    dz_all[me] = dz_in[...]
    l_copies = []
    for k in range(1, 8):
        peer = peer_of(place, k // 4, (k // 2) % 2, k % 2)
        l_copies.append(push(loss_in, l_all.at[me], l_send.at[k], l_recv.at[k], peer))
        l_copies.append(push(dz_in, dz_all.at[me], z_send.at[k], z_recv.at[k], peer))
    in_copies[1].wait()
    h_copy = push(h_all.at[:, :, c], h_all.at[:, :, c], h_sem.at[0], h_sem.at[1], peer_of(place, 0, 0, 1))

    per = rows_t.shape[3] // ROWS_BLK

    def rows_copy(i):
        b = i // per
        here = (b // 4, (b // 2) % 2, b % 2, pl.ds(pl.multiple_of((i % per) * ROWS_BLK, ROWS_BLK), ROWS_BLK))
        return pltpu.make_async_copy(rows_t.at[here], rows_out.at[here], rows_sem.at[i])

    def rows_pass(first, last):

        @pl.loop(first, last)
        def _(i):
            b = i // per
            by, bx, bc = b // 4, (b // 2) % 2, b % 2
            rows = pl.ds(pl.multiple_of((i % per) * ROWS_BLK, ROWS_BLK), ROWS_BLK)
            columns = []
            for k in range(ROWS_BLK // 128):
                line = dz_all[b, pl.ds((i % per) * (ROWS_BLK // 128) + k, 1), :]
                columns.append(jnp.broadcast_to(line, (128, 128)).T)
            column = jnp.concatenate(columns, axis=0)
            column = jnp.concatenate([column] * (width // 128), axis=1)
            grad = (scale * column * h_all[by, bx, bc, rows, :].astype(jnp.float32)).astype(jnp.bfloat16)
            q = tower_back(raw_all[by, bx, bc, rows, :], wi_one[...], wi_two[...], grad)[0]
            rows_t[by, bx, bc, rows, :] = by_transpose(q, wi_one[...]).astype(jnp.bfloat16)
            rows_copy(i).start()

    def put(data, first, value):
        n = value.shape[0] // 8
        for b in range(8):
            data[b // 4, (b // 2) % 2, b % 2, first : first + n, :] = value[b * n : (b + 1) * n, :]

    def own(red, full):
        first, second = red.last()
        half = first.shape[0]
        full[y, x, c, 0:half, :] = first
        full[y, x, c, half : 2 * half, :] = second

    for copy in in_copies[4:]:
        copy.wait()
    t_q, t_hid = tower_back(targ_raw[...], wi_one[...], wi_two[...], d_targ[...])
    red_u[0].two()
    red_u[1].two()
    in_copies[2].wait()
    q_q, q_hid = tower_back(tokens[...], w_one[...], w_two[...], d_query[...])
    dw_one = over_rows(tokens[...], q_q)
    put(wa_data, 0, dw_one[:, :width])
    put(wa_data, 128, dw_one[:, width:])
    put(wa_data, 256, over_rows(q_hid, d_query[...]))
    red_a.one()
    in_copies[3].wait()
    for copy in l_copies:
        copy.wait()
    h_copy.wait()
    loss_out[...] = jnp.sum(l_all[...], axis=0)
    rows_pass(0, 3)
    red_u[0].three()
    red_u[1].three()
    red_a.two()
    rows_pass(3, 6)
    parts = []
    for k in range(2):
        first, second = red_u[k].last()
        parts += [first, second]
    d_cand = (jnp.concatenate(parts, axis=0) * scale).astype(jnp.bfloat16)
    c_q, c_hid = tower_back(cand_raw[...], wi_one[...], wi_two[...], d_cand)
    back_c[y, x, c] = by_transpose(c_q, wi_one[...]).astype(jnp.bfloat16)
    ag_c.one()
    dwi_one = over_rows(targ_raw[...], t_q) + over_rows(cand_raw[...], c_q)
    put(wb_data, 0, dwi_one[:, :width])
    put(wb_data, 32, dwi_one[:, width:])
    put(wb_data, 64, over_rows(t_hid, d_targ[...]) + over_rows(c_hid, d_cand))
    red_b.one()
    red_a.three()
    red_b.two()
    ag_c.two()
    rows_pass(6, 8)
    own(red_a, wa_full)
    ag_a.one()
    red_b.three()
    rows_pass(8, 13)
    ag_a.two()
    own(red_b, wb_full)
    ag_b.one()
    ag_c.three()
    rows_pass(13, 16)
    ag_b.two()
    ag_c.last()
    out_copies = [pltpu.make_async_copy(back_c, cand_out, out_sem.at[0])]
    out_copies[0].start()
    ag_a.three()
    ag_b.three()
    ag_a.last()
    out_copies.append(pltpu.make_async_copy(wa_full, wa_out, out_sem.at[1]))
    out_copies[1].start()
    ag_b.last()
    out_copies.append(pltpu.make_async_copy(wb_full, wb_out, out_sem.at[2]))
    out_copies[2].start()
    for part in red_u + [red_a, red_b, ag_c, ag_a, ag_b]:
        part.drain()
    for i in range(rows_sem.shape[0]):
        rows_copy(i).wait()
    for copy in out_copies:
        copy.wait()


def back_rows(d_part, tokens, raw_all, h_part, operands, loss_part, dz):
    n_mine, width = d_part.shape[3:]
    vmem = pl.BlockSpec(memory_space=pltpu.VMEM)
    hbm = pl.BlockSpec(memory_space=pl.ANY)
    eight = pltpu.SemaphoreType.DMA((8,))
    scratch = reduce_scratch(2, PIECE, width, jnp.float32) + reduce_scratch(1, WA_ROWS, width, jnp.float32) + reduce_scratch(1, WB_ROWS, width, jnp.float32)
    scratch += gather_sems() + gather_sems() + gather_sems() + [eight] * 4 + [pltpu.SemaphoreType.DMA((2,))]
    scratch += [pltpu.VMEM((2, 2, 2, WA_ROWS, width), jnp.float32), pltpu.VMEM((2, 2, 2, WB_ROWS, width), jnp.float32), pltpu.VMEM((8, 8, 128), jnp.float32), pltpu.VMEM((8, 8, 128), jnp.float32)]
    scratch += [pltpu.VMEM(d_part.shape, jnp.float32), pltpu.VMEM(tokens.shape, jnp.bfloat16), pltpu.VMEM(raw_all.shape, jnp.bfloat16), pltpu.VMEM(raw_all.shape, jnp.bfloat16), pltpu.SemaphoreType.DMA((4 + len(operands),))]
    scratch += [pltpu.VMEM(raw_all.shape, jnp.bfloat16), pltpu.VMEM((2, 2, 2, n_mine, width), jnp.bfloat16), pltpu.VMEM((2, 2, 2, WA_ROWS, width), jnp.float32), pltpu.VMEM((2, 2, 2, WB_ROWS, width), jnp.float32)]
    scratch += [pltpu.SemaphoreType.DMA((8 * raw_all.shape[3] // ROWS_BLK,)), pltpu.SemaphoreType.DMA((3,))]
    scratch += [pltpu.VMEM(operand.shape, operand.dtype) for operand in operands]
    return pl.pallas_call(
        back_body,
        out_shape=(
            jax.ShapeDtypeStruct(raw_all.shape, jnp.bfloat16),
            jax.ShapeDtypeStruct((2, 2, 2, n_mine, width), jnp.bfloat16),
            jax.ShapeDtypeStruct((2, 2, 2, WA_ROWS, width), jnp.float32),
            jax.ShapeDtypeStruct((2, 2, 2, WB_ROWS, width), jnp.float32),
            jax.ShapeDtypeStruct((8, 128), jnp.float32),
        ),
        in_specs=[hbm] * 12 + [vmem] * 2,
        out_specs=(hbm,) * 4 + (vmem,),
        scratch_shapes=scratch,
        compiler_params=pltpu.CompilerParams(vmem_limit_bytes=VMEM_LIMIT, collective_id=2, has_side_effects=True),
        name="back_rows",
    )(d_part, tokens, raw_all, h_part, *operands, loss_part, dz)


def solution(mesh):
    num_dev = mesh.shape["dp"]

    def local_step(tokens, w_one, w_two, wi_one, wi_two, table_loc, cand_ids, log_q, targ_loc):
        rows_loc, width = table_loc.shape
        n_cand = cand_ids.shape[0]
        n_tok = tokens.shape[0]
        tok_total = n_tok * num_dev
        ids_two, query = prepare(targ_loc, cand_ids, tokens, w_one, w_two, rows_loc)
        data_c, data_t = pick_rows(ids_two, table_loc, n_cand)
        data_c = data_c.reshape(2, 2, 2, n_cand // 8, width)
        data_t = data_t.reshape(2, 2, 2, n_tok, width)
        cand_raw, targ_raw, loss_part, d_query, d_targ, d_part, dz, h_part = score(tok_total, data_c, data_t, wi_one, wi_two, query, log_q, cand_ids, targ_loc)
        rows_t, back_c, wa, wb, loss = back_rows(d_part.reshape(2, 2, 2, n_cand // 8, width), tokens, data_t, h_part, (d_targ, targ_raw, wi_one, wi_two, d_query, w_one, w_two, cand_raw), loss_part, dz)
        d_table, dw_one, dw_two, dwi_one, dwi_two, loss = scatter_rows(tok_total, ids_two, loss, back_c.reshape(-1, width), rows_t.reshape(-1, width), wa.reshape(8, WA_ROWS, width), wb.reshape(8, WB_ROWS, width), rows_loc, tokens.shape[1])
        return loss.reshape(()), d_table, dw_one, dw_two, dwi_one, dwi_two

    return jax.shard_map(local_step, mesh=mesh, in_specs=(P("dp", None), P(), P(), P(), P(), P("dp", None), P(), P(), P("dp")), out_specs=(P(), P("dp", None), P(), P(), P(), P()), check_vma=False)
```

```python
import functools
import math
import jax
import jax.numpy as jnp
from jax import lax
from jax.experimental import pallas as pl
from jax.experimental.pallas import tpu as pltpu
from jax.sharding import PartitionSpec as P

SCORE_GAIN = 3.0
HIT_VALUE = -1e9


def tower_fwd(row_block, w_in, w_out):
    pre_act = jnp.dot(row_block, w_in, preferred_element_type=jnp.float32)
    hidden = jax.nn.gelu(pre_act).astype(jnp.bfloat16)
    tower_out = jnp.dot(hidden, w_out, preferred_element_type=jnp.float32).astype(jnp.bfloat16)
    return tower_out


def over_rows(a, b):
    return lax.dot_general(a, b, (((0,), (0,)), ((), ())), preferred_element_type=jnp.float32)


def by_transpose(a, b):
    return lax.dot_general(a, b, (((1,), (1,)), ((), ())), preferred_element_type=jnp.float32)


def tower_back(row_block, w_in, w_out, grad_out):
    pre_act = jnp.dot(row_block, w_in, preferred_element_type=jnp.float32)
    hidden, gelu_back = jax.vjp(jax.nn.gelu, pre_act)
    grad_hidden = by_transpose(grad_out, w_out)
    return gelu_back(grad_hidden)[0].astype(jnp.bfloat16), hidden.astype(jnp.bfloat16)


VMEM_LIMIT = 63 * 1024 * 1024
BATCH = 128
SPARE = 256
GROUP = 16
STAGE_ROWS = 2048
OUT_ROWS = 1024
IN_SLOTS = 12
OUT_SLOTS = 8


def pick_body(ids_s, table, cand_hbm, targ_hbm, wide, stage, rows_f, cand_out, targ_out, stage_sem, out_sem):
    rows_loc, width = table.shape
    lane = width // 2
    n_stage = rows_loc // STAGE_ROWS

    def stage_copy(i, slot):
        return pltpu.make_async_copy(table.at[pl.ds(i * STAGE_ROWS, STAGE_ROWS)], stage.at[slot], stage_sem.at[slot])

    for i in range(IN_SLOTS - 1):
        stage_copy(i, i).start()
    wide[pl.ds(2 * rows_loc, 2 * SPARE), :] = jnp.zeros((2 * SPARE, lane), jnp.float32)

    @pl.loop(0, n_stage)
    def _(i):
        slot = i % IN_SLOTS

        @pl.when(i + IN_SLOTS - 1 < n_stage)
        def _():
            stage_copy(i + IN_SLOTS - 1, (i + IN_SLOTS - 1) % IN_SLOTS).start()

        stage_copy(i, slot).wait()

        @pl.loop(0, STAGE_ROWS // 128)
        def _(j):
            block = stage[slot, pl.ds(pl.multiple_of(j * 128, 128), 128), :].astype(jnp.float32)
            base = pl.multiple_of((i * STAGE_ROWS + j * 128) * 2, 256)
            wide[pl.ds(base, 128, 2), :] = block[:, :lane]
            wide[pl.ds(base + 1, 128, 2), :] = block[:, lane:]

    copies = []

    def fill(out, hbm, first, count, ids_row):
        @pl.loop(0, count // BATCH)
        def _(b):
            for r in range(BATCH):
                at = pl.multiple_of(ids_s[ids_row + b, r], 2)
                rows_f[pl.ds(2 * r, 2), :] = wide[pl.ds(at, 2), :]
            rows = pl.ds(pl.multiple_of(first + b * BATCH, BATCH), BATCH)
            out[rows, :lane] = rows_f[pl.ds(0, BATCH, 2), :].astype(jnp.bfloat16)
            out[rows, lane:] = rows_f[pl.ds(1, BATCH, 2), :].astype(jnp.bfloat16)

        copy = pltpu.make_async_copy(out.at[pl.ds(first, count)], hbm.at[pl.ds(first, count)], out_sem.at[len(copies)])
        copy.start()
        copies.append(copy)

    n_cand = cand_out.shape[0]
    part = targ_out.shape[0] // 4
    fill(cand_out, cand_hbm, 0, n_cand, 0)
    for k in range(4):
        fill(targ_out, targ_hbm, k * part, part, (n_cand + k * part) // BATCH)
    for copy in copies:
        copy.wait()


def pick_rows(ids_two, table_loc, n_cand):
    rows_loc, width = table_loc.shape
    n_targ = ids_two.size - n_cand
    hbm = pl.BlockSpec(memory_space=pl.ANY)
    return pl.pallas_call(
        pick_body,
        out_shape=(jax.ShapeDtypeStruct((n_cand, width), jnp.bfloat16), jax.ShapeDtypeStruct((n_targ, width), jnp.bfloat16)),
        in_specs=[pl.BlockSpec(memory_space=pltpu.SMEM), hbm],
        out_specs=(hbm, hbm),
        scratch_shapes=[
            pltpu.VMEM((2 * (rows_loc + SPARE), width // 2), jnp.float32),
            pltpu.VMEM((IN_SLOTS, STAGE_ROWS, width), jnp.bfloat16),
            pltpu.VMEM((2 * BATCH, width // 2), jnp.float32),
            pltpu.VMEM((n_cand, width), jnp.bfloat16),
            pltpu.VMEM((n_targ, width), jnp.bfloat16),
            pltpu.SemaphoreType.DMA((IN_SLOTS,)),
            pltpu.SemaphoreType.DMA((5,)),
        ],
        compiler_params=pltpu.CompilerParams(vmem_limit_bytes=VMEM_LIMIT),
        name="pick_rows",
    )(ids_two, table_loc)


def scatter_body(tok_total, ids_s, ids_v, loss_s, cand_hbm, targ_hbm, wa_hbm, wb_hbm, out_ref, dw_one, dw_two, dwi_one, dwi_two, loss_out, acc, g2, cand_ref, targ_ref, wa, wb, flag_v, flag_s, out_stage, sem, in_sem, flag_sem, w_sem):
    rows, width = out_ref.shape
    lane = width // 2
    n_cand = cand_ref.shape[0]
    loss_out[0, 0] = loss_s[0, 0] * (1.0 / tok_total)
    n_all = n_cand + targ_ref.shape[0]
    in_copies = [pltpu.make_async_copy(src, dst, in_sem.at[k]) for k, (src, dst) in enumerate([(cand_hbm, cand_ref), (targ_hbm, targ_ref), (wa_hbm, wa), (wb_hbm, wb)])]
    for copy in in_copies:
        copy.start()

    ids = ids_v[...]
    place = lax.broadcasted_iota(jnp.int32, ids.shape, 1) % GROUP
    twice = jnp.zeros(ids.shape, jnp.int32)
    for k in range(1, GROUP):
        twice = jnp.where((ids == pltpu.roll(ids, k, 1)) & (place >= k), 1, twice)
    flag_v[...] = jnp.broadcast_to(jnp.max(twice, axis=1, keepdims=True), ids.shape)
    flag_copy = pltpu.make_async_copy(flag_v, flag_s, flag_sem)
    flag_copy.start()

    @pl.loop(0, 2 * rows // 512)
    def _(i):
        acc[pl.ds(pl.multiple_of(i * 512, 512), 512), :] = jnp.zeros((512, lane), jnp.float32)

    def one_batch(b, src, src_base):
        rows_b = pl.ds(pl.multiple_of(b * BATCH - src_base, BATCH), BATCH)
        repeated = flag_s[b, 0]

        @pl.when(repeated == 0)
        def _():
            part = src[rows_b, :].astype(jnp.float32)
            g2[pl.ds(0, BATCH, 2), :] = part[:, :lane]
            g2[pl.ds(1, BATCH, 2), :] = part[:, lane:]

        @pl.when(repeated != 0)
        def _():
            row_i = lax.broadcasted_iota(jnp.int32, (BATCH, BATCH), 0) // GROUP
            col_i = lax.broadcasted_iota(jnp.int32, (BATCH, BATCH), 1) // GROUP
            idr = jnp.broadcast_to(ids_v[pl.ds(b, 1), :], (BATCH, BATCH))
            same = jnp.where((idr == idr.T) & (row_i == col_i), 1.0, 0.0).astype(jnp.bfloat16)
            part = jnp.dot(same, src[rows_b, :], preferred_element_type=jnp.float32)
            g2[pl.ds(0, BATCH, 2), :] = part[:, :lane]
            g2[pl.ds(1, BATCH, 2), :] = part[:, lane:]

        for g in range(BATCH // GROUP):
            at = [pl.multiple_of(ids_s[b, g * GROUP + r], 2) for r in range(GROUP)]
            new = [acc[pl.ds(at[r], 2), :] + g2[pl.ds(2 * (g * GROUP + r), 2), :] for r in range(GROUP)]
            for r in range(GROUP):
                acc[pl.ds(at[r], 2), :] = new[r]

    for copy in in_copies:
        copy.wait()
    w_copies = []

    def place_block(src, dst):
        copy = pltpu.make_async_copy(src, dst, w_sem)
        copy.start()
        w_copies.append(copy)

    for b in range(8):
        place_block(wa.at[b, pl.ds(0, 128)], dw_one.at[pl.ds(b * 128, 128), pl.ds(0, width)])
        place_block(wa.at[b, pl.ds(128, 128)], dw_one.at[pl.ds(b * 128, 128), pl.ds(width, width)])
        place_block(wa.at[b, pl.ds(256, 64)], dw_two.at[pl.ds(b * 64, 64)])
        place_block(wb.at[b, pl.ds(0, 32)], dwi_one.at[pl.ds(b * 32, 32), pl.ds(0, width)])
        place_block(wb.at[b, pl.ds(32, 32)], dwi_one.at[pl.ds(b * 32, 32), pl.ds(width, width)])
        place_block(wb.at[b, pl.ds(64, 64)], dwi_two.at[pl.ds(b * 64, 64)])
    flag_copy.wait()

    @pl.loop(0, n_cand // BATCH)
    def _(b):
        one_batch(b, cand_ref, 0)

    @pl.loop(n_cand // BATCH, n_all // BATCH)
    def _(b):
        one_batch(b, targ_ref, n_cand)

    n_out = rows // OUT_ROWS

    def out_copy(i, slot):
        return pltpu.make_async_copy(out_stage.at[slot], out_ref.at[pl.ds(i * OUT_ROWS, OUT_ROWS)], sem.at[slot])

    @pl.loop(0, n_out)
    def _(i):
        slot = i % OUT_SLOTS

        @pl.when(i >= OUT_SLOTS)
        def _():
            out_copy(i - OUT_SLOTS, slot).wait()

        @pl.loop(0, OUT_ROWS // 128)
        def _(j):
            base = pl.multiple_of((i * OUT_ROWS + j * 128) * 2, 256)
            here = pl.ds(pl.multiple_of(j * 128, 128), 128)
            out_stage[slot, here, :lane] = acc[pl.ds(base, 128, 2), :]
            out_stage[slot, here, lane:] = acc[pl.ds(base + 1, 128, 2), :]

        out_copy(i, slot).start()

    for i in range(n_out - OUT_SLOTS, n_out):
        out_copy(i, i % OUT_SLOTS).wait()
    for copy in w_copies:
        copy.wait()


def scatter_rows(tok_total, ids_two, loss, back_cand, back_targ, wa, wb, rows_loc, din):
    width = back_cand.shape[1]
    n_batch = ids_two.shape[0]
    vmem = pl.BlockSpec(memory_space=pltpu.VMEM)
    hbm = pl.BlockSpec(memory_space=pl.ANY)
    smem = pl.BlockSpec(memory_space=pltpu.SMEM)
    shapes = [(rows_loc, width), (din, 2 * width), (2 * width, width), (width, 2 * width), (2 * width, width), (1, 1)]
    return pl.pallas_call(
        functools.partial(scatter_body, tok_total),
        out_shape=tuple(jax.ShapeDtypeStruct(shape, jnp.float32) for shape in shapes),
        in_specs=[smem, vmem, smem] + [hbm] * 4,
        out_specs=(hbm,) * 5 + (smem,),
        scratch_shapes=[
            pltpu.VMEM((2 * (rows_loc + SPARE), width // 2), jnp.float32),
            pltpu.VMEM((2 * BATCH, width // 2), jnp.float32),
            pltpu.VMEM(back_cand.shape, jnp.bfloat16),
            pltpu.VMEM(back_targ.shape, jnp.bfloat16),
            pltpu.VMEM(wa.shape, jnp.float32),
            pltpu.VMEM(wb.shape, jnp.float32),
            pltpu.VMEM((n_batch, BATCH), jnp.int32),
            pltpu.SMEM((n_batch, BATCH), jnp.int32),
            pltpu.VMEM((OUT_SLOTS, OUT_ROWS, width), jnp.float32),
            pltpu.SemaphoreType.DMA((OUT_SLOTS,)),
            pltpu.SemaphoreType.DMA((4,)),
            pltpu.SemaphoreType.DMA,
            pltpu.SemaphoreType.DMA,
        ],
        compiler_params=pltpu.CompilerParams(vmem_limit_bytes=VMEM_LIMIT),
        cost_estimate=pl.CostEstimate(flops=60_000_000_000, bytes_accessed=40 << 20, transcendentals=0),
        name="scatter_rows",
    )(ids_two, ids_two, loss, back_cand, back_targ, wa, wb)


CHUNK = 512
SUB = 128
COLS = 256


def logits_pass(u_at, n_cand, h, lq_ref, cid_ref, tid, z_a, z_b, e_s, m_s, s_s):
    n_tok, width = h.shape
    scale = SCORE_GAIN / math.sqrt(width)
    ht = h.T
    n_chunk = n_cand // CHUNK

    def multiply(i, z_ref):
        z_ref[...] = jnp.dot(u_at(jnp.minimum(i, n_chunk - 1)), ht, preferred_element_type=jnp.float32)

    def absorb(i, z_ref):
        off = pl.multiple_of(i * CHUNK, CHUNK)
        for col in range(0, n_tok, COLS):
            cols = slice(col, col + COLS)
            m8 = m_s[0, :, cols]
            s8 = s_s[:, cols]
            for k in range(CHUNK // SUB):
                rows = pl.ds(pl.multiple_of(off + k * SUB, SUB), SUB)
                lq = jnp.concatenate([lq_ref[rows, :]] * (COLS // 128), axis=1)
                cid = jnp.concatenate([cid_ref[rows, :]] * (COLS // 128), axis=1)
                z = z_ref[k * SUB : (k + 1) * SUB, cols] * scale - lq
                z = jnp.where(cid == tid[:, cols], HIT_VALUE, z).reshape(SUB // 8, 8, COLS)
                m_new = jnp.maximum(m8, jnp.max(z, axis=0))
                e = jnp.exp(z - m_new[None])
                s8 = s8 * jnp.exp(m8 - m_new) + jnp.sum(e, axis=0)
                m8 = m_new
                e_s[rows, cols] = e.reshape(SUB, COLS)
                m_s[1 + i * (CHUNK // SUB) + k, :, cols] = m8
            m_s[0, :, cols] = m8
            s_s[:, cols] = s8

    m_s[0] = jnp.full((8, n_tok), jnp.finfo(jnp.float32).min, jnp.float32)
    s_s[...] = jnp.zeros_like(s_s)
    multiply(0, z_a)

    def two_chunks(i):
        multiply(2 * i + 1, z_b)
        absorb(2 * i, z_a)
        multiply(2 * i + 2, z_a)
        absorb(2 * i + 1, z_b)

    pl.loop(0, n_chunk // 2)(two_chunks)


def loss_pass(tok_total, u_at, ut_s, h, v, e_s, m_s, s_s, fac_s, dz_a, dz_b, dht_s, loss_ref, dh_ref, dv_ref, du_ref, dz_ref, du_copy):
    n_cand, width = du_ref.shape
    n_tok = h.shape[0]
    scale = SCORE_GAIN / math.sqrt(width)
    n_chunk = n_cand // CHUNK
    hf = h.astype(jnp.float32)
    vf = v.astype(jnp.float32)
    zt = jnp.sum(hf * vf, axis=1, keepdims=True) * scale
    zt = jnp.broadcast_to(zt, (n_tok, 128)).T[0:1, :]
    m8 = m_s[0]
    m = jnp.maximum(zt, jnp.max(m8, axis=0, keepdims=True))
    et = jnp.exp(zt - m)
    den = et + jnp.sum(s_s[...] * jnp.exp(m8 - m), axis=0, keepdims=True)
    part = jnp.sum(jnp.log(den) + m - zt, axis=1, keepdims=True)
    loss_ref[...] = jnp.broadcast_to(part, loss_ref.shape)
    dzt = ((et / den - 1.0) / tok_total).astype(jnp.bfloat16).astype(jnp.float32)
    inv = 1.0 / den / tok_total
    fac_s[0:8, :] = jnp.broadcast_to(m, (8, n_tok))
    fac_s[8:16, :] = jnp.broadcast_to(inv, (8, n_tok))
    for i in range(n_chunk):
        ut_s[:, i * CHUNK : (i + 1) * CHUNK] = u_at(i).T
    for i in range(8):
        dz_ref[i : i + 1, :] = dzt[:, i * 128 : (i + 1) * 128]

    def gradient(i, out):
        i = jnp.minimum(i, n_chunk - 1)
        off = pl.multiple_of(i * CHUNK, CHUNK)
        for col in range(0, n_tok, COLS):
            cols = slice(col, col + COLS)
            for k in range(CHUNK // SUB):
                rows = pl.ds(pl.multiple_of(off + k * SUB, SUB), SUB)
                fac = jnp.exp(m_s[1 + i * (CHUNK // SUB) + k, :, cols] - fac_s[0:8, cols]) * fac_s[8:16, cols]
                out[k * SUB : (k + 1) * SUB, cols] = (e_s[rows, cols].reshape(SUB // 8, 8, COLS) * fac[None]).reshape(SUB, COLS).astype(jnp.bfloat16)

    def spread(i, dz_c):
        off = pl.multiple_of(i * CHUNK, CHUNK)
        du_ref[pl.ds(off, CHUNK), :] = jnp.dot(dz_c[...], h, preferred_element_type=jnp.float32)
        du_copy(i).start()
        dht_s[...] += jnp.dot(ut_s[:, pl.ds(off, CHUNK)], dz_c[...], preferred_element_type=jnp.float32)

    dht_s[...] = jnp.zeros_like(dht_s)
    gradient(0, dz_a)

    @pl.loop(0, n_chunk // 2)
    def _(i):
        gradient(2 * i + 1, dz_b)
        spread(2 * i, dz_a)
        gradient(2 * i + 2, dz_a)
        spread(2 * i + 1, dz_b)

    dzt_c = jnp.broadcast_to(dzt, (128, n_tok)).T[:, 0:1]
    dh_ref[...] = ((dzt_c * vf + dht_s[...].T) * scale).astype(jnp.bfloat16)
    dv_ref[...] = (scale * dzt_c * hf).astype(jnp.bfloat16)


def softmax_scratch(n_cand, n_tok, width):
    return [
        pltpu.VMEM((CHUNK, n_tok), jnp.float32),
        pltpu.VMEM((CHUNK, n_tok), jnp.float32),
        pltpu.VMEM((n_cand, n_tok), jnp.float32),
        pltpu.VMEM((1 + n_cand // SUB, 8, n_tok), jnp.float32),
        pltpu.VMEM((8, n_tok), jnp.float32),
        pltpu.VMEM((width, n_cand), jnp.bfloat16),
        pltpu.VMEM((16, n_tok), jnp.float32),
        pltpu.VMEM((CHUNK, n_tok), jnp.bfloat16),
        pltpu.VMEM((CHUNK, n_tok), jnp.bfloat16),
        pltpu.VMEM((width, n_tok), jnp.float32),
    ]


MESH = pl.DeviceIdType.MESH


def my_place():
    me = lax.axis_index("dp")
    return me, me // 4, (me // 2) % 2, me % 2


def peer_of(place, dy, dx, dc):
    me, y, x, c = place
    return me + dy * (4 - 8 * y) + dx * (2 - 4 * x) + dc * (1 - 2 * c)


def greet(place):
    barrier = pltpu.get_barrier_semaphore()
    for k in range(1, 8):
        pl.semaphore_signal(barrier, inc=1, device_id=(peer_of(place, k // 4, (k // 2) % 2, k % 2),), device_id_type=MESH)


def meet(place):
    greet(place)
    pl.semaphore_wait(pltpu.get_barrier_semaphore(), 7)


def push(src, dst, send_sem, recv_sem, peer):
    copy = pltpu.make_async_remote_copy(src_ref=src, dst_ref=dst, send_sem=send_sem, recv_sem=recv_sem, device_id=(peer,), device_id_type=MESH)
    copy.start()
    return copy


class Reduce:
    def __init__(self, place, data, in_one, mid, in_xa, in_yb, part_a, part_b, in_ya, in_xb, send_sem, recv_sem):
        self.place, self.data = place, data
        self.in_one, self.mid, self.in_xa, self.in_yb = in_one, mid, in_xa, in_yb
        self.part_a, self.part_b, self.in_ya, self.in_xb = part_a, part_b, in_ya, in_xb
        self.send_sem, self.recv_sem = send_sem, recv_sem
        self.half = data.shape[3] // 2
        self.copies = []

    def push(self, k, src, dst, dy, dx, dc):
        copy = push(src, dst, self.send_sem.at[k], self.recv_sem.at[k], peer_of(self.place, dy, dx, dc))
        self.copies.append(copy)

    def one(self):
        c = self.place[3]
        self.push(0, self.data.at[:, :, 1 - c], self.in_one, 0, 0, 1)

    def two(self):
        _, y, x, c = self.place
        half = self.half
        self.copies[0].wait_recv()
        for i in range(2):
            for j in range(2):
                self.mid[i, j] = self.data[i, j, c] + self.in_one[i, j]
        self.push(1, self.mid.at[:, 1 - x, pl.ds(0, half)], self.in_xa, 0, 1, 0)
        self.push(2, self.mid.at[1 - y, :, pl.ds(half, half)], self.in_yb, 1, 0, 0)

    def three(self):
        _, y, x, c = self.place
        half = self.half
        self.copies[1].wait_recv()
        for i in range(2):
            self.part_a[i] = self.mid[i, x, 0:half] + self.in_xa[i]
        self.push(3, self.part_a.at[1 - y], self.in_ya, 1, 0, 0)
        self.copies[2].wait_recv()
        for i in range(2):
            self.part_b[i] = self.mid[y, i, half : 2 * half] + self.in_yb[i]
        self.push(4, self.part_b.at[1 - x], self.in_xb, 0, 1, 0)

    def last(self):
        _, y, x, c = self.place
        self.copies[3].wait_recv()
        first = self.part_a[y] + self.in_ya[...]
        self.copies[4].wait_recv()
        return first, self.part_b[x] + self.in_xb[...]

    def drain(self):
        for copy in self.copies:
            copy.wait_send()


def reduce_scratch(n, rows, width, dtype):
    half = rows // 2
    return [
        pltpu.VMEM((n, 2, 2, rows, width), dtype),
        pltpu.VMEM((n, 2, 2, rows, width), dtype),
        pltpu.VMEM((n, 2, half, width), dtype),
        pltpu.VMEM((n, 2, half, width), dtype),
        pltpu.VMEM((n, 2, half, width), dtype),
        pltpu.VMEM((n, 2, half, width), dtype),
        pltpu.VMEM((n, half, width), dtype),
        pltpu.VMEM((n, half, width), dtype),
        pltpu.SemaphoreType.DMA((n, 5)),
        pltpu.SemaphoreType.DMA((n, 5)),
    ]


class Gather:
    def __init__(self, place, full, send_sem, recv_sem):
        self.place, self.full = place, full
        self.send_sem, self.recv_sem = send_sem, recv_sem
        self.half = full.shape[3] // 2
        self.copies = []

    def push(self, k, ref, dy, dx, dc):
        copy = push(ref, ref, self.send_sem.at[k], self.recv_sem.at[k], peer_of(self.place, dy, dx, dc))
        self.copies.append(copy)

    def one(self):
        _, y, x, c = self.place
        half = self.half
        self.push(0, self.full.at[y, x, c, pl.ds(0, half)], 0, 1, 0)
        self.push(1, self.full.at[y, x, c, pl.ds(half, half)], 1, 0, 0)

    def two(self):
        _, y, x, c = self.place
        half = self.half
        self.copies[0].wait_recv()
        self.push(2, self.full.at[y, :, c, pl.ds(0, half)], 1, 0, 0)
        self.copies[1].wait_recv()
        self.push(3, self.full.at[:, x, c, pl.ds(half, half)], 0, 1, 0)

    def three(self):
        c = self.place[3]
        self.copies[2].wait_recv()
        self.copies[3].wait_recv()
        self.push(4, self.full.at[:, :, c], 0, 0, 1)

    def last(self):
        self.copies[4].wait_recv()

    def drain(self):
        for copy in self.copies:
            copy.wait_send()


def gather_sems():
    return [pltpu.SemaphoreType.DMA((5,)), pltpu.SemaphoreType.DMA((5,))]


def prepare_body(rows_loc, mine, cand_ids, tokens, w_one, w_two, ids_two, query, full, send_sem, recv_sem):
    place = my_place()
    me = place[0]
    greet(place)
    half = tokens.shape[0] // 2
    query[0:half, :] = tower_fwd(tokens[0:half, :], w_one[...], w_two[...])
    pl.semaphore_wait(pltpu.get_barrier_semaphore(), 7)
    full[me] = mine[...]
    copies = []
    for k in range(1, 8):
        copies.append(push(mine, full.at[me], send_sem.at[k], recv_sem.at[k], peer_of(place, k // 4, (k // 2) % 2, k % 2)))

    def owned(ids):
        local = ids - me * rows_loc
        spare = rows_loc + (lax.broadcasted_iota(jnp.int32, ids.shape, 0) % 2) * 128 + lax.broadcasted_iota(jnp.int32, ids.shape, 1)
        return 2 * jnp.where((local >= 0) & (local < rows_loc), local, spare)

    n_c = cand_ids.shape[0]
    ids_two[0:n_c, :] = owned(cand_ids[...])
    query[half : 2 * half, :] = tower_fwd(tokens[half : 2 * half, :], w_one[...], w_two[...])
    for copy in copies:
        copy.wait()
    ids_two[n_c : n_c + 64, :] = owned(full[...].reshape(64, 128))


def prepare(targ_loc, cand_ids, tokens, w_one, w_two, rows_loc):
    n_tok = tokens.shape[0]
    n_c = cand_ids.shape[0] // 128
    vmem = pl.BlockSpec(memory_space=pltpu.VMEM)
    return pl.pallas_call(
        functools.partial(prepare_body, rows_loc),
        out_shape=(jax.ShapeDtypeStruct((n_c + 64, 128), jnp.int32), jax.ShapeDtypeStruct((n_tok, w_two.shape[1]), jnp.bfloat16)),
        in_specs=[vmem] * 5,
        out_specs=(vmem,) * 2,
        scratch_shapes=[pltpu.VMEM((8, 8, 128), jnp.int32), pltpu.SemaphoreType.DMA((8,)), pltpu.SemaphoreType.DMA((8,))],
        compiler_params=pltpu.CompilerParams(vmem_limit_bytes=VMEM_LIMIT, collective_id=0, has_side_effects=True),
        name="prepare",
    )(targ_loc.reshape(8, 128), cand_ids.reshape(n_c, 128), tokens, w_one, w_two)


PIECE = 256


def score_body(tok_total, c_hbm, t_hbm, wi_one, wi_two, h_ref, lq_ref, cid_ref, tid_ref, cand_raw, targ_raw, loss_ref, dh_ref, dv_ref, du_hbm, dz_ref, h_part, *scratch):
    place = my_place()
    me, y, x, c = place
    half = PIECE // 2
    data_c, data_t, in_sem, cand_vec, lq_b, cid_b, rs, ag_send, ag_recv = scratch[0:6] + (scratch[6:16],) + scratch[16:18]
    z_a, z_b, e_s, m_s, s_s, ut_s, fac_s, dz_a, dz_b, dht_s, h_send, h_recv, du_ref, du_sem = scratch[18:32]
    n_cand, width = du_ref.shape
    in_copies = [pltpu.make_async_copy(c_hbm, data_c, in_sem.at[0]), pltpu.make_async_copy(t_hbm, data_t, in_sem.at[1])]
    for copy in in_copies:
        copy.start()
    ag_h = Gather((me, y, x, 0), h_part, h_send, h_recv)
    h_part[y, x, 0] = h_ref[...]
    meet(place)
    ag_h.one()
    reduces = []
    for k in range(6):
        data = data_c.at[:, :, :, pl.ds(k * PIECE, PIECE)] if k < 2 else data_t.at[:, :, :, pl.ds((k - 2) * PIECE, PIECE)]
        reduces.append(Reduce(place, data, *[r.at[k] for r in rs]))
    ag = Gather(place, cand_vec, ag_send, ag_recv)

    def close(k, out, base):
        first, second = reduces[k].last()
        out[base : base + half, :] = first
        out[base + half : base + PIECE, :] = second

    in_copies[0].wait()
    reduces[0].one()
    reduces[1].one()
    in_copies[1].wait()
    for k in range(2, 6):
        reduces[k].one()
    reduces[0].two()
    reduces[1].two()
    reduces[0].three()
    reduces[1].three()
    reduces[2].two()
    reduces[3].two()

    @pl.loop(0, n_cand // 128)
    def _(i):
        rows = pl.ds(pl.multiple_of(i * 128, 128), 128)
        lq_b[rows, :] = jnp.broadcast_to(lq_ref[pl.ds(i, 1), :], (128, 128)).T
        cid_b[rows, :] = jnp.broadcast_to(cid_ref[pl.ds(i, 1), :], (128, 128)).T

    close(0, cand_raw, 0)
    close(1, cand_raw, PIECE)
    cand_vec[y, x, c] = tower_fwd(cand_raw[...], wi_one[...], wi_two[...])
    ag.one()
    reduces[4].two()
    ag.two()
    reduces[5].two()
    reduces[2].three()
    reduces[3].three()
    reduces[4].three()
    ag.three()
    reduces[5].three()
    ag_h.two()
    ag.last()

    def du_copy(i):
        rows = pl.ds(pl.multiple_of(i * CHUNK, CHUNK), CHUNK)
        return pltpu.make_async_copy(du_ref.at[rows], du_hbm.at[rows], du_sem.at[i])

    def u_at(i):
        return cand_vec[i // 4, (i // 2) % 2, i % 2]

    h = h_ref[...]
    logits_pass(u_at, n_cand, h, lq_b, cid_b, tid_ref[...], z_a, z_b, e_s, m_s, s_s)
    for k in range(4):
        close(k + 2, targ_raw, k * PIECE)
    v = tower_fwd(targ_raw[...], wi_one[...], wi_two[...])
    loss_pass(tok_total, u_at, ut_s, h, v, e_s, m_s, s_s, fac_s, dz_a, dz_b, dht_s, loss_ref, dh_ref, dv_ref, du_ref, dz_ref, du_copy)
    for i in range(n_cand // CHUNK):
        du_copy(i).wait()
    ag_h.copies[2].wait_recv()
    ag_h.copies[3].wait_recv()
    for red in reduces:
        red.drain()
    ag.drain()
    ag_h.drain()


def score(tok_total, data_c, data_t, wi_one, wi_two, query, log_q, cand_ids, targ_loc):
    n_mine, width = data_c.shape[3:]
    n_tok = data_t.shape[3]
    n_cand = 8 * n_mine
    vmem = pl.BlockSpec(memory_space=pltpu.VMEM)
    hbm = pl.BlockSpec(memory_space=pl.ANY)
    scratch = [pltpu.VMEM(data_c.shape, jnp.bfloat16), pltpu.VMEM(data_t.shape, jnp.bfloat16), pltpu.SemaphoreType.DMA((2,))]
    scratch += [pltpu.VMEM(data_c.shape, jnp.bfloat16), pltpu.VMEM((n_cand, 128), jnp.float32), pltpu.VMEM((n_cand, 128), jnp.int32)]
    scratch += reduce_scratch(6, PIECE, width, jnp.bfloat16) + gather_sems() + softmax_scratch(n_cand, n_tok, width)
    scratch += gather_sems() + [pltpu.VMEM((n_cand, width), jnp.float32), pltpu.SemaphoreType.DMA((n_cand // CHUNK,))]
    rows = [jax.ShapeDtypeStruct((n, width), jnp.bfloat16) for n in (n_mine, n_tok, n_tok, n_tok)]
    return pl.pallas_call(
        functools.partial(score_body, tok_total),
        out_shape=(rows[0], rows[1], jax.ShapeDtypeStruct((8, 128), jnp.float32), rows[2], rows[3], jax.ShapeDtypeStruct((n_cand, width), jnp.float32), jax.ShapeDtypeStruct((8, 128), jnp.float32), jax.ShapeDtypeStruct((2, 2, 1, n_tok, width), jnp.bfloat16)),
        in_specs=[hbm, hbm] + [vmem] * 6,
        out_specs=(vmem,) * 5 + (hbm,) + (vmem,) * 2,
        scratch_shapes=scratch,
        compiler_params=pltpu.CompilerParams(vmem_limit_bytes=VMEM_LIMIT, collective_id=1, has_side_effects=True),
        name="score",
    )(data_c, data_t, wi_one, wi_two, query, log_q.reshape(-1, 128), cand_ids.reshape(-1, 128), targ_loc.reshape(1, n_tok))


WA_ROWS = 320
WB_ROWS = 128


ROWS_BLK = 512


def back_body(part_hbm, tok_hbm, raw_hbm, h_hbm, *rest):
    operands, (loss_in, dz_in, rows_out, cand_out, wa_out, wb_out, loss_out), scratch = rest[0:8], rest[8:15], rest[15:]
    place = my_place()
    me, y, x, c = place
    rs_u, rs_a, rs_b = scratch[0:10], scratch[10:20], scratch[20:30]
    ac_send, ac_recv, aa_send, aa_recv, ab_send, ab_recv, l_send, l_recv, z_send, z_recv, h_sem, wa_data, wb_data, l_all, dz_all, d_part, tokens, raw_all, h_all, in_sem, rows_t, back_c, wa_full, wb_full, rows_sem, out_sem = scratch[30:56]
    d_targ, targ_raw, wi_one, wi_two, d_query, w_one, w_two, cand_raw = scratch[56:64]
    width = d_query.shape[1]
    scale = SCORE_GAIN / math.sqrt(width)
    pairs = [(part_hbm, d_part), (h_hbm.at[:, :, 0], h_all.at[:, :, c]), (tok_hbm, tokens), (raw_hbm, raw_all)] + list(zip(operands, scratch[56:64]))
    in_copies = [pltpu.make_async_copy(src, dst, in_sem.at[k]) for k, (src, dst) in enumerate(pairs)]
    in_copies[0].start()
    for copy in in_copies[4:]:
        copy.start()
    meet(place)
    for copy in in_copies[1:4]:
        copy.start()
    red_u = []
    for k in range(2):
        red_u.append(Reduce(place, d_part.at[:, :, :, pl.ds(k * PIECE, PIECE)], *[r.at[k] for r in rs_u]))
    red_a = Reduce(place, wa_data, *[r.at[0] for r in rs_a])
    red_b = Reduce(place, wb_data, *[r.at[0] for r in rs_b])
    ag_a = Gather(place, wa_full, aa_send, aa_recv)
    ag_b = Gather(place, wb_full, ab_send, ab_recv)
    ag_c = Gather(place, back_c, ac_send, ac_recv)
    in_copies[0].wait()
    red_u[0].one()
    red_u[1].one()
    l_all[me] = loss_in[...]
    dz_all[me] = dz_in[...]
    l_copies = []
    for k in range(1, 8):
        peer = peer_of(place, k // 4, (k // 2) % 2, k % 2)
        l_copies.append(push(loss_in, l_all.at[me], l_send.at[k], l_recv.at[k], peer))
        l_copies.append(push(dz_in, dz_all.at[me], z_send.at[k], z_recv.at[k], peer))
    in_copies[1].wait()
    h_copy = push(h_all.at[:, :, c], h_all.at[:, :, c], h_sem.at[0], h_sem.at[1], peer_of(place, 0, 0, 1))

    per = rows_t.shape[3] // ROWS_BLK

    def rows_copy(i):
        b = i // per
        here = (b // 4, (b // 2) % 2, b % 2, pl.ds(pl.multiple_of((i % per) * ROWS_BLK, ROWS_BLK), ROWS_BLK))
        return pltpu.make_async_copy(rows_t.at[here], rows_out.at[here], rows_sem.at[i])

    def rows_pass(first, last):

        @pl.loop(first, last)
        def _(i):
            b = i // per
            by, bx, bc = b // 4, (b // 2) % 2, b % 2
            rows = pl.ds(pl.multiple_of((i % per) * ROWS_BLK, ROWS_BLK), ROWS_BLK)
            columns = []
            for k in range(ROWS_BLK // 128):
                line = dz_all[b, pl.ds((i % per) * (ROWS_BLK // 128) + k, 1), :]
                columns.append(jnp.broadcast_to(line, (128, 128)).T)
            column = jnp.concatenate(columns, axis=0)
            column = jnp.concatenate([column] * (width // 128), axis=1)
            grad = (scale * column * h_all[by, bx, bc, rows, :].astype(jnp.float32)).astype(jnp.bfloat16)
            q = tower_back(raw_all[by, bx, bc, rows, :], wi_one[...], wi_two[...], grad)[0]
            rows_t[by, bx, bc, rows, :] = by_transpose(q, wi_one[...]).astype(jnp.bfloat16)
            rows_copy(i).start()

    def put(data, first, value):
        n = value.shape[0] // 8
        for b in range(8):
            data[b // 4, (b // 2) % 2, b % 2, first : first + n, :] = value[b * n : (b + 1) * n, :]

    def own(red, full):
        first, second = red.last()
        half = first.shape[0]
        full[y, x, c, 0:half, :] = first
        full[y, x, c, half : 2 * half, :] = second

    for copy in in_copies[4:]:
        copy.wait()
    t_q, t_hid = tower_back(targ_raw[...], wi_one[...], wi_two[...], d_targ[...])
    red_u[0].two()
    red_u[1].two()
    in_copies[2].wait()
    q_q, q_hid = tower_back(tokens[...], w_one[...], w_two[...], d_query[...])
    dw_one = over_rows(tokens[...], q_q)
    put(wa_data, 0, dw_one[:, :width])
    put(wa_data, 128, dw_one[:, width:])
    put(wa_data, 256, over_rows(q_hid, d_query[...]))
    red_a.one()
    in_copies[3].wait()
    for copy in l_copies:
        copy.wait()
    h_copy.wait()
    loss_out[...] = jnp.sum(l_all[...], axis=0)
    rows_pass(0, 3)
    red_u[0].three()
    red_u[1].three()
    red_a.two()
    rows_pass(3, 6)
    parts = []
    for k in range(2):
        first, second = red_u[k].last()
        parts += [first, second]
    d_cand = (jnp.concatenate(parts, axis=0) * scale).astype(jnp.bfloat16)
    c_q, c_hid = tower_back(cand_raw[...], wi_one[...], wi_two[...], d_cand)
    back_c[y, x, c] = by_transpose(c_q, wi_one[...]).astype(jnp.bfloat16)
    ag_c.one()
    dwi_one = over_rows(targ_raw[...], t_q) + over_rows(cand_raw[...], c_q)
    put(wb_data, 0, dwi_one[:, :width])
    put(wb_data, 32, dwi_one[:, width:])
    put(wb_data, 64, over_rows(t_hid, d_targ[...]) + over_rows(c_hid, d_cand))
    red_b.one()
    red_a.three()
    red_b.two()
    ag_c.two()
    rows_pass(6, 8)
    own(red_a, wa_full)
    ag_a.one()
    red_b.three()
    rows_pass(8, 13)
    ag_a.two()
    own(red_b, wb_full)
    ag_b.one()
    ag_c.three()
    rows_pass(13, 16)
    ag_b.two()
    ag_c.last()
    out_copies = [pltpu.make_async_copy(back_c, cand_out, out_sem.at[0])]
    out_copies[0].start()
    ag_a.three()
    ag_b.three()
    ag_a.last()
    out_copies.append(pltpu.make_async_copy(wa_full, wa_out, out_sem.at[1]))
    out_copies[1].start()
    ag_b.last()
    out_copies.append(pltpu.make_async_copy(wb_full, wb_out, out_sem.at[2]))
    out_copies[2].start()
    for part in red_u + [red_a, red_b, ag_c, ag_a, ag_b]:
        part.drain()
    for i in range(rows_sem.shape[0]):
        rows_copy(i).wait()
    for copy in out_copies:
        copy.wait()


def back_rows(d_part, tokens, raw_all, h_part, operands, loss_part, dz):
    n_mine, width = d_part.shape[3:]
    vmem = pl.BlockSpec(memory_space=pltpu.VMEM)
    hbm = pl.BlockSpec(memory_space=pl.ANY)
    eight = pltpu.SemaphoreType.DMA((8,))
    scratch = reduce_scratch(2, PIECE, width, jnp.float32) + reduce_scratch(1, WA_ROWS, width, jnp.float32) + reduce_scratch(1, WB_ROWS, width, jnp.float32)
    scratch += gather_sems() + gather_sems() + gather_sems() + [eight] * 4 + [pltpu.SemaphoreType.DMA((2,))]
    scratch += [pltpu.VMEM((2, 2, 2, WA_ROWS, width), jnp.float32), pltpu.VMEM((2, 2, 2, WB_ROWS, width), jnp.float32), pltpu.VMEM((8, 8, 128), jnp.float32), pltpu.VMEM((8, 8, 128), jnp.float32)]
    scratch += [pltpu.VMEM(d_part.shape, jnp.float32), pltpu.VMEM(tokens.shape, jnp.bfloat16), pltpu.VMEM(raw_all.shape, jnp.bfloat16), pltpu.VMEM(raw_all.shape, jnp.bfloat16), pltpu.SemaphoreType.DMA((4 + len(operands),))]
    scratch += [pltpu.VMEM(raw_all.shape, jnp.bfloat16), pltpu.VMEM((2, 2, 2, n_mine, width), jnp.bfloat16), pltpu.VMEM((2, 2, 2, WA_ROWS, width), jnp.float32), pltpu.VMEM((2, 2, 2, WB_ROWS, width), jnp.float32)]
    scratch += [pltpu.SemaphoreType.DMA((8 * raw_all.shape[3] // ROWS_BLK,)), pltpu.SemaphoreType.DMA((3,))]
    scratch += [pltpu.VMEM(operand.shape, operand.dtype) for operand in operands]
    return pl.pallas_call(
        back_body,
        out_shape=(
            jax.ShapeDtypeStruct(raw_all.shape, jnp.bfloat16),
            jax.ShapeDtypeStruct((2, 2, 2, n_mine, width), jnp.bfloat16),
            jax.ShapeDtypeStruct((2, 2, 2, WA_ROWS, width), jnp.float32),
            jax.ShapeDtypeStruct((2, 2, 2, WB_ROWS, width), jnp.float32),
            jax.ShapeDtypeStruct((8, 128), jnp.float32),
        ),
        in_specs=[hbm] * 12 + [vmem] * 2,
        out_specs=(hbm,) * 4 + (vmem,),
        scratch_shapes=scratch,
        compiler_params=pltpu.CompilerParams(vmem_limit_bytes=VMEM_LIMIT, collective_id=2, has_side_effects=True),
        name="back_rows",
    )(d_part, tokens, raw_all, h_part, *operands, loss_part, dz)


def solution(mesh):
    num_dev = mesh.shape["dp"]

    def local_step(tokens, w_one, w_two, wi_one, wi_two, table_loc, cand_ids, log_q, targ_loc):
        rows_loc, width = table_loc.shape
        n_cand = cand_ids.shape[0]
        n_tok = tokens.shape[0]
        tok_total = n_tok * num_dev
        ids_two, query = prepare(targ_loc, cand_ids, tokens, w_one, w_two, rows_loc)
        data_c, data_t = pick_rows(ids_two, table_loc, n_cand)
        data_c = data_c.reshape(2, 2, 2, n_cand // 8, width)
        data_t = data_t.reshape(2, 2, 2, n_tok, width)
        cand_raw, targ_raw, loss_part, d_query, d_targ, d_part, dz, h_part = score(tok_total, data_c, data_t, wi_one, wi_two, query, log_q, cand_ids, targ_loc)
        rows_t, back_c, wa, wb, loss = back_rows(d_part.reshape(2, 2, 2, n_cand // 8, width), tokens, data_t, h_part, (d_targ, targ_raw, wi_one, wi_two, d_query, w_one, w_two, cand_raw), loss_part, dz)
        d_table, dw_one, dw_two, dwi_one, dwi_two, loss = scatter_rows(tok_total, ids_two, loss, back_c.reshape(-1, width), rows_t.reshape(-1, width), wa.reshape(8, WA_ROWS, width), wb.reshape(8, WB_ROWS, width), rows_loc, tokens.shape[1])
        return loss.reshape(()), d_table, dw_one, dw_two, dwi_one, dwi_two

    return jax.shard_map(local_step, mesh=mesh, in_specs=(P("dp", None), P(), P(), P(), P(), P("dp", None), P(), P(), P("dp")), out_specs=(P(), P("dp", None), P(), P(), P(), P()), check_vma=False)
```
